8 devices in a mesh: part: 1 (over z), dp: 2 (over y), tp: 4 (over x, core).
Axes of the slice: x: 2, y: 2, z: 1, core: 2. Of those that a mesh axis runs over, the one named last changes fastest.
Arguments:
- hidden: bfloat16 [4, 256, 1280], P(('part', 'dp'))
- weight: bfloat16 [1280, 65536], P(None, 'tp')
- labels: int32 [4, 32], P(('part', 'dp'))
- in_len: int32 [4], P(('part', 'dp'))
- lab_len: int32 [4], P(('part', 'dp'))
Outputs:
- output 1: float32 [4], P(('part', 'dp'))
- output 2: float32 [1280, 65536], P(('part', 'dp'), 'tp')
- output 3: float32 [4, 256, 1280], P(('part', 'dp'))
All inputs are finite; a program needn't handle non-finite values.
Results may differ from the reference program's by a relative error of at most 0.00238044.
Values are sent between devices in bfloat16 or wider.
A program may use at most 1 GiB of HBM per device.

```python
import jax
import jax.numpy as jnp
from jax import lax

MODEL_DIM = 1280
VOCAB_SIZE = 65536
FRAMES = 256
MAX_LABELS = 32
BATCH_SIZE = 4
NEG_BIG = -1.0e30


def setup_inputs(seed: int = 0, part: int = 0) -> dict:
    root_key = jax.random.key(seed)
    shared_key, group_root = jax.random.split(root_key)
    group_key = jax.random.fold_in(group_root, part)
    key_hidden, key_labels, key_lab_len, key_in_len = jax.random.split(group_key, 4)
    hidden = jax.random.normal(key_hidden, (BATCH_SIZE, FRAMES, MODEL_DIM), jnp.float32)
    weight = jax.random.normal(shared_key, (MODEL_DIM, VOCAB_SIZE), jnp.float32) * (2.0 * MODEL_DIM ** -0.5)
    labels = jax.random.randint(key_labels, (BATCH_SIZE, MAX_LABELS), 1, VOCAB_SIZE, dtype=jnp.int32)
    lab_len = jax.random.randint(key_lab_len, (BATCH_SIZE,), (MAX_LABELS + 1) // 2, MAX_LABELS + 1, dtype=jnp.int32)
    lab_len = lab_len.at[0].set(MAX_LABELS)
    len_slack = FRAMES - 2 * lab_len - 1
    in_len = 2 * lab_len + 1 + jax.random.randint(key_in_len, (BATCH_SIZE,), 0, len_slack + 1, dtype=jnp.int32)
    in_len = in_len.at[BATCH_SIZE - 1].set(FRAMES)
    return {"hidden": hidden.astype(jnp.bfloat16), "weight": weight.astype(jnp.bfloat16), "labels": labels, "in_len": in_len, "lab_len": lab_len}


def log_sum3(val_a, val_b, val_c):
    top_val = jnp.maximum(jnp.maximum(val_a, val_b), val_c)
    return top_val + jnp.log(jnp.exp(val_a - top_val) + jnp.exp(val_b - top_val) + jnp.exp(val_c - top_val))


def ctc_lattice(lab_logp, labels, in_len, lab_len):
    batch_loc, frames, n_slots = lab_logp.shape
    n_lab = n_slots - 1
    states = 2 * n_lab + 1
    blank_lp = lab_logp[:, :, :1]
    pair_lp = jnp.stack([jnp.broadcast_to(blank_lp, (batch_loc, frames, n_lab)), lab_logp[:, :, 1:]], axis=3)
    ext_lp = jnp.concatenate([pair_lp.reshape(batch_loc, frames, 2 * n_lab), blank_lp], axis=2)
    ext_lp = jnp.moveaxis(ext_lp, 1, 0)
    zero_lab = jnp.zeros_like(labels)
    ext_lab = jnp.concatenate([jnp.stack([zero_lab, labels], axis=2).reshape(batch_loc, 2 * n_lab), zero_lab[:, :1]], axis=1)
    prev_lab = jnp.pad(ext_lab[:, :-2], ((0, 0), (2, 0)), constant_values=-1)
    state_ids = jnp.arange(states)
    skip_ok = ((state_ids % 2) == 1)[None, :] & (ext_lab != prev_lab)
    skip_up = jnp.pad(skip_ok[:, 2:], ((0, 0), (0, 2)), constant_values=False)
    end_mask = (state_ids[None, :] == 2 * lab_len[:, None]) | (state_ids[None, :] == 2 * lab_len[:, None] - 1)
    zeros_bs = jnp.zeros((batch_loc, states), lab_logp.dtype)
    neg_bs = zeros_bs + NEG_BIG
    start_vec = jnp.where(state_ids[None, :] < 2, zeros_bs, neg_bs)
    end_vec = jnp.where(end_mask, zeros_bs, neg_bs)
    frame_ids = jnp.arange(frames)
    is_live = frame_ids[:, None] < in_len[None, :]
    is_last = frame_ids[:, None] == in_len[None, :] - 1

    def fwd_step(prev_vec, step_in):
        step_lp, step_live, is_first = step_in
        down_one = jnp.pad(prev_vec[:, :-1], ((0, 0), (1, 0)), constant_values=NEG_BIG)
        down_two = jnp.where(skip_ok, jnp.pad(prev_vec[:, :-2], ((0, 0), (2, 0)), constant_values=NEG_BIG), NEG_BIG)
        new_vec = step_lp + jnp.where(is_first, start_vec, log_sum3(prev_vec, down_one, down_two))
        new_vec = jnp.where(step_live[:, None], new_vec, prev_vec)
        return new_vec, new_vec

    alpha_last, alpha_all = lax.scan(fwd_step, neg_bs, (ext_lp, is_live, frame_ids == 0))
    final_alpha = jnp.where(end_mask, alpha_last, NEG_BIG)
    top_val = jnp.max(final_alpha, axis=1)
    seq_loss = -(top_val + jnp.log(jnp.sum(jnp.exp(final_alpha - top_val[:, None]), axis=1)))

    def bwd_step(next_vec, step_in):
        step_lp, step_live, step_last = step_in
        up_one = jnp.pad(next_vec[:, 1:], ((0, 0), (0, 1)), constant_values=NEG_BIG)
        up_two = jnp.where(skip_up, jnp.pad(next_vec[:, 2:], ((0, 0), (0, 2)), constant_values=NEG_BIG), NEG_BIG)
        new_vec = step_lp + jnp.where(step_last[:, None], end_vec, log_sum3(next_vec, up_one, up_two))
        new_vec = jnp.where(step_live[:, None], new_vec, next_vec)
        return new_vec, new_vec

    beta_carry, beta_all = lax.scan(bwd_step, end_vec, (ext_lp, is_live, is_last), reverse=True)
    log_occ = alpha_all + beta_all - ext_lp + seq_loss[None, :, None]
    occ_ext = jnp.where(is_live[:, :, None], jnp.exp(log_occ), 0.0)
    occ_pairs = occ_ext[:, :, :2 * n_lab].reshape(frames, batch_loc, n_lab, 2)
    blank_occ = jnp.sum(occ_pairs[:, :, :, 0], axis=2) + occ_ext[:, :, 2 * n_lab]
    occ_lab = jnp.concatenate([blank_occ[:, :, None], occ_pairs[:, :, :, 1]], axis=2)
    return seq_loss, jnp.moveaxis(occ_lab, 0, 1)


def reference(hidden, weight, labels, in_len, lab_len):
    frame_ids = jnp.arange(FRAMES)

    def one_sequence(grad_acc, row_in):
        h_seq, lab_seq, seq_in, seq_lab = row_in
        logits = jnp.dot(h_seq, weight, preferred_element_type=jnp.float32)
        row_max = jnp.max(logits, axis=1, keepdims=True)
        log_norm = row_max + jnp.log(jnp.sum(jnp.exp(logits - row_max), axis=1, keepdims=True))
        columns = jnp.concatenate([jnp.zeros((1,), jnp.int32), lab_seq])
        lab_logp = jnp.take(logits, columns, axis=1) - log_norm
        seq_loss, occ_lab = ctc_lattice(lab_logp[None], lab_seq[None], seq_in[None], seq_lab[None])
        soft_probs = jnp.exp(logits - log_norm)
        grad_z = soft_probs.at[:, columns].add(-occ_lab[0])
        grad_z = jnp.where((frame_ids < seq_in)[:, None], grad_z, 0.0).astype(jnp.bfloat16)
        grad_acc = grad_acc + jnp.dot(h_seq.T, grad_z, preferred_element_type=jnp.float32)
        grad_seq = jnp.dot(grad_z, weight.T, preferred_element_type=jnp.float32)
        return grad_acc, (seq_loss[0], grad_seq)

    grad_weight, (seq_loss, grad_hidden) = lax.scan(one_sequence, jnp.zeros((MODEL_DIM, VOCAB_SIZE), jnp.float32), (hidden, labels, in_len, lab_len))
    return seq_loss, grad_weight, grad_hidden
```

```python
import functools

import jax
import jax.numpy as jnp
from jax import lax
from jax.experimental import pallas as pl
from jax.experimental.pallas import tpu as pltpu
from jax.sharding import PartitionSpec as P

NEG_BIG = -1.0e30
F32 = jnp.float32
BF16 = jnp.bfloat16
TILE = 512
LANES = 128
MIB = 1 << 20


def vmem_spec():
    return pl.BlockSpec(memory_space=pltpu.VMEM)


def smem_spec():
    return pl.BlockSpec(memory_space=pltpu.SMEM)


def any_spec():
    return pl.BlockSpec(memory_space=pl.ANY)


def params(limit):
    return pltpu.CompilerParams(vmem_limit_bytes=limit)


def label_col(meta_refs, i):
    n_slots = meta_refs[0].shape[1] - 1
    seq, item = i // n_slots, lax.rem(i, n_slots)
    n_seq = meta_refs[0].shape[0]
    at = lax.max(item - 1, 0)
    col = meta_refs[0][lax.rem(seq, n_seq), at]
    for k in range(1, len(meta_refs)):
        col = jnp.where(seq >= k * n_seq, meta_refs[k][lax.rem(seq, n_seq), at], col)
    return jnp.where(item == 0, 0, col)


def build_lists(meta_refs, vocab_loc, head, nxt):
    n_items = len(meta_refs) * meta_refs[0].shape[0] * (meta_refs[0].shape[1] - 1)
    col_start = lax.axis_index("tp") * vocab_loc
    n_tiles = vocab_loc // TILE

    def clear(i, c):
        head[i] = -1
        return c

    lax.fori_loop(0, n_tiles, clear, 0)

    def insert(i, c):
        loc = label_col(meta_refs, i) - col_start
        tile = lax.max(loc, 0) // TILE

        @pl.when((loc >= 0) & (loc < vocab_loc))
        def _():
            nxt[i] = head[tile]
            head[tile] = i

        return c

    lax.fori_loop(0, n_items, insert, 0)
    return col_start


def walk_list(head, nxt, tile, visit):
    def body(i):
        visit(i)
        return nxt[i]

    lax.while_loop(lambda i: i >= 0, body, head[tile])


class TileStream:
    def __init__(self, src, buf, sem, depth, n_tiles, view):
        self.src, self.buf, self.sem, self.depth, self.n, self.view = src, buf, sem, depth, n_tiles, view

    def copy(self, j):
        slot = lax.rem(j, self.depth)
        return pltpu.make_async_copy(self.view(self.src, j), self.buf.at[slot], self.sem.at[slot])

    def prime(self):
        for j in range(self.depth - 1):
            self.copy(j).start()

    def get(self, j):
        self.copy(j).wait()

        @pl.when(j + self.depth - 1 < self.n)
        def _():
            self.copy(j + self.depth - 1).start()

        return lax.rem(j, self.depth)


def w_view(src, j):
    return src.at[:, pl.ds(pl.multiple_of(j * TILE, TILE), TILE)]


def z_view(src, j):
    return src.at[j]


def tile_stats(z, m_ref, s_ref):
    n_chunks = z.shape[1] // LANES
    m_old = m_ref[...]
    m_new = m_old
    for k in range(n_chunks):
        m_new = jnp.maximum(m_new, z[:, k * LANES:(k + 1) * LANES])
    s_new = s_ref[...] * jnp.exp(m_old - m_new)
    for k in range(n_chunks):
        s_new = s_new + jnp.exp(z[:, k * LANES:(k + 1) * LANES] - m_new)
    m_ref[...] = m_new
    s_ref[...] = s_new


def emit_stats(m_ref, s_ref, stats_ref):
    row_m = jnp.max(m_ref[...], axis=1, keepdims=True)
    row_s = jnp.sum(s_ref[...] * jnp.exp(m_ref[...] - row_m), axis=1, keepdims=True)
    rows = m_ref.shape[0]
    m_t = jnp.broadcast_to(row_m, (rows, LANES)).T
    s_t = jnp.broadcast_to(row_s, (rows, LANES)).T
    stats_ref[0:8, :] = m_t[0:8, :]
    stats_ref[8:16, :] = s_t[0:8, :]


def z_own_kernel(n_slots, h_ref, w_hbm, meta_ref, z_hbm, stats_ref, pick_ref, wbuf, wsem, zbuf, zsem, m_ref, s_ref, head, nxt):
    n_tiles = z_hbm.shape[0]
    rows = h_ref.shape[0]
    n_seq = meta_ref.shape[0]
    frames = rows // n_seq
    stream = TileStream(w_hbm, wbuf, wsem, wbuf.shape[0], n_tiles, w_view)
    stream.prime()
    col_start = build_lists([meta_ref], n_tiles * TILE, head, nxt)
    m_ref[...] = jnp.full(m_ref.shape, NEG_BIG, F32)
    s_ref[...] = jnp.zeros(s_ref.shape, F32)
    pick_ref[...] = jnp.zeros(pick_ref.shape, F32)
    lane = lax.broadcasted_iota(jnp.int32, (frames, LANES), 1)

    def out_copy(j):
        slot = lax.rem(j, 2)
        return pltpu.make_async_copy(zbuf.at[slot], z_hbm.at[j], zsem.at[slot])

    def step(j, c):
        slot = stream.get(j)

        @pl.when(j >= 2)
        def _():
            out_copy(j - 2).wait()

        zslot = lax.rem(j, 2)
        z = jnp.dot(h_ref[...], wbuf[slot], preferred_element_type=F32)
        zbuf[zslot] = z
        tile_stats(z, m_ref, s_ref)
        out_copy(j).start()

        def visit(i):
            seq, item = i // n_slots, lax.rem(i, n_slots)
            off = label_col([meta_ref], i) - col_start - j * TILE
            blk = off // LANES
            r0 = pl.multiple_of(seq * frames, frames)
            zb = zbuf[zslot, pl.ds(r0, frames), pl.ds(pl.multiple_of(blk * LANES, LANES), LANES)]
            at = item + 64 * seq
            moved = pltpu.roll(zb, lax.rem(at - (off - blk * LANES) + 2 * LANES, LANES), 1)
            pick_ref[...] = jnp.where(lane == at, moved, pick_ref[...])

        walk_list(head, nxt, j, visit)
        return c

    lax.fori_loop(0, n_tiles, step, 0)
    emit_stats(m_ref, s_ref, stats_ref)
    out_copy(n_tiles - 2).wait()
    out_copy(n_tiles - 1).wait()


def z_oth_loop(lo, hi, h_ref, w_hbm, z_hbm, wbuf, wsem, zbuf, zsem, m_ref, s_ref, sections):
    stream = TileStream(w_hbm, wbuf, wsem, wbuf.shape[0], hi - lo, lambda src, j: w_view(src, lo + j))
    stream.prime()

    def out_copy(j):
        slot = lax.rem(j, 2)
        return pltpu.make_async_copy(zbuf.at[slot], z_hbm.at[lo + j], zsem.at[slot])

    base = 0
    for n, side, make_carry in sections:
        carry = make_carry()

        def step(k, c, base=base, side=side):
            j = base + k
            slot = stream.get(j)

            @pl.when(j >= 2)
            def _():
                out_copy(j - 2).wait()

            z = jnp.dot(h_ref[...], wbuf[slot], preferred_element_type=F32)
            zbuf[lax.rem(j, 2)] = z
            tile_stats(z, m_ref, s_ref)
            c = side(k, c)
            out_copy(j).start()
            return c

        last = lax.fori_loop(0, n, step, carry)
        yield last
        base += n
    out_copy(hi - lo - 2).wait()
    out_copy(hi - lo - 1).wait()


def join_rows(h_got, h_core, h_ref):
    n = h_got.shape[0]
    core = lax.rem(lax.axis_index("tp"), 2)
    h_ref[pl.ds(pl.multiple_of(core * n, n), n), :] = h_got[...]
    h_ref[pl.ds(pl.multiple_of((1 - core) * n, n), n), :] = h_core[...]


def z_first_kernel(lo, hi, h_got, h_core, w_hbm, meta_oth, z_hbm, m_ref, s_ref, h_ref, wbuf, wsem, zbuf, zsem):
    join_rows(h_got, h_core, h_ref)
    m_ref[...] = jnp.full(m_ref.shape, NEG_BIG, F32)
    s_ref[...] = jnp.zeros(s_ref.shape, F32)
    for _ in z_oth_loop(lo, hi, h_ref, w_hbm, z_hbm, wbuf, wsem, zbuf, zsem, m_ref, s_ref, [(hi - lo, lambda k, c: c, lambda: 0)]):
        pass


def z_last_kernel(lo, hi, h_ref, w_hbm, m_in, s_in, z_in, z_hbm, stats_ref, wbuf, wsem, zbuf, zsem, m_ref, s_ref):
    m_ref[...] = m_in[...]
    s_ref[...] = s_in[...]
    for _ in z_oth_loop(lo, hi, h_ref, w_hbm, z_hbm, wbuf, wsem, zbuf, zsem, m_ref, s_ref, [(hi - lo, lambda k, c: c, lambda: 0)]):
        pass
    emit_stats(m_ref, s_ref, stats_ref)


def z_lattice_kernel(lo, hi, n_lat, n_lab, h_ref, w_hbm, m_in, s_in, p0, p1, p2, p3, meta_ref, z_in,
                     z_hbm, m_ref, s_ref, occ_ref, loss_ref,
                     wbuf, wsem, zbuf, zsem, e_lab, e_blk, a_lab, a_blk, b_lab, b_blk, o_t):
    n_blk = e_lab.shape[0]
    frames = n_blk * 64
    m_ref[...] = m_in[...]
    s_ref[...] = s_in[...]
    lane128 = lax.broadcasted_iota(jnp.int32, (LANES, LANES), 1)
    row32 = lax.broadcasted_iota(jnp.int32, (n_lab, LANES), 0)
    row8 = lax.broadcasted_iota(jnp.int32, (8, LANES), 0)
    lane32 = lax.broadcasted_iota(jnp.int32, (n_lab, LANES), 1)
    lane8 = lax.broadcasted_iota(jnp.int32, (8, LANES), 1)
    n_seq = meta_ref.shape[0]
    labs = jnp.zeros((n_lab, LANES), jnp.int32)
    lab_row = jnp.zeros((8, LANES), jnp.int32)
    live8 = jnp.zeros((8, LANES), jnp.int32)
    used8 = jnp.zeros((8, LANES), jnp.int32)
    for s in range(n_seq):
        for k in range(n_lab):
            labs = jnp.where((row32 == k) & (lane32 == s), meta_ref[s, k], labs)
            lab_row = jnp.where((row8 == s) & (lane8 == k), meta_ref[s, k], lab_row)
        live8 = jnp.where(lane8 == s, meta_ref[s, n_lab], live8)
        used8 = jnp.where(lane8 == s, meta_ref[s, n_lab + 1], used8)
    live32 = jnp.broadcast_to(live8[0:1], (n_lab, LANES))
    used32 = jnp.broadcast_to(used8[0:1], (n_lab, LANES))
    skip_dn = labs != pltpu.roll(labs, 1, 0)
    skip_up = labs != pltpu.roll(labs, n_lab - 1, 0)
    end_lab = row32 == used32 - 1
    end_blk = row32 == used32
    end_top = (row8 == 0) & (used8 == n_lab)
    shift0 = jnp.zeros((1, LANES), F32)
    seq1 = lane8[0:1] >= 64
    half_len = jnp.where(seq1, meta_ref[1, n_lab], meta_ref[0, n_lab])
    for j in range(n_blk):
        part = functools.reduce(jnp.add, [p[pl.ds(64 * j, 64), :] for p in (p0, p1, p2, p3)])
        blk = jnp.concatenate([part, pltpu.roll(part, 64, 1)], axis=0)
        blk = jnp.where(lane128 <= n_lab, blk, NEG_BIG)
        x = blk.T
        top = jnp.max(x[0:n_lab + 8], axis=0, keepdims=True)
        e_blk[j] = jnp.broadcast_to(x[0:1] - top, (8, LANES))
        e_lab[j] = pltpu.roll(x, LANES - 1, 0)[0:n_lab] - top
        shift0 = shift0 + jnp.where(lax.rem(lane8[0:1], 64) + 64 * j < half_len, top, 0.0)
    shift_seq0 = jnp.sum(jnp.where(seq1, 0.0, shift0), axis=1, keepdims=True)
    shift_seq1 = jnp.sum(jnp.where(seq1, shift0, 0.0), axis=1, keepdims=True)

    def lse2(a, b):
        hi_v = jnp.maximum(a, b)
        return hi_v + jnp.log(1.0 + jnp.exp(jnp.minimum(a, b) - hi_v))

    def lse3(a, b, c):
        hi_v = jnp.maximum(a, b)
        lo_v = jnp.minimum(a, b)
        top = jnp.maximum(hi_v, c)
        mid = jnp.minimum(hi_v, c)
        return top + jnp.log(1.0 + jnp.exp(lo_v - top) + jnp.exp(mid - top))

    def emission(t):
        j, u = t // 64, lax.rem(t, 64)
        idx32 = jnp.where(lane32 == 1, 64 + u, u)
        idx8 = jnp.where(lane8 == 1, 64 + u, u)
        el = jnp.take_along_axis(e_lab[j], idx32, axis=1)
        eb = jnp.take_along_axis(e_blk[j], idx8, axis=1)
        return el, eb

    neg32 = jnp.full((n_lab, LANES), NEG_BIG, F32)
    neg8 = jnp.full((8, LANES), NEG_BIG, F32)
    start32 = jnp.where(row32 == 0, 0.0, NEG_BIG)
    fin_l = jnp.where(end_lab, 0.0, NEG_BIG)
    fin_b = jnp.where(end_blk, 0.0, NEG_BIG)
    fin_t = jnp.where(end_top, 0.0, NEG_BIG)

    def lat_step(i, carry):
        al, ab, at, bl, bb, bt = carry
        el, eb = emission(i)
        eb32 = jnp.broadcast_to(eb[0:1], (n_lab, LANES))
        rolled = pltpu.roll(al, 1, 0)
        prev = jnp.where(row32 == 0, NEG_BIG, rolled)
        prev_t = jnp.where(row8 == 0, rolled[0:8], NEG_BIG)
        first = i == 0
        nl = jnp.where(first, start32, lse3(al, ab, jnp.where(skip_dn, prev, NEG_BIG)))
        nb = jnp.where(first, start32, lse2(ab, prev))
        nt = jnp.where(first, neg8, lse2(at, prev_t))
        a_lab[i] = nl
        a_blk[i, 0:n_lab] = nb
        a_blk[i, n_lab:n_lab + 8] = nt
        al = jnp.where(i < live32, el + nl, al)
        ab = jnp.where(i < live32, eb32 + nb, ab)
        at = jnp.where(i < live8, eb + nt, at)
        t = frames - 1 - i
        fl, fb = emission(t)
        fb32 = jnp.broadcast_to(fb[0:1], (n_lab, LANES))
        last = row32 == n_lab - 1
        up_l = jnp.where(last, NEG_BIG, pltpu.roll(bl, n_lab - 1, 0))
        up_b = jnp.where(last, jnp.broadcast_to(bt[0:1], (n_lab, LANES)), pltpu.roll(bb, n_lab - 1, 0))
        is_end32 = t == live32 - 1
        is_end8 = t == live8 - 1
        ml = fl + jnp.where(is_end32, fin_l, lse3(bl, up_b, jnp.where(skip_up, up_l, NEG_BIG)))
        mb = fb32 + jnp.where(is_end32, fin_b, lse2(bb, bl))
        mt = fb + jnp.where(is_end8, fin_t, bt)
        bl = jnp.where(t < live32, ml, bl)
        bb = jnp.where(t < live32, mb, bb)
        bt = jnp.where(t < live8, mt, bt)
        b_lab[t] = bl
        b_blk[t, 0:n_lab] = bb
        b_blk[t, n_lab:n_lab + 8] = bt
        return al, ab, at, bl, bb, bt

    per_tile = frames // n_lat

    def lattice_side(k, carry):
        for u in range(per_tile):
            carry = lat_step(k * per_tile + u, carry)
        return carry

    n_occ = hi - lo - n_lat
    occ_group = frames // n_occ // 64
    back32 = jnp.where(lane32 >= 64, 1, 0)
    back8 = jnp.where(lane8 >= 64, 1, 0)
    run = z_oth_loop(lo, hi, h_ref, w_hbm, z_hbm, wbuf, wsem, zbuf, zsem, m_ref, s_ref,
                     [(n_lat, lattice_side, lambda: (neg32, neg32, neg8, fin_l, fin_b, fin_t)),
                      (n_occ, lambda k, c: occ_side(k, c), lambda: 0)])
    al, ab, at, _, _, _ = next(run)

    last_l = jnp.where(end_lab, al, NEG_BIG)
    last_b = jnp.where(end_blk, ab, NEG_BIG)
    last_t = jnp.where(end_top, at, NEG_BIG)
    top = jnp.maximum(jnp.maximum(jnp.max(last_l, axis=0, keepdims=True), jnp.max(last_b, axis=0, keepdims=True)), jnp.max(last_t, axis=0, keepdims=True))
    total = jnp.sum(jnp.exp(last_l - top), axis=0, keepdims=True) + jnp.sum(jnp.exp(last_b - top), axis=0, keepdims=True) + jnp.sum(jnp.exp(last_t - top), axis=0, keepdims=True)
    loss = -(top + jnp.log(total))
    loss32 = jnp.broadcast_to(loss, (n_lab, LANES))
    loss8 = jnp.broadcast_to(loss, (8, LANES))
    lane1 = lane8[0:1]
    loss_ref[...] = jnp.broadcast_to(loss - jnp.where(lane1 == 0, shift_seq0, jnp.where(lane1 == 1, shift_seq1, 0.0)), (8, LANES))

    def occ_frame(i, u, acc_l, acc_b):
        occ_l = jnp.where(i < live32, jnp.exp(a_lab[i] + b_lab[i] + loss32), 0.0)
        occ_b = jnp.exp(a_blk[i, 0:n_lab] + b_blk[i, 0:n_lab] + loss32)
        occ_u = jnp.exp(a_blk[i, n_lab:n_lab + 8] + b_blk[i, n_lab:n_lab + 8] + loss8)
        blank = jnp.sum(occ_b, axis=0, keepdims=True) + occ_u[0:1]
        blank = jnp.where(i < live8, jnp.broadcast_to(blank, (8, LANES)), 0.0)
        acc_l = jnp.where(lax.rem(lane32, 64) == u, jnp.take_along_axis(occ_l, back32, axis=1), acc_l)
        acc_b = jnp.where(lax.rem(lane8, 64) == u, jnp.take_along_axis(blank, back8, axis=1), acc_b)
        return acc_l, acc_b

    def occ_side(k, c):
        for g in range(occ_group):
            j = k * occ_group + g
            acc_l = jnp.zeros((n_lab, LANES), F32)
            acc_b = jnp.zeros((8, LANES), F32)
            for u in range(64):
                acc_l, acc_b = occ_frame(j * 64 + u, u, acc_l, acc_b)
            o_t[j, 0:n_lab] = acc_l
            o_t[j, n_lab:n_lab + 8] = acc_b
            o_t[j, 8 + n_lab:LANES] = jnp.zeros((LANES - 8 - n_lab, LANES), F32)
        return c

    for _ in run:
        pass
    row128 = lax.broadcasted_iota(jnp.int32, (LANES, LANES), 0)
    inner = (row128 < n_lab) & (lane128 < n_lab)
    same = []
    for s in range(n_seq):
        down = jnp.full((n_lab, LANES), -1, jnp.int32)
        for k in range(n_lab):
            down = jnp.where(row32 == k, meta_ref[s, k], down)
        down = jnp.concatenate([down, jnp.full((LANES - n_lab, LANES), -1, jnp.int32)], axis=0)
        across = jnp.broadcast_to(lab_row[s:s + 1], (LANES, LANES))
        same.append(jnp.where((inner & (down == across)) | (row128 == lane128), 1.0, 0.0))
    for j in range(n_blk):
        y = o_t[j].T
        for s in range(2):
            occ_ref[pl.ds(s * frames + 64 * j, 64), :] = jnp.dot(y[64 * s:64 * (s + 1), :], same[s], precision=lax.Precision.HIGHEST, preferred_element_type=F32)


def combine_stats(refs):
    m = functools.reduce(jnp.maximum, [r[0:8, :] for r in refs])
    tot = functools.reduce(jnp.add, [r[8:16, :] * jnp.exp(r[0:8, :] - m) for r in refs])
    return m + jnp.log(tot)


def spread_lse(refs, meta_ref, lse_ref, r0, frames):
    row = combine_stats(refs)
    n = row.shape[1]
    cols = jnp.broadcast_to(row[0:1, :], (LANES, n)).T
    t = lax.broadcasted_iota(jnp.int32, (frames, LANES), 0)
    sums = []
    for s in range(n // frames):
        part = cols[s * frames:(s + 1) * frames]
        live = t < meta_ref[s, meta_ref.shape[1] - 2]
        lse_ref[pl.ds(r0 + s * frames, frames), :] = jnp.where(live, part, 1.0e30)
        sums.append(jnp.sum(jnp.where(live, part, 0.0), axis=0, keepdims=True))
    return sums


def patch_tile(n_slots, frames, meta_refs, col_start, j, i, z_block, lse_ref, occ_ref, g_ref, lane):
    seq, item = i // n_slots, lax.rem(i, n_slots)
    off = label_col(meta_refs, i) - col_start - j * TILE
    blk = off // LANES
    r0 = pl.multiple_of(seq * frames, frames)
    c0 = pl.multiple_of(blk * LANES, LANES)
    zb = z_block(seq, c0)
    slot_lane = jnp.where(item == 0, n_slots - 1, item - 1)
    occ = jnp.sum(jnp.where(lane == slot_lane, occ_ref[pl.ds(r0, frames), :], 0.0), axis=1, keepdims=True)
    fresh = jnp.exp(zb - lse_ref[pl.ds(r0, frames), :]) - occ
    old = g_ref[pl.ds(r0, frames), pl.ds(c0, LANES)].astype(F32)
    g_ref[pl.ds(r0, frames), pl.ds(c0, LANES)] = jnp.where(lane == off - blk * LANES, fresh, old).astype(BF16)


def softmax_tile(z, lse, out, r0, n):
    for k in range(TILE // LANES):
        sl = slice(k * LANES, (k + 1) * LANES)
        out[r0:r0 + n, sl] = jnp.exp(z[:, sl] - lse[r0:r0 + n, :]).astype(BF16)


def grad_h_kernel(n_slots, z_hbm, w_hbm, st0, st1, st2, st3, occ_ref, part_loss, meta_ref, keep_ref, send_ref, loss_ref,
                  wbuf, wsem, zbuf, zsem, acc, lse_ref, g0, g1, head, nxt):
    n_tiles, rows = z_hbm.shape[0], z_hbm.shape[1]
    frames = rows // meta_ref.shape[0]
    meta_refs = [meta_ref]
    stream = TileStream(w_hbm, wbuf, wsem, wbuf.shape[0], n_tiles, w_view)
    zs = TileStream(z_hbm, zbuf, zsem, zbuf.shape[0], n_tiles, z_view)
    zs.prime()
    stream.prime()
    col_start = build_lists(meta_refs, n_tiles * TILE, head, nxt)
    sums = spread_lse([st0, st1, st2, st3], meta_ref, lse_ref, 0, frames)
    lane1 = lax.broadcasted_iota(jnp.int32, (8, LANES), 1)
    loss_ref[...] = part_loss[...] + jnp.where(lane1 == 0, sums[0], sums[1])
    lane = lax.broadcasted_iota(jnp.int32, (frames, LANES), 1)

    def make_g(slot, g):
        softmax_tile(zbuf.at[slot], lse_ref, g, 0, rows)

    def patch(j, slot, g):
        def z_block(seq, c0):
            return zbuf[slot, pl.ds(pl.multiple_of(seq * frames, frames), frames), pl.ds(c0, LANES)]

        walk_list(head, nxt, j, lambda i: patch_tile(n_slots, frames, meta_refs, col_start, j, i, z_block, lse_ref, occ_ref, g, lane))

    acc[...] = jnp.zeros(acc.shape, F32)
    slot0 = zs.get(0)
    make_g(slot0, g0)
    patch(0, slot0, g0)

    def half(j, g_now, g_next):
        slot = stream.get(j)
        nj = lax.min(j + 1, n_tiles - 1)

        @pl.when(j + 1 < n_tiles)
        def _():
            zs.get(nj)

        zslot = lax.rem(nj, zbuf.shape[0])
        acc[...] += lax.dot_general(g_now[...], wbuf[slot], (((1,), (1,)), ((), ())), preferred_element_type=F32)
        make_g(zslot, g_next)
        patch(nj, zslot, g_next)

    def step(i, c):
        half(2 * i, g0, g1)
        half(2 * i + 1, g1, g0)
        return c

    lax.fori_loop(0, n_tiles // 2, step, 0)
    core = lax.rem(lax.axis_index("tp"), 2)
    n = rows // 2
    keep_ref[...] = acc[pl.ds(pl.multiple_of(core * n, n), n), :]
    send_ref[...] = acc[pl.ds(pl.multiple_of((1 - core) * n, n), n), :]


def grad_w_kernel(n_slots, zo_hbm, zx_hbm, h_own_ref, h_oth_ref, st0, st1, st2, st3, sx0, sx1, sx2, sx3, occ_own_ref, occ_oth_ref, meta_own, meta_oth, gw_hbm,
                  zo_buf, zo_sem, zx_buf, zx_sem, obuf, osem, ht, lse_ref, occ_ref, g0, g1, head, nxt):
    n_tiles, rows = zo_hbm.shape[0], zo_hbm.shape[1]
    meta_refs = [meta_own, meta_oth]
    n_half = meta_own.shape[0]
    frames = rows // n_half
    d_loc = ht.shape[0]
    zo = TileStream(zo_hbm, zo_buf, zo_sem, zo_buf.shape[0], n_tiles, z_view)
    zx = TileStream(zx_hbm, zx_buf, zx_sem, zx_buf.shape[0], n_tiles, z_view)
    zo.prime()
    zx.prime()
    col_start = build_lists(meta_refs, n_tiles * TILE, head, nxt)
    d0 = pl.multiple_of(lax.axis_index("dp") * d_loc, LANES)
    ht[:, 0:rows] = h_own_ref[:, pl.ds(d0, d_loc)].T
    ht[:, rows:2 * rows] = h_oth_ref[:, pl.ds(d0, d_loc)].T
    spread_lse([st0, st1, st2, st3], meta_own, lse_ref, 0, frames)
    spread_lse([sx0, sx1, sx2, sx3], meta_oth, lse_ref, rows, frames)
    occ_ref[0:rows] = occ_own_ref[...]
    occ_ref[rows:2 * rows] = occ_oth_ref[...]
    lane = lax.broadcasted_iota(jnp.int32, (frames, LANES), 1)

    def make_g(slot, g):
        softmax_tile(zo_buf.at[slot], lse_ref, g, 0, rows)
        softmax_tile(zx_buf.at[slot], lse_ref, g, rows, rows)

    def patch(j, slot, g):
        def z_own(seq, c0):
            return zo_buf[slot, pl.ds(pl.multiple_of(seq * frames, frames), frames), pl.ds(c0, LANES)]

        def z_oth(seq, c0):
            return zx_buf[slot, pl.ds(pl.multiple_of((seq - n_half) * frames, frames), frames), pl.ds(c0, LANES)]

        def visit(i):
            @pl.when(i < n_half * n_slots)
            def _():
                patch_tile(n_slots, frames, meta_refs, col_start, j, i, z_own, lse_ref, occ_ref, g, lane)

            @pl.when(i >= n_half * n_slots)
            def _():
                patch_tile(n_slots, frames, meta_refs, col_start, j, i, z_oth, lse_ref, occ_ref, g, lane)

        walk_list(head, nxt, j, visit)

    def out_copy(j):
        slot = lax.rem(j, 2)
        return pltpu.make_async_copy(obuf.at[slot], w_view(gw_hbm, j), osem.at[slot])

    slot0 = zo.get(0)
    zx.get(0)
    make_g(slot0, g0)
    patch(0, slot0, g0)

    def half(j, g_now, g_next):
        @pl.when(j >= 2)
        def _():
            out_copy(j - 2).wait()

        nj = lax.min(j + 1, n_tiles - 1)

        @pl.when(j + 1 < n_tiles)
        def _():
            zo.get(nj)
            zx.get(nj)

        slot = lax.rem(nj, zo_buf.shape[0])
        obuf[lax.rem(j, 2)] = jnp.dot(ht[...], g_now[...], preferred_element_type=F32)
        make_g(slot, g_next)
        out_copy(j).start()
        patch(nj, slot, g_next)

    def step(i, c):
        half(2 * i, g0, g1)
        half(2 * i + 1, g1, g0)
        return c

    lax.fori_loop(0, n_tiles // 2, step, 0)
    out_copy(n_tiles - 2).wait()
    out_copy(n_tiles - 1).wait()


def cost(flops, nbytes, trans=0):
    return pl.CostEstimate(flops=flops, bytes_accessed=nbytes, transcendentals=trans)


def solution(mesh):
    batch_axes = ("part", "dp")
    n_tp = mesh.shape["tp"]
    n_dp = mesh.shape["dp"]
    dp_swap = [(i, n_dp - 1 - i) for i in range(n_dp)]

    def tp_xor(x, mask):
        return lax.ppermute(x, "tp", [(i, i ^ mask) for i in range(n_tp)])

    def local_step(hidden, w_loc, labels, in_len, lab_len):
        batch_loc, frames, model_dim = hidden.shape
        vocab_loc = w_loc.shape[1]
        n_lab = labels.shape[1]
        n_slots = n_lab + 1
        rows = batch_loc * frames
        n_tiles = vocab_loc // TILE
        d_loc = model_dim // n_dp
        dma = pltpu.SemaphoreType.DMA
        i32 = jnp.int32
        cut_a, cut_c, n_lat = 8, 28, 16
        h_own = hidden.reshape(rows, model_dim)
        core = lax.rem(lax.axis_index("tp"), 2)
        h_half = lax.dynamic_index_in_dim(h_own.reshape(2, rows // 2, model_dim), core, 0, keepdims=False)
        h_got = lax.ppermute(h_half, "dp", dp_swap)
        meta = jnp.concatenate([labels, in_len[:, None], lab_len[:, None]], axis=1)
        meta_oth = lax.ppermute(meta, "dp", dp_swap)
        flops = 2 * rows * model_dim * TILE
        wbytes = model_dim * TILE * 2
        zbytes = rows * TILE * 4
        z_type = jax.ShapeDtypeStruct((n_tiles, rows, TILE), F32)
        run_type = jax.ShapeDtypeStruct((rows, LANES), F32)
        pick_type = jax.ShapeDtypeStruct((frames, LANES), F32)
        stat_type = jax.ShapeDtypeStruct((16, rows), F32)
        w_scratch = [pltpu.VMEM((3, model_dim, TILE), BF16), dma((3,))]
        zo_scratch = [pltpu.VMEM((2, rows, TILE), F32), dma((2,))]
        zi_scratch = [pltpu.VMEM((3, rows, TILE), F32), dma((3,))]
        run_scratch = [pltpu.VMEM((rows, LANES), F32), pltpu.VMEM((rows, LANES), F32)]

        def lists(n_sets):
            return [pltpu.SMEM((n_tiles,), i32), pltpu.SMEM((n_sets * batch_loc * n_slots,), i32)]

        z_own, stats_own, pick = pl.pallas_call(
            functools.partial(z_own_kernel, n_slots),
            out_shape=(z_type, stat_type, pick_type),
            in_specs=[vmem_spec(), any_spec(), smem_spec()],
            out_specs=(any_spec(), vmem_spec(), vmem_spec()),
            scratch_shapes=w_scratch + zo_scratch + run_scratch + lists(1),
            compiler_params=params(48 * MIB),
            cost_estimate=cost(n_tiles * flops, n_tiles * (wbytes + zbytes)),
            name="z_own",
        )(h_own, w_loc, meta)

        h_got, stats_own = lax.optimization_barrier((h_got, stats_own))
        h_core = tp_xor(h_got, 1)
        picks = [pick] + [tp_xor(pick, k) for k in (1, 2, 3)]
        st_own = [stats_own] + [tp_xor(stats_own, k) for k in (1, 2, 3)]

        z_part, run_m, run_s, h_oth = pl.pallas_call(
            functools.partial(z_first_kernel, 0, cut_a),
            out_shape=(z_type, run_type, run_type, jax.ShapeDtypeStruct((rows, model_dim), BF16)),
            in_specs=[vmem_spec(), vmem_spec(), any_spec(), smem_spec()],
            out_specs=(any_spec(), vmem_spec(), vmem_spec(), vmem_spec()),
            scratch_shapes=w_scratch + zo_scratch,
            compiler_params=params(48 * MIB),
            cost_estimate=cost(cut_a * flops, cut_a * (wbytes + zbytes)),
            name="z_first",
        )(h_got, h_core, w_loc, meta_oth)

        n_blk = frames // 64
        z_part, run_m, run_s, occ, part_loss = pl.pallas_call(
            functools.partial(z_lattice_kernel, cut_a, cut_c, n_lat, n_lab),
            out_shape=(z_type, run_type, run_type, run_type, jax.ShapeDtypeStruct((8, LANES), F32)),
            in_specs=[vmem_spec(), any_spec()] + [vmem_spec()] * 6 + [smem_spec(), any_spec()],
            out_specs=(any_spec(),) + (vmem_spec(),) * 4,
            input_output_aliases={9: 0},
            scratch_shapes=w_scratch + zo_scratch + [
                pltpu.VMEM((n_blk, n_lab, LANES), F32), pltpu.VMEM((n_blk, 8, LANES), F32),
                pltpu.VMEM((frames, n_lab, LANES), F32), pltpu.VMEM((frames, n_lab + 8, LANES), F32),
                pltpu.VMEM((frames, n_lab, LANES), F32), pltpu.VMEM((frames, n_lab + 8, LANES), F32),
                pltpu.VMEM((n_blk, LANES, LANES), F32)],
            compiler_params=params(48 * MIB),
            cost_estimate=cost((cut_c - cut_a) * flops, (cut_c - cut_a) * (wbytes + zbytes)),
            name="z_lattice",
        )(h_oth, w_loc, run_m, run_s, *picks, meta, z_part)

        keep, send, loss = pl.pallas_call(
            functools.partial(grad_h_kernel, n_slots),
            out_shape=(jax.ShapeDtypeStruct((rows // 2, model_dim), F32), jax.ShapeDtypeStruct((rows // 2, model_dim), F32), jax.ShapeDtypeStruct((8, LANES), F32)),
            in_specs=[any_spec(), any_spec()] + [vmem_spec()] * 6 + [smem_spec()],
            out_specs=(vmem_spec(),) * 3,
            scratch_shapes=w_scratch + zi_scratch + [pltpu.VMEM((rows, model_dim), F32), pltpu.VMEM((rows, LANES), F32),
                                                     pltpu.VMEM((rows, TILE), BF16), pltpu.VMEM((rows, TILE), BF16)] + lists(1),
            compiler_params=params(48 * MIB),
            cost_estimate=cost(n_tiles * flops, n_tiles * (wbytes + zbytes)),
            name="grad_h",
        )(z_own, w_loc, *st_own, occ, part_loss, meta)
        occ_oth = lax.ppermute(occ, "dp", dp_swap)

        h_late, send = lax.optimization_barrier((h_oth, send))
        recv = tp_xor(send, 1)
        z_oth, stats_oth = pl.pallas_call(
            functools.partial(z_last_kernel, cut_c, n_tiles),
            out_shape=(z_type, stat_type),
            in_specs=[vmem_spec(), any_spec(), vmem_spec(), vmem_spec(), any_spec()],
            out_specs=(any_spec(), vmem_spec()),
            input_output_aliases={4: 0},
            scratch_shapes=w_scratch + zo_scratch + run_scratch,
            compiler_params=params(48 * MIB),
            cost_estimate=cost((n_tiles - cut_c) * flops, (n_tiles - cut_c) * (wbytes + zbytes)),
            name="z_last",
        )(h_late, w_loc, run_m, run_s, z_part)
        keep, stats_oth = lax.optimization_barrier((keep, stats_oth))
        chip_sum = keep + recv
        across = tp_xor(chip_sum, 2)
        st_oth = [stats_oth] + [tp_xor(stats_oth, k) for k in (1, 2, 3)]

        grad_weight = pl.pallas_call(
            functools.partial(grad_w_kernel, n_slots),
            out_shape=jax.ShapeDtypeStruct((d_loc, vocab_loc), F32),
            in_specs=[any_spec(), any_spec()] + [vmem_spec()] * 12 + [smem_spec()] * 2,
            out_specs=any_spec(),
            scratch_shapes=zi_scratch + zi_scratch + [
                pltpu.VMEM((2, d_loc, TILE), F32), dma((2,)),
                pltpu.VMEM((d_loc, 2 * rows), BF16), pltpu.VMEM((2 * rows, LANES), F32), pltpu.VMEM((2 * rows, LANES), F32),
                pltpu.VMEM((2 * rows, TILE), BF16), pltpu.VMEM((2 * rows, TILE), BF16)] + lists(2),
            compiler_params=params(48 * MIB),
            cost_estimate=cost(n_tiles * flops, n_tiles * (2 * zbytes + d_loc * TILE * 4)),
            name="grad_w",
        )(z_own, z_oth, h_own, h_oth, *st_own, *st_oth, occ, occ_oth, meta, meta_oth)

        chip_sum, grad_weight = lax.optimization_barrier((chip_sum, grad_weight))
        full_half = chip_sum + across
        other_half = tp_xor(full_half, 1)
        grad_hidden = jnp.where(core == 0, jnp.stack([full_half, other_half]), jnp.stack([other_half, full_half])).reshape(batch_loc, frames, model_dim)
        return loss[0, :batch_loc], grad_weight, grad_hidden

    return jax.shard_map(
        local_step,
        mesh=mesh,
        in_specs=(P(batch_axes, None, None), P(None, "tp"), P(batch_axes, None), P(batch_axes), P(batch_axes)),
        out_specs=(P(batch_axes), P(batch_axes, "tp"), P(batch_axes, None, None)),
        check_vma=False,
    )
```

```python
import functools

import jax
import jax.numpy as jnp
from jax import lax
from jax.experimental import pallas as pl
from jax.experimental.pallas import tpu as pltpu
from jax.sharding import PartitionSpec as P

NEG_BIG = -1.0e30
F32 = jnp.float32
BF16 = jnp.bfloat16
TILE = 512
LANES = 128
MIB = 1 << 20


def vmem_spec():
    return pl.BlockSpec(memory_space=pltpu.VMEM)


def smem_spec():
    return pl.BlockSpec(memory_space=pltpu.SMEM)


def any_spec():
    return pl.BlockSpec(memory_space=pl.ANY)


def params(limit):
    return pltpu.CompilerParams(vmem_limit_bytes=limit)


def label_col(meta_refs, i):
    n_slots = meta_refs[0].shape[1] - 1
    seq, item = i // n_slots, lax.rem(i, n_slots)
    n_seq = meta_refs[0].shape[0]
    at = lax.max(item - 1, 0)
    col = meta_refs[0][lax.rem(seq, n_seq), at]
    for k in range(1, len(meta_refs)):
        col = jnp.where(seq >= k * n_seq, meta_refs[k][lax.rem(seq, n_seq), at], col)
    return jnp.where(item == 0, 0, col)


def build_lists(meta_refs, vocab_loc, head, nxt):
    n_items = len(meta_refs) * meta_refs[0].shape[0] * (meta_refs[0].shape[1] - 1)
    col_start = lax.axis_index("tp") * vocab_loc
    n_tiles = vocab_loc // TILE

    def clear(i, c):
        head[i] = -1
        return c

    lax.fori_loop(0, n_tiles, clear, 0)

    def insert(i, c):
        loc = label_col(meta_refs, i) - col_start
        tile = lax.max(loc, 0) // TILE

        @pl.when((loc >= 0) & (loc < vocab_loc))
        def _():
            nxt[i] = head[tile]
            head[tile] = i

        return c

    lax.fori_loop(0, n_items, insert, 0)
    return col_start


def walk_list(head, nxt, tile, visit):
    def body(i):
        visit(i)
        return nxt[i]

    lax.while_loop(lambda i: i >= 0, body, head[tile])


class TileStream:
    def __init__(self, src, buf, sem, depth, n_tiles, view):
        self.src, self.buf, self.sem, self.depth, self.n, self.view = src, buf, sem, depth, n_tiles, view

    def copy(self, j):
        slot = lax.rem(j, self.depth)
        return pltpu.make_async_copy(self.view(self.src, j), self.buf.at[slot], self.sem.at[slot])

    def prime(self):
        for j in range(self.depth - 1):
            self.copy(j).start()

    def get(self, j):
        self.copy(j).wait()

        @pl.when(j + self.depth - 1 < self.n)
        def _():
            self.copy(j + self.depth - 1).start()

        return lax.rem(j, self.depth)


def w_view(src, j, n=1):
    return src.at[:, pl.ds(pl.multiple_of(j * n * TILE, TILE), n * TILE)]


def z_view(src, j, n):
    return src.at[pl.ds(j * n, n)]


def exact_zero(x):
    total = x[0:16, 0:LANES]
    for c in range(x.shape[1] // LANES):
        for r in range(x.shape[0] // 16):
            if r or c:
                total = total + x[16 * r:16 * (r + 1), c * LANES:(c + 1) * LANES]
    return jnp.minimum(total, 0.0).astype(BF16)


def after(lhs, zero):
    if zero is None:
        return lhs
    corner = lhs[0:16, 0:LANES] + zero
    return jnp.concatenate([jnp.concatenate([corner, lhs[0:16, LANES:]], axis=1), lhs[16:]], axis=0)


def unit_stats(z, m_old, s_old):
    n_chunks = z.shape[1] // LANES
    m_new = m_old
    for k in range(n_chunks):
        m_new = jnp.maximum(m_new, z[:, k * LANES:(k + 1) * LANES])
    s_new = s_old * jnp.exp(m_old - m_new)
    for k in range(n_chunks):
        s_new = s_new + jnp.exp(z[:, k * LANES:(k + 1) * LANES] - m_new)
    return m_new, s_new


def z_group(h_ref, w, z_out, m_ref, s_ref):
    n_tiles = z_out.shape[0]
    n = h_ref.shape[0] // 2
    zeros = []
    for t in range(n_tiles):
        for r in range(2):
            rows = slice(r * n, (r + 1) * n)
            lhs = after(h_ref[rows, :], zeros[-2] if len(zeros) >= 2 else None)
            z = jnp.dot(lhs, w[:, t * TILE:(t + 1) * TILE], preferred_element_type=F32)
            z_out[t, rows, :] = z
            m_new, s_new = unit_stats(z, m_ref[rows, :], s_ref[rows, :])
            m_ref[rows, :] = m_new
            s_ref[rows, :] = s_new
            zeros.append(exact_zero(s_new))


def emit_stats(m_ref, s_ref, stats_ref):
    row_m = jnp.max(m_ref[...], axis=1, keepdims=True)
    row_s = jnp.sum(s_ref[...] * jnp.exp(m_ref[...] - row_m), axis=1, keepdims=True)
    rows = m_ref.shape[0]
    m_t = jnp.broadcast_to(row_m, (rows, LANES)).T
    s_t = jnp.broadcast_to(row_s, (rows, LANES)).T
    stats_ref[0:8, :] = m_t[0:8, :]
    stats_ref[8:16, :] = s_t[0:8, :]


def z_own_kernel(n_slots, h_ref, w_hbm, meta_ref, z_hbm, stats_ref, pick_ref, wbuf, wsem, zbuf, zsem, m_ref, s_ref, head, nxt):
    n_tiles = z_hbm.shape[0]
    rows = h_ref.shape[0]
    n_seq = meta_ref.shape[0]
    frames = rows // n_seq
    group = zbuf.shape[1]
    stream = TileStream(w_hbm, wbuf, wsem, wbuf.shape[0], n_tiles // group, lambda src, j: w_view(src, j, group))
    stream.prime()
    col_start = build_lists([meta_ref], n_tiles * TILE, head, nxt)
    m_ref[...] = jnp.full(m_ref.shape, NEG_BIG, F32)
    s_ref[...] = jnp.zeros(s_ref.shape, F32)
    pick_ref[...] = jnp.zeros(pick_ref.shape, F32)
    lane = lax.broadcasted_iota(jnp.int32, (frames, LANES), 1)

    def out_copy(j):
        slot = lax.rem(j, 2)
        return pltpu.make_async_copy(zbuf.at[slot], z_view(z_hbm, j, group), zsem.at[slot])

    def step(j, c):
        slot = stream.get(j)

        @pl.when(j >= 2)
        def _():
            out_copy(j - 2).wait()

        zslot = lax.rem(j, 2)
        z_group(h_ref, wbuf.at[slot], zbuf.at[zslot], m_ref, s_ref)
        out_copy(j).start()

        for t in range(group):
            def visit(i, t=t):
                seq, item = i // n_slots, lax.rem(i, n_slots)
                off = label_col([meta_ref], i) - col_start - (j * group + t) * TILE
                blk = off // LANES
                r0 = pl.multiple_of(seq * frames, frames)
                zb = zbuf[zslot, t, pl.ds(r0, frames), pl.ds(pl.multiple_of(blk * LANES, LANES), LANES)]
                at = item + 64 * seq
                moved = pltpu.roll(zb, lax.rem(at - (off - blk * LANES) + 2 * LANES, LANES), 1)
                pick_ref[...] = jnp.where(lane == at, moved, pick_ref[...])

            walk_list(head, nxt, j * group + t, visit)
        return c

    n_groups = n_tiles // group
    lax.fori_loop(0, n_groups, step, 0)
    emit_stats(m_ref, s_ref, stats_ref)
    out_copy(n_groups - 2).wait()
    out_copy(n_groups - 1).wait()


def z_oth_loop(lo, hi, h_ref, w_hbm, z_hbm, wbuf, wsem, zbuf, zsem, m_ref, s_ref, sections):
    group = zbuf.shape[1]
    lo, n_groups = lo // group, (hi - lo) // group
    stream = TileStream(w_hbm, wbuf, wsem, wbuf.shape[0], n_groups, lambda src, j: w_view(src, lo + j, group))
    stream.prime()

    def out_copy(j):
        slot = lax.rem(j, 2)
        return pltpu.make_async_copy(zbuf.at[slot], z_view(z_hbm, lo + j, group), zsem.at[slot])

    base = 0
    for n, side, make_carry in sections:
        carry = make_carry()

        def step(k, c, base=base, side=side):
            j = base + k
            slot = stream.get(j)

            @pl.when(j >= 2)
            def _():
                out_copy(j - 2).wait()

            z_group(h_ref, wbuf.at[slot], zbuf.at[lax.rem(j, 2)], m_ref, s_ref)
            c = side(k, c)
            out_copy(j).start()
            return c

        last = lax.fori_loop(0, n, step, carry)
        yield last
        base += n
    for j in range(max(n_groups - 2, 0), n_groups):
        out_copy(j).wait()


def join_rows(h_got, h_core, h_ref):
    n = h_got.shape[0]
    core = lax.rem(lax.axis_index("tp"), 2)
    h_ref[pl.ds(pl.multiple_of(core * n, n), n), :] = h_got[...]
    h_ref[pl.ds(pl.multiple_of((1 - core) * n, n), n), :] = h_core[...]


def z_first_kernel(lo, hi, h_got, h_core, w_hbm, meta_oth, z_hbm, m_ref, s_ref, h_ref, wbuf, wsem, zbuf, zsem):
    join_rows(h_got, h_core, h_ref)
    m_ref[...] = jnp.full(m_ref.shape, NEG_BIG, F32)
    s_ref[...] = jnp.zeros(s_ref.shape, F32)
    for _ in z_oth_loop(lo, hi, h_ref, w_hbm, z_hbm, wbuf, wsem, zbuf, zsem, m_ref, s_ref, [((hi - lo) // zbuf.shape[1], lambda k, c: c, lambda: 0)]):
        pass


def z_last_kernel(lo, hi, h_ref, w_hbm, m_in, s_in, z_in, z_hbm, stats_ref, wbuf, wsem, zbuf, zsem, m_ref, s_ref):
    m_ref[...] = m_in[...]
    s_ref[...] = s_in[...]
    for _ in z_oth_loop(lo, hi, h_ref, w_hbm, z_hbm, wbuf, wsem, zbuf, zsem, m_ref, s_ref, [((hi - lo) // zbuf.shape[1], lambda k, c: c, lambda: 0)]):
        pass
    emit_stats(m_ref, s_ref, stats_ref)


def z_lattice_kernel(lo, hi, n_lat, n_lab, h_ref, w_hbm, m_in, s_in, p0, p1, p2, p3, meta_ref, z_in,
                     z_hbm, m_ref, s_ref, occ_ref, loss_ref,
                     wbuf, wsem, zbuf, zsem, e_lab, e_blk, a_lab, a_blk, b_lab, b_blk, o_t):
    n_blk = e_lab.shape[0]
    frames = n_blk * 64
    m_ref[...] = m_in[...]
    s_ref[...] = s_in[...]
    lane128 = lax.broadcasted_iota(jnp.int32, (LANES, LANES), 1)
    row32 = lax.broadcasted_iota(jnp.int32, (n_lab, LANES), 0)
    row8 = lax.broadcasted_iota(jnp.int32, (8, LANES), 0)
    lane32 = lax.broadcasted_iota(jnp.int32, (n_lab, LANES), 1)
    lane8 = lax.broadcasted_iota(jnp.int32, (8, LANES), 1)
    n_seq = meta_ref.shape[0]
    labs = jnp.zeros((n_lab, LANES), jnp.int32)
    lab_row = jnp.zeros((8, LANES), jnp.int32)
    live8 = jnp.zeros((8, LANES), jnp.int32)
    used8 = jnp.zeros((8, LANES), jnp.int32)
    for s in range(n_seq):
        for k in range(n_lab):
            labs = jnp.where((row32 == k) & (lane32 == s), meta_ref[s, k], labs)
            lab_row = jnp.where((row8 == s) & (lane8 == k), meta_ref[s, k], lab_row)
        live8 = jnp.where(lane8 == s, meta_ref[s, n_lab], live8)
        used8 = jnp.where(lane8 == s, meta_ref[s, n_lab + 1], used8)
    live32 = jnp.broadcast_to(live8[0:1], (n_lab, LANES))
    used32 = jnp.broadcast_to(used8[0:1], (n_lab, LANES))
    skip_dn = labs != pltpu.roll(labs, 1, 0)
    skip_up = labs != pltpu.roll(labs, n_lab - 1, 0)
    end_lab = row32 == used32 - 1
    end_blk = row32 == used32
    end_top = (row8 == 0) & (used8 == n_lab)
    shift0 = jnp.zeros((1, LANES), F32)
    seq1 = lane8[0:1] >= 64
    half_len = jnp.where(seq1, meta_ref[1, n_lab], meta_ref[0, n_lab])
    for j in range(n_blk):
        part = functools.reduce(jnp.add, [p[pl.ds(64 * j, 64), :] for p in (p0, p1, p2, p3)])
        blk = jnp.concatenate([part, pltpu.roll(part, 64, 1)], axis=0)
        blk = jnp.where(lane128 <= n_lab, blk, NEG_BIG)
        x = blk.T
        top = jnp.max(x[0:n_lab + 8], axis=0, keepdims=True)
        e_blk[j] = jnp.broadcast_to(x[0:1] - top, (8, LANES))
        e_lab[j] = pltpu.roll(x, LANES - 1, 0)[0:n_lab] - top
        shift0 = shift0 + jnp.where(lax.rem(lane8[0:1], 64) + 64 * j < half_len, top, 0.0)
    shift_seq0 = jnp.sum(jnp.where(seq1, 0.0, shift0), axis=1, keepdims=True)
    shift_seq1 = jnp.sum(jnp.where(seq1, shift0, 0.0), axis=1, keepdims=True)

    def lse2(a, b):
        hi_v = jnp.maximum(a, b)
        return hi_v + jnp.log(1.0 + jnp.exp(jnp.minimum(a, b) - hi_v))

    def lse3(a, b, c):
        hi_v = jnp.maximum(a, b)
        lo_v = jnp.minimum(a, b)
        top = jnp.maximum(hi_v, c)
        mid = jnp.minimum(hi_v, c)
        return top + jnp.log(1.0 + jnp.exp(lo_v - top) + jnp.exp(mid - top))

    def emission(t):
        j, u = t // 64, lax.rem(t, 64)
        idx32 = jnp.where(lane32 == 1, 64 + u, u)
        idx8 = jnp.where(lane8 == 1, 64 + u, u)
        el = jnp.take_along_axis(e_lab[j], idx32, axis=1)
        eb = jnp.take_along_axis(e_blk[j], idx8, axis=1)
        return el, eb

    neg32 = jnp.full((n_lab, LANES), NEG_BIG, F32)
    neg8 = jnp.full((8, LANES), NEG_BIG, F32)
    start32 = jnp.where(row32 == 0, 0.0, NEG_BIG)
    fin_l = jnp.where(end_lab, 0.0, NEG_BIG)
    fin_b = jnp.where(end_blk, 0.0, NEG_BIG)
    fin_t = jnp.where(end_top, 0.0, NEG_BIG)

    def lat_step(i, carry):
        al, ab, at, bl, bb, bt = carry
        el, eb = emission(i)
        eb32 = jnp.broadcast_to(eb[0:1], (n_lab, LANES))
        rolled = pltpu.roll(al, 1, 0)
        prev = jnp.where(row32 == 0, NEG_BIG, rolled)
        prev_t = jnp.where(row8 == 0, rolled[0:8], NEG_BIG)
        first = i == 0
        nl = jnp.where(first, start32, lse3(al, ab, jnp.where(skip_dn, prev, NEG_BIG)))
        nb = jnp.where(first, start32, lse2(ab, prev))
        nt = jnp.where(first, neg8, lse2(at, prev_t))
        a_lab[i] = nl
        a_blk[i, 0:n_lab] = nb
        a_blk[i, n_lab:n_lab + 8] = nt
        al = jnp.where(i < live32, el + nl, al)
        ab = jnp.where(i < live32, eb32 + nb, ab)
        at = jnp.where(i < live8, eb + nt, at)
        t = frames - 1 - i
        fl, fb = emission(t)
        fb32 = jnp.broadcast_to(fb[0:1], (n_lab, LANES))
        last = row32 == n_lab - 1
        up_l = jnp.where(last, NEG_BIG, pltpu.roll(bl, n_lab - 1, 0))
        up_b = jnp.where(last, jnp.broadcast_to(bt[0:1], (n_lab, LANES)), pltpu.roll(bb, n_lab - 1, 0))
        is_end32 = t == live32 - 1
        is_end8 = t == live8 - 1
        ml = fl + jnp.where(is_end32, fin_l, lse3(bl, up_b, jnp.where(skip_up, up_l, NEG_BIG)))
        mb = fb32 + jnp.where(is_end32, fin_b, lse2(bb, bl))
        mt = fb + jnp.where(is_end8, fin_t, bt)
        bl = jnp.where(t < live32, ml, bl)
        bb = jnp.where(t < live32, mb, bb)
        bt = jnp.where(t < live8, mt, bt)
        b_lab[t] = bl
        b_blk[t, 0:n_lab] = bb
        b_blk[t, n_lab:n_lab + 8] = bt
        return al, ab, at, bl, bb, bt

    group = zbuf.shape[1]
    n_lat_groups = n_lat // group
    per_tile = frames // n_lat_groups

    def lattice_side(k, carry):
        for u in range(per_tile):
            carry = lat_step(k * per_tile + u, carry)
        return carry

    n_occ = (hi - lo - n_lat) // group
    occ_group = frames // n_occ // 64
    back32 = jnp.where(lane32 >= 64, 1, 0)
    back8 = jnp.where(lane8 >= 64, 1, 0)
    run = z_oth_loop(lo, hi, h_ref, w_hbm, z_hbm, wbuf, wsem, zbuf, zsem, m_ref, s_ref,
                     [(n_lat_groups, lattice_side, lambda: (neg32, neg32, neg8, fin_l, fin_b, fin_t)),
                      (n_occ, lambda k, c: occ_side(k, c), lambda: 0)])
    al, ab, at, _, _, _ = next(run)

    last_l = jnp.where(end_lab, al, NEG_BIG)
    last_b = jnp.where(end_blk, ab, NEG_BIG)
    last_t = jnp.where(end_top, at, NEG_BIG)
    top = jnp.maximum(jnp.maximum(jnp.max(last_l, axis=0, keepdims=True), jnp.max(last_b, axis=0, keepdims=True)), jnp.max(last_t, axis=0, keepdims=True))
    total = jnp.sum(jnp.exp(last_l - top), axis=0, keepdims=True) + jnp.sum(jnp.exp(last_b - top), axis=0, keepdims=True) + jnp.sum(jnp.exp(last_t - top), axis=0, keepdims=True)
    loss = -(top + jnp.log(total))
    loss32 = jnp.broadcast_to(loss, (n_lab, LANES))
    loss8 = jnp.broadcast_to(loss, (8, LANES))
    lane1 = lane8[0:1]
    loss_ref[...] = jnp.broadcast_to(loss - jnp.where(lane1 == 0, shift_seq0, jnp.where(lane1 == 1, shift_seq1, 0.0)), (8, LANES))

    def occ_frame(i, u, acc_l, acc_b):
        occ_l = jnp.where(i < live32, jnp.exp(a_lab[i] + b_lab[i] + loss32), 0.0)
        occ_b = jnp.exp(a_blk[i, 0:n_lab] + b_blk[i, 0:n_lab] + loss32)
        occ_u = jnp.exp(a_blk[i, n_lab:n_lab + 8] + b_blk[i, n_lab:n_lab + 8] + loss8)
        blank = jnp.sum(occ_b, axis=0, keepdims=True) + occ_u[0:1]
        blank = jnp.where(i < live8, jnp.broadcast_to(blank, (8, LANES)), 0.0)
        acc_l = jnp.where(lax.rem(lane32, 64) == u, jnp.take_along_axis(occ_l, back32, axis=1), acc_l)
        acc_b = jnp.where(lax.rem(lane8, 64) == u, jnp.take_along_axis(blank, back8, axis=1), acc_b)
        return acc_l, acc_b

    def occ_side(k, c):
        for g in range(occ_group):
            j = k * occ_group + g
            acc_l = jnp.zeros((n_lab, LANES), F32)
            acc_b = jnp.zeros((8, LANES), F32)
            for u in range(64):
                acc_l, acc_b = occ_frame(j * 64 + u, u, acc_l, acc_b)
            o_t[j, 0:n_lab] = acc_l
            o_t[j, n_lab:n_lab + 8] = acc_b
            o_t[j, 8 + n_lab:LANES] = jnp.zeros((LANES - 8 - n_lab, LANES), F32)
        return c

    for _ in run:
        pass
    row128 = lax.broadcasted_iota(jnp.int32, (LANES, LANES), 0)
    inner = (row128 < n_lab) & (lane128 < n_lab)
    same = []
    for s in range(n_seq):
        down = jnp.full((n_lab, LANES), -1, jnp.int32)
        for k in range(n_lab):
            down = jnp.where(row32 == k, meta_ref[s, k], down)
        down = jnp.concatenate([down, jnp.full((LANES - n_lab, LANES), -1, jnp.int32)], axis=0)
        across = jnp.broadcast_to(lab_row[s:s + 1], (LANES, LANES))
        same.append(jnp.where((inner & (down == across)) | (row128 == lane128), 1.0, 0.0))
    for j in range(n_blk):
        y = o_t[j].T
        for s in range(2):
            occ_ref[pl.ds(s * frames + 64 * j, 64), :] = jnp.dot(y[64 * s:64 * (s + 1), :], same[s], precision=lax.Precision.HIGHEST, preferred_element_type=F32)


def combine_stats(refs):
    m = functools.reduce(jnp.maximum, [r[0:8, :] for r in refs])
    tot = functools.reduce(jnp.add, [r[8:16, :] * jnp.exp(r[0:8, :] - m) for r in refs])
    return m + jnp.log(tot)


def spread_lse(refs, meta_ref, lse_ref, r0, frames):
    row = combine_stats(refs)
    n = row.shape[1]
    cols = jnp.broadcast_to(row[0:1, :], (LANES, n)).T
    t = lax.broadcasted_iota(jnp.int32, (frames, LANES), 0)
    sums = []
    for s in range(n // frames):
        part = cols[s * frames:(s + 1) * frames]
        live = t < meta_ref[s, meta_ref.shape[1] - 2]
        lse_ref[pl.ds(r0 + s * frames, frames), :] = jnp.where(live, part, 1.0e30)
        sums.append(jnp.sum(jnp.where(live, part, 0.0), axis=0, keepdims=True))
    return sums


def patch_tile(n_slots, frames, meta_refs, col_start, j, i, z_block, lse_ref, occ_ref, g_ref, g_col, lane):
    seq, item = i // n_slots, lax.rem(i, n_slots)
    off = label_col(meta_refs, i) - col_start - j * TILE
    blk = off // LANES
    r0 = pl.multiple_of(seq * frames, frames)
    c0 = pl.multiple_of(blk * LANES, LANES)
    zb = z_block(seq, c0)
    slot_lane = jnp.where(item == 0, n_slots - 1, item - 1)
    occ = jnp.sum(jnp.where(lane == slot_lane, occ_ref[pl.ds(r0, frames), :], 0.0), axis=1, keepdims=True)
    fresh = jnp.exp(zb - lse_ref[pl.ds(r0, frames), :]) - occ
    gc = pl.multiple_of(g_col + c0, LANES)
    old = g_ref[pl.ds(r0, frames), pl.ds(gc, LANES)].astype(F32)
    g_ref[pl.ds(r0, frames), pl.ds(gc, LANES)] = jnp.where(lane == off - blk * LANES, fresh, old).astype(BF16)


def softmax_unit(z, lse_ref, out, r0, c0):
    n = z.shape[0]
    total = None
    for k in range(z.shape[1] // LANES):
        e = jnp.exp(z[:, k * LANES:(k + 1) * LANES] - lse_ref[r0:r0 + n, :])
        out[r0:r0 + n, c0 + k * LANES:c0 + (k + 1) * LANES] = e.astype(BF16)
        total = e if total is None else total + e
    return exact_zero(total)


def grad_h_kernel(n_slots, z_hbm, w_hbm, st0, st1, st2, st3, occ_ref, part_loss, meta_ref, keep_ref, send_ref, loss_ref,
                  wbuf, wsem, zbuf, zsem, acc, lse_ref, g0, g1, head, nxt):
    n_tiles, rows = z_hbm.shape[0], z_hbm.shape[1]
    frames = rows // meta_ref.shape[0]
    meta_refs = [meta_ref]
    group = zbuf.shape[1]
    n_groups = n_tiles // group
    stream = TileStream(w_hbm, wbuf, wsem, wbuf.shape[0], n_groups, lambda src, j: w_view(src, j, group))
    zs = TileStream(z_hbm, zbuf, zsem, zbuf.shape[0], n_groups, lambda src, j: z_view(src, j, group))
    zs.prime()
    stream.prime()
    col_start = build_lists(meta_refs, n_tiles * TILE, head, nxt)
    sums = spread_lse([st0, st1, st2, st3], meta_ref, lse_ref, 0, frames)
    lane1 = lax.broadcasted_iota(jnp.int32, (8, LANES), 1)
    loss_ref[...] = part_loss[...] + jnp.where(lane1 == 0, sums[0], sums[1])
    lane = lax.broadcasted_iota(jnp.int32, (frames, LANES), 1)

    def patch(j, slot, g):
        for t in range(group):
            def z_block(seq, c0, t=t):
                return zbuf[slot, t, pl.ds(pl.multiple_of(seq * frames, frames), frames), pl.ds(c0, LANES)]

            walk_list(head, nxt, j * group + t,
                      lambda i, t=t, z_block=z_block: patch_tile(n_slots, frames, meta_refs, col_start, j * group + t, i, z_block, lse_ref, occ_ref, g, t * TILE, lane))

    acc[...] = jnp.zeros(acc.shape, F32)
    slot0 = zs.get(0)
    for t in range(group):
        softmax_unit(zbuf.at[slot0, t], lse_ref, g0, 0, t * TILE)
    patch(0, slot0, g0)
    n_units = acc.shape[0] // 256

    def half(j, g_now, g_next):
        slot = stream.get(j)
        nj = lax.min(j + 1, n_groups - 1)

        @pl.when(j + 1 < n_groups)
        def _():
            zs.get(nj)

        zslot = lax.rem(nj, zbuf.shape[0])
        zeros = [None, None]
        for u in range(n_units):
            d_rows = slice(u * 256, (u + 1) * 256)
            lhs = after(wbuf[slot, d_rows, :], zeros[u])
            acc[d_rows, :] += lax.dot_general(lhs, g_now[...], (((1,), (1,)), ((), ())), preferred_element_type=F32)
            if u < group:
                zeros.append(softmax_unit(zbuf.at[zslot, u], lse_ref, g_next, 0, u * TILE))
        patch(nj, zslot, g_next)

    def step(i, c):
        half(2 * i, g0, g1)
        half(2 * i + 1, g1, g0)
        return c

    lax.fori_loop(0, n_groups // 2, step, 0)
    core = lax.rem(lax.axis_index("tp"), 2)
    n = rows // 2
    keep_ref[...] = acc[:, pl.ds(pl.multiple_of(core * n, n), n)].T
    send_ref[...] = acc[:, pl.ds(pl.multiple_of((1 - core) * n, n), n)].T


def grad_w_kernel(n_slots, zo_hbm, zx_hbm, h_own_ref, h_oth_ref, st0, st1, st2, st3, sx0, sx1, sx2, sx3, occ_own_ref, occ_oth_ref, meta_own, meta_oth, gw_hbm,
                  zo_buf, zo_sem, zx_buf, zx_sem, obuf, osem, ht, lse_ref, occ_ref, g0, g1, head, nxt):
    n_tiles, rows = zo_hbm.shape[0], zo_hbm.shape[1]
    meta_refs = [meta_own, meta_oth]
    n_half = meta_own.shape[0]
    frames = rows // n_half
    d_loc = ht.shape[0]
    group = zo_buf.shape[1]
    n_groups = n_tiles // group
    zo = TileStream(zo_hbm, zo_buf, zo_sem, zo_buf.shape[0], n_groups, lambda src, j: z_view(src, j, group))
    zx = TileStream(zx_hbm, zx_buf, zx_sem, zx_buf.shape[0], n_groups, lambda src, j: z_view(src, j, group))
    zo.prime()
    zx.prime()
    col_start = build_lists(meta_refs, n_tiles * TILE, head, nxt)
    d0 = pl.multiple_of(lax.axis_index("dp") * d_loc, LANES)
    ht[:, 0:rows] = h_own_ref[:, pl.ds(d0, d_loc)].T
    ht[:, rows:2 * rows] = h_oth_ref[:, pl.ds(d0, d_loc)].T
    spread_lse([st0, st1, st2, st3], meta_own, lse_ref, 0, frames)
    spread_lse([sx0, sx1, sx2, sx3], meta_oth, lse_ref, rows, frames)
    occ_ref[0:rows] = occ_own_ref[...]
    occ_ref[rows:2 * rows] = occ_oth_ref[...]
    lane = lax.broadcasted_iota(jnp.int32, (frames, LANES), 1)

    def patch(j, slot, g):
        for t in range(group):
            def z_own(seq, c0, t=t):
                return zo_buf[slot, t, pl.ds(pl.multiple_of(seq * frames, frames), frames), pl.ds(c0, LANES)]

            def z_oth(seq, c0, t=t):
                return zx_buf[slot, t, pl.ds(pl.multiple_of((seq - n_half) * frames, frames), frames), pl.ds(c0, LANES)]

            def visit(i, t=t, z_own=z_own, z_oth=z_oth):
                @pl.when(i < n_half * n_slots)
                def _():
                    patch_tile(n_slots, frames, meta_refs, col_start, j * group + t, i, z_own, lse_ref, occ_ref, g, t * TILE, lane)

                @pl.when(i >= n_half * n_slots)
                def _():
                    patch_tile(n_slots, frames, meta_refs, col_start, j * group + t, i, z_oth, lse_ref, occ_ref, g, t * TILE, lane)

            walk_list(head, nxt, j * group + t, visit)

    def out_copy(j):
        slot = lax.rem(j, 2)
        return pltpu.make_async_copy(obuf.at[slot], w_view(gw_hbm, j, group), osem.at[slot])

    def make_g(slot, u, g):
        t, side = u // 2, u % 2
        src = (zo_buf, zx_buf)[side]
        return softmax_unit(src.at[slot, t], lse_ref, g, side * rows, t * TILE)

    slot0 = zo.get(0)
    zx.get(0)
    for u in range(2 * group):
        make_g(slot0, u, g0)
    patch(0, slot0, g0)
    d_half = d_loc // 2

    def half(j, g_now, g_next):
        @pl.when(j >= 2)
        def _():
            out_copy(j - 2).wait()

        nj = lax.min(j + 1, n_groups - 1)

        @pl.when(j + 1 < n_groups)
        def _():
            zo.get(nj)
            zx.get(nj)

        slot = lax.rem(nj, zo_buf.shape[0])
        oslot = lax.rem(j, 2)
        zero = None
        for u in range(2 * group):
            t, r = u // 2, u % 2
            d_rows = slice(r * d_half, (r + 1) * d_half)
            lhs = after(ht[d_rows, :], zero)
            obuf[oslot, d_rows, t * TILE:(t + 1) * TILE] = jnp.dot(lhs, g_now[:, t * TILE:(t + 1) * TILE], preferred_element_type=F32)
            zero = make_g(slot, u, g_next)
        out_copy(j).start()
        patch(nj, slot, g_next)

    def step(i, c):
        half(2 * i, g0, g1)
        half(2 * i + 1, g1, g0)
        return c

    lax.fori_loop(0, n_groups // 2, step, 0)
    out_copy(n_groups - 2).wait()
    out_copy(n_groups - 1).wait()


def cost(flops, nbytes, trans=0):
    return pl.CostEstimate(flops=flops, bytes_accessed=nbytes, transcendentals=trans)


def solution(mesh):
    batch_axes = ("part", "dp")
    n_tp = mesh.shape["tp"]
    n_dp = mesh.shape["dp"]
    dp_swap = [(i, n_dp - 1 - i) for i in range(n_dp)]

    def tp_xor(x, mask):
        return lax.ppermute(x, "tp", [(i, i ^ mask) for i in range(n_tp)])

    def local_step(hidden, w_loc, labels, in_len, lab_len):
        batch_loc, frames, model_dim = hidden.shape
        vocab_loc = w_loc.shape[1]
        n_lab = labels.shape[1]
        n_slots = n_lab + 1
        rows = batch_loc * frames
        n_tiles = vocab_loc // TILE
        d_loc = model_dim // n_dp
        dma = pltpu.SemaphoreType.DMA
        i32 = jnp.int32
        cut_a, cut_c, n_lat = 8, 28, 16
        h_own = hidden.reshape(rows, model_dim)
        core = lax.rem(lax.axis_index("tp"), 2)
        h_half = lax.dynamic_index_in_dim(h_own.reshape(2, rows // 2, model_dim), core, 0, keepdims=False)
        h_got = lax.ppermute(h_half, "dp", dp_swap)
        meta = jnp.concatenate([labels, in_len[:, None], lab_len[:, None]], axis=1)
        meta_oth = lax.ppermute(meta, "dp", dp_swap)
        flops = 2 * rows * model_dim * TILE
        wbytes = model_dim * TILE * 2
        zbytes = rows * TILE * 4
        z_type = jax.ShapeDtypeStruct((n_tiles, rows, TILE), F32)
        run_type = jax.ShapeDtypeStruct((rows, LANES), F32)
        pick_type = jax.ShapeDtypeStruct((frames, LANES), F32)
        stat_type = jax.ShapeDtypeStruct((16, rows), F32)
        def w_scratch(n):
            return [pltpu.VMEM((2, model_dim, n * TILE), BF16), dma((2,))]

        def z_scratch(n):
            return [pltpu.VMEM((2, n, rows, TILE), F32), dma((2,))]

        run_scratch = [pltpu.VMEM((rows, LANES), F32), pltpu.VMEM((rows, LANES), F32)]

        def lists(n_sets):
            return [pltpu.SMEM((n_tiles,), i32), pltpu.SMEM((n_sets * batch_loc * n_slots,), i32)]

        z_own, stats_own, pick = pl.pallas_call(
            functools.partial(z_own_kernel, n_slots),
            out_shape=(z_type, stat_type, pick_type),
            in_specs=[vmem_spec(), any_spec(), smem_spec()],
            out_specs=(any_spec(), vmem_spec(), vmem_spec()),
            scratch_shapes=w_scratch(4) + z_scratch(4) + run_scratch + lists(1),
            compiler_params=params(56 * MIB),
            cost_estimate=cost(n_tiles * flops, n_tiles * (wbytes + zbytes)),
            name="z_own",
        )(h_own, w_loc, meta)

        h_got, stats_own = lax.optimization_barrier((h_got, stats_own))
        h_core = tp_xor(h_got, 1)
        picks = [pick] + [tp_xor(pick, k) for k in (1, 2, 3)]
        st_own = [stats_own] + [tp_xor(stats_own, k) for k in (1, 2, 3)]

        z_part, run_m, run_s, h_oth = pl.pallas_call(
            functools.partial(z_first_kernel, 0, cut_a),
            out_shape=(z_type, run_type, run_type, jax.ShapeDtypeStruct((rows, model_dim), BF16)),
            in_specs=[vmem_spec(), vmem_spec(), any_spec(), smem_spec()],
            out_specs=(any_spec(), vmem_spec(), vmem_spec(), vmem_spec()),
            scratch_shapes=w_scratch(4) + z_scratch(4),
            compiler_params=params(56 * MIB),
            cost_estimate=cost(cut_a * flops, cut_a * (wbytes + zbytes)),
            name="z_first",
        )(h_got, h_core, w_loc, meta_oth)

        n_blk = frames // 64
        z_part, run_m, run_s, occ, part_loss = pl.pallas_call(
            functools.partial(z_lattice_kernel, cut_a, cut_c, n_lat, n_lab),
            out_shape=(z_type, run_type, run_type, run_type, jax.ShapeDtypeStruct((8, LANES), F32)),
            in_specs=[vmem_spec(), any_spec()] + [vmem_spec()] * 6 + [smem_spec(), any_spec()],
            out_specs=(any_spec(),) + (vmem_spec(),) * 4,
            input_output_aliases={9: 0},
            scratch_shapes=w_scratch(2) + z_scratch(2) + [
                pltpu.VMEM((n_blk, n_lab, LANES), F32), pltpu.VMEM((n_blk, 8, LANES), F32),
                pltpu.VMEM((frames, n_lab, LANES), F32), pltpu.VMEM((frames, n_lab + 8, LANES), F32),
                pltpu.VMEM((frames, n_lab, LANES), F32), pltpu.VMEM((frames, n_lab + 8, LANES), F32),
                pltpu.VMEM((n_blk, LANES, LANES), F32)],
            compiler_params=params(56 * MIB),
            cost_estimate=cost((cut_c - cut_a) * flops, (cut_c - cut_a) * (wbytes + zbytes)),
            name="z_lattice",
        )(h_oth, w_loc, run_m, run_s, *picks, meta, z_part)

        keep, send, loss = pl.pallas_call(
            functools.partial(grad_h_kernel, n_slots),
            out_shape=(jax.ShapeDtypeStruct((rows // 2, model_dim), F32), jax.ShapeDtypeStruct((rows // 2, model_dim), F32), jax.ShapeDtypeStruct((8, LANES), F32)),
            in_specs=[any_spec(), any_spec()] + [vmem_spec()] * 6 + [smem_spec()],
            out_specs=(vmem_spec(),) * 3,
            scratch_shapes=w_scratch(4) + z_scratch(4) + [pltpu.VMEM((model_dim, rows), F32), pltpu.VMEM((rows, LANES), F32),
                                                     pltpu.VMEM((rows, 4 * TILE), BF16), pltpu.VMEM((rows, 4 * TILE), BF16)] + lists(1),
            compiler_params=params(56 * MIB),
            cost_estimate=cost(n_tiles * flops, n_tiles * (wbytes + zbytes)),
            name="grad_h",
        )(z_own, w_loc, *st_own, occ, part_loss, meta)
        occ_oth = lax.ppermute(occ, "dp", dp_swap)

        h_late, send = lax.optimization_barrier((h_oth, send))
        recv = tp_xor(send, 1)
        z_oth, stats_oth = pl.pallas_call(
            functools.partial(z_last_kernel, cut_c, n_tiles),
            out_shape=(z_type, stat_type),
            in_specs=[vmem_spec(), any_spec(), vmem_spec(), vmem_spec(), any_spec()],
            out_specs=(any_spec(), vmem_spec()),
            input_output_aliases={4: 0},
            scratch_shapes=w_scratch(4) + z_scratch(4) + run_scratch,
            compiler_params=params(56 * MIB),
            cost_estimate=cost((n_tiles - cut_c) * flops, (n_tiles - cut_c) * (wbytes + zbytes)),
            name="z_last",
        )(h_late, w_loc, run_m, run_s, z_part)
        keep, stats_oth = lax.optimization_barrier((keep, stats_oth))
        chip_sum = keep + recv
        across = tp_xor(chip_sum, 2)
        st_oth = [stats_oth] + [tp_xor(stats_oth, k) for k in (1, 2, 3)]

        grad_weight = pl.pallas_call(
            functools.partial(grad_w_kernel, n_slots),
            out_shape=jax.ShapeDtypeStruct((d_loc, vocab_loc), F32),
            in_specs=[any_spec(), any_spec()] + [vmem_spec()] * 12 + [smem_spec()] * 2,
            out_specs=any_spec(),
            scratch_shapes=z_scratch(2) + z_scratch(2) + [
                pltpu.VMEM((2, d_loc, 2 * TILE), F32), dma((2,)),
                pltpu.VMEM((d_loc, 2 * rows), BF16), pltpu.VMEM((2 * rows, LANES), F32), pltpu.VMEM((2 * rows, LANES), F32),
                pltpu.VMEM((2 * rows, 2 * TILE), BF16), pltpu.VMEM((2 * rows, 2 * TILE), BF16)] + lists(2),
            compiler_params=params(56 * MIB),
            cost_estimate=cost(n_tiles * flops, n_tiles * (2 * zbytes + d_loc * TILE * 4)),
            name="grad_w",
        )(z_own, z_oth, h_own, h_oth, *st_own, *st_oth, occ, occ_oth, meta, meta_oth)

        chip_sum, grad_weight = lax.optimization_barrier((chip_sum, grad_weight))
        full_half = chip_sum + across
        other_half = tp_xor(full_half, 1)
        grad_hidden = jnp.where(core == 0, jnp.stack([full_half, other_half]), jnp.stack([other_half, full_half])).reshape(batch_loc, frames, model_dim)
        return loss[0, :batch_loc], grad_weight, grad_hidden

    return jax.shard_map(
        local_step,
        mesh=mesh,
        in_specs=(P(batch_axes, None, None), P(None, "tp"), P(batch_axes, None), P(batch_axes), P(batch_axes)),
        out_specs=(P(batch_axes), P(batch_axes, "tp"), P(batch_axes, None, None)),
        check_vma=False,
    )
```

```python
import functools

import jax
import jax.numpy as jnp
from jax import lax
from jax.experimental import pallas as pl
from jax.experimental.pallas import tpu as pltpu
from jax.sharding import PartitionSpec as P

NEG_BIG = -1.0e30
F32 = jnp.float32
BF16 = jnp.bfloat16
TILE = 512
LANES = 128
MIB = 1 << 20


def vmem_spec():
    return pl.BlockSpec(memory_space=pltpu.VMEM)


def smem_spec():
    return pl.BlockSpec(memory_space=pltpu.SMEM)


def any_spec():
    return pl.BlockSpec(memory_space=pl.ANY)


def params(limit):
    return pltpu.CompilerParams(vmem_limit_bytes=limit)


def label_col(meta_refs, i):
    n_slots = meta_refs[0].shape[1] - 1
    seq, item = i // n_slots, lax.rem(i, n_slots)
    n_seq = meta_refs[0].shape[0]
    at = lax.max(item - 1, 0)
    col = meta_refs[0][lax.rem(seq, n_seq), at]
    for k in range(1, len(meta_refs)):
        col = jnp.where(seq >= k * n_seq, meta_refs[k][lax.rem(seq, n_seq), at], col)
    return jnp.where(item == 0, 0, col)


def build_lists(meta_refs, vocab_loc, head, nxt):
    n_items = len(meta_refs) * meta_refs[0].shape[0] * (meta_refs[0].shape[1] - 1)
    col_start = lax.axis_index("tp") * vocab_loc
    n_tiles = vocab_loc // TILE

    def clear(i, c):
        head[i] = -1
        return c

    lax.fori_loop(0, n_tiles, clear, 0)

    def insert(i, c):
        loc = label_col(meta_refs, i) - col_start
        tile = lax.max(loc, 0) // TILE

        @pl.when((loc >= 0) & (loc < vocab_loc))
        def _():
            nxt[i] = head[tile]
            head[tile] = i

        return c

    lax.fori_loop(0, n_items, insert, 0)
    return col_start


def walk_list(head, nxt, tile, visit):
    def body(i):
        visit(i)
        return nxt[i]

    lax.while_loop(lambda i: i >= 0, body, head[tile])


class TileStream:
    def __init__(self, src, buf, sem, depth, n_tiles, view):
        self.src, self.buf, self.sem, self.depth, self.n, self.view = src, buf, sem, depth, n_tiles, view

    def copy(self, j):
        slot = lax.rem(j, self.depth)
        return pltpu.make_async_copy(self.view(self.src, j), self.buf.at[slot], self.sem.at[slot])

    def prime(self):
        for j in range(min(self.depth - 1, self.n)):
            self.copy(j).start()

    def get(self, j):
        self.copy(j).wait()

        @pl.when(j + self.depth - 1 < self.n)
        def _():
            self.copy(j + self.depth - 1).start()

        return lax.rem(j, self.depth)


def w_view(src, j, n=1):
    return src.at[:, pl.ds(pl.multiple_of(j * n * TILE, TILE), n * TILE)]


def z_view(src, j, n):
    return src.at[pl.ds(j * n, n)]


def exact_zero(total):
    return jnp.minimum(total[0:16] + total[16:32], 0.0).astype(BF16)


def after(lhs, zero):
    if zero is None:
        return lhs
    corner = lhs[0:16, 0:LANES] + zero
    return jnp.concatenate([jnp.concatenate([corner, lhs[0:16, LANES:]], axis=1), lhs[16:]], axis=0)


def unit_stats(z, m_ref, s_ref, r0):
    n_chunks = z.shape[1] // LANES
    total = None
    for b in range(z.shape[0] // 32):
        zb = [z[32 * b:32 * (b + 1), k * LANES:(k + 1) * LANES] for k in range(n_chunks)]
        rows = slice(r0 + 32 * b, r0 + 32 * (b + 1))
        m_old = m_ref[rows, :]
        m_new = functools.reduce(jnp.maximum, zb, m_old)
        s_new = s_ref[rows, :] * jnp.exp(m_old - m_new)
        for part in zb:
            s_new = s_new + jnp.exp(part - m_new)
        m_ref[rows, :] = m_new
        s_ref[rows, :] = s_new
        total = s_new if total is None else total + s_new
    return exact_zero(total)


def z_group(h_ref, w, z_out, m_ref, s_ref):
    n_tiles = z_out.shape[0]
    n = h_ref.shape[0] // 2
    zeros = []
    for t in range(n_tiles):
        for r in range(2):
            rows = slice(r * n, (r + 1) * n)
            lhs = after(h_ref[rows, :], zeros[-2] if len(zeros) >= 2 else None)
            z = jnp.dot(lhs, w[:, t * TILE:(t + 1) * TILE], preferred_element_type=F32)
            z_out[t, rows, :] = z
            zeros.append(unit_stats(z, m_ref, s_ref, r * n))


def emit_stats(m_ref, s_ref, stats_ref):
    row_m = jnp.max(m_ref[...], axis=1, keepdims=True)
    row_s = jnp.sum(s_ref[...] * jnp.exp(m_ref[...] - row_m), axis=1, keepdims=True)
    rows = m_ref.shape[0]
    m_t = jnp.broadcast_to(row_m, (rows, LANES)).T
    s_t = jnp.broadcast_to(row_s, (rows, LANES)).T
    stats_ref[0:8, :] = m_t[0:8, :]
    stats_ref[8:16, :] = s_t[0:8, :]


def z_own_kernel(n_slots, h_ref, w_hbm, meta_ref, z_hbm, stats_ref, pick_ref, wbuf, wsem, zbuf, zsem, m_ref, s_ref, head, nxt):
    n_tiles = z_hbm.shape[0]
    rows = h_ref.shape[0]
    n_seq = meta_ref.shape[0]
    frames = rows // n_seq
    group = zbuf.shape[1]
    stream = TileStream(w_hbm, wbuf, wsem, wbuf.shape[0], n_tiles // group, lambda src, j: w_view(src, j, group))
    stream.prime()
    col_start = build_lists([meta_ref], n_tiles * TILE, head, nxt)
    m_ref[...] = jnp.full(m_ref.shape, NEG_BIG, F32)
    s_ref[...] = jnp.zeros(s_ref.shape, F32)
    pick_ref[...] = jnp.zeros(pick_ref.shape, F32)
    lane = lax.broadcasted_iota(jnp.int32, (frames, LANES), 1)

    def out_copy(j):
        slot = lax.rem(j, zbuf.shape[0])
        return pltpu.make_async_copy(zbuf.at[slot], z_view(z_hbm, j, group), zsem.at[slot])

    def step(j, c):
        slot = stream.get(j)

        @pl.when(j >= 3)
        def _():
            out_copy(j - 3).wait()

        zslot = lax.rem(j, zbuf.shape[0])
        z_group(h_ref, wbuf.at[slot], zbuf.at[zslot], m_ref, s_ref)
        out_copy(j).start()

        for t in range(group):
            def visit(i, t=t):
                seq, item = i // n_slots, lax.rem(i, n_slots)
                off = label_col([meta_ref], i) - col_start - (j * group + t) * TILE
                blk = off // LANES
                r0 = pl.multiple_of(seq * frames, frames)
                zb = zbuf[zslot, t, pl.ds(r0, frames), pl.ds(pl.multiple_of(blk * LANES, LANES), LANES)]
                at = item + 64 * seq
                moved = pltpu.roll(zb, lax.rem(at - (off - blk * LANES) + 2 * LANES, LANES), 1)
                pick_ref[...] = jnp.where(lane == at, moved, pick_ref[...])

            walk_list(head, nxt, j * group + t, visit)
        return c

    n_groups = n_tiles // group
    lax.fori_loop(0, n_groups, step, 0)
    emit_stats(m_ref, s_ref, stats_ref)
    for j in range(n_groups - 3, n_groups):
        out_copy(j).wait()


def z_oth_loop(lo, hi, h_ref, w_hbm, z_hbm, wbuf, wsem, zbuf, zsem, m_ref, s_ref, sections):
    group = zbuf.shape[1]
    lo, n_groups = lo // group, (hi - lo) // group
    stream = TileStream(w_hbm, wbuf, wsem, wbuf.shape[0], n_groups, lambda src, j: w_view(src, lo + j, group))
    stream.prime()

    def out_copy(j):
        slot = lax.rem(j, zbuf.shape[0])
        return pltpu.make_async_copy(zbuf.at[slot], z_view(z_hbm, lo + j, group), zsem.at[slot])

    base = 0
    for n, side, make_carry in sections:
        carry = make_carry()

        def step(k, c, base=base, side=side):
            j = base + k
            slot = stream.get(j)

            @pl.when(j >= 3)
            def _():
                out_copy(j - 3).wait()

            z_group(h_ref, wbuf.at[slot], zbuf.at[lax.rem(j, zbuf.shape[0])], m_ref, s_ref)
            c = side(k, c)
            out_copy(j).start()
            return c

        last = lax.fori_loop(0, n, step, carry)
        yield last
        base += n
    for j in range(max(n_groups - 3, 0), n_groups):
        out_copy(j).wait()


def join_rows(h_got, h_core, h_ref):
    n = h_got.shape[0]
    core = lax.rem(lax.axis_index("tp"), 2)
    h_ref[pl.ds(pl.multiple_of(core * n, n), n), :] = h_got[...]
    h_ref[pl.ds(pl.multiple_of((1 - core) * n, n), n), :] = h_core[...]


def z_first_kernel(lo, hi, h_got, h_core, w_hbm, meta_oth, z_hbm, m_ref, s_ref, h_ref, wbuf, wsem, zbuf, zsem):
    join_rows(h_got, h_core, h_ref)
    m_ref[...] = jnp.full(m_ref.shape, NEG_BIG, F32)
    s_ref[...] = jnp.zeros(s_ref.shape, F32)
    for _ in z_oth_loop(lo, hi, h_ref, w_hbm, z_hbm, wbuf, wsem, zbuf, zsem, m_ref, s_ref, [((hi - lo) // zbuf.shape[1], lambda k, c: c, lambda: 0)]):
        pass


def z_last_kernel(lo, hi, h_ref, w_hbm, m_in, s_in, z_in, z_hbm, stats_ref, wbuf, wsem, zbuf, zsem, m_ref, s_ref):
    m_ref[...] = m_in[...]
    s_ref[...] = s_in[...]
    for _ in z_oth_loop(lo, hi, h_ref, w_hbm, z_hbm, wbuf, wsem, zbuf, zsem, m_ref, s_ref, [((hi - lo) // zbuf.shape[1], lambda k, c: c, lambda: 0)]):
        pass
    emit_stats(m_ref, s_ref, stats_ref)


def z_lattice_kernel(lo, hi, n_lat, n_lab, h_ref, w_hbm, m_in, s_in, p0, p1, p2, p3, meta_ref, z_in,
                     z_hbm, m_ref, s_ref, occ_ref, loss_ref,
                     wbuf, wsem, zbuf, zsem, e_lab, e_blk, a_lab, a_blk, b_lab, b_blk, o_t):
    n_blk = e_lab.shape[0]
    frames = n_blk * 64
    m_ref[...] = m_in[...]
    s_ref[...] = s_in[...]
    lane128 = lax.broadcasted_iota(jnp.int32, (LANES, LANES), 1)
    row32 = lax.broadcasted_iota(jnp.int32, (n_lab, LANES), 0)
    row8 = lax.broadcasted_iota(jnp.int32, (8, LANES), 0)
    lane32 = lax.broadcasted_iota(jnp.int32, (n_lab, LANES), 1)
    lane8 = lax.broadcasted_iota(jnp.int32, (8, LANES), 1)
    n_seq = meta_ref.shape[0]
    labs = jnp.zeros((n_lab, LANES), jnp.int32)
    lab_row = jnp.zeros((8, LANES), jnp.int32)
    live8 = jnp.zeros((8, LANES), jnp.int32)
    used8 = jnp.zeros((8, LANES), jnp.int32)
    for s in range(n_seq):
        for k in range(n_lab):
            labs = jnp.where((row32 == k) & (lane32 == s), meta_ref[s, k], labs)
            lab_row = jnp.where((row8 == s) & (lane8 == k), meta_ref[s, k], lab_row)
        live8 = jnp.where(lane8 == s, meta_ref[s, n_lab], live8)
        used8 = jnp.where(lane8 == s, meta_ref[s, n_lab + 1], used8)
    live32 = jnp.broadcast_to(live8[0:1], (n_lab, LANES))
    used32 = jnp.broadcast_to(used8[0:1], (n_lab, LANES))
    skip_dn = labs != pltpu.roll(labs, 1, 0)
    skip_up = labs != pltpu.roll(labs, n_lab - 1, 0)
    end_lab = row32 == used32 - 1
    end_blk = row32 == used32
    end_top = (row8 == 0) & (used8 == n_lab)
    shift0 = jnp.zeros((1, LANES), F32)
    seq1 = lane8[0:1] >= 64
    half_len = jnp.where(seq1, meta_ref[1, n_lab], meta_ref[0, n_lab])
    for j in range(n_blk):
        part = functools.reduce(jnp.add, [p[pl.ds(64 * j, 64), :] for p in (p0, p1, p2, p3)])
        blk = jnp.concatenate([part, pltpu.roll(part, 64, 1)], axis=0)
        blk = jnp.where(lane128 <= n_lab, blk, NEG_BIG)
        x = blk.T
        top = jnp.max(x[0:n_lab + 8], axis=0, keepdims=True)
        e_blk[j] = jnp.broadcast_to(x[0:1] - top, (8, LANES))
        e_lab[j] = pltpu.roll(x, LANES - 1, 0)[0:n_lab] - top
        shift0 = shift0 + jnp.where(lax.rem(lane8[0:1], 64) + 64 * j < half_len, top, 0.0)
    shift_seq0 = jnp.sum(jnp.where(seq1, 0.0, shift0), axis=1, keepdims=True)
    shift_seq1 = jnp.sum(jnp.where(seq1, shift0, 0.0), axis=1, keepdims=True)

    def lse2(a, b):
        hi_v = jnp.maximum(a, b)
        return hi_v + jnp.log(1.0 + jnp.exp(jnp.minimum(a, b) - hi_v))

    def lse3(a, b, c):
        hi_v = jnp.maximum(a, b)
        lo_v = jnp.minimum(a, b)
        top = jnp.maximum(hi_v, c)
        mid = jnp.minimum(hi_v, c)
        return top + jnp.log(1.0 + jnp.exp(lo_v - top) + jnp.exp(mid - top))

    def emission(t):
        j, u = t // 64, lax.rem(t, 64)
        idx32 = jnp.where(lane32 == 1, 64 + u, u)
        idx8 = jnp.where(lane8 == 1, 64 + u, u)
        el = jnp.take_along_axis(e_lab[j], idx32, axis=1)
        eb = jnp.take_along_axis(e_blk[j], idx8, axis=1)
        return el, eb

    neg32 = jnp.full((n_lab, LANES), NEG_BIG, F32)
    neg8 = jnp.full((8, LANES), NEG_BIG, F32)
    start32 = jnp.where(row32 == 0, 0.0, NEG_BIG)
    fin_l = jnp.where(end_lab, 0.0, NEG_BIG)
    fin_b = jnp.where(end_blk, 0.0, NEG_BIG)
    fin_t = jnp.where(end_top, 0.0, NEG_BIG)

    def lat_step(i, carry):
        al, ab, at, bl, bb, bt = carry
        el, eb = emission(i)
        eb32 = jnp.broadcast_to(eb[0:1], (n_lab, LANES))
        rolled = pltpu.roll(al, 1, 0)
        prev = jnp.where(row32 == 0, NEG_BIG, rolled)
        prev_t = jnp.where(row8 == 0, rolled[0:8], NEG_BIG)
        first = i == 0
        nl = jnp.where(first, start32, lse3(al, ab, jnp.where(skip_dn, prev, NEG_BIG)))
        nb = jnp.where(first, start32, lse2(ab, prev))
        nt = jnp.where(first, neg8, lse2(at, prev_t))
        a_lab[i] = nl
        a_blk[i, 0:n_lab] = nb
        a_blk[i, n_lab:n_lab + 8] = nt
        al = jnp.where(i < live32, el + nl, al)
        ab = jnp.where(i < live32, eb32 + nb, ab)
        at = jnp.where(i < live8, eb + nt, at)
        t = frames - 1 - i
        fl, fb = emission(t)
        fb32 = jnp.broadcast_to(fb[0:1], (n_lab, LANES))
        last = row32 == n_lab - 1
        up_l = jnp.where(last, NEG_BIG, pltpu.roll(bl, n_lab - 1, 0))
        up_b = jnp.where(last, jnp.broadcast_to(bt[0:1], (n_lab, LANES)), pltpu.roll(bb, n_lab - 1, 0))
        is_end32 = t == live32 - 1
        is_end8 = t == live8 - 1
        ml = fl + jnp.where(is_end32, fin_l, lse3(bl, up_b, jnp.where(skip_up, up_l, NEG_BIG)))
        mb = fb32 + jnp.where(is_end32, fin_b, lse2(bb, bl))
        mt = fb + jnp.where(is_end8, fin_t, bt)
        bl = jnp.where(t < live32, ml, bl)
        bb = jnp.where(t < live32, mb, bb)
        bt = jnp.where(t < live8, mt, bt)
        b_lab[t] = bl
        b_blk[t, 0:n_lab] = bb
        b_blk[t, n_lab:n_lab + 8] = bt
        return al, ab, at, bl, bb, bt

    group = zbuf.shape[1]
    n_lat_groups = n_lat // group
    per_tile = frames // n_lat_groups

    def lattice_side(k, carry):
        for u in range(per_tile):
            carry = lat_step(k * per_tile + u, carry)
        return carry

    n_occ = (hi - lo - n_lat) // group
    occ_group = frames // n_occ // 64
    back32 = jnp.where(lane32 >= 64, 1, 0)
    back8 = jnp.where(lane8 >= 64, 1, 0)
    run = z_oth_loop(lo, hi, h_ref, w_hbm, z_hbm, wbuf, wsem, zbuf, zsem, m_ref, s_ref,
                     [(n_lat_groups, lattice_side, lambda: (neg32, neg32, neg8, fin_l, fin_b, fin_t)),
                      (n_occ, lambda k, c: occ_side(k, c), lambda: 0)])
    al, ab, at, _, _, _ = next(run)

    last_l = jnp.where(end_lab, al, NEG_BIG)
    last_b = jnp.where(end_blk, ab, NEG_BIG)
    last_t = jnp.where(end_top, at, NEG_BIG)
    top = jnp.maximum(jnp.maximum(jnp.max(last_l, axis=0, keepdims=True), jnp.max(last_b, axis=0, keepdims=True)), jnp.max(last_t, axis=0, keepdims=True))
    total = jnp.sum(jnp.exp(last_l - top), axis=0, keepdims=True) + jnp.sum(jnp.exp(last_b - top), axis=0, keepdims=True) + jnp.sum(jnp.exp(last_t - top), axis=0, keepdims=True)
    loss = -(top + jnp.log(total))
    loss32 = jnp.broadcast_to(loss, (n_lab, LANES))
    loss8 = jnp.broadcast_to(loss, (8, LANES))
    lane1 = lane8[0:1]
    loss_ref[...] = jnp.broadcast_to(loss - jnp.where(lane1 == 0, shift_seq0, jnp.where(lane1 == 1, shift_seq1, 0.0)), (8, LANES))

    def occ_frame(i, u, acc_l, acc_b):
        occ_l = jnp.where(i < live32, jnp.exp(a_lab[i] + b_lab[i] + loss32), 0.0)
        occ_b = jnp.exp(a_blk[i, 0:n_lab] + b_blk[i, 0:n_lab] + loss32)
        occ_u = jnp.exp(a_blk[i, n_lab:n_lab + 8] + b_blk[i, n_lab:n_lab + 8] + loss8)
        blank = jnp.sum(occ_b, axis=0, keepdims=True) + occ_u[0:1]
        blank = jnp.where(i < live8, jnp.broadcast_to(blank, (8, LANES)), 0.0)
        acc_l = jnp.where(lax.rem(lane32, 64) == u, jnp.take_along_axis(occ_l, back32, axis=1), acc_l)
        acc_b = jnp.where(lax.rem(lane8, 64) == u, jnp.take_along_axis(blank, back8, axis=1), acc_b)
        return acc_l, acc_b

    def occ_side(k, c):
        for g in range(occ_group):
            j = k * occ_group + g
            acc_l = jnp.zeros((n_lab, LANES), F32)
            acc_b = jnp.zeros((8, LANES), F32)
            for u in range(64):
                acc_l, acc_b = occ_frame(j * 64 + u, u, acc_l, acc_b)
            o_t[j, 0:n_lab] = acc_l
            o_t[j, n_lab:n_lab + 8] = acc_b
            o_t[j, 8 + n_lab:LANES] = jnp.zeros((LANES - 8 - n_lab, LANES), F32)
        return c

    for _ in run:
        pass
    row128 = lax.broadcasted_iota(jnp.int32, (LANES, LANES), 0)
    inner = (row128 < n_lab) & (lane128 < n_lab)
    same = []
    for s in range(n_seq):
        down = jnp.full((n_lab, LANES), -1, jnp.int32)
        for k in range(n_lab):
            down = jnp.where(row32 == k, meta_ref[s, k], down)
        down = jnp.concatenate([down, jnp.full((LANES - n_lab, LANES), -1, jnp.int32)], axis=0)
        across = jnp.broadcast_to(lab_row[s:s + 1], (LANES, LANES))
        same.append(jnp.where((inner & (down == across)) | (row128 == lane128), 1.0, 0.0))
    for j in range(n_blk):
        y = o_t[j].T
        for s in range(2):
            occ_ref[pl.ds(s * frames + 64 * j, 64), :] = jnp.dot(y[64 * s:64 * (s + 1), :], same[s], precision=lax.Precision.HIGHEST, preferred_element_type=F32)


def combine_stats(refs):
    m = functools.reduce(jnp.maximum, [r[0:8, :] for r in refs])
    tot = functools.reduce(jnp.add, [r[8:16, :] * jnp.exp(r[0:8, :] - m) for r in refs])
    return m + jnp.log(tot)


def spread_lse(refs, meta_ref, lse_ref, r0, frames):
    row = combine_stats(refs)
    n = row.shape[1]
    cols = jnp.broadcast_to(row[0:1, :], (LANES, n)).T
    t = lax.broadcasted_iota(jnp.int32, (frames, LANES), 0)
    sums = []
    for s in range(n // frames):
        part = cols[s * frames:(s + 1) * frames]
        live = t < meta_ref[s, meta_ref.shape[1] - 2]
        lse_ref[pl.ds(r0 + s * frames, frames), :] = jnp.where(live, part, 1.0e30)
        sums.append(jnp.sum(jnp.where(live, part, 0.0), axis=0, keepdims=True))
    return sums


def patch_tile(n_slots, frames, meta_refs, col_start, j, i, z_block, lse_ref, occ_ref, g_ref, g_col, lane):
    seq, item = i // n_slots, lax.rem(i, n_slots)
    off = label_col(meta_refs, i) - col_start - j * TILE
    blk = off // LANES
    r0 = pl.multiple_of(seq * frames, frames)
    c0 = pl.multiple_of(blk * LANES, LANES)
    zb = z_block(seq, c0)
    slot_lane = jnp.where(item == 0, n_slots - 1, item - 1)
    occ = jnp.sum(jnp.where(lane == slot_lane, occ_ref[pl.ds(r0, frames), :], 0.0), axis=1, keepdims=True)
    fresh = jnp.exp(zb - lse_ref[pl.ds(r0, frames), :]) - occ
    gc = pl.multiple_of(g_col + c0, LANES)
    old = g_ref[pl.ds(r0, frames), pl.ds(gc, LANES)].astype(F32)
    g_ref[pl.ds(r0, frames), pl.ds(gc, LANES)] = jnp.where(lane == off - blk * LANES, fresh, old).astype(BF16)


def softmax_unit(z, z_row, lse_ref, out, r0, n, c0):
    total = None
    for b in range(n // 32):
        lse = lse_ref[r0 + 32 * b:r0 + 32 * (b + 1), :]
        for k in range(TILE // LANES):
            e = jnp.exp(z[z_row + 32 * b:z_row + 32 * (b + 1), k * LANES:(k + 1) * LANES] - lse)
            out[r0 + 32 * b:r0 + 32 * (b + 1), c0 + k * LANES:c0 + (k + 1) * LANES] = e.astype(BF16)
            total = e if total is None else total + e
    return exact_zero(total)


def grad_h_kernel(n_slots, z_hbm, w_hbm, st0, st1, st2, st3, occ_ref, part_loss, meta_ref, keep_ref, send_ref, loss_ref,
                  wbuf, wsem, zbuf, zsem, acc, lse_ref, g0, g1, head, nxt):
    n_tiles, rows = z_hbm.shape[0], z_hbm.shape[1]
    frames = rows // meta_ref.shape[0]
    meta_refs = [meta_ref]
    group = zbuf.shape[1]
    n_groups = n_tiles // group
    stream = TileStream(w_hbm, wbuf, wsem, wbuf.shape[0], n_groups, lambda src, j: w_view(src, j, group))
    zs = TileStream(z_hbm, zbuf, zsem, zbuf.shape[0], n_groups, lambda src, j: z_view(src, j, group))
    zs.prime()
    stream.prime()
    col_start = build_lists(meta_refs, n_tiles * TILE, head, nxt)
    sums = spread_lse([st0, st1, st2, st3], meta_ref, lse_ref, 0, frames)
    lane1 = lax.broadcasted_iota(jnp.int32, (8, LANES), 1)
    loss_ref[...] = part_loss[...] + jnp.where(lane1 == 0, sums[0], sums[1])
    lane = lax.broadcasted_iota(jnp.int32, (frames, LANES), 1)

    def patch(j, slot, g):
        for t in range(group):
            def z_block(seq, c0, t=t):
                return zbuf[slot, t, pl.ds(pl.multiple_of(seq * frames, frames), frames), pl.ds(c0, LANES)]

            walk_list(head, nxt, j * group + t,
                      lambda i, t=t, z_block=z_block: patch_tile(n_slots, frames, meta_refs, col_start, j * group + t, i, z_block, lse_ref, occ_ref, g, t * TILE, lane))

    def make_g(slot, u, g):
        t, r = u // 2, u % 2
        return softmax_unit(zbuf.at[slot, t], r * rows // 2, lse_ref, g, r * rows // 2, rows // 2, t * TILE)

    acc[...] = jnp.zeros(acc.shape, F32)
    slot0 = zs.get(0)
    for u in range(2 * group):
        make_g(slot0, u, g0)
    patch(0, slot0, g0)
    n_units = acc.shape[0] // 256

    def half(j, g_now, g_next):
        slot = stream.get(j)
        nj = lax.min(j + 1, n_groups - 1)

        @pl.when(j + 1 < n_groups)
        def _():
            zs.get(nj)

        zslot = lax.rem(nj, zbuf.shape[0])
        zero = None
        for u in range(n_units):
            d_rows = slice(u * 256, (u + 1) * 256)
            lhs = after(wbuf[slot, d_rows, :], zero)
            acc[d_rows, :] += lax.dot_general(lhs, g_now[...], (((1,), (1,)), ((), ())), preferred_element_type=F32)
            if u < 2 * group:
                zero = make_g(zslot, u, g_next)
        patch(nj, zslot, g_next)

    def step(i, c):
        half(2 * i, g0, g1)
        half(2 * i + 1, g1, g0)
        return c

    lax.fori_loop(0, n_groups // 2, step, 0)
    core = lax.rem(lax.axis_index("tp"), 2)
    n = rows // 2
    keep_ref[...] = acc[:, pl.ds(pl.multiple_of(core * n, n), n)].T
    send_ref[...] = acc[:, pl.ds(pl.multiple_of((1 - core) * n, n), n)].T


def grad_w_kernel(n_slots, zo_hbm, zx_hbm, h_own_ref, h_oth_ref, st0, st1, st2, st3, sx0, sx1, sx2, sx3, occ_own_ref, occ_oth_ref, meta_own, meta_oth, gw_hbm,
                  zo_buf, zo_sem, zx_buf, zx_sem, obuf, osem, ht, lse_ref, occ_ref, g0, g1, head, nxt):
    n_tiles, rows = zo_hbm.shape[0], zo_hbm.shape[1]
    meta_refs = [meta_own, meta_oth]
    n_half = meta_own.shape[0]
    frames = rows // n_half
    d_loc = ht.shape[0]
    group = zo_buf.shape[1]
    n_groups = n_tiles // group
    zo = TileStream(zo_hbm, zo_buf, zo_sem, zo_buf.shape[0], n_groups, lambda src, j: z_view(src, j, group))
    zx = TileStream(zx_hbm, zx_buf, zx_sem, zx_buf.shape[0], n_groups, lambda src, j: z_view(src, j, group))
    zo.prime()
    zx.prime()
    col_start = build_lists(meta_refs, n_tiles * TILE, head, nxt)
    d0 = pl.multiple_of(lax.axis_index("dp") * d_loc, LANES)
    ht[:, 0:rows] = h_own_ref[:, pl.ds(d0, d_loc)].T
    ht[:, rows:2 * rows] = h_oth_ref[:, pl.ds(d0, d_loc)].T
    spread_lse([st0, st1, st2, st3], meta_own, lse_ref, 0, frames)
    spread_lse([sx0, sx1, sx2, sx3], meta_oth, lse_ref, rows, frames)
    occ_ref[0:rows] = occ_own_ref[...]
    occ_ref[rows:2 * rows] = occ_oth_ref[...]
    lane = lax.broadcasted_iota(jnp.int32, (frames, LANES), 1)

    def patch(j, slot, g):
        for t in range(group):
            def z_own(seq, c0, t=t):
                return zo_buf[slot, t, pl.ds(pl.multiple_of(seq * frames, frames), frames), pl.ds(c0, LANES)]

            def z_oth(seq, c0, t=t):
                return zx_buf[slot, t, pl.ds(pl.multiple_of((seq - n_half) * frames, frames), frames), pl.ds(c0, LANES)]

            def visit(i, t=t, z_own=z_own, z_oth=z_oth):
                @pl.when(i < n_half * n_slots)
                def _():
                    patch_tile(n_slots, frames, meta_refs, col_start, j * group + t, i, z_own, lse_ref, occ_ref, g, t * TILE, lane)

                @pl.when(i >= n_half * n_slots)
                def _():
                    patch_tile(n_slots, frames, meta_refs, col_start, j * group + t, i, z_oth, lse_ref, occ_ref, g, t * TILE, lane)

            walk_list(head, nxt, j * group + t, visit)

    def out_copy(j):
        slot = lax.rem(j, obuf.shape[0])
        return pltpu.make_async_copy(obuf.at[slot], w_view(gw_hbm, j, group), osem.at[slot])

    def make_g(slot, u, g):
        t, side = u // 2, u % 2
        src = (zo_buf, zx_buf)[side]
        return softmax_unit(src.at[slot, t], 0, lse_ref, g, side * rows, rows, t * TILE)

    slot0 = zo.get(0)
    zx.get(0)
    for u in range(2 * group):
        make_g(slot0, u, g0)
    patch(0, slot0, g0)
    d_half = d_loc // 2

    def half(j, g_now, g_next):
        @pl.when(j >= 3)
        def _():
            out_copy(j - 3).wait()

        nj = lax.min(j + 1, n_groups - 1)

        @pl.when(j + 1 < n_groups)
        def _():
            zo.get(nj)
            zx.get(nj)

        slot = lax.rem(nj, zo_buf.shape[0])
        oslot = lax.rem(j, obuf.shape[0])
        zero = None
        for u in range(2 * group):
            t, r = u // 2, u % 2
            d_rows = slice(r * d_half, (r + 1) * d_half)
            lhs = after(ht[d_rows, :], zero)
            obuf[oslot, d_rows, t * TILE:(t + 1) * TILE] = jnp.dot(lhs, g_now[:, t * TILE:(t + 1) * TILE], preferred_element_type=F32)
            zero = make_g(slot, u, g_next)
        out_copy(j).start()
        patch(nj, slot, g_next)

    def step(i, c):
        half(2 * i, g0, g1)
        half(2 * i + 1, g1, g0)
        return c

    lax.fori_loop(0, n_groups // 2, step, 0)
    for j in range(n_groups - 3, n_groups):
        out_copy(j).wait()


def cost(flops, nbytes, trans=0):
    return pl.CostEstimate(flops=flops, bytes_accessed=nbytes, transcendentals=trans)


def solution(mesh):
    batch_axes = ("part", "dp")
    n_tp = mesh.shape["tp"]
    n_dp = mesh.shape["dp"]
    dp_swap = [(i, n_dp - 1 - i) for i in range(n_dp)]

    def tp_xor(x, mask):
        return lax.ppermute(x, "tp", [(i, i ^ mask) for i in range(n_tp)])

    def local_step(hidden, w_loc, labels, in_len, lab_len):
        batch_loc, frames, model_dim = hidden.shape
        vocab_loc = w_loc.shape[1]
        n_lab = labels.shape[1]
        n_slots = n_lab + 1
        rows = batch_loc * frames
        n_tiles = vocab_loc // TILE
        d_loc = model_dim // n_dp
        dma = pltpu.SemaphoreType.DMA
        i32 = jnp.int32
        cut_a, cut_c, n_lat = 8, 28, 16
        h_own = hidden.reshape(rows, model_dim)
        core = lax.rem(lax.axis_index("tp"), 2)
        h_half = lax.dynamic_index_in_dim(h_own.reshape(2, rows // 2, model_dim), core, 0, keepdims=False)
        h_got = lax.ppermute(h_half, "dp", dp_swap)
        meta = jnp.concatenate([labels, in_len[:, None], lab_len[:, None]], axis=1)
        meta_oth = lax.ppermute(meta, "dp", dp_swap)
        flops = 2 * rows * model_dim * TILE
        wbytes = model_dim * TILE * 2
        zbytes = rows * TILE * 4
        z_type = jax.ShapeDtypeStruct((n_tiles, rows, TILE), F32)
        run_type = jax.ShapeDtypeStruct((rows, LANES), F32)
        pick_type = jax.ShapeDtypeStruct((frames, LANES), F32)
        stat_type = jax.ShapeDtypeStruct((16, rows), F32)
        def w_scratch(n):
            return [pltpu.VMEM((3, model_dim, n * TILE), BF16), dma((3,))]

        def z_scratch(n):
            return [pltpu.VMEM((3, n, rows, TILE), F32), dma((3,))]

        run_scratch = [pltpu.VMEM((rows, LANES), F32), pltpu.VMEM((rows, LANES), F32)]

        def lists(n_sets):
            return [pltpu.SMEM((n_tiles,), i32), pltpu.SMEM((n_sets * batch_loc * n_slots,), i32)]

        z_own, stats_own, pick = pl.pallas_call(
            functools.partial(z_own_kernel, n_slots),
            out_shape=(z_type, stat_type, pick_type),
            in_specs=[vmem_spec(), any_spec(), smem_spec()],
            out_specs=(any_spec(), vmem_spec(), vmem_spec()),
            scratch_shapes=w_scratch(2) + z_scratch(2) + run_scratch + lists(1),
            compiler_params=params(56 * MIB),
            cost_estimate=cost(n_tiles * flops, n_tiles * (wbytes + zbytes)),
            name="z_own",
        )(h_own, w_loc, meta)

        h_got, stats_own = lax.optimization_barrier((h_got, stats_own))
        h_core = tp_xor(h_got, 1)
        picks = [pick] + [tp_xor(pick, k) for k in (1, 2, 3)]
        st_own = [stats_own] + [tp_xor(stats_own, k) for k in (1, 2, 3)]

        z_part, run_m, run_s, h_oth = pl.pallas_call(
            functools.partial(z_first_kernel, 0, cut_a),
            out_shape=(z_type, run_type, run_type, jax.ShapeDtypeStruct((rows, model_dim), BF16)),
            in_specs=[vmem_spec(), vmem_spec(), any_spec(), smem_spec()],
            out_specs=(any_spec(), vmem_spec(), vmem_spec(), vmem_spec()),
            scratch_shapes=w_scratch(2) + z_scratch(2),
            compiler_params=params(56 * MIB),
            cost_estimate=cost(cut_a * flops, cut_a * (wbytes + zbytes)),
            name="z_first",
        )(h_got, h_core, w_loc, meta_oth)

        n_blk = frames // 64
        z_part, run_m, run_s, occ, part_loss = pl.pallas_call(
            functools.partial(z_lattice_kernel, cut_a, cut_c, n_lat, n_lab),
            out_shape=(z_type, run_type, run_type, run_type, jax.ShapeDtypeStruct((8, LANES), F32)),
            in_specs=[vmem_spec(), any_spec()] + [vmem_spec()] * 6 + [smem_spec(), any_spec()],
            out_specs=(any_spec(),) + (vmem_spec(),) * 4,
            input_output_aliases={9: 0},
            scratch_shapes=w_scratch(2) + z_scratch(2) + [
                pltpu.VMEM((n_blk, n_lab, LANES), F32), pltpu.VMEM((n_blk, 8, LANES), F32),
                pltpu.VMEM((frames, n_lab, LANES), F32), pltpu.VMEM((frames, n_lab + 8, LANES), F32),
                pltpu.VMEM((frames, n_lab, LANES), F32), pltpu.VMEM((frames, n_lab + 8, LANES), F32),
                pltpu.VMEM((n_blk, LANES, LANES), F32)],
            compiler_params=params(56 * MIB),
            cost_estimate=cost((cut_c - cut_a) * flops, (cut_c - cut_a) * (wbytes + zbytes)),
            name="z_lattice",
        )(h_oth, w_loc, run_m, run_s, *picks, meta, z_part)

        keep, send, loss = pl.pallas_call(
            functools.partial(grad_h_kernel, n_slots),
            out_shape=(jax.ShapeDtypeStruct((rows // 2, model_dim), F32), jax.ShapeDtypeStruct((rows // 2, model_dim), F32), jax.ShapeDtypeStruct((8, LANES), F32)),
            in_specs=[any_spec(), any_spec()] + [vmem_spec()] * 6 + [smem_spec()],
            out_specs=(vmem_spec(),) * 3,
            scratch_shapes=w_scratch(2) + z_scratch(2) + [pltpu.VMEM((model_dim, rows), F32), pltpu.VMEM((rows, LANES), F32),
                                                     pltpu.VMEM((rows, 2 * TILE), BF16), pltpu.VMEM((rows, 2 * TILE), BF16)] + lists(1),
            compiler_params=params(56 * MIB),
            cost_estimate=cost(n_tiles * flops, n_tiles * (wbytes + zbytes)),
            name="grad_h",
        )(z_own, w_loc, *st_own, occ, part_loss, meta)
        occ_oth = lax.ppermute(occ, "dp", dp_swap)

        h_late, send = lax.optimization_barrier((h_oth, send))
        recv = tp_xor(send, 1)
        z_oth, stats_oth = pl.pallas_call(
            functools.partial(z_last_kernel, cut_c, n_tiles),
            out_shape=(z_type, stat_type),
            in_specs=[vmem_spec(), any_spec(), vmem_spec(), vmem_spec(), any_spec()],
            out_specs=(any_spec(), vmem_spec()),
            input_output_aliases={4: 0},
            scratch_shapes=w_scratch(2) + z_scratch(2) + run_scratch,
            compiler_params=params(56 * MIB),
            cost_estimate=cost((n_tiles - cut_c) * flops, (n_tiles - cut_c) * (wbytes + zbytes)),
            name="z_last",
        )(h_late, w_loc, run_m, run_s, z_part)
        keep, stats_oth = lax.optimization_barrier((keep, stats_oth))
        chip_sum = keep + recv
        across = tp_xor(chip_sum, 2)
        st_oth = [stats_oth] + [tp_xor(stats_oth, k) for k in (1, 2, 3)]

        grad_weight = pl.pallas_call(
            functools.partial(grad_w_kernel, n_slots),
            out_shape=jax.ShapeDtypeStruct((d_loc, vocab_loc), F32),
            in_specs=[any_spec(), any_spec()] + [vmem_spec()] * 12 + [smem_spec()] * 2,
            out_specs=any_spec(),
            scratch_shapes=z_scratch(2) + z_scratch(2) + [
                pltpu.VMEM((3, d_loc, 2 * TILE), F32), dma((3,)),
                pltpu.VMEM((d_loc, 2 * rows), BF16), pltpu.VMEM((2 * rows, LANES), F32), pltpu.VMEM((2 * rows, LANES), F32),
                pltpu.VMEM((2 * rows, 2 * TILE), BF16), pltpu.VMEM((2 * rows, 2 * TILE), BF16)] + lists(2),
            compiler_params=params(56 * MIB),
            cost_estimate=cost(n_tiles * flops, n_tiles * (2 * zbytes + d_loc * TILE * 4)),
            name="grad_w",
        )(z_own, z_oth, h_own, h_oth, *st_own, *st_oth, occ, occ_oth, meta, meta_oth)

        chip_sum, grad_weight = lax.optimization_barrier((chip_sum, grad_weight))
        full_half = chip_sum + across
        other_half = tp_xor(full_half, 1)
        grad_hidden = jnp.where(core == 0, jnp.stack([full_half, other_half]), jnp.stack([other_half, full_half])).reshape(batch_loc, frames, model_dim)
        return loss[0, :batch_loc], grad_weight, grad_hidden

    return jax.shard_map(
        local_step,
        mesh=mesh,
        in_specs=(P(batch_axes, None, None), P(None, "tp"), P(batch_axes, None), P(batch_axes), P(batch_axes)),
        out_specs=(P(batch_axes), P(batch_axes, "tp"), P(batch_axes, None, None)),
        check_vma=False,
    )
```

```python
import functools

import jax
import jax.numpy as jnp
from jax import lax
from jax.experimental import pallas as pl
from jax.experimental.pallas import tpu as pltpu
from jax.sharding import PartitionSpec as P

NEG_BIG = -1.0e30
LOG2E = 1.4426950408889634
F32 = jnp.float32
BF16 = jnp.bfloat16
TILE = 512
LANES = 128
MIB = 1 << 20


def vmem_spec():
    return pl.BlockSpec(memory_space=pltpu.VMEM)


def smem_spec():
    return pl.BlockSpec(memory_space=pltpu.SMEM)


def any_spec():
    return pl.BlockSpec(memory_space=pl.ANY)


def kernel_call(*args, **kw):
    return pl.pallas_call(*args, **kw)


def params():
    return pltpu.CompilerParams(vmem_limit_bytes=56 * MIB)


def label_col(meta_refs, i):
    n_slots = meta_refs[0].shape[1] - 1
    seq, item = i // n_slots, lax.rem(i, n_slots)
    n_seq = meta_refs[0].shape[0]
    at = lax.max(item - 1, 0)
    col = meta_refs[0][lax.rem(seq, n_seq), at]
    for k in range(1, len(meta_refs)):
        col = jnp.where(seq >= k * n_seq, meta_refs[k][lax.rem(seq, n_seq), at], col)
    return jnp.where(item == 0, 0, col)


def build_lists(meta_refs, vocab_loc, head, nxt):
    n_items = len(meta_refs) * meta_refs[0].shape[0] * (meta_refs[0].shape[1] - 1)
    col_start = lax.axis_index("tp") * vocab_loc
    n_tiles = vocab_loc // TILE

    def clear(i, c):
        head[i] = -1
        return c

    lax.fori_loop(0, n_tiles, clear, 0)

    def insert(i, c):
        loc = label_col(meta_refs, i) - col_start
        tile = lax.max(loc, 0) // TILE

        @pl.when((loc >= 0) & (loc < vocab_loc))
        def _():
            nxt[i] = head[tile]
            head[tile] = i

        return c

    lax.fori_loop(0, n_items, insert, 0)
    return col_start


def walk_list(head, nxt, tile, visit):
    def body(i):
        visit(i)
        return nxt[i]

    lax.while_loop(lambda i: i >= 0, body, head[tile])


class TileStream:
    def __init__(self, src, buf, sem, depth, n_tiles, view):
        self.src, self.buf, self.sem, self.depth, self.n, self.view = src, buf, sem, depth, n_tiles, view

    def copy(self, j):
        slot = lax.rem(j, self.depth)
        return pltpu.make_async_copy(self.view(self.src, j), self.buf.at[slot], self.sem.at[slot])

    def prime(self):
        for j in range(min(self.depth - 1, self.n)):
            self.copy(j).start()

    def get(self, j):
        self.copy(j).wait()

        @pl.when(j + self.depth - 1 < self.n)
        def _():
            self.copy(j + self.depth - 1).start()

        return lax.rem(j, self.depth)


def w_view(src, j, n=1):
    return src.at[:, pl.ds(pl.multiple_of(j * n * TILE, TILE), n * TILE)]


def z_view(src, j, n):
    return src.at[pl.ds(j * n, n)]


def exact_zero(total):
    return jnp.minimum(total[0:16] + total[16:32], 0.0).astype(BF16)


def after(lhs, zero):
    if zero is None:
        return lhs
    corner = lhs[0:16, 0:LANES] + zero
    return jnp.concatenate([jnp.concatenate([corner, lhs[0:16, LANES:]], axis=1), lhs[16:]], axis=0)


def unit_stats(z, m_ref, s_ref, r0):
    n_chunks = z.shape[1] // LANES
    total = None
    for b in range(z.shape[0] // 32):
        zb = [z[32 * b:32 * (b + 1), k * LANES:(k + 1) * LANES] for k in range(n_chunks)]
        rows = slice(r0 + 32 * b, r0 + 32 * (b + 1))
        m_old = m_ref[rows, :]
        m_new = functools.reduce(jnp.maximum, zb, m_old)
        s_new = s_ref[rows, :] * jnp.exp(m_old - m_new)
        for part in zb:
            s_new = s_new + jnp.exp(part - m_new)
        m_ref[rows, :] = m_new
        s_ref[rows, :] = s_new
        total = s_new if total is None else total + s_new
    return exact_zero(total)


def z_group(h_ref, w, z_out, m_ref, s_ref):
    n_tiles = z_out.shape[0]
    n = h_ref.shape[0] // 2
    zeros = []
    for t in range(n_tiles):
        for r in range(2):
            rows = slice(r * n, (r + 1) * n)
            lhs = after(h_ref[rows, :], zeros[-2] if len(zeros) >= 2 else None)
            z = jnp.dot(lhs, w[:, t * TILE:(t + 1) * TILE], preferred_element_type=F32)
            z_out[t, rows, :] = z
            zeros.append(unit_stats(z, m_ref, s_ref, r * n))


def emit_stats(m_ref, s_ref, out_ref, base):
    row_m = jnp.max(m_ref[...], axis=1, keepdims=True)
    row_s = jnp.sum(s_ref[...] * jnp.exp(m_ref[...] - row_m), axis=1, keepdims=True)
    rows = m_ref.shape[0]
    for k, v in enumerate((row_m, row_s)):
        flat = jnp.broadcast_to(v, (rows, LANES)).T
        for p in range(rows // LANES):
            at = base + 8 * k + p
            out_ref[at:at + 1, :] = flat[0:1, p * LANES:(p + 1) * LANES]


def z_own_kernel(n_slots, h_ref, w_hbm, labels_ref, in_len_ref, lab_len_ref, z_hbm, pick_ref, meta_ref, wbuf, wsem, zbuf, zsem, m_ref, s_ref, head, nxt):
    n_tiles = z_hbm.shape[0]
    rows = h_ref.shape[0]
    n_seq = meta_ref.shape[0]
    frames = rows // n_seq
    n_lab = n_slots - 1
    for q in range(n_seq):
        def put(k, c, q=q):
            meta_ref[q, k] = labels_ref[q, k]
            return c

        lax.fori_loop(0, n_lab, put, 0)
        meta_ref[q, n_lab] = in_len_ref[q]
        meta_ref[q, n_lab + 1] = lab_len_ref[q]
    group = zbuf.shape[1]
    stream = TileStream(w_hbm, wbuf, wsem, wbuf.shape[0], n_tiles // group, lambda src, j: w_view(src, j, group))
    stream.prime()
    col_start = build_lists([meta_ref], n_tiles * TILE, head, nxt)
    m_ref[...] = jnp.full(m_ref.shape, NEG_BIG, F32)
    s_ref[...] = jnp.zeros(s_ref.shape, F32)
    pick_ref[...] = jnp.zeros(pick_ref.shape, F32)
    lane = lax.broadcasted_iota(jnp.int32, (frames, LANES), 1)

    def out_copy(j):
        slot = lax.rem(j, zbuf.shape[0])
        return pltpu.make_async_copy(zbuf.at[slot], z_view(z_hbm, j, group), zsem.at[slot])

    def step(j, c):
        slot = stream.get(j)

        @pl.when(j >= 3)
        def _():
            out_copy(j - 3).wait()

        zslot = lax.rem(j, zbuf.shape[0])
        z_group(h_ref, wbuf.at[slot], zbuf.at[zslot], m_ref, s_ref)
        out_copy(j).start()

        for t in range(group):
            def visit(i, t=t):
                seq, item = i // n_slots, lax.rem(i, n_slots)
                off = label_col([meta_ref], i) - col_start - (j * group + t) * TILE
                blk = off // LANES
                r0 = pl.multiple_of(seq * frames, frames)
                zb = zbuf[zslot, t, pl.ds(r0, frames), pl.ds(pl.multiple_of(blk * LANES, LANES), LANES)]
                at = item + 64 * seq
                moved = pltpu.roll(zb, lax.rem(at - (off - blk * LANES) + 2 * LANES, LANES), 1)
                pick_ref[0:frames, :] = jnp.where(lane == at, moved, pick_ref[0:frames, :])

            walk_list(head, nxt, j * group + t, visit)
        return c

    n_groups = n_tiles // group
    lax.fori_loop(0, n_groups, step, 0)
    emit_stats(m_ref, s_ref, pick_ref, frames)
    for j in range(n_groups - 3, n_groups):
        out_copy(j).wait()


def z_oth_loop(lo, hi, h_ref, w_hbm, z_hbm, wbuf, wsem, zbuf, zsem, m_ref, s_ref, sections):
    group = zbuf.shape[1]
    lo, n_groups = lo // group, (hi - lo) // group
    stream = TileStream(w_hbm, wbuf, wsem, wbuf.shape[0], n_groups, lambda src, j: w_view(src, lo + j, group))
    stream.prime()

    def out_copy(j):
        slot = lax.rem(j, zbuf.shape[0])
        return pltpu.make_async_copy(zbuf.at[slot], z_view(z_hbm, lo + j, group), zsem.at[slot])

    base = 0
    for n, side, make_carry in sections:
        carry = make_carry()

        def step(k, c, base=base, side=side):
            j = base + k
            slot = stream.get(j)

            @pl.when(j >= 3)
            def _():
                out_copy(j - 3).wait()

            z_group(h_ref, wbuf.at[slot], zbuf.at[lax.rem(j, zbuf.shape[0])], m_ref, s_ref)
            c = side(k, c)
            out_copy(j).start()
            return c

        last = lax.fori_loop(0, n, step, carry)
        yield last
        base += n
    for j in range(max(n_groups - 3, 0), n_groups):
        out_copy(j).wait()


def join_rows(h_got, h_core, h_ref):
    n = h_got.shape[0]
    core = lax.rem(lax.axis_index("tp"), 2)
    h_ref[pl.ds(pl.multiple_of(core * n, n), n), :] = h_got[...]
    h_ref[pl.ds(pl.multiple_of((1 - core) * n, n), n), :] = h_core[...]


def z_first_kernel(lo, hi, h_got, h_core, w_hbm, z_hbm, m_ref, s_ref, h_ref, wbuf, wsem, zbuf, zsem):
    join_rows(h_got, h_core, h_ref)
    m_ref[...] = jnp.full(m_ref.shape, NEG_BIG, F32)
    s_ref[...] = jnp.zeros(s_ref.shape, F32)
    for _ in z_oth_loop(lo, hi, h_ref, w_hbm, z_hbm, wbuf, wsem, zbuf, zsem, m_ref, s_ref, [((hi - lo) // zbuf.shape[1], lambda k, c: c, lambda: 0)]):
        pass


def z_lattice_kernel(lo, hi, n_lat, n_lab, h_ref, w_hbm, m_in, s_in, p0, p1, p2, p3, meta_ref, z_in,
                     z_hbm, stats_ref, occ_ref, loss_ref, m_ref, s_ref,
                     wbuf, wsem, zbuf, zsem, e_lab, e_blk, a_lab, a_blk, b_lab, b_blk, o_t):
    n_blk = e_lab.shape[0]
    frames = n_blk * 64
    m_ref[...] = m_in[...]
    s_ref[...] = s_in[...]
    lane128 = lax.broadcasted_iota(jnp.int32, (LANES, LANES), 1)
    row32 = lax.broadcasted_iota(jnp.int32, (n_lab, LANES), 0)
    row8 = lax.broadcasted_iota(jnp.int32, (8, LANES), 0)
    lane32 = lax.broadcasted_iota(jnp.int32, (n_lab, LANES), 1)
    lane8 = lax.broadcasted_iota(jnp.int32, (8, LANES), 1)
    n_seq = meta_ref.shape[0]
    labs = jnp.zeros((n_lab, LANES), jnp.int32)
    lab_row = jnp.zeros((8, LANES), jnp.int32)
    live8 = jnp.zeros((8, LANES), jnp.int32)
    used8 = jnp.zeros((8, LANES), jnp.int32)
    for s in range(n_seq):
        for k in range(n_lab):
            labs = jnp.where((row32 == k) & (lane32 == s), meta_ref[s, k], labs)
            lab_row = jnp.where((row8 == s) & (lane8 == k), meta_ref[s, k], lab_row)
        live8 = jnp.where(lane8 == s, meta_ref[s, n_lab], live8)
        used8 = jnp.where(lane8 == s, meta_ref[s, n_lab + 1], used8)
    live32 = jnp.broadcast_to(live8[0:1], (n_lab, LANES))
    used32 = jnp.broadcast_to(used8[0:1], (n_lab, LANES))
    skip_dn = labs != pltpu.roll(labs, 1, 0)
    skip_up = labs != pltpu.roll(labs, n_lab - 1, 0)
    end_lab = row32 == used32 - 1
    end_blk = row32 == used32
    end_top = (row8 == 0) & (used8 == n_lab)
    shift0 = jnp.zeros((1, LANES), F32)
    seq1 = lane8[0:1] >= 64
    half_len = jnp.where(seq1, meta_ref[1, n_lab], meta_ref[0, n_lab])
    for j in range(n_blk):
        part = functools.reduce(jnp.add, [p[pl.ds(64 * j, 64), :] for p in (p0, p1, p2, p3)])
        blk = jnp.concatenate([part, pltpu.roll(part, 64, 1)], axis=0)
        blk = jnp.where(lane128 <= n_lab, blk, NEG_BIG)
        x = blk.T
        top = jnp.max(x[0:n_lab + 8], axis=0, keepdims=True)
        e_blk[j] = jnp.broadcast_to((x[0:1] - top) * LOG2E, (8, LANES))
        e_lab[j] = (pltpu.roll(x, LANES - 1, 0)[0:n_lab] - top) * LOG2E
        shift0 = shift0 + jnp.where(lax.rem(lane8[0:1], 64) + 64 * j < half_len, top, 0.0)
    shift_seq0 = jnp.sum(jnp.where(seq1, 0.0, shift0), axis=1, keepdims=True)
    shift_seq1 = jnp.sum(jnp.where(seq1, shift0, 0.0), axis=1, keepdims=True)

    def lse2(a, b):
        hi_v = jnp.maximum(a, b)
        return hi_v + jnp.log2(1.0 + jnp.exp2(jnp.minimum(a, b) - hi_v))

    def lse3(a, b, c):
        hi_v = jnp.maximum(a, b)
        lo_v = jnp.minimum(a, b)
        top = jnp.maximum(hi_v, c)
        mid = jnp.minimum(hi_v, c)
        return top + jnp.log2(1.0 + (jnp.exp2(lo_v - top) + jnp.exp2(mid - top)))

    def emission(t):
        j, u = t // 64, lax.rem(t, 64)
        idx32 = jnp.where(lane32 == 1, 64 + u, u)
        idx8 = jnp.where(lane8 == 1, 64 + u, u)
        el = jnp.take_along_axis(e_lab[j], idx32, axis=1)
        eb = jnp.take_along_axis(e_blk[j], idx8, axis=1)
        return el, eb

    neg32 = jnp.full((n_lab, LANES), NEG_BIG, F32)
    neg8 = jnp.full((8, LANES), NEG_BIG, F32)
    start32 = jnp.where(row32 == 0, 0.0, NEG_BIG)
    fin_b = jnp.where(end_blk, 0.0, NEG_BIG)
    fin_t = jnp.where(end_top, 0.0, NEG_BIG)
    skip_dn = skip_dn & (row32 > 0)
    skip_up = skip_up & (row32 < n_lab - 1)

    def lat_step(i, carry):
        al, ab, at, bl, bb, bt = carry
        el, eb = emission(i)
        eb32 = jnp.broadcast_to(eb[0:1], (n_lab, LANES))
        rolled = pltpu.roll(al, 1, 0)
        prev = jnp.where(row32 == 0, NEG_BIG, rolled)
        prev_t = jnp.where(row8 == 0, rolled[0:8], NEG_BIG)
        nl = lse3(al, ab, jnp.where(skip_dn, rolled, NEG_BIG))
        nb = lse2(ab, prev)
        nt = lse2(at, prev_t)
        a_lab[i] = nl
        a_blk[i, 0:n_lab] = nb
        a_blk[i, n_lab:n_lab + 8] = nt
        al = jnp.where(i < live32, el + nl, al)
        ab = jnp.where(i < live32, eb32 + nb, ab)
        at = jnp.where(i < live8, eb + nt, at)
        t = frames - 1 - i
        fl, fb = emission(t)
        fb32 = jnp.broadcast_to(fb[0:1], (n_lab, LANES))
        last = row32 == n_lab - 1
        up_l = jnp.where(skip_up, pltpu.roll(bl, n_lab - 1, 0), NEG_BIG)
        up_b = jnp.where(last, jnp.broadcast_to(bt[0:1], (n_lab, LANES)), pltpu.roll(bb, n_lab - 1, 0))
        ml = fl + lse3(bl, up_b, up_l)
        mb = fb32 + lse2(bb, bl)
        mt = fb + bt
        bl = jnp.where(t < live32, ml, bl)
        bb = jnp.where(t < live32, mb, bb)
        bt = jnp.where(t < live8, mt, bt)
        b_lab[t] = bl
        b_blk[t, 0:n_lab] = bb
        b_blk[t, n_lab:n_lab + 8] = bt
        return al, ab, at, bl, bb, bt

    group = zbuf.shape[1]
    n_lat_groups = n_lat // group
    per_tile = frames // n_lat_groups

    def lattice_side(k, carry):
        for u in range(per_tile):
            carry = lat_step(k * per_tile + u, carry)
        return carry

    n_occ = (hi - lo - n_lat) // group
    occ_group = frames // n_occ // 64
    back32 = jnp.where(lane32 >= 64, 1, 0)
    back8 = jnp.where(lane8 >= 64, 1, 0)
    run = z_oth_loop(lo, hi, h_ref, w_hbm, z_hbm, wbuf, wsem, zbuf, zsem, m_ref, s_ref,
                     [(n_lat_groups, lattice_side, lambda: (neg32, start32, neg8, neg32, fin_b, fin_t)),
                      (n_occ, lambda k, c: occ_side(k, c), lambda: 0)])
    al, ab, at, _, _, _ = next(run)

    lasts = [jnp.where(end, v, NEG_BIG) for end, v in ((end_lab, al), (end_blk, ab), (end_top, at))]
    top = functools.reduce(jnp.maximum, [jnp.max(v, axis=0, keepdims=True) for v in lasts])
    total = functools.reduce(jnp.add, [jnp.sum(jnp.exp2(v - top), axis=0, keepdims=True) for v in lasts])
    loss = -(top + jnp.log2(total))
    loss32 = jnp.broadcast_to(loss, (n_lab, LANES))
    loss8 = jnp.broadcast_to(loss, (8, LANES))
    lane1 = lane8[0:1]
    loss_ref[...] = jnp.broadcast_to(loss * (1.0 / LOG2E) - jnp.where(lane1 == 0, shift_seq0, jnp.where(lane1 == 1, shift_seq1, 0.0)), (8, LANES))

    def occ_frame(i, u, acc_l, acc_b):
        occ_l = jnp.where(i < live32, jnp.exp2(a_lab[i] + b_lab[i] + loss32), 0.0)
        occ_b = jnp.exp2(a_blk[i, 0:n_lab] + b_blk[i, 0:n_lab] + loss32)
        occ_u = jnp.exp2(a_blk[i, n_lab:n_lab + 8] + b_blk[i, n_lab:n_lab + 8] + loss8)
        blank = jnp.sum(occ_b, axis=0, keepdims=True) + occ_u[0:1]
        blank = jnp.where(i < live8, jnp.broadcast_to(blank, (8, LANES)), 0.0)
        acc_l = jnp.where(lax.rem(lane32, 64) == u, jnp.take_along_axis(occ_l, back32, axis=1), acc_l)
        acc_b = jnp.where(lax.rem(lane8, 64) == u, jnp.take_along_axis(blank, back8, axis=1), acc_b)
        return acc_l, acc_b

    def occ_side(k, c):
        for g in range(occ_group):
            j = k * occ_group + g
            acc_l = jnp.zeros((n_lab, LANES), F32)
            acc_b = jnp.zeros((8, LANES), F32)
            for u in range(64):
                acc_l, acc_b = occ_frame(j * 64 + u, u, acc_l, acc_b)
            o_t[j, 0:n_lab] = acc_l
            o_t[j, n_lab:n_lab + 8] = acc_b
            o_t[j, 8 + n_lab:LANES] = jnp.zeros((LANES - 8 - n_lab, LANES), F32)
        return c

    for _ in run:
        pass
    emit_stats(m_ref, s_ref, stats_ref, 0)
    row128 = lax.broadcasted_iota(jnp.int32, (LANES, LANES), 0)
    inner = (row128 < n_lab) & (lane128 < n_lab)
    same = []
    for s in range(n_seq):
        down = jnp.full((n_lab, LANES), -1, jnp.int32)
        for k in range(n_lab):
            down = jnp.where(row32 == k, meta_ref[s, k], down)
        down = jnp.concatenate([down, jnp.full((LANES - n_lab, LANES), -1, jnp.int32)], axis=0)
        across = jnp.broadcast_to(lab_row[s:s + 1], (LANES, LANES))
        same.append(jnp.where((inner & (down == across)) | (row128 == lane128), 1.0, 0.0))
    for j in range(n_blk):
        y = o_t[j].T
        for s in range(2):
            occ_ref[pl.ds(s * frames + 64 * j, 64), :] = jnp.dot(y[64 * s:64 * (s + 1), :], same[s], precision=lax.Precision.HIGHEST, preferred_element_type=F32)


def spread_lse(refs, base, meta_ref, lse_ref, r0, frames):
    m = functools.reduce(jnp.maximum, [r[base:base + 8, :] for r in refs])
    tot = functools.reduce(jnp.add, [r[base + 8:base + 16, :] * jnp.exp(r[base:base + 8, :] - m) for r in refs])
    lse = m + jnp.log(tot)
    t = lax.broadcasted_iota(jnp.int32, (LANES, LANES), 0)
    n_part = frames // LANES
    sums = []
    for q in range(meta_ref.shape[0]):
        live_sum = jnp.zeros((1, LANES), F32)
        for p in range(n_part):
            at = q * n_part + p
            part = jnp.broadcast_to(lse[at:at + 1, :], (LANES, LANES)).T
            live = t + p * LANES < meta_ref[q, meta_ref.shape[1] - 2]
            lse_ref[r0 + at * LANES:r0 + (at + 1) * LANES, :] = jnp.where(live, part, 1.0e30)
            live_sum = live_sum + jnp.sum(jnp.where(live, part, 0.0), axis=0, keepdims=True)
        sums.append(live_sum)
    return sums


def patch_tile(n_slots, frames, meta_refs, col_start, j, i, z_block, lse_ref, occ_ref, g_ref, g_col, lane):
    seq, item = i // n_slots, lax.rem(i, n_slots)
    off = label_col(meta_refs, i) - col_start - j * TILE
    blk = off // LANES
    r0 = pl.multiple_of(seq * frames, frames)
    c0 = pl.multiple_of(blk * LANES, LANES)
    zb = z_block(seq, c0)
    slot_lane = jnp.where(item == 0, n_slots - 1, item - 1)
    occ = jnp.sum(jnp.where(lane == slot_lane, occ_ref[pl.ds(r0, frames), :], 0.0), axis=1, keepdims=True)
    fresh = jnp.exp(zb - lse_ref[pl.ds(r0, frames), :]) - occ
    gc = pl.multiple_of(g_col + c0, LANES)
    old = g_ref[pl.ds(r0, frames), pl.ds(gc, LANES)].astype(F32)
    g_ref[pl.ds(r0, frames), pl.ds(gc, LANES)] = jnp.where(lane == off - blk * LANES, fresh, old).astype(BF16)


def softmax_unit(z, z_row, lse_ref, out, r0, n, c0):
    total = None
    for b in range(n // 32):
        lse = lse_ref[r0 + 32 * b:r0 + 32 * (b + 1), :]
        for k in range(TILE // LANES):
            e = jnp.exp(z[z_row + 32 * b:z_row + 32 * (b + 1), k * LANES:(k + 1) * LANES] - lse)
            out[r0 + 32 * b:r0 + 32 * (b + 1), c0 + k * LANES:c0 + (k + 1) * LANES] = e.astype(BF16)
            total = e if total is None else total + e
    return exact_zero(total)


def grad_h_kernel(n_slots, z_hbm, w_hbm, st0, st1, st2, st3, occ_ref, part_loss, meta_ref, keep_ref, send_ref, loss_ref, g_hbm,
                  wbuf, wsem, zbuf, zsem, acc, lse_ref, g0, g1, gsem, head, nxt):
    n_tiles, rows = z_hbm.shape[0], z_hbm.shape[1]
    frames = rows // meta_ref.shape[0]
    meta_refs = [meta_ref]
    group = zbuf.shape[1]
    n_groups = n_tiles // group
    stream = TileStream(w_hbm, wbuf, wsem, wbuf.shape[0], n_groups, lambda src, j: w_view(src, j, group))
    zs = TileStream(z_hbm, zbuf, zsem, zbuf.shape[0], n_groups, lambda src, j: z_view(src, j, group))
    zs.prime()
    stream.prime()
    col_start = build_lists(meta_refs, n_tiles * TILE, head, nxt)
    sums = spread_lse([st0, st1, st2, st3], frames, meta_ref, lse_ref, 0, frames)
    lane1 = lax.broadcasted_iota(jnp.int32, (8, LANES), 1)
    loss_ref[...] = part_loss[...] + jnp.where(lane1 == 0, sums[0], sums[1])
    lane = lax.broadcasted_iota(jnp.int32, (frames, LANES), 1)

    def patch(j, slot, g):
        for t in range(group):
            def z_block(seq, c0, t=t):
                return zbuf[slot, t, pl.ds(pl.multiple_of(seq * frames, frames), frames), pl.ds(c0, LANES)]

            walk_list(head, nxt, j * group + t,
                      lambda i, t=t, z_block=z_block: patch_tile(n_slots, frames, meta_refs, col_start, j * group + t, i, z_block, lse_ref, occ_ref, g, t * TILE, lane))

    def make_g(slot, u, g):
        t, r = u // 2, u % 2
        return softmax_unit(zbuf.at[slot, t], r * rows // 2, lse_ref, g, r * rows // 2, rows // 2, t * TILE)

    acc[...] = jnp.zeros(acc.shape, F32)
    slot0 = zs.get(0)
    for u in range(2 * group):
        make_g(slot0, u, g0)
    patch(0, slot0, g0)
    n_units = acc.shape[0] // 256

    def g_copy(j, g, k):
        return pltpu.make_async_copy(g, g_hbm.at[j], gsem.at[k])

    def half(j, g_now, g_next, k):
        slot = stream.get(j)
        nj = lax.min(j + 1, n_groups - 1)

        @pl.when(j + 1 < n_groups)
        def _():
            zs.get(nj)

        @pl.when(j >= 1)
        def _():
            g_copy(j - 1, g_next, 1 - k).wait()

        g_copy(j, g_now, k).start()

        zslot = lax.rem(nj, zbuf.shape[0])
        zero = None
        for u in range(n_units):
            d_rows = slice(u * 256, (u + 1) * 256)
            lhs = after(wbuf[slot, d_rows, :], zero)
            acc[d_rows, :] += lax.dot_general(lhs, g_now[...], (((1,), (1,)), ((), ())), preferred_element_type=F32)
            if u < 2 * group:
                zero = make_g(zslot, u, g_next)
        patch(nj, zslot, g_next)

    def step(i, c):
        half(2 * i, g0, g1, 0)
        half(2 * i + 1, g1, g0, 1)
        return c

    lax.fori_loop(0, n_groups // 2, step, 0)
    g_copy(n_groups - 1, g1, 1).wait()
    core = lax.rem(lax.axis_index("tp"), 2)
    n = rows // 2
    keep_ref[...] = acc[:, pl.ds(pl.multiple_of(core * n, n), n)].T
    send_ref[...] = acc[:, pl.ds(pl.multiple_of((1 - core) * n, n), n)].T


def grad_w_kernel(n_slots, g_hbm, z_hbm, h_own_ref, h_oth_ref, st0, st1, st2, st3, occ_ref, meta_ref, gw_hbm,
                  zbuf, zsem, gsem, obuf, osem, ht, lse_ref, g0, g1, head, nxt):
    n_tiles, rows = z_hbm.shape[0], z_hbm.shape[1]
    frames = rows // meta_ref.shape[0]
    d_loc = ht.shape[0]
    group = zbuf.shape[1]
    n_groups = n_tiles // group
    zs = TileStream(z_hbm, zbuf, zsem, zbuf.shape[0], n_groups, lambda src, j: z_view(src, j, group))

    def g_copy(j, g, k):
        return pltpu.make_async_copy(g_hbm.at[j], g.at[0:rows, :], gsem.at[k])

    g_copy(0, g0, 0).start()
    zs.prime()
    col_start = build_lists([meta_ref], n_tiles * TILE, head, nxt)
    d0 = pl.multiple_of(lax.axis_index("dp") * d_loc, LANES)
    ht[:, 0:rows] = h_own_ref[:, pl.ds(d0, d_loc)].T
    ht[:, rows:2 * rows] = h_oth_ref[:, pl.ds(d0, d_loc)].T
    spread_lse([st0, st1, st2, st3], 0, meta_ref, lse_ref, 0, frames)
    lane = lax.broadcasted_iota(jnp.int32, (frames, LANES), 1)
    n_units = 2 * group

    def make_g(slot, u, g):
        t, r = u // 2, u % 2
        return softmax_unit(zbuf.at[slot, t], r * rows // 2, lse_ref, g.at[rows:2 * rows, :], r * rows // 2, rows // 2, t * TILE)

    def patch(j, slot, g):
        for t in range(group):
            def z_block(seq, c0, t=t):
                return zbuf[slot, t, pl.ds(pl.multiple_of(seq * frames, frames), frames), pl.ds(c0, LANES)]

            walk_list(head, nxt, j * group + t,
                      lambda i, t=t, z_block=z_block: patch_tile(n_slots, frames, [meta_ref], col_start, j * group + t, i, z_block, lse_ref, occ_ref, g.at[rows:2 * rows, :], t * TILE, lane))

    def out_copy(j):
        slot = lax.rem(j, obuf.shape[0])
        return pltpu.make_async_copy(obuf.at[slot], w_view(gw_hbm, j, group), osem.at[slot])

    slot0 = zs.get(0)
    for u in range(n_units):
        make_g(slot0, u, g0)
    patch(0, slot0, g0)
    d_half = d_loc // 2

    def half(j, g_now, g_next, k):
        @pl.when(j >= 3)
        def _():
            out_copy(j - 3).wait()

        nj = lax.min(j + 1, n_groups - 1)

        @pl.when(j + 1 < n_groups)
        def _():
            zs.get(nj)
            g_copy(nj, g_next, 1 - k).start()

        g_copy(j, g_now, k).wait()
        slot = lax.rem(nj, zbuf.shape[0])
        oslot = lax.rem(j, obuf.shape[0])
        zero = None
        for u in range(n_units):
            t, r = u // 2, u % 2
            d_rows = slice(r * d_half, (r + 1) * d_half)
            lhs = after(ht[d_rows, :], zero)
            obuf[oslot, d_rows, t * TILE:(t + 1) * TILE] = jnp.dot(lhs, g_now[:, t * TILE:(t + 1) * TILE], preferred_element_type=F32)
            zero = make_g(slot, u, g_next)
        out_copy(j).start()
        patch(nj, slot, g_next)

    def step(i, c):
        half(2 * i, g0, g1, 0)
        half(2 * i + 1, g1, g0, 1)
        return c

    lax.fori_loop(0, n_groups // 2, step, 0)
    for j in range(n_groups - 3, n_groups):
        out_copy(j).wait()


def cost(flops, nbytes):
    return pl.CostEstimate(flops=flops, bytes_accessed=nbytes, transcendentals=0)


def solution(mesh):
    batch_axes = ("part", "dp")
    n_tp = mesh.shape["tp"]
    n_dp = mesh.shape["dp"]
    dp_swap = [(i, n_dp - 1 - i) for i in range(n_dp)]

    others = range(1, n_tp)

    def tp_xor(x, mask):
        return lax.ppermute(x, "tp", [(i, i ^ mask) for i in range(n_tp)])

    def swap_dp(x):
        return lax.ppermute(x, "dp", dp_swap)

    def local_body(hidden, w_loc, labels, in_len, lab_len):
        batch_loc, frames, model_dim = hidden.shape
        vocab_loc = w_loc.shape[1]
        n_lab = labels.shape[1]
        n_slots = n_lab + 1
        rows = batch_loc * frames
        n_tiles = vocab_loc // TILE
        d_loc = model_dim // n_dp
        dma = pltpu.SemaphoreType.DMA
        i32 = jnp.int32
        cut_a, n_lat = 8, 16
        h_own = hidden.reshape(rows, model_dim)
        core = lax.rem(lax.axis_index("tp"), 2)
        h_half = lax.dynamic_index_in_dim(h_own.reshape(2, rows // 2, model_dim), core, 0, keepdims=False)
        h_got = swap_dp(h_half)
        flops = 2 * rows * model_dim * TILE
        wbytes = model_dim * TILE * 2
        zbytes = rows * TILE * 4
        z_type = jax.ShapeDtypeStruct((n_tiles, rows, TILE), F32)
        run_type = jax.ShapeDtypeStruct((rows, LANES), F32)
        pick_type = jax.ShapeDtypeStruct((frames + 16, LANES), F32)
        meta_type = jax.ShapeDtypeStruct((batch_loc, n_slots + 1), i32)
        g_type = jax.ShapeDtypeStruct((n_tiles // 2, rows, 2 * TILE), BF16)
        stat_type = jax.ShapeDtypeStruct((16, LANES), F32)

        def w_scratch(n):
            return [pltpu.VMEM((3, model_dim, n * TILE), BF16), dma((3,))]

        def z_scratch(n):
            return [pltpu.VMEM((3, n, rows, TILE), F32), dma((3,))]

        run_scratch = [pltpu.VMEM((rows, LANES), F32), pltpu.VMEM((rows, LANES), F32)]

        def lists(n_sets):
            return [pltpu.SMEM((n_tiles,), i32), pltpu.SMEM((n_sets * batch_loc * n_slots,), i32)]

        z_own, pick, meta = kernel_call(
            functools.partial(z_own_kernel, n_slots),
            out_shape=(z_type, pick_type, meta_type),
            in_specs=[vmem_spec(), any_spec(), smem_spec(), smem_spec(), smem_spec()],
            out_specs=(any_spec(), vmem_spec(), smem_spec()),
            scratch_shapes=w_scratch(2) + z_scratch(2) + run_scratch + lists(1),
            compiler_params=params(),
            cost_estimate=cost(n_tiles * flops, n_tiles * (wbytes + zbytes)),
        )(h_own, w_loc, labels, in_len, lab_len)

        h_got, pick = lax.optimization_barrier((h_got, pick))
        h_core = tp_xor(h_got, 1)
        picks = [pick] + [tp_xor(pick, k) for k in others]

        z_part, run_m, run_s, h_oth = kernel_call(
            functools.partial(z_first_kernel, 0, cut_a),
            out_shape=(z_type, run_type, run_type, jax.ShapeDtypeStruct((rows, model_dim), BF16)),
            in_specs=[vmem_spec(), vmem_spec(), any_spec()],
            out_specs=(any_spec(), vmem_spec(), vmem_spec(), vmem_spec()),
            scratch_shapes=w_scratch(2) + z_scratch(2),
            compiler_params=params(),
            cost_estimate=cost(cut_a * flops, cut_a * (wbytes + zbytes)),
        )(h_got, h_core, w_loc)

        n_blk = frames // 64
        z_oth, stats_oth, occ, part_loss = kernel_call(
            functools.partial(z_lattice_kernel, cut_a, n_tiles, n_lat, n_lab),
            out_shape=(z_type, stat_type, run_type, jax.ShapeDtypeStruct((8, LANES), F32)),
            in_specs=[vmem_spec(), any_spec()] + [vmem_spec()] * 6 + [smem_spec(), any_spec()],
            out_specs=(any_spec(),) + (vmem_spec(),) * 3,
            input_output_aliases={9: 0},
            scratch_shapes=run_scratch + w_scratch(2) + z_scratch(2) + [
                pltpu.VMEM((n_blk, n_lab, LANES), F32), pltpu.VMEM((n_blk, 8, LANES), F32),
                pltpu.VMEM((frames, n_lab, LANES), F32), pltpu.VMEM((frames, n_lab + 8, LANES), F32),
                pltpu.VMEM((frames, n_lab, LANES), F32), pltpu.VMEM((frames, n_lab + 8, LANES), F32),
                pltpu.VMEM((n_blk, LANES, LANES), F32)],
            compiler_params=params(),
            cost_estimate=cost((n_tiles - cut_a) * flops, (n_tiles - cut_a) * (wbytes + zbytes)),
        )(h_oth, w_loc, run_m, run_s, *picks, meta, z_part)

        st_oth = [stats_oth] + [tp_xor(stats_oth, k) for k in others]
        occ_oth = swap_dp(occ)
        meta_oth = swap_dp(meta)
        keep, send, loss, g_own = kernel_call(
            functools.partial(grad_h_kernel, n_slots),
            out_shape=(jax.ShapeDtypeStruct((rows // 2, model_dim), F32), jax.ShapeDtypeStruct((rows // 2, model_dim), F32), jax.ShapeDtypeStruct((8, LANES), F32), g_type),
            in_specs=[any_spec(), any_spec()] + [vmem_spec()] * 6 + [smem_spec()],
            out_specs=(vmem_spec(),) * 3 + (any_spec(),),
            scratch_shapes=w_scratch(2) + z_scratch(2) + [pltpu.VMEM((model_dim, rows), F32), pltpu.VMEM((rows, LANES), F32),
                                                     pltpu.VMEM((rows, 2 * TILE), BF16), pltpu.VMEM((rows, 2 * TILE), BF16), dma((2,))] + lists(1),
            compiler_params=params(),
            cost_estimate=cost(n_tiles * flops, n_tiles * (wbytes + zbytes)),
        )(z_own, w_loc, *picks, occ, part_loss, meta)

        recv = tp_xor(send, 1)
        chip_sum = keep + recv
        across = tp_xor(chip_sum, 2)

        grad_weight = kernel_call(
            functools.partial(grad_w_kernel, n_slots),
            out_shape=jax.ShapeDtypeStruct((d_loc, vocab_loc), F32),
            in_specs=[any_spec(), any_spec()] + [vmem_spec()] * 7 + [smem_spec()],
            out_specs=any_spec(),
            scratch_shapes=z_scratch(2) + [
                dma((2,)), pltpu.VMEM((3, d_loc, 2 * TILE), F32), dma((3,)),
                pltpu.VMEM((d_loc, 2 * rows), BF16), pltpu.VMEM((rows, LANES), F32),
                pltpu.VMEM((2 * rows, 2 * TILE), BF16), pltpu.VMEM((2 * rows, 2 * TILE), BF16)] + lists(1),
            compiler_params=params(),
            cost_estimate=cost(n_tiles * flops, n_tiles * (2 * zbytes + d_loc * TILE * 4)),
        )(g_own, z_oth, h_own, h_oth, *st_oth, occ_oth, meta_oth)

        chip_sum, grad_weight = lax.optimization_barrier((chip_sum, grad_weight))
        full_half = chip_sum + across
        other_half = tp_xor(full_half, 1)
        grad_hidden = jnp.where(core == 0, jnp.stack([full_half, other_half]), jnp.stack([other_half, full_half])).reshape(batch_loc, frames, model_dim)
        return loss[0, :batch_loc], grad_weight, grad_hidden


    return jax.shard_map(
        local_body,
        mesh=mesh,
        in_specs=(P(batch_axes, None, None), P(None, "tp"), P(batch_axes, None), P(batch_axes), P(batch_axes)),
        out_specs=(P(batch_axes), P(batch_axes, "tp"), P(batch_axes, None, None)),
        check_vma=False,
    )
```

```python
import functools

import jax
import jax.numpy as jnp
from jax import lax
from jax.experimental import pallas as pl
from jax.experimental.pallas import tpu as pltpu
from jax.sharding import PartitionSpec as P

NEG_BIG = -1.0e30
LOG2E = 1.4426950408889634
F32 = jnp.float32
BF16 = jnp.bfloat16
TILE = 512
LANES = 128
MIB = 1 << 20


def vmem_spec():
    return pl.BlockSpec(memory_space=pltpu.VMEM)


def smem_spec():
    return pl.BlockSpec(memory_space=pltpu.SMEM)


def any_spec():
    return pl.BlockSpec(memory_space=pl.ANY)


def kernel_call(*args, **kw):
    return pl.pallas_call(*args, **kw)


def params():
    return pltpu.CompilerParams(vmem_limit_bytes=56 * MIB)


def label_col(meta_refs, i):
    n_slots = meta_refs[0].shape[1] - 1
    seq, item = i // n_slots, lax.rem(i, n_slots)
    n_seq = meta_refs[0].shape[0]
    at = lax.max(item - 1, 0)
    col = meta_refs[0][lax.rem(seq, n_seq), at]
    for k in range(1, len(meta_refs)):
        col = jnp.where(seq >= k * n_seq, meta_refs[k][lax.rem(seq, n_seq), at], col)
    return jnp.where(item == 0, 0, col)


def build_lists(meta_refs, vocab_loc, head, nxt):
    n_items = len(meta_refs) * meta_refs[0].shape[0] * (meta_refs[0].shape[1] - 1)
    col_start = lax.axis_index("tp") * vocab_loc
    n_tiles = vocab_loc // TILE

    def clear(i, c):
        head[i] = -1
        return c

    lax.fori_loop(0, n_tiles, clear, 0)

    def insert(i, c):
        loc = label_col(meta_refs, i) - col_start
        tile = lax.max(loc, 0) // TILE

        @pl.when((loc >= 0) & (loc < vocab_loc))
        def _():
            nxt[i] = head[tile]
            head[tile] = i

        return c

    lax.fori_loop(0, n_items, insert, 0)
    return col_start


def walk_list(head, nxt, tile, visit):
    def body(i):
        visit(i)
        return nxt[i]

    lax.while_loop(lambda i: i >= 0, body, head[tile])


class TileStream:
    def __init__(self, src, buf, sem, depth, n_tiles, view):
        self.src, self.buf, self.sem, self.depth, self.n, self.view = src, buf, sem, depth, n_tiles, view

    def copy(self, j):
        slot = lax.rem(j, self.depth)
        return pltpu.make_async_copy(self.view(self.src, j), self.buf.at[slot], self.sem.at[slot])

    def prime(self):
        for j in range(min(self.depth - 1, self.n)):
            self.copy(j).start()

    def get(self, j):
        self.copy(j).wait()

        @pl.when(j + self.depth - 1 < self.n)
        def _():
            self.copy(j + self.depth - 1).start()

        return lax.rem(j, self.depth)


def w_view(src, j, n=1):
    return src.at[:, pl.ds(pl.multiple_of(j * n * TILE, TILE), n * TILE)]


def z_view(src, j, n):
    return src.at[pl.ds(j * n, n)]


def exact_zero(total):
    return jnp.minimum(total[0:16] + total[16:32], 0.0).astype(BF16)


def after(lhs, zero):
    if zero is None:
        return lhs
    corner = lhs[0:16, 0:LANES] + zero
    return jnp.concatenate([jnp.concatenate([corner, lhs[0:16, LANES:]], axis=1), lhs[16:]], axis=0)


def unit_stats(z, m_ref, s_ref, r0):
    n_chunks = z.shape[1] // LANES
    total = None
    for b in range(z.shape[0] // 32):
        zb = [z[32 * b:32 * (b + 1), k * LANES:(k + 1) * LANES] for k in range(n_chunks)]
        rows = slice(r0 + 32 * b, r0 + 32 * (b + 1))
        m_old = m_ref[rows, :]
        m_new = functools.reduce(jnp.maximum, zb, m_old)
        s_new = s_ref[rows, :] * jnp.exp(m_old - m_new)
        for part in zb:
            s_new = s_new + jnp.exp(part - m_new)
        m_ref[rows, :] = m_new
        s_ref[rows, :] = s_new
        total = s_new if total is None else total + s_new
    return exact_zero(total)


def z_group(h_ref, w, z_out, m_ref, s_ref):
    n_tiles = z_out.shape[0]
    n = h_ref.shape[0] // 2
    zeros = []
    for t in range(n_tiles):
        for r in range(2):
            rows = slice(r * n, (r + 1) * n)
            lhs = after(h_ref[rows, :], zeros[-2] if len(zeros) >= 2 else None)
            z = jnp.dot(lhs, w[:, t * TILE:(t + 1) * TILE], preferred_element_type=F32)
            z_out[t, rows, :] = z
            zeros.append(unit_stats(z, m_ref, s_ref, r * n))


def emit_stats(m_ref, s_ref, out_ref, base):
    row_m = jnp.max(m_ref[...], axis=1, keepdims=True)
    row_s = jnp.sum(s_ref[...] * jnp.exp(m_ref[...] - row_m), axis=1, keepdims=True)
    rows = m_ref.shape[0]
    for k, v in enumerate((row_m, row_s)):
        flat = jnp.broadcast_to(v, (rows, LANES)).T
        for p in range(rows // LANES):
            at = base + 8 * k + p
            out_ref[at:at + 1, :] = flat[0:1, p * LANES:(p + 1) * LANES]


def z_own_kernel(n_slots, h_hbm, w_hbm, labels_ref, in_len_ref, lab_len_ref, z_hbm, pick_ref, meta_ref, h_ref, hsem, wbuf, wsem, zbuf, zsem, m_ref, s_ref, head, nxt):
    n_tiles = z_hbm.shape[0]
    rows = h_ref.shape[0]
    n_seq = meta_ref.shape[0]
    frames = rows // n_seq
    h_copy = pltpu.make_async_copy(h_hbm, h_ref, hsem.at[0])
    h_copy.start()
    n_lab = n_slots - 1
    for q in range(n_seq):
        def put(k, c, q=q):
            meta_ref[q, k] = labels_ref[q, k]
            return c

        lax.fori_loop(0, n_lab, put, 0)
        meta_ref[q, n_lab] = in_len_ref[q]
        meta_ref[q, n_lab + 1] = lab_len_ref[q]
    group = zbuf.shape[1]
    stream = TileStream(w_hbm, wbuf, wsem, wbuf.shape[0], n_tiles // group, lambda src, j: w_view(src, j, group))
    stream.prime()
    col_start = build_lists([meta_ref], n_tiles * TILE, head, nxt)
    m_ref[...] = jnp.full(m_ref.shape, NEG_BIG, F32)
    s_ref[...] = jnp.zeros(s_ref.shape, F32)
    pick_ref[...] = jnp.zeros(pick_ref.shape, F32)
    h_copy.wait()
    lane = lax.broadcasted_iota(jnp.int32, (frames, LANES), 1)

    def out_copy(j):
        slot = lax.rem(j, zbuf.shape[0])
        return pltpu.make_async_copy(zbuf.at[slot], z_view(z_hbm, j, group), zsem.at[slot])

    def step(j, c):
        slot = stream.get(j)

        @pl.when(j >= 3)
        def _():
            out_copy(j - 3).wait()

        zslot = lax.rem(j, zbuf.shape[0])
        z_group(h_ref, wbuf.at[slot], zbuf.at[zslot], m_ref, s_ref)
        out_copy(j).start()

        for t in range(group):
            def visit(i, t=t):
                seq, item = i // n_slots, lax.rem(i, n_slots)
                off = label_col([meta_ref], i) - col_start - (j * group + t) * TILE
                blk = off // LANES
                r0 = pl.multiple_of(seq * frames, frames)
                zb = zbuf[zslot, t, pl.ds(r0, frames), pl.ds(pl.multiple_of(blk * LANES, LANES), LANES)]
                at = item + 64 * seq
                moved = pltpu.roll(zb, lax.rem(at - (off - blk * LANES) + 2 * LANES, LANES), 1)
                pick_ref[0:frames, :] = jnp.where(lane == at, moved, pick_ref[0:frames, :])

            walk_list(head, nxt, j * group + t, visit)
        return c

    n_groups = n_tiles // group
    lax.fori_loop(0, n_groups, step, 0)
    emit_stats(m_ref, s_ref, pick_ref, frames)
    for j in range(n_groups - 3, n_groups):
        out_copy(j).wait()


def z_oth_loop(lo, hi, join, h_ref, w_hbm, z_hbm, wbuf, wsem, zbuf, zsem, m_ref, s_ref, sections):
    group = zbuf.shape[1]
    lo, n_groups = lo // group, (hi - lo) // group
    stream = TileStream(w_hbm, wbuf, wsem, wbuf.shape[0], n_groups, lambda src, j: w_view(src, lo + j, group))
    stream.prime()

    def out_copy(j):
        slot = lax.rem(j, zbuf.shape[0])
        return pltpu.make_async_copy(zbuf.at[slot], z_view(z_hbm, lo + j, group), zsem.at[slot])

    base = 0
    join.wait()
    for n, side, make_carry in sections:
        carry = make_carry()

        def step(k, c, base=base, side=side):
            j = base + k
            slot = stream.get(j)

            @pl.when(j >= 3)
            def _():
                out_copy(j - 3).wait()

            z_group(h_ref, wbuf.at[slot], zbuf.at[lax.rem(j, zbuf.shape[0])], m_ref, s_ref)
            c = side(k, c)
            out_copy(j).start()
            return c

        last = lax.fori_loop(0, n, step, carry)
        yield last
        base += n
    for j in range(max(n_groups - 3, 0), n_groups):
        out_copy(j).wait()


class JoinRows:
    def __init__(self, h_got, h_core, h_ref, hsem):
        n = h_got.shape[0]
        core = lax.rem(lax.axis_index("tp"), 2)
        self.copies = [pltpu.make_async_copy(src, h_ref.at[pl.ds(pl.multiple_of(at * n, n), n), :], hsem.at[k])
                       for k, (src, at) in enumerate(((h_got, core), (h_core, 1 - core)))]

    def start(self):
        for c in self.copies:
            c.start()

    def wait(self):
        for c in self.copies:
            c.wait()


def z_first_kernel(lo, hi, h_got, h_core, w_hbm, z_hbm, m_ref, s_ref, h_ref, hsem, wbuf, wsem, zbuf, zsem):
    join = JoinRows(h_got, h_core, h_ref, hsem)
    join.start()
    m_ref[...] = jnp.full(m_ref.shape, NEG_BIG, F32)
    s_ref[...] = jnp.zeros(s_ref.shape, F32)
    for _ in z_oth_loop(lo, hi, join, h_ref, w_hbm, z_hbm, wbuf, wsem, zbuf, zsem, m_ref, s_ref, [((hi - lo) // zbuf.shape[1], lambda k, c: c, lambda: 0)]):
        pass


def z_lattice_part(lo, hi, n_lat, n_lab, before_tail, h_got, h_core, w_hbm, m_in, s_in, p0, p1, p2, p3, meta_ref,
                     z_hbm, stats_ref, occ_ref, loss_ref, m_ref, s_ref,
                     h_ref, hsem, wbuf, wsem, zbuf, zsem, e_lab, e_blk, a_lab, a_blk, b_lab, b_blk, o_t):
    join = JoinRows(h_got, h_core, h_ref, hsem)
    join.start()
    n_blk = e_lab.shape[0]
    frames = n_blk * 64
    m_ref[...] = m_in[...]
    s_ref[...] = s_in[...]
    lane128 = lax.broadcasted_iota(jnp.int32, (LANES, LANES), 1)
    row32 = lax.broadcasted_iota(jnp.int32, (n_lab, LANES), 0)
    row8 = lax.broadcasted_iota(jnp.int32, (8, LANES), 0)
    lane32 = lax.broadcasted_iota(jnp.int32, (n_lab, LANES), 1)
    lane8 = lax.broadcasted_iota(jnp.int32, (8, LANES), 1)
    n_seq = meta_ref.shape[0]
    labs = jnp.zeros((n_lab, LANES), jnp.int32)
    lab_row = jnp.zeros((8, LANES), jnp.int32)
    live8 = jnp.zeros((8, LANES), jnp.int32)
    used8 = jnp.zeros((8, LANES), jnp.int32)
    for s in range(n_seq):
        for k in range(n_lab):
            labs = jnp.where((row32 == k) & (lane32 == s), meta_ref[s, k], labs)
            lab_row = jnp.where((row8 == s) & (lane8 == k), meta_ref[s, k], lab_row)
        live8 = jnp.where(lane8 == s, meta_ref[s, n_lab], live8)
        used8 = jnp.where(lane8 == s, meta_ref[s, n_lab + 1], used8)
    live32 = jnp.broadcast_to(live8[0:1], (n_lab, LANES))
    used32 = jnp.broadcast_to(used8[0:1], (n_lab, LANES))
    skip_dn = labs != pltpu.roll(labs, 1, 0)
    skip_up = labs != pltpu.roll(labs, n_lab - 1, 0)
    end_lab = row32 == used32 - 1
    end_blk = row32 == used32
    end_top = (row8 == 0) & (used8 == n_lab)
    shift0 = jnp.zeros((1, LANES), F32)
    seq1 = lane8[0:1] >= 64
    half_len = jnp.where(seq1, meta_ref[1, n_lab], meta_ref[0, n_lab])
    for j in range(n_blk):
        part = functools.reduce(jnp.add, [p[pl.ds(64 * j, 64), :] for p in (p0, p1, p2, p3)])
        blk = jnp.concatenate([part, pltpu.roll(part, 64, 1)], axis=0)
        blk = jnp.where(lane128 <= n_lab, blk, NEG_BIG)
        x = blk.T
        top = jnp.max(x[0:n_lab + 8], axis=0, keepdims=True)
        e_blk[j] = jnp.broadcast_to((x[0:1] - top) * LOG2E, (8, LANES))
        e_lab[j] = (pltpu.roll(x, LANES - 1, 0)[0:n_lab] - top) * LOG2E
        shift0 = shift0 + jnp.where(lax.rem(lane8[0:1], 64) + 64 * j < half_len, top, 0.0)
    shift_seq0 = jnp.sum(jnp.where(seq1, 0.0, shift0), axis=1, keepdims=True)
    shift_seq1 = jnp.sum(jnp.where(seq1, shift0, 0.0), axis=1, keepdims=True)

    def lse2(a, b):
        hi_v = jnp.maximum(a, b)
        return hi_v + jnp.log2(1.0 + jnp.exp2(jnp.minimum(a, b) - hi_v))

    def lse3(a, b, c):
        hi_v = jnp.maximum(a, b)
        lo_v = jnp.minimum(a, b)
        top = jnp.maximum(hi_v, c)
        mid = jnp.minimum(hi_v, c)
        return top + jnp.log2(1.0 + (jnp.exp2(lo_v - top) + jnp.exp2(mid - top)))

    pick32 = jnp.where(lane32 == 1, 64, 0)
    pick8 = jnp.where(lane8 == 1, 64, 0)

    def lanes_of(x, idx):
        return jnp.take_along_axis(x, idx, axis=1, mode="promise_in_bounds")

    def emission(j, u):
        return lanes_of(e_lab[j], pick32 + u), lanes_of(e_blk[j], pick8 + u)

    neg32 = jnp.full((n_lab, LANES), NEG_BIG, F32)
    neg8 = jnp.full((8, LANES), NEG_BIG, F32)
    start32 = jnp.where(row32 == 0, 0.0, NEG_BIG)
    fin_b = jnp.where(end_blk, 0.0, NEG_BIG)
    fin_t = jnp.where(end_top, 0.0, NEG_BIG)
    skip_dn = skip_dn & (row32 > 0)
    skip_up = skip_up & (row32 < n_lab - 1)

    def lat_step(i, j, u, carry):
        al, ab, at, bl, bb, bt = carry
        el, eb = emission(j, u)
        eb32 = jnp.broadcast_to(eb[0:1], (n_lab, LANES))
        rolled = pltpu.roll(al, 1, 0)
        prev = jnp.where(row32 == 0, NEG_BIG, rolled)
        prev_t = jnp.where(row8 == 0, rolled[0:8], NEG_BIG)
        nl = lse3(al, ab, jnp.where(skip_dn, rolled, NEG_BIG))
        nb = lse2(ab, prev)
        nt = lse2(at, prev_t)
        a_lab[i] = nl
        a_blk[i, 0:n_lab] = nb
        a_blk[i, n_lab:n_lab + 8] = nt
        al = jnp.where(i < live32, el + nl, al)
        ab = jnp.where(i < live32, eb32 + nb, ab)
        at = jnp.where(i < live8, eb + nt, at)
        t = frames - 1 - i
        fl, fb = emission(n_blk - 1 - j, 63 - u)
        fb32 = jnp.broadcast_to(fb[0:1], (n_lab, LANES))
        last = row32 == n_lab - 1
        up_l = jnp.where(skip_up, pltpu.roll(bl, n_lab - 1, 0), NEG_BIG)
        up_b = jnp.where(last, jnp.broadcast_to(bt[0:1], (n_lab, LANES)), pltpu.roll(bb, n_lab - 1, 0))
        ml = fl + lse3(bl, up_b, up_l)
        mb = fb32 + lse2(bb, bl)
        mt = fb + bt
        bl = jnp.where(t < live32, ml, bl)
        bb = jnp.where(t < live32, mb, bb)
        bt = jnp.where(t < live8, mt, bt)
        b_lab[t] = bl
        b_blk[t, 0:n_lab] = bb
        b_blk[t, n_lab:n_lab + 8] = bt
        return al, ab, at, bl, bb, bt

    group = zbuf.shape[1]
    n_lat_groups = n_lat // group
    per_tile = frames // n_lat_groups

    def lattice_side(k, carry):
        i = k * per_tile
        j = lax.div(i, 64)
        for u in range(per_tile):
            carry = lat_step(i + u, j, i - 64 * j + u, carry)
        return carry

    n_occ = (hi - lo - n_lat) // group
    occ_group = frames // n_occ // 64
    back32 = jnp.where(lane32 >= 64, 1, 0)
    back8 = jnp.where(lane8 >= 64, 1, 0)
    run = z_oth_loop(lo, hi, join, h_ref, w_hbm, z_hbm, wbuf, wsem, zbuf, zsem, m_ref, s_ref,
                     [(n_lat_groups, lattice_side, lambda: (neg32, start32, neg8, neg32, fin_b, fin_t)),
                      (n_occ, lambda k, c: occ_side(k, c), lambda: 0)])
    al, ab, at, _, _, _ = next(run)

    lasts = [jnp.where(end, v, NEG_BIG) for end, v in ((end_lab, al), (end_blk, ab), (end_top, at))]
    top = functools.reduce(jnp.maximum, [jnp.max(v, axis=0, keepdims=True) for v in lasts])
    total = functools.reduce(jnp.add, [jnp.sum(jnp.exp2(v - top), axis=0, keepdims=True) for v in lasts])
    loss = -(top + jnp.log2(total))
    loss32 = jnp.broadcast_to(loss, (n_lab, LANES))
    loss8 = jnp.broadcast_to(loss, (8, LANES))
    lane1 = lane8[0:1]
    loss_ref[...] = jnp.broadcast_to(loss * (1.0 / LOG2E) - jnp.where(lane1 == 0, shift_seq0, jnp.where(lane1 == 1, shift_seq1, 0.0)), (8, LANES))

    def occ_frame(i, u, acc_l, acc_b):
        occ_l = jnp.where(i < live32, jnp.exp2(a_lab[i] + b_lab[i] + loss32), 0.0)
        occ_b = jnp.exp2(a_blk[i, 0:n_lab] + b_blk[i, 0:n_lab] + loss32)
        occ_u = jnp.exp2(a_blk[i, n_lab:n_lab + 8] + b_blk[i, n_lab:n_lab + 8] + loss8)
        blank = jnp.sum(occ_b, axis=0, keepdims=True) + occ_u[0:1]
        blank = jnp.where(i < live8, jnp.broadcast_to(blank, (8, LANES)), 0.0)
        acc_l = jnp.where(lax.rem(lane32, 64) == u, lanes_of(occ_l, back32), acc_l)
        acc_b = jnp.where(lax.rem(lane8, 64) == u, lanes_of(blank, back8), acc_b)
        return acc_l, acc_b

    def occ_side(k, c):
        for g in range(occ_group):
            j = k * occ_group + g
            acc_l = jnp.zeros((n_lab, LANES), F32)
            acc_b = jnp.zeros((8, LANES), F32)
            for u in range(64):
                acc_l, acc_b = occ_frame(j * 64 + u, u, acc_l, acc_b)
            o_t[j, 0:n_lab] = acc_l
            o_t[j, n_lab:n_lab + 8] = acc_b
            o_t[j, 8 + n_lab:LANES] = jnp.zeros((LANES - 8 - n_lab, LANES), F32)
        return c

    next(run)
    before_tail()
    for _ in run:
        pass
    emit_stats(m_ref, s_ref, stats_ref, 0)
    row128 = lax.broadcasted_iota(jnp.int32, (LANES, LANES), 0)
    inner = (row128 < n_lab) & (lane128 < n_lab)
    same = []
    for s in range(n_seq):
        down = jnp.full((n_lab, LANES), -1, jnp.int32)
        for k in range(n_lab):
            down = jnp.where(row32 == k, meta_ref[s, k], down)
        down = jnp.concatenate([down, jnp.full((LANES - n_lab, LANES), -1, jnp.int32)], axis=0)
        across = jnp.broadcast_to(lab_row[s:s + 1], (LANES, LANES))
        same.append(jnp.where((inner & (down == across)) | (row128 == lane128), 1.0, 0.0))
    for j in range(n_blk):
        y = o_t[j].T
        for s in range(2):
            occ_ref[pl.ds(s * frames + 64 * j, 64), :] = jnp.dot(y[64 * s:64 * (s + 1), :], same[s], precision=lax.Precision.HIGHEST, preferred_element_type=F32)


def spread_lse(refs, base, meta_ref, lse_ref, r0, frames):
    m = functools.reduce(jnp.maximum, [r[base:base + 8, :] for r in refs])
    tot = functools.reduce(jnp.add, [r[base + 8:base + 16, :] * jnp.exp(r[base:base + 8, :] - m) for r in refs])
    lse = m + jnp.log(tot)
    t = lax.broadcasted_iota(jnp.int32, (LANES, LANES), 0)
    n_part = frames // LANES
    sums = []
    for q in range(meta_ref.shape[0]):
        live_sum = jnp.zeros((1, LANES), F32)
        for p in range(n_part):
            at = q * n_part + p
            part = jnp.broadcast_to(lse[at:at + 1, :], (LANES, LANES)).T
            live = t + p * LANES < meta_ref[q, meta_ref.shape[1] - 2]
            lse_ref[r0 + at * LANES:r0 + (at + 1) * LANES, :] = jnp.where(live, part, 1.0e30)
            live_sum = live_sum + jnp.sum(jnp.where(live, part, 0.0), axis=0, keepdims=True)
        sums.append(live_sum)
    return sums


def patch_tile(n_slots, frames, meta_refs, col_start, j, i, z_block, lse_ref, occ_ref, g_ref, g_col, lane):
    seq, item = i // n_slots, lax.rem(i, n_slots)
    off = label_col(meta_refs, i) - col_start - j * TILE
    blk = off // LANES
    r0 = pl.multiple_of(seq * frames, frames)
    c0 = pl.multiple_of(blk * LANES, LANES)
    zb = z_block(seq, c0)
    slot_lane = jnp.where(item == 0, n_slots - 1, item - 1)
    occ = jnp.sum(jnp.where(lane == slot_lane, occ_ref[pl.ds(r0, frames), :], 0.0), axis=1, keepdims=True)
    fresh = jnp.exp(zb - lse_ref[pl.ds(r0, frames), :]) - occ
    gc = pl.multiple_of(g_col + c0, LANES)
    old = g_ref[pl.ds(r0, frames), pl.ds(gc, LANES)].astype(F32)
    g_ref[pl.ds(r0, frames), pl.ds(gc, LANES)] = jnp.where(lane == off - blk * LANES, fresh, old).astype(BF16)


def softmax_unit(z, z_row, lse_ref, out, r0, n, c0):
    total = None
    for b in range(n // 32):
        lse = lse_ref[r0 + 32 * b:r0 + 32 * (b + 1), :]
        for k in range(TILE // LANES):
            e = jnp.exp(z[z_row + 32 * b:z_row + 32 * (b + 1), k * LANES:(k + 1) * LANES] - lse)
            out[r0 + 32 * b:r0 + 32 * (b + 1), c0 + k * LANES:c0 + (k + 1) * LANES] = e.astype(BF16)
            total = e if total is None else total + e
    return exact_zero(total)


def grad_h_part(n_slots, z_hbm, w_hbm, st0, st1, st2, st3, occ_ref, part_loss, meta_ref, keep_ref, send_ref, loss_ref, g_hbm,
                  wbuf, wsem, zbuf, zsem, acc, lse_ref, g0, g1, gsem, head, nxt):
    n_tiles, rows = z_hbm.shape[0], z_hbm.shape[1]
    frames = rows // meta_ref.shape[0]
    meta_refs = [meta_ref]
    group = zbuf.shape[1]
    n_groups = n_tiles // group
    stream = TileStream(w_hbm, wbuf, wsem, wbuf.shape[0], n_groups, lambda src, j: w_view(src, j, group))
    zs = TileStream(z_hbm, zbuf, zsem, zbuf.shape[0], n_groups, lambda src, j: z_view(src, j, group))
    zs.prime()
    yield stream.prime
    col_start = build_lists(meta_refs, n_tiles * TILE, head, nxt)
    sums = spread_lse([st0, st1, st2, st3], frames, meta_ref, lse_ref, 0, frames)
    lane1 = lax.broadcasted_iota(jnp.int32, (8, LANES), 1)
    loss_ref[...] = part_loss[...] + jnp.where(lane1 == 0, sums[0], sums[1])
    lane = lax.broadcasted_iota(jnp.int32, (frames, LANES), 1)

    def patch(j, slot, g):
        for t in range(group):
            def z_block(seq, c0, t=t):
                return zbuf[slot, t, pl.ds(pl.multiple_of(seq * frames, frames), frames), pl.ds(c0, LANES)]

            walk_list(head, nxt, j * group + t,
                      lambda i, t=t, z_block=z_block: patch_tile(n_slots, frames, meta_refs, col_start, j * group + t, i, z_block, lse_ref, occ_ref, g, t * TILE, lane))

    def make_g(slot, u, g):
        t, r = u // 2, u % 2
        return softmax_unit(zbuf.at[slot, t], r * rows // 2, lse_ref, g, r * rows // 2, rows // 2, t * TILE)

    acc[...] = jnp.zeros(acc.shape, F32)
    slot0 = zs.get(0)
    for u in range(2 * group):
        make_g(slot0, u, g0)
    patch(0, slot0, g0)
    n_units = acc.shape[0] // 256

    def g_copy(j, g, k):
        return pltpu.make_async_copy(g, g_hbm.at[j], gsem.at[k])

    def half(j, g_now, g_next, k):
        slot = stream.get(j)
        nj = lax.min(j + 1, n_groups - 1)

        @pl.when(j + 1 < n_groups)
        def _():
            zs.get(nj)

        @pl.when(j >= 1)
        def _():
            g_copy(j - 1, g_next, 1 - k).wait()

        g_copy(j, g_now, k).start()

        zslot = lax.rem(nj, zbuf.shape[0])
        zero = None
        for u in range(n_units):
            d_rows = slice(u * 256, (u + 1) * 256)
            lhs = after(wbuf[slot, d_rows, :], zero)
            acc[d_rows, :] += lax.dot_general(lhs, g_now[...], (((1,), (1,)), ((), ())), preferred_element_type=F32)
            if u < 2 * group:
                zero = make_g(zslot, u, g_next)
        patch(nj, zslot, g_next)

    def step(i, c):
        half(2 * i, g0, g1, 0)
        half(2 * i + 1, g1, g0, 1)
        return c

    lax.fori_loop(0, n_groups // 2, step, 0)
    g_copy(n_groups - 1, g1, 1).wait()
    core = lax.rem(lax.axis_index("tp"), 2)
    n = rows // 2
    keep_ref[...] = acc[:, pl.ds(pl.multiple_of(core * n, n), n)].T
    send_ref[...] = acc[:, pl.ds(pl.multiple_of((1 - core) * n, n), n)].T


def mid_kernel(lo, hi, n_lat, n_lab, h_got, h_core, w_hbm, m_in, s_in, p0, p1, p2, p3, z_own, meta_ref, z_in,
               z_hbm, stats_ref, occ_ref, keep_ref, send_ref, loss_ref, g_hbm,
               part_loss, m_ref, s_ref, h_ref, hsem, wbuf, wsem, zbuf, zsem, e_lab, e_blk, a_lab, a_blk, b_lab, b_blk, o_t,
               zin_buf, zin_sem, acc, lse_ref, g0, g1, gsem, head, nxt):
    second = grad_h_part(n_lab + 1, z_own, w_hbm, p0, p1, p2, p3, occ_ref, part_loss, meta_ref, keep_ref, send_ref, loss_ref, g_hbm,
                         wbuf, wsem, zin_buf, zin_sem, acc, lse_ref, g0, g1, gsem, head, nxt)
    prime_w = next(second)
    z_lattice_part(lo, hi, n_lat, n_lab, prime_w, h_got, h_core, w_hbm, m_in, s_in, p0, p1, p2, p3, meta_ref,
                   z_hbm, stats_ref, occ_ref, part_loss, m_ref, s_ref,
                   h_ref, hsem, wbuf, wsem, zbuf, zsem, e_lab, e_blk, a_lab, a_blk, b_lab, b_blk, o_t)
    for _ in second:
        pass


def grad_w_kernel(n_slots, g_hbm, z_hbm, h_own_ref, h_got, h_core, st0, st1, st2, st3, occ_ref, meta_ref, gw_hbm,
                  h_ref, hsem, zbuf, zsem, gsem, obuf, osem, ht, lse_ref, g0, g1, head, nxt):
    n_tiles, rows = z_hbm.shape[0], z_hbm.shape[1]
    frames = rows // meta_ref.shape[0]
    d_loc = ht.shape[0]
    group = zbuf.shape[1]
    n_groups = n_tiles // group
    zs = TileStream(z_hbm, zbuf, zsem, zbuf.shape[0], n_groups, lambda src, j: z_view(src, j, group))

    def g_copy(j, g, k):
        return pltpu.make_async_copy(g_hbm.at[j], g.at[0:rows, :], gsem.at[k])

    join = JoinRows(h_got, h_core, h_ref, hsem)
    join.start()
    zs.prime()
    g_copy(0, g0, 0).start()
    col_start = build_lists([meta_ref], n_tiles * TILE, head, nxt)
    d0 = pl.multiple_of(lax.axis_index("dp") * d_loc, LANES)
    ht[:, 0:rows] = h_own_ref[:, pl.ds(d0, d_loc)].T
    spread_lse([st0, st1, st2, st3], 0, meta_ref, lse_ref, 0, frames)
    join.wait()
    ht[:, rows:2 * rows] = h_ref[:, pl.ds(d0, d_loc)].T
    lane = lax.broadcasted_iota(jnp.int32, (frames, LANES), 1)
    n_units = 2 * group

    def make_g(slot, u, g):
        t, r = u // 2, u % 2
        return softmax_unit(zbuf.at[slot, t], r * rows // 2, lse_ref, g.at[rows:2 * rows, :], r * rows // 2, rows // 2, t * TILE)

    def patch(j, slot, g):
        for t in range(group):
            def z_block(seq, c0, t=t):
                return zbuf[slot, t, pl.ds(pl.multiple_of(seq * frames, frames), frames), pl.ds(c0, LANES)]

            walk_list(head, nxt, j * group + t,
                      lambda i, t=t, z_block=z_block: patch_tile(n_slots, frames, [meta_ref], col_start, j * group + t, i, z_block, lse_ref, occ_ref, g.at[rows:2 * rows, :], t * TILE, lane))

    def out_copy(j):
        slot = lax.rem(j, obuf.shape[0])
        return pltpu.make_async_copy(obuf.at[slot], w_view(gw_hbm, j, group), osem.at[slot])

    slot0 = zs.get(0)
    for u in range(n_units):
        make_g(slot0, u, g0)
    patch(0, slot0, g0)
    d_half = d_loc // 2

    def half(j, g_now, g_next, k):
        @pl.when(j >= 3)
        def _():
            out_copy(j - 3).wait()

        nj = lax.min(j + 1, n_groups - 1)

        @pl.when(j + 1 < n_groups)
        def _():
            zs.get(nj)
            g_copy(nj, g_next, 1 - k).start()

        g_copy(j, g_now, k).wait()
        slot = lax.rem(nj, zbuf.shape[0])
        oslot = lax.rem(j, obuf.shape[0])
        zero = None
        for u in range(n_units):
            t, r = u // 2, u % 2
            d_rows = slice(r * d_half, (r + 1) * d_half)
            lhs = after(ht[d_rows, :], zero)
            obuf[oslot, d_rows, t * TILE:(t + 1) * TILE] = jnp.dot(lhs, g_now[:, t * TILE:(t + 1) * TILE], preferred_element_type=F32)
            zero = make_g(slot, u, g_next)
        out_copy(j).start()
        patch(nj, slot, g_next)

    def step(i, c):
        half(2 * i, g0, g1, 0)
        half(2 * i + 1, g1, g0, 1)
        return c

    lax.fori_loop(0, n_groups // 2, step, 0)
    for j in range(n_groups - 3, n_groups):
        out_copy(j).wait()


def cost(flops, nbytes):
    return pl.CostEstimate(flops=flops, bytes_accessed=nbytes, transcendentals=0)


def solution(mesh):
    batch_axes = ("part", "dp")
    n_tp = mesh.shape["tp"]
    n_dp = mesh.shape["dp"]
    dp_swap = [(i, n_dp - 1 - i) for i in range(n_dp)]

    others = range(1, n_tp)

    def tp_xor(x, mask):
        return lax.ppermute(x, "tp", [(i, i ^ mask) for i in range(n_tp)])

    def in_hbm(x):
        return pltpu.with_memory_space_constraint(x, pltpu.HBM)

    def swap_dp(x):
        return lax.ppermute(x, "dp", dp_swap)

    def local_body(hidden, w_loc, labels, in_len, lab_len):
        batch_loc, frames, model_dim = hidden.shape
        vocab_loc = w_loc.shape[1]
        n_lab = labels.shape[1]
        n_slots = n_lab + 1
        rows = batch_loc * frames
        n_tiles = vocab_loc // TILE
        d_loc = model_dim // n_dp
        dma = pltpu.SemaphoreType.DMA
        i32 = jnp.int32
        cut_a, n_lat = 8, 16
        h_own = hidden.reshape(rows, model_dim)
        core = lax.rem(lax.axis_index("tp"), 2)
        h_half = lax.dynamic_index_in_dim(h_own.reshape(2, rows // 2, model_dim), core, 0, keepdims=False)
        h_got = swap_dp(h_half)
        flops = 2 * rows * model_dim * TILE
        wbytes = model_dim * TILE * 2
        zbytes = rows * TILE * 4
        z_type = jax.ShapeDtypeStruct((n_tiles, rows, TILE), F32)
        run_type = jax.ShapeDtypeStruct((rows, LANES), F32)
        pick_type = jax.ShapeDtypeStruct((frames + 16, LANES), F32)
        meta_type = jax.ShapeDtypeStruct((batch_loc, n_slots + 1), i32)
        g_type = jax.ShapeDtypeStruct((n_tiles // 2, rows, 2 * TILE), BF16)
        stat_type = jax.ShapeDtypeStruct((16, LANES), F32)
        g_scratch = [pltpu.VMEM((rows, 2 * TILE), BF16)] * 2

        def w_scratch(n):
            return [pltpu.VMEM((3, model_dim, n * TILE), BF16), dma((3,))]

        def z_scratch(n):
            return [pltpu.VMEM((3, n, rows, TILE), F32), dma((3,))]

        h_scratch = [pltpu.VMEM((rows, model_dim), BF16), dma((2,))]
        run_scratch = [pltpu.VMEM((rows, LANES), F32), pltpu.VMEM((rows, LANES), F32)]

        def lists(n_sets):
            return [pltpu.SMEM((n_tiles,), i32), pltpu.SMEM((n_sets * batch_loc * n_slots,), i32)]

        z_own, pick, meta = kernel_call(
            functools.partial(z_own_kernel, n_slots),
            out_shape=(z_type, pick_type, meta_type),
            in_specs=[any_spec(), any_spec(), smem_spec(), smem_spec(), smem_spec()],
            out_specs=(any_spec(), vmem_spec(), smem_spec()),
            scratch_shapes=h_scratch + w_scratch(4) + z_scratch(4) + run_scratch + lists(1),
            compiler_params=params(),
            cost_estimate=cost(n_tiles * flops, n_tiles * (wbytes + zbytes)),
        )(in_hbm(h_own), w_loc, labels, in_len, lab_len)

        h_got, pick = lax.optimization_barrier((h_got, pick))
        h_core = in_hbm(tp_xor(h_got, 1))
        h_got = in_hbm(h_got)
        picks = [pick] + [tp_xor(pick, k) for k in others]

        z_part, run_m, run_s = kernel_call(
            functools.partial(z_first_kernel, 0, cut_a),
            out_shape=(z_type, run_type, run_type),
            in_specs=[any_spec()] * 3,
            out_specs=(any_spec(), vmem_spec(), vmem_spec()),
            scratch_shapes=h_scratch + w_scratch(4) + z_scratch(4),
            compiler_params=params(),
            cost_estimate=cost(cut_a * flops, cut_a * (wbytes + zbytes)),
        )(h_got, h_core, w_loc)

        n_blk = frames // 64
        half_type = jax.ShapeDtypeStruct((rows // 2, model_dim), F32)
        loss_type = jax.ShapeDtypeStruct((8, LANES), F32)
        z_oth, stats_oth, occ, keep, send, loss, g_own = kernel_call(
            functools.partial(mid_kernel, cut_a, n_tiles, n_lat, n_lab),
            out_shape=(z_type, stat_type, run_type, half_type, half_type, loss_type, g_type),
            in_specs=[any_spec()] * 3 + [vmem_spec()] * 6 + [any_spec(), smem_spec(), any_spec()],
            out_specs=(any_spec(),) + (vmem_spec(),) * 5 + (any_spec(),),
            input_output_aliases={11: 0},
            scratch_shapes=[pltpu.VMEM((8, LANES), F32)] + run_scratch + h_scratch + w_scratch(2) + z_scratch(2) + [
                pltpu.VMEM((n_blk, n_lab, LANES), F32), pltpu.VMEM((n_blk, 8, LANES), F32),
                pltpu.VMEM((frames, n_lab, LANES), F32), pltpu.VMEM((frames, n_lab + 8, LANES), F32),
                pltpu.VMEM((frames, n_lab, LANES), F32), pltpu.VMEM((frames, n_lab + 8, LANES), F32),
                pltpu.VMEM((n_blk, LANES, LANES), F32)] + z_scratch(2) + [
                pltpu.VMEM((model_dim, rows), F32), pltpu.VMEM((rows, LANES), F32)] + g_scratch + [dma((2,))] + lists(1),
            compiler_params=params(),
            cost_estimate=cost((2 * n_tiles - cut_a) * flops, (2 * n_tiles - cut_a) * (wbytes + zbytes)),
        )(h_got, h_core, w_loc, run_m, run_s, *picks, z_own, meta, z_part)
        st_oth = [stats_oth] + [tp_xor(stats_oth, k) for k in others]
        occ_oth = swap_dp(occ)
        meta_oth = swap_dp(meta)
        recv = tp_xor(send, 1)
        chip_sum = keep + recv
        across = tp_xor(chip_sum, 2)

        grad_weight = kernel_call(
            functools.partial(grad_w_kernel, n_slots),
            out_shape=jax.ShapeDtypeStruct((d_loc, vocab_loc), F32),
            in_specs=[any_spec(), any_spec(), vmem_spec(), any_spec(), any_spec()] + [vmem_spec()] * 5 + [smem_spec()],
            out_specs=any_spec(),
            scratch_shapes=h_scratch + z_scratch(2) + [
                dma((2,)), pltpu.VMEM((3, d_loc, 2 * TILE), F32), dma((3,)),
                pltpu.VMEM((d_loc, 2 * rows), BF16), pltpu.VMEM((rows, LANES), F32),
                pltpu.VMEM((2 * rows, 2 * TILE), BF16), pltpu.VMEM((2 * rows, 2 * TILE), BF16)] + lists(1),
            compiler_params=params(),
            cost_estimate=cost(n_tiles * flops, n_tiles * (2 * zbytes + d_loc * TILE * 4)),
        )(g_own, z_oth, h_own, h_got, h_core, *st_oth, occ_oth, meta_oth)

        chip_sum, grad_weight = lax.optimization_barrier((chip_sum, grad_weight))
        full_half = chip_sum + across
        other_half = tp_xor(full_half, 1)
        grad_hidden = jnp.where(core == 0, jnp.stack([full_half, other_half]), jnp.stack([other_half, full_half])).reshape(batch_loc, frames, model_dim)
        return loss[0, :batch_loc], grad_weight, grad_hidden


    return jax.shard_map(
        local_body,
        mesh=mesh,
        in_specs=(P(batch_axes, None, None), P(None, "tp"), P(batch_axes, None), P(batch_axes), P(batch_axes)),
        out_specs=(P(batch_axes), P(batch_axes, "tp"), P(batch_axes, None, None)),
        check_vma=False,
    )
```

```python
import functools

import jax
import jax.numpy as jnp
from jax import lax
from jax.experimental import pallas as pl
from jax.experimental.pallas import tpu as pltpu
from jax.sharding import PartitionSpec as P

NEG_BIG = -1.0e30
LOG2E = 1.4426950408889634
F32 = jnp.float32
DOWN = dict(axis=0, keepdims=True)
ALONG = dict(axis=1, keepdims=True)
BF16 = jnp.bfloat16
TILE = 512
LANES = 128
HALF = LANES // 2
MIB = 1 << 20


def vmem_spec():
    return pl.BlockSpec(memory_space=pltpu.VMEM)


def smem_spec():
    return pl.BlockSpec(memory_space=pltpu.SMEM)


def any_spec():
    return pl.BlockSpec(memory_space=pl.ANY)


def kernel_call(*args, **kw):
    return pl.pallas_call(*args, **kw)


def params():
    return pltpu.CompilerParams(vmem_limit_bytes=56 * MIB)


def label_col(meta_refs, i):
    n_slots = meta_refs[0].shape[1] - 1
    seq, item = i // n_slots, lax.rem(i, n_slots)
    n_seq = meta_refs[0].shape[0]
    at = lax.max(item - 1, 0)
    col = meta_refs[0][lax.rem(seq, n_seq), at]
    for k in range(1, len(meta_refs)):
        col = jnp.where(seq >= k * n_seq, meta_refs[k][lax.rem(seq, n_seq), at], col)
    return jnp.where(item == 0, 0, col)


def build_lists(meta_refs, vocab_loc, head, nxt):
    n_items = len(meta_refs) * meta_refs[0].shape[0] * (meta_refs[0].shape[1] - 1)
    col_start = lax.axis_index("tp") * vocab_loc
    n_tiles = vocab_loc // TILE

    def clear(i, c):
        head[i] = -1
        return c

    lax.fori_loop(0, n_tiles, clear, 0)

    def insert(i, c):
        loc = label_col(meta_refs, i) - col_start
        tile = lax.max(loc, 0) // TILE

        @pl.when((loc >= 0) & (loc < vocab_loc))
        def _():
            nxt[i] = head[tile]
            head[tile] = i

        return c

    lax.fori_loop(0, n_items, insert, 0)
    return col_start


def walk_list(head, nxt, tile, visit):
    def body(i):
        visit(i)
        return nxt[i]

    lax.while_loop(lambda i: i >= 0, body, head[tile])


class TileStream:
    def __init__(self, src, buf, sem, depth, n_tiles, view):
        self.src, self.buf, self.sem, self.depth, self.n, self.view = src, buf, sem, depth, n_tiles, view

    def copy(self, j):
        slot = lax.rem(j, self.depth)
        return pltpu.make_async_copy(self.view(self.src, j), self.buf.at[slot], self.sem.at[slot])

    def prime(self):
        for j in range(min(self.depth - 1, self.n)):
            self.copy(j).start()

    def get(self, j):
        self.copy(j).wait()

        @pl.when(j + self.depth - 1 < self.n)
        def _():
            self.copy(j + self.depth - 1).start()

        return lax.rem(j, self.depth)


def w_view(src, j, n=1):
    return src.at[:, pl.ds(pl.multiple_of(j * n * TILE, TILE), n * TILE)]


def z_view(src, j, n):
    return src.at[pl.ds(j * n, n)]


def exact_zero(total):
    return jnp.minimum(total[0:16] + total[16:32], 0.0).astype(BF16)


def after(lhs, zero):
    if zero is None:
        return lhs
    corner = lhs[0:16, 0:LANES] + zero
    return jnp.concatenate([jnp.concatenate([corner, lhs[0:16, LANES:]], axis=1), lhs[16:]], axis=0)


def unit_stats(z, m_ref, s_ref, r0):
    n_chunks = z.shape[1] // LANES
    total = None
    for b in range(z.shape[0] // 32):
        zb = [z[32 * b:32 * (b + 1), k * LANES:(k + 1) * LANES] for k in range(n_chunks)]
        rows = slice(r0 + 32 * b, r0 + 32 * (b + 1))
        m_old = m_ref[rows, :]
        m_new = functools.reduce(jnp.maximum, zb, m_old)
        s_new = s_ref[rows, :] * jnp.exp(m_old - m_new)
        for part in zb:
            s_new = s_new + jnp.exp(part - m_new)
        m_ref[rows, :] = m_new
        s_ref[rows, :] = s_new
        total = s_new if total is None else total + s_new
    return exact_zero(total)


def z_group(h_ref, w, z_out, m_ref, s_ref):
    n_tiles = z_out.shape[0]
    n = h_ref.shape[0] // 2
    zeros = []
    for t in range(n_tiles):
        for r in range(2):
            rows = slice(r * n, (r + 1) * n)
            lhs = after(h_ref[rows, :], zeros[-2] if len(zeros) >= 2 else None)
            z = jnp.dot(lhs, w[:, t * TILE:(t + 1) * TILE], preferred_element_type=F32)
            z_out[t, rows, :] = z
            zeros.append(unit_stats(z, m_ref, s_ref, r * n))


def emit_stats(m_ref, s_ref, out_ref, base):
    row_m = jnp.max(m_ref[...], **ALONG)
    row_s = jnp.sum(s_ref[...] * jnp.exp(m_ref[...] - row_m), **ALONG)
    rows = m_ref.shape[0]
    for k, v in enumerate((row_m, row_s)):
        flat = jnp.broadcast_to(v, (rows, LANES)).T
        for p in range(rows // LANES):
            at = base + 8 * k + p
            out_ref[at:at + 1, :] = flat[0:1, p * LANES:(p + 1) * LANES]


def z_own_kernel(n_slots, h_hbm, w_hbm, labels_ref, in_len_ref, lab_len_ref, z_hbm, pick_ref, meta_ref, h_ref, hsem, wbuf, wsem, zbuf, zsem, m_ref, s_ref, blank, head, nxt):
    n_tiles = z_hbm.shape[0]
    rows = h_ref.shape[0]
    n_seq = meta_ref.shape[0]
    frames = rows // n_seq
    h_copy = pltpu.make_async_copy(h_hbm, h_ref, hsem.at[0])
    h_copy.start()
    n_lab = n_slots - 1
    for q in range(n_seq):
        def put(k, c, q=q):
            meta_ref[q, k] = labels_ref[q, k]
            return c

        lax.fori_loop(0, n_lab, put, 0)
        meta_ref[q, n_lab] = in_len_ref[q]
        meta_ref[q, n_lab + 1] = lab_len_ref[q]
    group = zbuf.shape[1]
    stream = TileStream(w_hbm, wbuf, wsem, wbuf.shape[0], n_tiles // group, lambda src, j: w_view(src, j, group))
    stream.prime()
    col_start = build_lists([meta_ref], n_tiles * TILE, head, nxt)
    m_ref[...] = jnp.full(m_ref.shape, NEG_BIG, F32)
    s_ref[...] = jnp.zeros(s_ref.shape, F32)
    pick_ref[...] = jnp.zeros(pick_ref.shape, F32)
    blank[...] = jnp.zeros(blank.shape, F32)
    half = frames // 2
    h_copy.wait()
    lane = lax.broadcasted_iota(jnp.int32, (half, LANES), 1)

    def out_copy(j):
        slot = lax.rem(j, zbuf.shape[0])
        return pltpu.make_async_copy(zbuf.at[slot], z_view(z_hbm, j, group), zsem.at[slot])

    def step(j, c):
        slot = stream.get(j)

        @pl.when(j >= 3)
        def _():
            out_copy(j - 3).wait()

        zslot = lax.rem(j, zbuf.shape[0])
        z_group(h_ref, wbuf.at[slot], zbuf.at[zslot], m_ref, s_ref)
        out_copy(j).start()

        for t in range(group):
            def visit(i, t=t):
                seq, item = i // n_slots, lax.rem(i, n_slots)
                off = label_col([meta_ref], i) - col_start - (j * group + t) * TILE
                blk = off // LANES
                r0 = pl.multiple_of(seq * frames, frames)
                src = off - blk * LANES
                c0 = pl.multiple_of(blk * LANES, LANES)

                def moved(p, at):
                    zb = zbuf[zslot, t, pl.ds(r0 + p * half, half), pl.ds(c0, LANES)]
                    return pltpu.roll(zb, lax.rem(at - src + LANES, LANES), 1)

                @pl.when(item > 0)
                def _():
                    for p in range(2):
                        at = item - 1 + n_lab * seq + HALF * p
                        pick_ref[0:half, :] = jnp.where(lane == at, moved(p, at), pick_ref[0:half, :])

                @pl.when(item == 0)
                def _():
                    for p in range(2):
                        at = 2 * seq + p
                        blank[...] = jnp.where(lane == at, moved(p, at), blank[...])

            walk_list(head, nxt, j * group + t, visit)
        return c

    n_groups = n_tiles // group
    lax.fori_loop(0, n_groups, step, 0)
    emit_stats(m_ref, s_ref, pick_ref, half)
    pick_ref[half + 16:half + 24, :] = blank[...].T[0:8]
    for j in range(n_groups - 3, n_groups):
        out_copy(j).wait()


def z_oth_loop(lo, hi, join, h_ref, w_hbm, z_hbm, wbuf, wsem, zbuf, zsem, m_ref, s_ref, sections):
    group = zbuf.shape[1]
    lo, n_groups = lo // group, (hi - lo) // group
    stream = TileStream(w_hbm, wbuf, wsem, wbuf.shape[0], n_groups, lambda src, j: w_view(src, lo + j, group))
    stream.prime()

    def out_copy(j):
        slot = lax.rem(j, zbuf.shape[0])
        return pltpu.make_async_copy(zbuf.at[slot], z_view(z_hbm, lo + j, group), zsem.at[slot])

    base = 0
    join.wait()
    for n, side, make_carry in sections:
        carry = make_carry()

        def step(k, c, base=base, side=side):
            j = base + k
            slot = stream.get(j)

            @pl.when(j >= 3)
            def _():
                out_copy(j - 3).wait()

            z_group(h_ref, wbuf.at[slot], zbuf.at[lax.rem(j, zbuf.shape[0])], m_ref, s_ref)
            c = side(k, c)
            out_copy(j).start()
            return c

        last = lax.fori_loop(0, n, step, carry)
        yield last
        base += n
    for j in range(max(n_groups - 3, 0), n_groups):
        out_copy(j).wait()


class JoinRows:
    def __init__(self, h_got, h_core, h_ref, hsem):
        n = h_got.shape[0]
        core = lax.rem(lax.axis_index("tp"), 2)
        self.copies = [pltpu.make_async_copy(src, h_ref.at[pl.ds(pl.multiple_of(at * n, n), n), :], hsem.at[k])
                       for k, (src, at) in enumerate(((h_got, core), (h_core, 1 - core)))]

    def start(self):
        for c in self.copies:
            c.start()

    def wait(self):
        for c in self.copies:
            c.wait()


def z_lattice_part(lo, hi, n_lat, per_group, n_lab, before_tail, h_got, h_core, w_hbm, p0, p1, p2, p3, meta_ref,
                     z_hbm, stats_ref, occ_ref, loss_ref, m_ref, s_ref,
                     h_ref, hsem, wbuf, wsem, zbuf, zsem, e_lab, e_blk, a_lab, a_blk, b_lab, b_blk, o_t):
    join = JoinRows(h_got, h_core, h_ref, hsem)
    join.start()
    n_blk = e_lab.shape[0]
    frames = n_blk * HALF
    m_ref[...] = jnp.full(m_ref.shape, NEG_BIG, F32)
    s_ref[...] = jnp.zeros(s_ref.shape, F32)
    lane128 = lax.broadcasted_iota(jnp.int32, (LANES, LANES), 1)
    row32 = lax.broadcasted_iota(jnp.int32, (n_lab, LANES), 0)
    row8 = lax.broadcasted_iota(jnp.int32, (8, LANES), 0)
    lane32 = lax.broadcasted_iota(jnp.int32, (n_lab, LANES), 1)
    lane8 = lax.broadcasted_iota(jnp.int32, (8, LANES), 1)
    n_seq = meta_ref.shape[0]
    labs = jnp.zeros((n_lab, LANES), jnp.int32)
    lab_row = jnp.zeros((8, LANES), jnp.int32)
    live8 = jnp.zeros((8, LANES), jnp.int32)
    used8 = jnp.zeros((8, LANES), jnp.int32)
    for s in range(n_seq):
        for k in range(n_lab):
            labs = jnp.where((row32 == k) & (lane32 == s), meta_ref[s, k], labs)
            lab_row = jnp.where((row8 == s) & (lane8 == k), meta_ref[s, k], lab_row)
        live8 = jnp.where(lane8 == s, meta_ref[s, n_lab], live8)
        used8 = jnp.where(lane8 == s, meta_ref[s, n_lab + 1], used8)
    live32 = jnp.broadcast_to(live8[0:1], (n_lab, LANES))
    used32 = jnp.broadcast_to(used8[0:1], (n_lab, LANES))
    skip_dn = labs != pltpu.roll(labs, 1, 0)
    skip_up = labs != pltpu.roll(labs, n_lab - 1, 0)
    end_lab = row32 == used32 - 1
    end_blk = row32 == used32
    end_top = (row8 == 0) & (used8 == n_lab)
    shift0 = jnp.zeros((1, LANES), F32)
    seq1 = lane8[0:1] >= HALF
    half_len = jnp.where(seq1, meta_ref[1, n_lab], meta_ref[0, n_lab])
    half = frames // 2
    packed = functools.reduce(jnp.add, [p[0:half, :] for p in (p0, p1, p2, p3)])
    blanks = functools.reduce(jnp.add, [p[half + 16:half + 24, :] for p in (p0, p1, p2, p3)])
    for j in range(n_blk):
        far, near = j // 2, HALF * (j % 2)
        part = packed[near:near + HALF]
        x = jnp.concatenate([pltpu.roll(part, (LANES - HALF * far - n_lab * q) % LANES, 1) for q in range(2)], axis=0).T[0:n_lab]
        rows_b = [pltpu.roll(blanks, (HALF * q - near) % LANES, 1)[2 * q + far:2 * q + far + 1] for q in range(2)]
        x_blank = jnp.where(seq1, rows_b[1], rows_b[0])
        top = jnp.maximum(jnp.max(x, **DOWN), x_blank)
        e_blk[j] = jnp.broadcast_to((x_blank - top) * LOG2E, (8, LANES))
        e_lab[j] = (x - top) * LOG2E
        shift0 = shift0 + jnp.where(lax.rem(lane8[0:1], HALF) + HALF * j < half_len, top, 0.0)
    shift_seq0 = jnp.sum(jnp.where(seq1, 0.0, shift0), **ALONG)
    shift_seq1 = jnp.sum(jnp.where(seq1, shift0, 0.0), **ALONG)

    def lse2(a, b):
        hi_v = jnp.maximum(a, b)
        return hi_v + jnp.log2(1.0 + jnp.exp2(jnp.minimum(a, b) - hi_v))

    def lse3(a, b, c):
        hi_v = jnp.maximum(a, b)
        lo_v = jnp.minimum(a, b)
        top = jnp.maximum(hi_v, c)
        mid = jnp.minimum(hi_v, c)
        return top + jnp.log2(1.0 + (jnp.exp2(lo_v - top) + jnp.exp2(mid - top)))

    pick32 = jnp.where(lane32 == 1, HALF, 0)
    pick8 = jnp.where(lane8 == 1, HALF, 0)

    def lanes_of(x, idx):
        return jnp.take_along_axis(x, idx, axis=1, mode="promise_in_bounds")

    def emission(j, u):
        return lanes_of(e_lab[j], pick32 + u), lanes_of(e_blk[j], pick8 + u)

    neg32 = jnp.full((n_lab, LANES), NEG_BIG, F32)
    neg8 = jnp.full((8, LANES), NEG_BIG, F32)
    start32 = jnp.where(row32 == 0, 0.0, NEG_BIG)
    fin_b = jnp.where(end_blk, 0.0, NEG_BIG)
    fin_t = jnp.where(end_top, 0.0, NEG_BIG)
    skip_dn = skip_dn & (row32 > 0)
    skip_up = skip_up & (row32 < n_lab - 1)

    def lat_step(i, j, u, carry):
        al, ab, at, bl, bb, bt = carry
        el, eb = emission(j, u)
        eb32 = jnp.broadcast_to(eb[0:1], (n_lab, LANES))
        rolled = pltpu.roll(al, 1, 0)
        prev = jnp.where(row32 == 0, NEG_BIG, rolled)
        prev_t = jnp.where(row8 == 0, rolled[0:8], NEG_BIG)
        nl = lse3(al, ab, jnp.where(skip_dn, rolled, NEG_BIG))
        nb = lse2(ab, prev)
        nt = lse2(at, prev_t)
        a_lab[i] = nl
        a_blk[i, 0:n_lab] = nb
        a_blk[i, n_lab:n_lab + 8] = nt
        al = jnp.where(i < live32, el + nl, al)
        ab = jnp.where(i < live32, eb32 + nb, ab)
        at = jnp.where(i < live8, eb + nt, at)
        t = frames - 1 - i
        fl, fb = emission(n_blk - 1 - j, 63 - u)
        fb32 = jnp.broadcast_to(fb[0:1], (n_lab, LANES))
        last = row32 == n_lab - 1
        up_l = jnp.where(skip_up, pltpu.roll(bl, n_lab - 1, 0), NEG_BIG)
        up_b = jnp.where(last, jnp.broadcast_to(bt[0:1], (n_lab, LANES)), pltpu.roll(bb, n_lab - 1, 0))
        ml = fl + lse3(bl, up_b, up_l)
        mb = fb32 + lse2(bb, bl)
        mt = fb + bt
        bl = jnp.where(t < live32, ml, bl)
        bb = jnp.where(t < live32, mb, bb)
        bt = jnp.where(t < live8, mt, bt)
        b_lab[t + pad] = bl
        b_blk[t + pad, 0:n_lab] = bb
        b_blk[t + pad, n_lab:n_lab + 8] = bt
        return al, ab, at, bl, bb, bt

    group = zbuf.shape[1]
    n_lat_groups = n_lat // group
    pad = b_lab.shape[0] - frames

    def lattice_side(k, carry):
        for u in range(per_group):
            i = k * per_group + u
            j = lax.min(lax.div(i, HALF), n_blk - 1)
            carry = lat_step(i, j, lax.rem(i, HALF), carry)
        return carry

    n_occ = (hi - lo - n_lat) // group
    occ_group = frames // n_occ // HALF
    back32 = jnp.where(lane32 >= HALF, 1, 0)
    back8 = jnp.where(lane8 >= HALF, 1, 0)
    run = z_oth_loop(lo, hi, join, h_ref, w_hbm, z_hbm, wbuf, wsem, zbuf, zsem, m_ref, s_ref,
                     [(n_lat_groups, lattice_side, lambda: (neg32, start32, neg8, neg32, fin_b, fin_t)),
                      (n_occ, lambda k, c: occ_side(k, c), lambda: 0)])
    al, ab, at, _, _, _ = next(run)

    lasts = [jnp.where(end, v, NEG_BIG) for end, v in ((end_lab, al), (end_blk, ab), (end_top, at))]
    top = functools.reduce(jnp.maximum, [jnp.max(v, **DOWN) for v in lasts])
    total = functools.reduce(jnp.add, [jnp.sum(jnp.exp2(v - top), **DOWN) for v in lasts])
    loss = -(top + jnp.log2(total))
    loss32 = jnp.broadcast_to(loss, (n_lab, LANES))
    loss8 = jnp.broadcast_to(loss, (8, LANES))
    lane1 = lane8[0:1]
    loss_ref[...] = jnp.broadcast_to(loss * (1.0 / LOG2E) - jnp.where(lane1 == 0, shift_seq0, jnp.where(lane1 == 1, shift_seq1, 0.0)), (8, LANES))

    def occ_frame(i, u, acc_l, acc_b):
        occ_l = jnp.where(i < live32, jnp.exp2(a_lab[i] + b_lab[i + pad] + loss32), 0.0)
        occ_b = jnp.exp2(a_blk[i, 0:n_lab] + b_blk[i + pad, 0:n_lab] + loss32)
        occ_u = jnp.exp2(a_blk[i, n_lab:n_lab + 8] + b_blk[i + pad, n_lab:n_lab + 8] + loss8)
        blank = jnp.sum(occ_b, **DOWN) + occ_u[0:1]
        blank = jnp.where(i < live8, jnp.broadcast_to(blank, (8, LANES)), 0.0)
        acc_l = jnp.where(lax.rem(lane32, HALF) == u, lanes_of(occ_l, back32), acc_l)
        acc_b = jnp.where(lax.rem(lane8, HALF) == u, lanes_of(blank, back8), acc_b)
        return acc_l, acc_b

    def occ_side(k, c):
        for g in range(occ_group):
            j = k * occ_group + g
            acc_l = jnp.zeros((n_lab, LANES), F32)
            acc_b = jnp.zeros((8, LANES), F32)
            for u in range(HALF):
                acc_l, acc_b = occ_frame(j * HALF + u, u, acc_l, acc_b)
            o_t[j, 0:n_lab] = acc_l
            o_t[j, n_lab:n_lab + 8] = acc_b
            o_t[j, 8 + n_lab:LANES] = jnp.zeros((LANES - 8 - n_lab, LANES), F32)
        return c

    next(run)
    before_tail()
    for _ in run:
        pass
    emit_stats(m_ref, s_ref, stats_ref, 0)
    row128 = lax.broadcasted_iota(jnp.int32, (LANES, LANES), 0)
    same = []
    for s in range(n_seq):
        down = jnp.full((n_lab, LANES), -1, jnp.int32)
        for k in range(n_lab):
            down = jnp.where(row32 == k, meta_ref[s, k], down)
        down = jnp.concatenate([down, jnp.full((LANES - n_lab, LANES), -1, jnp.int32)], axis=0)
        across = pltpu.roll(jnp.broadcast_to(lab_row[s:s + 1], (LANES, LANES)), HALF * s, 1)
        own = lane128 - HALF * s
        inner = (row128 < n_lab) & (own >= 0) & (own < n_lab)
        same.append(jnp.where((inner & (down == across)) | ((row128 == own) & (own < HALF)), 1.0, 0.0))
    for j in range(n_blk):
        y = o_t[j].T
        occ_ref[HALF * j:HALF * (j + 1), :] = functools.reduce(jnp.add, [
            jnp.dot(y[HALF * q:HALF * (q + 1), :], same[q], precision=lax.Precision.HIGHEST, preferred_element_type=F32) for q in range(n_seq)])


def spread_lse(refs, base, meta_ref, lse_ref, r0, frames):
    m = functools.reduce(jnp.maximum, [r[base:base + 8, :] for r in refs])
    tot = functools.reduce(jnp.add, [r[base + 8:base + 16, :] * jnp.exp(r[base:base + 8, :] - m) for r in refs])
    lse = m + jnp.log(tot)
    t = lax.broadcasted_iota(jnp.int32, (LANES, LANES), 0)
    n_part = frames // LANES
    sums = []
    for q in range(meta_ref.shape[0]):
        live_sum = jnp.zeros((1, LANES), F32)
        for p in range(n_part):
            at = q * n_part + p
            part = jnp.broadcast_to(lse[at:at + 1, :], (LANES, LANES)).T
            live = t + p * LANES < meta_ref[q, meta_ref.shape[1] - 2]
            lse_ref[r0 + at * LANES:r0 + (at + 1) * LANES, :] = jnp.where(live, part, 1.0e30)
            live_sum = live_sum + jnp.sum(jnp.where(live, part, 0.0), **DOWN)
        sums.append(live_sum)
    return sums


def patch_tile(n_slots, frames, meta_refs, col_start, j, i, z_block, lse_ref, occ_ref, g_ref, g_col, lane):
    seq, item = i // n_slots, lax.rem(i, n_slots)
    off = label_col(meta_refs, i) - col_start - j * TILE
    blk = off // LANES
    r0 = pl.multiple_of(seq * frames, frames)
    c0 = pl.multiple_of(blk * LANES, LANES)
    zb = z_block(seq, c0)
    slot_lane = jnp.where(item == 0, n_slots - 1, item - 1) + HALF * seq
    occ = jnp.sum(jnp.where(lane == slot_lane, occ_ref[...], 0.0), **ALONG)
    fresh = jnp.exp(zb - lse_ref[pl.ds(r0, frames), :]) - occ
    gc = pl.multiple_of(g_col + c0, LANES)
    old = g_ref[pl.ds(r0, frames), pl.ds(gc, LANES)].astype(F32)
    g_ref[pl.ds(r0, frames), pl.ds(gc, LANES)] = jnp.where(lane == off - blk * LANES, fresh, old).astype(BF16)


def softmax_unit(z, z_row, lse_ref, out, r0, n, c0):
    total = None
    for b in range(n // 32):
        lse = lse_ref[r0 + 32 * b:r0 + 32 * (b + 1), :]
        for k in range(TILE // LANES):
            e = jnp.exp(z[z_row + 32 * b:z_row + 32 * (b + 1), k * LANES:(k + 1) * LANES] - lse)
            out[r0 + 32 * b:r0 + 32 * (b + 1), c0 + k * LANES:c0 + (k + 1) * LANES] = e.astype(BF16)
            total = e if total is None else total + e
    return exact_zero(total)


def grad_h_part(n_slots, z_hbm, w_hbm, st0, st1, st2, st3, occ_ref, part_loss, meta_ref, keep_ref, send_ref, loss_ref, g_hbm,
                  wbuf, wsem, zbuf, zsem, acc, lse_ref, g0, g1, gsem, head, nxt):
    n_tiles, rows = z_hbm.shape[0], z_hbm.shape[1]
    frames = rows // meta_ref.shape[0]
    meta_refs = [meta_ref]
    group = zbuf.shape[1]
    n_groups = n_tiles // group
    stream = TileStream(w_hbm, wbuf, wsem, wbuf.shape[0], n_groups, lambda src, j: w_view(src, j, group))
    zs = TileStream(z_hbm, zbuf, zsem, zbuf.shape[0], n_groups, lambda src, j: z_view(src, j, group))
    zs.prime()
    yield stream.prime
    col_start = build_lists(meta_refs, n_tiles * TILE, head, nxt)
    sums = spread_lse([st0, st1, st2, st3], frames // 2, meta_ref, lse_ref, 0, frames)
    lane1 = lax.broadcasted_iota(jnp.int32, (8, LANES), 1)
    loss_ref[...] = part_loss[...] + jnp.where(lane1 == 0, sums[0], sums[1])
    lane = lax.broadcasted_iota(jnp.int32, (frames, LANES), 1)

    def patch(j, slot, g):
        for t in range(group):
            def z_block(seq, c0, t=t):
                return zbuf[slot, t, pl.ds(pl.multiple_of(seq * frames, frames), frames), pl.ds(c0, LANES)]

            walk_list(head, nxt, j * group + t,
                      lambda i, t=t, z_block=z_block: patch_tile(n_slots, frames, meta_refs, col_start, j * group + t, i, z_block, lse_ref, occ_ref, g, t * TILE, lane))

    def make_g(slot, u, g):
        t, r = u // 2, u % 2
        return softmax_unit(zbuf.at[slot, t], r * rows // 2, lse_ref, g, r * rows // 2, rows // 2, t * TILE)

    acc[...] = jnp.zeros(acc.shape, F32)
    slot0 = zs.get(0)
    for u in range(2 * group):
        make_g(slot0, u, g0)
    patch(0, slot0, g0)
    n_units = acc.shape[0] // 256

    def g_copy(j, g, k):
        return pltpu.make_async_copy(g, g_hbm.at[j], gsem.at[k])

    def half(j, g_now, g_next, k):
        slot = stream.get(j)
        nj = lax.min(j + 1, n_groups - 1)

        @pl.when(j + 1 < n_groups)
        def _():
            zs.get(nj)

        @pl.when(j >= 1)
        def _():
            g_copy(j - 1, g_next, 1 - k).wait()

        g_copy(j, g_now, k).start()

        zslot = lax.rem(nj, zbuf.shape[0])
        zero = None
        for u in range(n_units):
            d_rows = slice(u * 256, (u + 1) * 256)
            lhs = after(wbuf[slot, d_rows, :], zero)
            acc[d_rows, :] += lax.dot_general(lhs, g_now[...], (((1,), (1,)), ((), ())), preferred_element_type=F32)
            if u < 2 * group:
                zero = make_g(zslot, u, g_next)
        patch(nj, zslot, g_next)

    def step(i, c):
        half(2 * i, g0, g1, 0)
        half(2 * i + 1, g1, g0, 1)
        return c

    lax.fori_loop(0, n_groups // 2, step, 0)
    g_copy(n_groups - 1, g1, 1).wait()
    core = lax.rem(lax.axis_index("tp"), 2)
    n = rows // 2
    keep_ref[...] = acc[:, pl.ds(pl.multiple_of(core * n, n), n)].T
    send_ref[...] = acc[:, pl.ds(pl.multiple_of((1 - core) * n, n), n)].T


def mid_kernel(lo, hi, n_lat, per_group, n_lab, h_got, h_core, w_hbm, p0, p1, p2, p3, z_own, meta_ref,
               z_hbm, stats_ref, occ_ref, keep_ref, send_ref, loss_ref, g_hbm,
               part_loss, m_ref, s_ref, h_ref, hsem, wbuf, wsem, zbuf, zsem, e_lab, e_blk, a_lab, a_blk, b_lab, b_blk, o_t,
               zin_buf, zin_sem, acc, lse_ref, g0, g1, gsem, head, nxt):
    second = grad_h_part(n_lab + 1, z_own, w_hbm, p0, p1, p2, p3, occ_ref, part_loss, meta_ref, keep_ref, send_ref, loss_ref, g_hbm,
                         wbuf, wsem, zin_buf, zin_sem, acc, lse_ref, g0, g1, gsem, head, nxt)
    prime_w = next(second)
    z_lattice_part(lo, hi, n_lat, per_group, n_lab, prime_w, h_got, h_core, w_hbm, p0, p1, p2, p3, meta_ref,
                   z_hbm, stats_ref, occ_ref, part_loss, m_ref, s_ref,
                   h_ref, hsem, wbuf, wsem, zbuf, zsem, e_lab, e_blk, a_lab, a_blk, b_lab, b_blk, o_t)
    for _ in second:
        pass


def grad_w_kernel(n_slots, g_hbm, z_hbm, h_own_ref, h_got, h_core, st0, st1, st2, st3, occ_ref, meta_ref, gw_hbm,
                  h_ref, hsem, zbuf, zsem, gsem, obuf, osem, ht, lse_ref, g0, g1, head, nxt):
    n_tiles, rows = z_hbm.shape[0], z_hbm.shape[1]
    frames = rows // meta_ref.shape[0]
    d_loc = ht.shape[0]
    group = zbuf.shape[1]
    n_groups = n_tiles // group
    zs = TileStream(z_hbm, zbuf, zsem, zbuf.shape[0], n_groups, lambda src, j: z_view(src, j, group))

    def g_copy(j, g, k):
        return pltpu.make_async_copy(g_hbm.at[j], g.at[0:rows, :], gsem.at[k])

    join = JoinRows(h_got, h_core, h_ref, hsem)
    join.start()
    zs.prime()
    g_copy(0, g0, 0).start()
    col_start = build_lists([meta_ref], n_tiles * TILE, head, nxt)
    d0 = pl.multiple_of(lax.axis_index("dp") * d_loc, LANES)
    ht[:, 0:rows] = h_own_ref[:, pl.ds(d0, d_loc)].T
    spread_lse([st0, st1, st2, st3], 0, meta_ref, lse_ref, 0, frames)
    join.wait()
    ht[:, rows:2 * rows] = h_ref[:, pl.ds(d0, d_loc)].T
    lane = lax.broadcasted_iota(jnp.int32, (frames, LANES), 1)
    n_units = 2 * group

    def make_g(slot, u, g):
        t, r = u // 2, u % 2
        return softmax_unit(zbuf.at[slot, t], r * rows // 2, lse_ref, g.at[rows:2 * rows, :], r * rows // 2, rows // 2, t * TILE)

    def patch(j, slot, g):
        for t in range(group):
            def z_block(seq, c0, t=t):
                return zbuf[slot, t, pl.ds(pl.multiple_of(seq * frames, frames), frames), pl.ds(c0, LANES)]

            walk_list(head, nxt, j * group + t,
                      lambda i, t=t, z_block=z_block: patch_tile(n_slots, frames, [meta_ref], col_start, j * group + t, i, z_block, lse_ref, occ_ref, g.at[rows:2 * rows, :], t * TILE, lane))

    def out_copy(j):
        slot = lax.rem(j, obuf.shape[0])
        return pltpu.make_async_copy(obuf.at[slot], w_view(gw_hbm, j, group), osem.at[slot])

    slot0 = zs.get(0)
    for u in range(n_units):
        make_g(slot0, u, g0)
    patch(0, slot0, g0)
    d_half = d_loc // 2

    def half(j, g_now, g_next, k):
        @pl.when(j >= 3)
        def _():
            out_copy(j - 3).wait()

        nj = lax.min(j + 1, n_groups - 1)

        @pl.when(j + 1 < n_groups)
        def _():
            zs.get(nj)
            g_copy(nj, g_next, 1 - k).start()

        g_copy(j, g_now, k).wait()
        slot = lax.rem(nj, zbuf.shape[0])
        oslot = lax.rem(j, obuf.shape[0])
        zero = None
        for u in range(n_units):
            t, r = u // 2, u % 2
            d_rows = slice(r * d_half, (r + 1) * d_half)
            lhs = after(ht[d_rows, :], zero)
            obuf[oslot, d_rows, t * TILE:(t + 1) * TILE] = jnp.dot(lhs, g_now[:, t * TILE:(t + 1) * TILE], preferred_element_type=F32)
            zero = make_g(slot, u, g_next)
        out_copy(j).start()
        patch(nj, slot, g_next)

    def step(i, c):
        half(2 * i, g0, g1, 0)
        half(2 * i + 1, g1, g0, 1)
        return c

    lax.fori_loop(0, n_groups // 2, step, 0)
    for j in range(n_groups - 3, n_groups):
        out_copy(j).wait()


def cost(flops, nbytes):
    return pl.CostEstimate(flops=flops, bytes_accessed=nbytes, transcendentals=0)


def solution(mesh):
    batch_axes = ("part", "dp")
    n_tp = mesh.shape["tp"]
    n_dp = mesh.shape["dp"]
    dp_swap = [(i, n_dp - 1 - i) for i in range(n_dp)]

    others = range(1, n_tp)

    def tp_xor(x, mask):
        return lax.ppermute(x, "tp", [(i, i ^ mask) for i in range(n_tp)])

    def in_hbm(x):
        return pltpu.with_memory_space_constraint(x, pltpu.HBM)

    def swap_dp(x):
        return lax.ppermute(x, "dp", dp_swap)

    def local_body(hidden, w_loc, labels, in_len, lab_len):
        batch_loc, frames, model_dim = hidden.shape
        vocab_loc = w_loc.shape[1]
        n_lab = labels.shape[1]
        n_slots = n_lab + 1
        rows = batch_loc * frames
        n_tiles = vocab_loc // TILE
        d_loc = model_dim // n_dp
        dma = pltpu.SemaphoreType.DMA
        i32 = jnp.int32
        n_lat, lat_steps, lat_pad = 24, 22, 8
        h_own = hidden.reshape(rows, model_dim)
        core = lax.rem(lax.axis_index("tp"), 2)
        h_half = lax.dynamic_index_in_dim(h_own.reshape(2, rows // 2, model_dim), core, 0, keepdims=False)
        h_got = swap_dp(h_half)
        flops = 2 * rows * model_dim * TILE
        wbytes = model_dim * TILE * 2
        zbytes = rows * TILE * 4
        z_type = jax.ShapeDtypeStruct((n_tiles, rows, TILE), F32)
        pick_type = jax.ShapeDtypeStruct((frames // 2 + 24, LANES), F32)
        meta_type = jax.ShapeDtypeStruct((batch_loc, n_slots + 1), i32)
        g_type = jax.ShapeDtypeStruct((n_tiles // 2, rows, 2 * TILE), BF16)
        stat_type = jax.ShapeDtypeStruct((16, LANES), F32)
        g_scratch = [pltpu.VMEM((rows, 2 * TILE), BF16)] * 2

        def w_scratch(n):
            return [pltpu.VMEM((3, model_dim, n * TILE), BF16), dma((3,))]

        def z_scratch(n):
            return [pltpu.VMEM((3, n, rows, TILE), F32), dma((3,))]

        h_scratch = [pltpu.VMEM((rows, model_dim), BF16), dma((2,))]
        run_scratch = [pltpu.VMEM((rows, LANES), F32), pltpu.VMEM((rows, LANES), F32)]

        def lists(n_sets):
            return [pltpu.SMEM((n_tiles,), i32), pltpu.SMEM((n_sets * batch_loc * n_slots,), i32)]

        z_own, pick, meta = kernel_call(
            functools.partial(z_own_kernel, n_slots),
            out_shape=(z_type, pick_type, meta_type),
            in_specs=[any_spec(), any_spec(), smem_spec(), smem_spec(), smem_spec()],
            out_specs=(any_spec(), vmem_spec(), smem_spec()),
            scratch_shapes=h_scratch + w_scratch(4) + z_scratch(4) + run_scratch + [pltpu.VMEM((frames // 2, LANES), F32)] + lists(1),
            compiler_params=params(),
            cost_estimate=cost(n_tiles * flops, n_tiles * (wbytes + zbytes)),
        )(in_hbm(h_own), w_loc, labels, in_len, lab_len)

        h_got, pick = lax.optimization_barrier((h_got, pick))
        h_core = in_hbm(tp_xor(h_got, 1))
        h_got = in_hbm(h_got)
        picks = [pick] + [tp_xor(pick, k) for k in others]

        n_blk = frames // HALF
        half_type = jax.ShapeDtypeStruct((rows // 2, model_dim), F32)
        occ_type = jax.ShapeDtypeStruct((frames, LANES), F32)
        loss_type = jax.ShapeDtypeStruct((8, LANES), F32)
        z_oth, stats_oth, occ, keep, send, loss, g_own = kernel_call(
            functools.partial(mid_kernel, 0, n_tiles, n_lat, lat_steps, n_lab),
            out_shape=(z_type, stat_type, occ_type, half_type, half_type, loss_type, g_type),
            in_specs=[any_spec()] * 3 + [vmem_spec()] * 4 + [any_spec(), smem_spec()],
            out_specs=(any_spec(),) + (vmem_spec(),) * 5 + (any_spec(),),
            scratch_shapes=[pltpu.VMEM((8, LANES), F32)] + run_scratch + h_scratch + w_scratch(2) + z_scratch(2) + [
                pltpu.VMEM((n_blk, n_lab, LANES), F32), pltpu.VMEM((n_blk, 8, LANES), F32),
                pltpu.VMEM((frames + lat_pad, n_lab, LANES), F32), pltpu.VMEM((frames + lat_pad, n_lab + 8, LANES), F32),
                pltpu.VMEM((frames + lat_pad, n_lab, LANES), F32), pltpu.VMEM((frames + lat_pad, n_lab + 8, LANES), F32),
                pltpu.VMEM((n_blk, LANES, LANES), F32)] + z_scratch(2) + [
                pltpu.VMEM((model_dim, rows), F32), pltpu.VMEM((rows, LANES), F32)] + g_scratch + [dma((2,))] + lists(1),
            compiler_params=params(),
            cost_estimate=cost((2 * n_tiles) * flops, (2 * n_tiles) * (wbytes + zbytes)),
        )(h_got, h_core, w_loc, *picks, z_own, meta)
        st_oth = [stats_oth] + [tp_xor(stats_oth, k) for k in others]
        occ_oth = swap_dp(occ)
        meta_oth = swap_dp(meta)
        recv = tp_xor(send, 1)
        chip_sum = keep + recv
        across = tp_xor(chip_sum, 2)

        grad_weight = kernel_call(
            functools.partial(grad_w_kernel, n_slots),
            out_shape=jax.ShapeDtypeStruct((d_loc, vocab_loc), F32),
            in_specs=[any_spec(), any_spec(), vmem_spec(), any_spec(), any_spec()] + [vmem_spec()] * 5 + [smem_spec()],
            out_specs=any_spec(),
            scratch_shapes=h_scratch + z_scratch(2) + [
                dma((2,)), pltpu.VMEM((3, d_loc, 2 * TILE), F32), dma((3,)),
                pltpu.VMEM((d_loc, 2 * rows), BF16), pltpu.VMEM((rows, LANES), F32),
                pltpu.VMEM((2 * rows, 2 * TILE), BF16), pltpu.VMEM((2 * rows, 2 * TILE), BF16)] + lists(1),
            compiler_params=params(),
            cost_estimate=cost(n_tiles * flops, n_tiles * (2 * zbytes + d_loc * TILE * 4)),
        )(g_own, z_oth, h_own, h_got, h_core, *st_oth, occ_oth, meta_oth)

        chip_sum, grad_weight = lax.optimization_barrier((chip_sum, grad_weight))
        full_half = chip_sum + across
        other_half = tp_xor(full_half, 1)
        grad_hidden = jnp.where(core == 0, jnp.stack([full_half, other_half]), jnp.stack([other_half, full_half])).reshape(batch_loc, frames, model_dim)
        return loss[0, :batch_loc], grad_weight, grad_hidden


    return jax.shard_map(
        local_body,
        mesh=mesh,
        in_specs=(P(batch_axes, None, None), P(None, "tp"), P(batch_axes, None), P(batch_axes), P(batch_axes)),
        out_specs=(P(batch_axes), P(batch_axes, "tp"), P(batch_axes, None, None)),
        check_vma=False,
    )
```

```python
import functools

import jax
import jax.numpy as jnp
from jax import lax
from jax.experimental import pallas as pl
from jax.experimental.pallas import tpu as pltpu
from jax.sharding import PartitionSpec as P

NEG_BIG = -1.0e30
LOG2E = 1.4426950408889634
F32 = jnp.float32
DOWN = dict(axis=0, keepdims=True)
ALONG = dict(axis=1, keepdims=True)
BF16 = jnp.bfloat16
TILE = 512
LANES = 128
HALF = LANES // 2
MIB = 1 << 20


def vmem_spec():
    return pl.BlockSpec(memory_space=pltpu.VMEM)


def smem_spec():
    return pl.BlockSpec(memory_space=pltpu.SMEM)


def any_spec():
    return pl.BlockSpec(memory_space=pl.ANY)


def kernel_call(*args, **kw):
    return pl.pallas_call(*args, **kw)


def params():
    return pltpu.CompilerParams(vmem_limit_bytes=56 * MIB)


def label_col(meta_refs, i):
    n_slots = meta_refs[0].shape[1] - 1
    seq, item = i // n_slots, lax.rem(i, n_slots)
    n_seq = meta_refs[0].shape[0]
    at = lax.max(item - 1, 0)
    col = meta_refs[0][lax.rem(seq, n_seq), at]
    for k in range(1, len(meta_refs)):
        col = jnp.where(seq >= k * n_seq, meta_refs[k][lax.rem(seq, n_seq), at], col)
    return jnp.where(item == 0, 0, col)


def build_lists(meta_refs, vocab_loc, head, nxt):
    n_items = len(meta_refs) * meta_refs[0].shape[0] * (meta_refs[0].shape[1] - 1)
    col_start = lax.axis_index("tp") * vocab_loc
    n_tiles = vocab_loc // TILE

    def clear(i, c):
        head[i] = -1
        return c

    lax.fori_loop(0, n_tiles, clear, 0)

    def insert(i, c):
        loc = label_col(meta_refs, i) - col_start
        tile = lax.max(loc, 0) // TILE

        @pl.when((loc >= 0) & (loc < vocab_loc))
        def _():
            nxt[i] = head[tile]
            head[tile] = i

        return c

    lax.fori_loop(0, n_items, insert, 0)
    return col_start


def walk_list(head, nxt, tile, visit):
    def body(i):
        visit(i)
        return nxt[i]

    lax.while_loop(lambda i: i >= 0, body, head[tile])


class TileStream:
    def __init__(self, src, buf, sem, depth, n_tiles, view):
        self.src, self.buf, self.sem, self.depth, self.n, self.view = src, buf, sem, depth, n_tiles, view

    def copy(self, j):
        slot = lax.rem(j, self.depth)
        return pltpu.make_async_copy(self.view(self.src, j), self.buf.at[slot], self.sem.at[slot])

    def prime(self):
        for j in range(min(self.depth - 1, self.n)):
            self.copy(j).start()

    def get(self, j):
        self.copy(j).wait()

        @pl.when(j + self.depth - 1 < self.n)
        def _():
            self.copy(j + self.depth - 1).start()

        return lax.rem(j, self.depth)


def w_view(src, j, n=1):
    return src.at[:, pl.ds(pl.multiple_of(j * n * TILE, TILE), n * TILE)]


def z_view(src, j, n):
    return src.at[pl.ds(j * n, n)]


def exact_zero(total):
    return jnp.minimum(total[0:16] + total[16:32], 0.0).astype(BF16)


def after(lhs, zero):
    if zero is None:
        return lhs
    corner = lhs[0:16, 0:LANES] + zero
    return jnp.concatenate([jnp.concatenate([corner, lhs[0:16, LANES:]], axis=1), lhs[16:]], axis=0)


def unit_stats(z, m_ref, s_ref, r0):
    n_chunks = z.shape[1] // LANES
    total = None
    for b in range(z.shape[0] // 32):
        zb = [z[32 * b:32 * (b + 1), k * LANES:(k + 1) * LANES] for k in range(n_chunks)]
        rows = slice(r0 + 32 * b, r0 + 32 * (b + 1))
        m_old = m_ref[rows, :]
        m_new = functools.reduce(jnp.maximum, zb, m_old)
        s_new = s_ref[rows, :] * jnp.exp(m_old - m_new)
        for part in zb:
            s_new = s_new + jnp.exp(part - m_new)
        m_ref[rows, :] = m_new
        s_ref[rows, :] = s_new
        total = s_new if total is None else total + s_new
    return exact_zero(total)


def z_group(h_ref, w, z_out, m_ref, s_ref):
    n_tiles = z_out.shape[0]
    n = h_ref.shape[0] // 2
    zeros = []
    for t in range(n_tiles):
        for r in range(2):
            rows = slice(r * n, (r + 1) * n)
            lhs = after(h_ref[rows, :], zeros[-2] if len(zeros) >= 2 else None)
            z = jnp.dot(lhs, w[:, t * TILE:(t + 1) * TILE], preferred_element_type=F32)
            z_out[t, rows, :] = z
            zeros.append(unit_stats(z, m_ref, s_ref, r * n))


def emit_stats(m_ref, s_ref, out_ref, base):
    row_m = jnp.max(m_ref[...], **ALONG)
    row_s = jnp.sum(s_ref[...] * jnp.exp(m_ref[...] - row_m), **ALONG)
    rows = m_ref.shape[0]
    for k, v in enumerate((row_m, row_s)):
        flat = jnp.broadcast_to(v, (rows, LANES)).T
        for p in range(rows // LANES):
            at = base + 8 * k + p
            out_ref[at:at + 1, :] = flat[0:1, p * LANES:(p + 1) * LANES]


def z_own_kernel(n_slots, h_hbm, w_hbm, labels_ref, in_len_ref, lab_len_ref, z_hbm, pick_ref, meta_ref, h_ref, hsem, wbuf, wsem, zbuf, zsem, m_ref, s_ref, blank, head, nxt):
    n_tiles = z_hbm.shape[0]
    rows = h_ref.shape[0]
    n_seq = meta_ref.shape[0]
    frames = rows // n_seq
    h_copy = pltpu.make_async_copy(h_hbm, h_ref, hsem.at[0])
    h_copy.start()
    n_lab = n_slots - 1
    for q in range(n_seq):
        def put(k, c, q=q):
            meta_ref[q, k] = labels_ref[q, k]
            return c

        lax.fori_loop(0, n_lab, put, 0)
        meta_ref[q, n_lab] = in_len_ref[q]
        meta_ref[q, n_lab + 1] = lab_len_ref[q]
    group = zbuf.shape[1]
    stream = TileStream(w_hbm, wbuf, wsem, wbuf.shape[0], n_tiles // group, lambda src, j: w_view(src, j, group))
    stream.prime()
    col_start = build_lists([meta_ref], n_tiles * TILE, head, nxt)
    m_ref[...] = jnp.full(m_ref.shape, NEG_BIG, F32)
    s_ref[...] = jnp.zeros(s_ref.shape, F32)
    pick_ref[...] = jnp.zeros(pick_ref.shape, F32)
    blank[...] = jnp.zeros(blank.shape, F32)
    half = frames // 2
    h_copy.wait()
    lane = lax.broadcasted_iota(jnp.int32, (half, LANES), 1)

    def out_copy(j):
        slot = lax.rem(j, zbuf.shape[0])
        return pltpu.make_async_copy(zbuf.at[slot], z_view(z_hbm, j, group), zsem.at[slot])

    def step(j, c):
        slot = stream.get(j)

        @pl.when(j >= 3)
        def _():
            out_copy(j - 3).wait()

        zslot = lax.rem(j, zbuf.shape[0])
        z_group(h_ref, wbuf.at[slot], zbuf.at[zslot], m_ref, s_ref)
        out_copy(j).start()

        for t in range(group):
            def visit(i, t=t):
                seq, item = i // n_slots, lax.rem(i, n_slots)
                off = label_col([meta_ref], i) - col_start - (j * group + t) * TILE
                blk = off // LANES
                r0 = pl.multiple_of(seq * frames, frames)
                src = off - blk * LANES
                c0 = pl.multiple_of(blk * LANES, LANES)

                def moved(p, at):
                    zb = zbuf[zslot, t, pl.ds(r0 + p * half, half), pl.ds(c0, LANES)]
                    return pltpu.roll(zb, lax.rem(at - src + LANES, LANES), 1)

                @pl.when(item > 0)
                def _():
                    for p in range(2):
                        at = item - 1 + n_lab * seq + HALF * p
                        pick_ref[0:half, :] = jnp.where(lane == at, moved(p, at), pick_ref[0:half, :])

                @pl.when(item == 0)
                def _():
                    for p in range(2):
                        at = 2 * seq + p
                        blank[...] = jnp.where(lane == at, moved(p, at), blank[...])

            walk_list(head, nxt, j * group + t, visit)
        return c

    n_groups = n_tiles // group
    lax.fori_loop(0, n_groups, step, 0)
    emit_stats(m_ref, s_ref, pick_ref, half)
    pick_ref[half + 16:half + 24, :] = blank[...].T[0:8]
    for j in range(n_groups - 3, n_groups):
        out_copy(j).wait()


def z_oth_loop(lo, hi, join, h_ref, w_hbm, z_hbm, wbuf, wsem, zbuf, zsem, m_ref, s_ref, sections):
    group = zbuf.shape[1]
    lo, n_groups = lo // group, (hi - lo) // group
    stream = TileStream(w_hbm, wbuf, wsem, wbuf.shape[0], n_groups, lambda src, j: w_view(src, lo + j, group))
    stream.prime()

    def out_copy(j):
        slot = lax.rem(j, zbuf.shape[0])
        return pltpu.make_async_copy(zbuf.at[slot], z_view(z_hbm, lo + j, group), zsem.at[slot])

    base = 0
    join.wait()
    for n, side, make_carry in sections:
        carry = make_carry()

        def step(k, c, base=base, side=side):
            j = base + k
            slot = stream.get(j)

            @pl.when(j >= 3)
            def _():
                out_copy(j - 3).wait()

            z_group(h_ref, wbuf.at[slot], zbuf.at[lax.rem(j, zbuf.shape[0])], m_ref, s_ref)
            c = side(k, c)
            out_copy(j).start()
            return c

        last = lax.fori_loop(0, n, step, carry)
        yield last
        base += n
    for j in range(max(n_groups - 3, 0), n_groups):
        out_copy(j).wait()


class JoinRows:
    def __init__(self, h_got, h_core, h_ref, hsem):
        n = h_got.shape[0]
        core = lax.rem(lax.axis_index("tp"), 2)
        self.copies = [pltpu.make_async_copy(src, h_ref.at[pl.ds(pl.multiple_of(at * n, n), n), :], hsem.at[k])
                       for k, (src, at) in enumerate(((h_got, core), (h_core, 1 - core)))]

    def start(self):
        for c in self.copies:
            c.start()

    def wait(self):
        for c in self.copies:
            c.wait()


def z_lattice_part(lo, hi, n_lat, per_group, n_lab, before_tail, h_got, h_core, w_hbm, p0, p1, p2, p3, meta_ref,
                     z_hbm, stats_ref, occ_ref, loss_ref, m_ref, s_ref,
                     h_ref, hsem, wbuf, wsem, zbuf, zsem, e_lab, e_blk, s_lab, s_blk, r_lab, r_blk, o_t):
    join = JoinRows(h_got, h_core, h_ref, hsem)
    join.start()
    n_blk = e_lab.shape[0]
    frames = n_blk * HALF
    m_ref[...] = jnp.full(m_ref.shape, NEG_BIG, F32)
    s_ref[...] = jnp.zeros(s_ref.shape, F32)
    lane128 = lax.broadcasted_iota(jnp.int32, (LANES, LANES), 1)
    row32 = lax.broadcasted_iota(jnp.int32, (n_lab, LANES), 0)
    row8 = lax.broadcasted_iota(jnp.int32, (8, LANES), 0)
    lane32 = lax.broadcasted_iota(jnp.int32, (n_lab, LANES), 1)
    lane8 = lax.broadcasted_iota(jnp.int32, (8, LANES), 1)
    n_seq = meta_ref.shape[0]
    labs = jnp.zeros((n_lab, LANES), jnp.int32)
    lab_row = jnp.zeros((8, LANES), jnp.int32)
    live8 = jnp.zeros((8, LANES), jnp.int32)
    used8 = jnp.zeros((8, LANES), jnp.int32)
    for s in range(n_seq):
        for k in range(n_lab):
            labs = jnp.where((row32 == k) & ((lane32 == s) | (lane32 == s + n_seq)), meta_ref[s, k], labs)
            lab_row = jnp.where((row8 == s) & (lane8 == k), meta_ref[s, k], lab_row)
        here = (lane8 == s) | (lane8 == s + n_seq)
        live8 = jnp.where(here, meta_ref[s, n_lab], live8)
        used8 = jnp.where(here, meta_ref[s, n_lab + 1], used8)
    live32 = jnp.broadcast_to(live8[0:1], (n_lab, LANES))
    used32 = jnp.broadcast_to(used8[0:1], (n_lab, LANES))
    skip_dn = labs != pltpu.roll(labs, 1, 0)
    skip_up = labs != pltpu.roll(labs, n_lab - 1, 0)
    end_lab = row32 == used32 - 1
    end_blk = row32 == used32
    end_top = (row8 == 0) & (used8 == n_lab)
    shift0 = jnp.zeros((1, LANES), F32)
    seq1 = lane8[0:1] >= HALF
    half_len = jnp.where(seq1, meta_ref[1, n_lab], meta_ref[0, n_lab])
    half = frames // 2
    packed = functools.reduce(jnp.add, [p[0:half, :] for p in (p0, p1, p2, p3)])
    blanks = functools.reduce(jnp.add, [p[half + 16:half + 24, :] for p in (p0, p1, p2, p3)])
    for j in range(n_blk):
        far, near = j // 2, HALF * (j % 2)
        part = packed[near:near + HALF]
        x = jnp.concatenate([pltpu.roll(part, (LANES - HALF * far - n_lab * q) % LANES, 1) for q in range(2)], axis=0).T[0:n_lab]
        rows_b = [pltpu.roll(blanks, (HALF * q - near) % LANES, 1)[2 * q + far:2 * q + far + 1] for q in range(2)]
        x_blank = jnp.where(seq1, rows_b[1], rows_b[0])
        top = jnp.maximum(jnp.max(x, **DOWN), x_blank)
        e_blk[j] = jnp.broadcast_to((x_blank - top) * LOG2E, (8, LANES))
        e_lab[j] = (x - top) * LOG2E
        shift0 = shift0 + jnp.where(lax.rem(lane8[0:1], HALF) + HALF * j < half_len, top, 0.0)
    shift_seq0 = jnp.sum(jnp.where(seq1, 0.0, shift0), **ALONG)
    shift_seq1 = jnp.sum(jnp.where(seq1, shift0, 0.0), **ALONG)

    def lse2(a, b):
        hi_v = jnp.maximum(a, b)
        return hi_v + jnp.log2(1.0 + jnp.exp2(jnp.minimum(a, b) - hi_v))

    def lse3(a, b, c):
        hi_v = jnp.maximum(a, b)
        lo_v = jnp.minimum(a, b)
        top = jnp.maximum(hi_v, c)
        mid = jnp.minimum(hi_v, c)
        return top + jnp.log2(1.0 + (jnp.exp2(lo_v - top) + jnp.exp2(mid - top)))

    fwd8, fwd32 = lane8 < n_seq, lane32 < n_seq
    ahead8 = fwd8 & (row8 == 0)
    behind8 = (lane8 >= n_seq) & (row8 == 7)
    base8 = jnp.where(fwd8, HALF * lane8, HALF * (lane8 - n_seq) + HALF - 1)
    base8 = jnp.where(lane8 < 2 * n_seq, base8, HALF)
    skip = jnp.where(fwd32, jnp.where(skip_dn & (row32 > 0), 1, 0), jnp.where(skip_up & (row32 < n_lab - 1), 1, 0)) > 0

    def lanes_of(x, idx):
        return jnp.take_along_axis(x, idx, axis=1, mode="promise_in_bounds")

    def tall(x):
        return jnp.concatenate([x] * (n_lab // 8), axis=0)

    neg32 = jnp.full((n_lab, LANES), NEG_BIG, F32)
    first_b = jnp.where(fwd32, jnp.where(row32 == 0, 0.0, NEG_BIG), jnp.where(end_blk, 0.0, NEG_BIG))
    first_t = jnp.where(fwd8, NEG_BIG, jnp.where(end_top, 0.0, NEG_BIG))

    def lat_step(i, j, u, carry):
        lab, blk, top_b = carry
        idx8 = base8 + jnp.where(fwd8, u, -u)
        idx32 = tall(idx8)
        back = n_blk - 1 - j
        e_l = jnp.where(fwd32, lanes_of(e_lab[j], idx32), lanes_of(e_lab[back], idx32))
        e_b = jnp.where(fwd8, lanes_of(e_blk[j], idx8), lanes_of(e_blk[back], idx8))
        lab_dn = pltpu.roll(lab, 1, 0)
        lab_up = pltpu.roll(lab, n_lab - 1, 0)
        blk_side = jnp.where(fwd32, blk, pltpu.roll(blk, n_lab - 1, 0))
        blk_side = jnp.concatenate([blk_side[:n_lab - 8], jnp.where(behind8, jnp.broadcast_to(top_b[0:1], (8, LANES)), blk_side[n_lab - 8:])], axis=0)
        lab_side = jnp.where(fwd32, lab_dn, lab)
        lab_side = jnp.concatenate([jnp.where(ahead8, NEG_BIG, lab_side[:8]), lab_side[8:]], axis=0)
        new_l = lse3(lab, blk_side, jnp.where(skip, jnp.where(fwd32, lab_dn, lab_up), NEG_BIG))
        new_b = lse2(blk, lab_side)
        new_t = lse2(top_b, jnp.where(ahead8, lab_dn[:8], NEG_BIG))
        s_lab[i] = new_l
        s_blk[i, 0:n_lab] = new_b
        s_blk[i, n_lab:n_lab + 8] = new_t
        behind = frames - 1 - i + pad
        r_lab[behind] = pltpu.roll(new_l, LANES - n_seq, 1)
        r_blk[behind, 0:n_lab] = pltpu.roll(new_b, LANES - n_seq, 1)
        r_blk[behind, n_lab:n_lab + 8] = pltpu.roll(new_t, LANES - n_seq, 1)
        at8 = jnp.where(fwd8, i, frames - 1 - i)
        live = tall(at8) < live32
        lab = jnp.where(live, e_l + new_l, lab)
        blk = jnp.where(live, tall(e_b) + new_b, blk)
        top_b = jnp.where(at8 < live8, e_b + new_t, top_b)
        return lab, blk, top_b

    group = zbuf.shape[1]
    n_lat_groups = n_lat // group
    pad = s_lab.shape[0] - frames

    def lattice_side(k, carry):
        for u in range(per_group):
            i = k * per_group + u
            j = lax.min(lax.div(i, HALF), n_blk - 1)
            carry = lat_step(i, j, lax.rem(i, HALF), carry)
        return carry

    n_occ = (hi - lo - n_lat) // group
    occ_group = frames // n_occ // HALF
    seq_of8 = jnp.where(lane8 >= HALF, 1, 0)
    run = z_oth_loop(lo, hi, join, h_ref, w_hbm, z_hbm, wbuf, wsem, zbuf, zsem, m_ref, s_ref,
                     [(n_lat_groups, lattice_side, lambda: (neg32, first_b, first_t)),
                      (n_occ, lambda k, c: occ_side(k, c), lambda: 0)])
    al, ab, at = next(run)

    lasts = [jnp.where(end, v, NEG_BIG) for end, v in ((end_lab, al), (end_blk, ab), (end_top, at))]
    top = functools.reduce(jnp.maximum, [jnp.max(v, **DOWN) for v in lasts])
    total = functools.reduce(jnp.add, [jnp.sum(jnp.exp2(v - top), **DOWN) for v in lasts])
    loss = -(top + jnp.log2(total))
    loss_at = lanes_of(jnp.broadcast_to(loss, (8, LANES)), seq_of8)
    lane1 = lane8[0:1]
    loss_ref[...] = jnp.broadcast_to(loss * (1.0 / LOG2E) - jnp.where(lane1 == 0, shift_seq0, jnp.where(lane1 == 1, shift_seq1, 0.0)), (8, LANES))

    def occ_side(k, c):
        for g in range(occ_group):
            j = k * occ_group + g
            seq_of32 = tall(seq_of8)
            logs = [neg32, neg32, neg32[0:8]]
            for u in range(HALF):
                i = j * HALF + u
                here8 = lax.rem(lane8, HALF) == u
                here32 = lax.rem(lane32, HALF) == u
                sum_l = s_lab[i] + r_lab[i + pad]
                sum_b = s_blk[i] + r_blk[i + pad]
                logs[0] = jnp.where(here32, lanes_of(sum_l, seq_of32), logs[0])
                logs[1] = jnp.where(here32, lanes_of(sum_b[:n_lab], seq_of32), logs[1])
                logs[2] = jnp.where(here8, lanes_of(sum_b[n_lab:], seq_of8), logs[2])
            rest = e_blk[j] + loss_at
            live = lax.rem(lane8, HALF) + HALF * j < jnp.broadcast_to(half_len, (8, LANES))
            occ_l = jnp.exp2(logs[0] + e_lab[j] + tall(loss_at))
            occ_b = jnp.sum(jnp.exp2(logs[1] + tall(rest)), **DOWN) + jnp.exp2(logs[2] + rest)[0:1]
            o_t[j, 0:n_lab] = jnp.where(tall(jnp.where(live, 1, 0)) > 0, occ_l, 0.0)
            o_t[j, n_lab:n_lab + 8] = jnp.where(live, jnp.broadcast_to(occ_b, (8, LANES)), 0.0)
            o_t[j, 8 + n_lab:LANES] = jnp.zeros((LANES - 8 - n_lab, LANES), F32)
        return c

    next(run)
    before_tail()
    for _ in run:
        pass
    emit_stats(m_ref, s_ref, stats_ref, 0)
    row128 = lax.broadcasted_iota(jnp.int32, (LANES, LANES), 0)
    same = []
    for s in range(n_seq):
        down = jnp.full((n_lab, LANES), -1, jnp.int32)
        for k in range(n_lab):
            down = jnp.where(row32 == k, meta_ref[s, k], down)
        down = jnp.concatenate([down, jnp.full((LANES - n_lab, LANES), -1, jnp.int32)], axis=0)
        across = pltpu.roll(jnp.broadcast_to(lab_row[s:s + 1], (LANES, LANES)), HALF * s, 1)
        own = lane128 - HALF * s
        inner = (row128 < n_lab) & (own >= 0) & (own < n_lab)
        same.append(jnp.where((inner & (down == across)) | ((row128 == own) & (own < HALF)), 1.0, 0.0))
    for j in range(n_blk):
        y = o_t[j].T
        occ_ref[HALF * j:HALF * (j + 1), :] = functools.reduce(jnp.add, [
            jnp.dot(y[HALF * q:HALF * (q + 1), :], same[q], precision=lax.Precision.HIGHEST, preferred_element_type=F32) for q in range(n_seq)])


def spread_lse(refs, base, meta_ref, lse_ref, r0, frames):
    m = functools.reduce(jnp.maximum, [r[base:base + 8, :] for r in refs])
    tot = functools.reduce(jnp.add, [r[base + 8:base + 16, :] * jnp.exp(r[base:base + 8, :] - m) for r in refs])
    lse = m + jnp.log(tot)
    t = lax.broadcasted_iota(jnp.int32, (LANES, LANES), 0)
    n_part = frames // LANES
    sums = []
    for q in range(meta_ref.shape[0]):
        live_sum = jnp.zeros((1, LANES), F32)
        for p in range(n_part):
            at = q * n_part + p
            part = jnp.broadcast_to(lse[at:at + 1, :], (LANES, LANES)).T
            live = t + p * LANES < meta_ref[q, meta_ref.shape[1] - 2]
            lse_ref[r0 + at * LANES:r0 + (at + 1) * LANES, :] = jnp.where(live, part, 1.0e30)
            live_sum = live_sum + jnp.sum(jnp.where(live, part, 0.0), **DOWN)
        sums.append(live_sum)
    return sums


def patch_tile(n_slots, frames, meta_refs, col_start, j, i, z_block, lse_ref, occ_ref, g_ref, g_col, lane):
    seq, item = i // n_slots, lax.rem(i, n_slots)
    off = label_col(meta_refs, i) - col_start - j * TILE
    blk = off // LANES
    r0 = pl.multiple_of(seq * frames, frames)
    c0 = pl.multiple_of(blk * LANES, LANES)
    zb = z_block(seq, c0)
    slot_lane = jnp.where(item == 0, n_slots - 1, item - 1) + HALF * seq
    occ = jnp.sum(jnp.where(lane == slot_lane, occ_ref[...], 0.0), **ALONG)
    fresh = jnp.exp(zb - lse_ref[pl.ds(r0, frames), :]) - occ
    gc = pl.multiple_of(g_col + c0, LANES)
    old = g_ref[pl.ds(r0, frames), pl.ds(gc, LANES)].astype(F32)
    g_ref[pl.ds(r0, frames), pl.ds(gc, LANES)] = jnp.where(lane == off - blk * LANES, fresh, old).astype(BF16)


def softmax_unit(z, z_row, lse_ref, out, r0, n, c0):
    total = None
    for b in range(n // 32):
        lse = lse_ref[r0 + 32 * b:r0 + 32 * (b + 1), :]
        for k in range(TILE // LANES):
            e = jnp.exp(z[z_row + 32 * b:z_row + 32 * (b + 1), k * LANES:(k + 1) * LANES] - lse)
            out[r0 + 32 * b:r0 + 32 * (b + 1), c0 + k * LANES:c0 + (k + 1) * LANES] = e.astype(BF16)
            total = e if total is None else total + e
    return exact_zero(total)


def grad_h_part(n_slots, z_hbm, w_hbm, st0, st1, st2, st3, occ_ref, part_loss, meta_ref, keep_ref, send_ref, loss_ref, g_hbm,
                  wbuf, wsem, zbuf, zsem, acc, lse_ref, g0, g1, gsem, head, nxt):
    n_tiles, rows = z_hbm.shape[0], z_hbm.shape[1]
    frames = rows // meta_ref.shape[0]
    meta_refs = [meta_ref]
    group = zbuf.shape[1]
    n_groups = n_tiles // group
    stream = TileStream(w_hbm, wbuf, wsem, wbuf.shape[0], n_groups, lambda src, j: w_view(src, j, group))
    zs = TileStream(z_hbm, zbuf, zsem, zbuf.shape[0], n_groups, lambda src, j: z_view(src, j, group))
    zs.prime()
    yield stream.prime
    col_start = build_lists(meta_refs, n_tiles * TILE, head, nxt)
    sums = spread_lse([st0, st1, st2, st3], frames // 2, meta_ref, lse_ref, 0, frames)
    lane1 = lax.broadcasted_iota(jnp.int32, (8, LANES), 1)
    loss_ref[...] = part_loss[...] + jnp.where(lane1 == 0, sums[0], sums[1])
    lane = lax.broadcasted_iota(jnp.int32, (frames, LANES), 1)

    def patch(j, slot, g):
        for t in range(group):
            def z_block(seq, c0, t=t):
                return zbuf[slot, t, pl.ds(pl.multiple_of(seq * frames, frames), frames), pl.ds(c0, LANES)]

            walk_list(head, nxt, j * group + t,
                      lambda i, t=t, z_block=z_block: patch_tile(n_slots, frames, meta_refs, col_start, j * group + t, i, z_block, lse_ref, occ_ref, g, t * TILE, lane))

    def make_g(slot, u, g):
        t, r = u // 2, u % 2
        return softmax_unit(zbuf.at[slot, t], r * rows // 2, lse_ref, g, r * rows // 2, rows // 2, t * TILE)

    acc[...] = jnp.zeros(acc.shape, F32)
    slot0 = zs.get(0)
    for u in range(2 * group):
        make_g(slot0, u, g0)
    patch(0, slot0, g0)
    n_units = acc.shape[0] // 256

    def g_copy(j, g, k):
        return pltpu.make_async_copy(g, g_hbm.at[j], gsem.at[k])

    def half(j, g_now, g_next, k):
        slot = stream.get(j)
        nj = lax.min(j + 1, n_groups - 1)

        @pl.when(j + 1 < n_groups)
        def _():
            zs.get(nj)

        @pl.when(j >= 1)
        def _():
            g_copy(j - 1, g_next, 1 - k).wait()

        g_copy(j, g_now, k).start()

        zslot = lax.rem(nj, zbuf.shape[0])
        zero = None
        for u in range(n_units):
            d_rows = slice(u * 256, (u + 1) * 256)
            lhs = after(wbuf[slot, d_rows, :], zero)
            acc[d_rows, :] += lax.dot_general(lhs, g_now[...], (((1,), (1,)), ((), ())), preferred_element_type=F32)
            if u < 2 * group:
                zero = make_g(zslot, u, g_next)
        patch(nj, zslot, g_next)

    def step(i, c):
        half(2 * i, g0, g1, 0)
        half(2 * i + 1, g1, g0, 1)
        return c

    lax.fori_loop(0, n_groups // 2, step, 0)
    g_copy(n_groups - 1, g1, 1).wait()
    core = lax.rem(lax.axis_index("tp"), 2)
    n = rows // 2
    keep_ref[...] = acc[:, pl.ds(pl.multiple_of(core * n, n), n)].T
    send_ref[...] = acc[:, pl.ds(pl.multiple_of((1 - core) * n, n), n)].T


def mid_kernel(lo, hi, n_lat, per_group, n_lab, h_got, h_core, w_hbm, p0, p1, p2, p3, z_own, meta_ref,
               z_hbm, stats_ref, occ_ref, keep_ref, send_ref, loss_ref, g_hbm,
               part_loss, m_ref, s_ref, h_ref, hsem, wbuf, wsem, zbuf, zsem, e_lab, e_blk, s_lab, s_blk, r_lab, r_blk, o_t,
               zin_buf, zin_sem, acc, lse_ref, g0, g1, gsem, head, nxt):
    second = grad_h_part(n_lab + 1, z_own, w_hbm, p0, p1, p2, p3, occ_ref, part_loss, meta_ref, keep_ref, send_ref, loss_ref, g_hbm,
                         wbuf, wsem, zin_buf, zin_sem, acc, lse_ref, g0, g1, gsem, head, nxt)
    prime_w = next(second)
    z_lattice_part(lo, hi, n_lat, per_group, n_lab, prime_w, h_got, h_core, w_hbm, p0, p1, p2, p3, meta_ref,
                   z_hbm, stats_ref, occ_ref, part_loss, m_ref, s_ref,
                   h_ref, hsem, wbuf, wsem, zbuf, zsem, e_lab, e_blk, s_lab, s_blk, r_lab, r_blk, o_t)
    for _ in second:
        pass


def grad_w_kernel(n_slots, g_hbm, z_hbm, h_own_ref, h_got, h_core, st0, st1, st2, st3, occ_ref, meta_ref, gw_hbm,
                  h_ref, hsem, zbuf, zsem, gsem, obuf, osem, ht, lse_ref, g0, g1, head, nxt):
    n_tiles, rows = z_hbm.shape[0], z_hbm.shape[1]
    frames = rows // meta_ref.shape[0]
    d_loc = ht.shape[0]
    group = zbuf.shape[1]
    n_groups = n_tiles // group
    zs = TileStream(z_hbm, zbuf, zsem, zbuf.shape[0], n_groups, lambda src, j: z_view(src, j, group))

    def g_copy(j, g, k):
        return pltpu.make_async_copy(g_hbm.at[j], g.at[0:rows, :], gsem.at[k])

    join = JoinRows(h_got, h_core, h_ref, hsem)
    join.start()
    zs.prime()
    g_copy(0, g0, 0).start()
    col_start = build_lists([meta_ref], n_tiles * TILE, head, nxt)
    d0 = pl.multiple_of(lax.axis_index("dp") * d_loc, LANES)
    ht[:, 0:rows] = h_own_ref[:, pl.ds(d0, d_loc)].T
    spread_lse([st0, st1, st2, st3], 0, meta_ref, lse_ref, 0, frames)
    join.wait()
    ht[:, rows:2 * rows] = h_ref[:, pl.ds(d0, d_loc)].T
    lane = lax.broadcasted_iota(jnp.int32, (frames, LANES), 1)
    n_units = 2 * group

    def make_g(slot, u, g):
        t, r = u // 2, u % 2
        return softmax_unit(zbuf.at[slot, t], r * rows // 2, lse_ref, g.at[rows:2 * rows, :], r * rows // 2, rows // 2, t * TILE)

    def patch(j, slot, g):
        for t in range(group):
            def z_block(seq, c0, t=t):
                return zbuf[slot, t, pl.ds(pl.multiple_of(seq * frames, frames), frames), pl.ds(c0, LANES)]

            walk_list(head, nxt, j * group + t,
                      lambda i, t=t, z_block=z_block: patch_tile(n_slots, frames, [meta_ref], col_start, j * group + t, i, z_block, lse_ref, occ_ref, g.at[rows:2 * rows, :], t * TILE, lane))

    def out_copy(j):
        slot = lax.rem(j, obuf.shape[0])
        return pltpu.make_async_copy(obuf.at[slot], w_view(gw_hbm, j, group), osem.at[slot])

    slot0 = zs.get(0)
    for u in range(n_units):
        make_g(slot0, u, g0)
    patch(0, slot0, g0)
    d_half = d_loc // 2

    def half(j, g_now, g_next, k):
        @pl.when(j >= 3)
        def _():
            out_copy(j - 3).wait()

        nj = lax.min(j + 1, n_groups - 1)

        @pl.when(j + 1 < n_groups)
        def _():
            zs.get(nj)
            g_copy(nj, g_next, 1 - k).start()

        g_copy(j, g_now, k).wait()
        slot = lax.rem(nj, zbuf.shape[0])
        oslot = lax.rem(j, obuf.shape[0])
        zero = None
        for u in range(n_units):
            t, r = u // 2, u % 2
            d_rows = slice(r * d_half, (r + 1) * d_half)
            lhs = after(ht[d_rows, :], zero)
            obuf[oslot, d_rows, t * TILE:(t + 1) * TILE] = jnp.dot(lhs, g_now[:, t * TILE:(t + 1) * TILE], preferred_element_type=F32)
            zero = make_g(slot, u, g_next)
        out_copy(j).start()
        patch(nj, slot, g_next)

    def step(i, c):
        half(2 * i, g0, g1, 0)
        half(2 * i + 1, g1, g0, 1)
        return c

    lax.fori_loop(0, n_groups // 2, step, 0)
    for j in range(n_groups - 3, n_groups):
        out_copy(j).wait()


def cost(flops, nbytes):
    return pl.CostEstimate(flops=flops, bytes_accessed=nbytes, transcendentals=0)


def solution(mesh):
    batch_axes = ("part", "dp")
    n_tp = mesh.shape["tp"]
    n_dp = mesh.shape["dp"]
    dp_swap = [(i, n_dp - 1 - i) for i in range(n_dp)]

    others = range(1, n_tp)

    def tp_xor(x, mask):
        return lax.ppermute(x, "tp", [(i, i ^ mask) for i in range(n_tp)])

    def in_hbm(x):
        return pltpu.with_memory_space_constraint(x, pltpu.HBM)

    def swap_dp(x):
        return lax.ppermute(x, "dp", dp_swap)

    def local_body(hidden, w_loc, labels, in_len, lab_len):
        batch_loc, frames, model_dim = hidden.shape
        vocab_loc = w_loc.shape[1]
        n_lab = labels.shape[1]
        n_slots = n_lab + 1
        rows = batch_loc * frames
        n_tiles = vocab_loc // TILE
        d_loc = model_dim // n_dp
        dma = pltpu.SemaphoreType.DMA
        i32 = jnp.int32
        n_lat, lat_steps, lat_pad = 24, 22, 8
        h_own = hidden.reshape(rows, model_dim)
        core = lax.rem(lax.axis_index("tp"), 2)
        h_half = lax.dynamic_index_in_dim(h_own.reshape(2, rows // 2, model_dim), core, 0, keepdims=False)
        h_got = swap_dp(h_half)
        flops = 2 * rows * model_dim * TILE
        wbytes = model_dim * TILE * 2
        zbytes = rows * TILE * 4
        z_type = jax.ShapeDtypeStruct((n_tiles, rows, TILE), F32)
        pick_type = jax.ShapeDtypeStruct((frames // 2 + 24, LANES), F32)
        meta_type = jax.ShapeDtypeStruct((batch_loc, n_slots + 1), i32)
        g_type = jax.ShapeDtypeStruct((n_tiles // 2, rows, 2 * TILE), BF16)
        stat_type = jax.ShapeDtypeStruct((16, LANES), F32)
        g_scratch = [pltpu.VMEM((rows, 2 * TILE), BF16)] * 2

        def w_scratch(n):
            return [pltpu.VMEM((3, model_dim, n * TILE), BF16), dma((3,))]

        def z_scratch(n):
            return [pltpu.VMEM((3, n, rows, TILE), F32), dma((3,))]

        h_scratch = [pltpu.VMEM((rows, model_dim), BF16), dma((2,))]
        run_scratch = [pltpu.VMEM((rows, LANES), F32), pltpu.VMEM((rows, LANES), F32)]

        def lists(n_sets):
            return [pltpu.SMEM((n_tiles,), i32), pltpu.SMEM((n_sets * batch_loc * n_slots,), i32)]

        z_own, pick, meta = kernel_call(
            functools.partial(z_own_kernel, n_slots),
            out_shape=(z_type, pick_type, meta_type),
            in_specs=[any_spec(), any_spec(), smem_spec(), smem_spec(), smem_spec()],
            out_specs=(any_spec(), vmem_spec(), smem_spec()),
            scratch_shapes=h_scratch + w_scratch(4) + z_scratch(4) + run_scratch + [pltpu.VMEM((frames // 2, LANES), F32)] + lists(1),
            compiler_params=params(),
            cost_estimate=cost(n_tiles * flops, n_tiles * (wbytes + zbytes)),
        )(in_hbm(h_own), w_loc, labels, in_len, lab_len)

        h_got, pick = lax.optimization_barrier((h_got, pick))
        h_core = in_hbm(tp_xor(h_got, 1))
        h_got = in_hbm(h_got)
        picks = [pick] + [tp_xor(pick, k) for k in others]

        n_blk = frames // HALF
        half_type = jax.ShapeDtypeStruct((rows // 2, model_dim), F32)
        occ_type = jax.ShapeDtypeStruct((frames, LANES), F32)
        loss_type = jax.ShapeDtypeStruct((8, LANES), F32)
        z_oth, stats_oth, occ, keep, send, loss, g_own = kernel_call(
            functools.partial(mid_kernel, 0, n_tiles, n_lat, lat_steps, n_lab),
            out_shape=(z_type, stat_type, occ_type, half_type, half_type, loss_type, g_type),
            in_specs=[any_spec()] * 3 + [vmem_spec()] * 4 + [any_spec(), smem_spec()],
            out_specs=(any_spec(),) + (vmem_spec(),) * 5 + (any_spec(),),
            scratch_shapes=[pltpu.VMEM((8, LANES), F32)] + run_scratch + h_scratch + w_scratch(2) + z_scratch(2) + [
                pltpu.VMEM((n_blk, n_lab, LANES), F32), pltpu.VMEM((n_blk, 8, LANES), F32),
                *[pltpu.VMEM((frames + lat_pad, n, LANES), F32) for n in (n_lab, n_lab + 8) * 2],
                pltpu.VMEM((n_blk, LANES, LANES), F32)] + z_scratch(2) + [
                pltpu.VMEM((model_dim, rows), F32), pltpu.VMEM((rows, LANES), F32)] + g_scratch + [dma((2,))] + lists(1),
            compiler_params=params(),
            cost_estimate=cost((2 * n_tiles) * flops, (2 * n_tiles) * (wbytes + zbytes)),
        )(h_got, h_core, w_loc, *picks, z_own, meta)
        st_oth = [stats_oth] + [tp_xor(stats_oth, k) for k in others]
        occ_oth = swap_dp(occ)
        meta_oth = swap_dp(meta)
        recv = tp_xor(send, 1)
        chip_sum = keep + recv
        across = tp_xor(chip_sum, 2)

        grad_weight = kernel_call(
            functools.partial(grad_w_kernel, n_slots),
            out_shape=jax.ShapeDtypeStruct((d_loc, vocab_loc), F32),
            in_specs=[any_spec(), any_spec(), vmem_spec(), any_spec(), any_spec()] + [vmem_spec()] * 5 + [smem_spec()],
            out_specs=any_spec(),
            scratch_shapes=h_scratch + z_scratch(2) + [
                dma((2,)), pltpu.VMEM((3, d_loc, 2 * TILE), F32), dma((3,)),
                pltpu.VMEM((d_loc, 2 * rows), BF16), pltpu.VMEM((rows, LANES), F32),
                pltpu.VMEM((2 * rows, 2 * TILE), BF16), pltpu.VMEM((2 * rows, 2 * TILE), BF16)] + lists(1),
            compiler_params=params(),
            cost_estimate=cost(n_tiles * flops, n_tiles * (2 * zbytes + d_loc * TILE * 4)),
        )(g_own, z_oth, h_own, h_got, h_core, *st_oth, occ_oth, meta_oth)

        chip_sum, grad_weight = lax.optimization_barrier((chip_sum, grad_weight))
        full_half = chip_sum + across
        other_half = tp_xor(full_half, 1)
        grad_hidden = jnp.where(core == 0, jnp.stack([full_half, other_half]), jnp.stack([other_half, full_half])).reshape(batch_loc, frames, model_dim)
        return loss[0, :batch_loc], grad_weight, grad_hidden


    return jax.shard_map(
        local_body,
        mesh=mesh,
        in_specs=(P(batch_axes, None, None), P(None, "tp"), P(batch_axes, None), P(batch_axes), P(batch_axes)),
        out_specs=(P(batch_axes), P(batch_axes, "tp"), P(batch_axes, None, None)),
        check_vma=False,
    )
```

```python
import functools

import jax
import jax.numpy as jnp
from jax import lax
from jax.experimental import pallas as pl
from jax.experimental.pallas import tpu as pltpu
from jax.sharding import PartitionSpec as P

NEG_BIG = -1.0e30
LOG2E = 1.4426950408889634
F32 = jnp.float32
DOWN = dict(axis=0, keepdims=True)
ALONG = dict(axis=1, keepdims=True)
BF16 = jnp.bfloat16
TILE = 512
LANES = 128
HALF = LANES // 2
MIB = 1 << 20


def vmem_spec():
    return pl.BlockSpec(memory_space=pltpu.VMEM)


def smem_spec():
    return pl.BlockSpec(memory_space=pltpu.SMEM)


def any_spec():
    return pl.BlockSpec(memory_space=pl.ANY)


def kernel_call(*args, **kw):
    return pl.pallas_call(*args, **kw)


def params():
    return pltpu.CompilerParams(vmem_limit_bytes=59 * MIB)


def label_col(meta_refs, i):
    n_slots = meta_refs[0].shape[1] - 1
    seq, item = i // n_slots, lax.rem(i, n_slots)
    n_seq = meta_refs[0].shape[0]
    at = lax.max(item - 1, 0)
    col = meta_refs[0][lax.rem(seq, n_seq), at]
    for k in range(1, len(meta_refs)):
        col = jnp.where(seq >= k * n_seq, meta_refs[k][lax.rem(seq, n_seq), at], col)
    return jnp.where(item == 0, 0, col)


def build_lists(meta_refs, vocab_loc, head, nxt):
    n_items = len(meta_refs) * meta_refs[0].shape[0] * (meta_refs[0].shape[1] - 1)
    col_start = lax.axis_index("tp") * vocab_loc
    n_tiles = vocab_loc // TILE

    def clear(i, c):
        head[i] = -1
        return c

    lax.fori_loop(0, n_tiles, clear, 0)

    def insert(i, c):
        loc = label_col(meta_refs, i) - col_start
        tile = lax.max(loc, 0) // TILE

        @pl.when((loc >= 0) & (loc < vocab_loc))
        def _():
            nxt[i] = head[tile]
            head[tile] = i

        return c

    lax.fori_loop(0, n_items, insert, 0)
    return col_start


def walk_list(head, nxt, tile, visit):
    def body(i):
        visit(i)
        return nxt[i]

    lax.while_loop(lambda i: i >= 0, body, head[tile])


class TileStream:
    def __init__(self, src, buf, sem, depth, n_tiles, view):
        self.src, self.buf, self.sem, self.depth, self.n, self.view = src, buf, sem, depth, n_tiles, view

    def copy(self, j):
        slot = lax.rem(j, self.depth)
        return pltpu.make_async_copy(self.view(self.src, j), self.buf.at[slot], self.sem.at[slot])

    def prime(self):
        for j in range(min(self.depth - 1, self.n)):
            self.copy(j).start()

    def get(self, j):
        self.copy(j).wait()

        @pl.when(j + self.depth - 1 < self.n)
        def _():
            self.copy(j + self.depth - 1).start()

        return lax.rem(j, self.depth)


def w_view(src, j, n=1):
    return src.at[:, pl.ds(pl.multiple_of(j * n * TILE, TILE), n * TILE)]


def z_view(src, j, n):
    return src.at[pl.ds(j * n, n)]


def exact_zero(total):
    return jnp.minimum(total[0:16] + total[16:32], 0.0).astype(BF16)


def after(lhs, zero):
    if zero is None:
        return lhs
    corner = lhs[0:16, 0:LANES] + zero
    return jnp.concatenate([jnp.concatenate([corner, lhs[0:16, LANES:]], axis=1), lhs[16:]], axis=0)


def unit_stats(z, m_ref, s_ref, r0):
    n_chunks = z.shape[1] // LANES
    total = None
    for b in range(z.shape[0] // 32):
        zb = [z[32 * b:32 * (b + 1), k * LANES:(k + 1) * LANES] for k in range(n_chunks)]
        rows = slice(r0 + 32 * b, r0 + 32 * (b + 1))
        m_old = m_ref[rows, :]
        m_new = functools.reduce(jnp.maximum, zb, m_old)
        s_new = s_ref[rows, :] * jnp.exp(m_old - m_new)
        for part in zb:
            s_new = s_new + jnp.exp(part - m_new)
        m_ref[rows, :] = m_new
        s_ref[rows, :] = s_new
        total = s_new if total is None else total + s_new
    return exact_zero(total)


def z_group(h_ref, w, z_out, m_ref, s_ref):
    n_tiles = z_out.shape[0]
    n = h_ref.shape[0] // 2
    zeros = []
    for t in range(n_tiles):
        for r in range(2):
            rows = slice(r * n, (r + 1) * n)
            lhs = after(h_ref[rows, :], zeros[-2] if len(zeros) >= 2 else None)
            z = jnp.dot(lhs, w[:, t * TILE:(t + 1) * TILE], preferred_element_type=F32)
            z_out[t, rows, :] = z
            zeros.append(unit_stats(z, m_ref, s_ref, r * n))


def emit_stats(m_ref, s_ref, out_ref, base):
    row_m = jnp.max(m_ref[...], **ALONG)
    row_s = jnp.sum(s_ref[...] * jnp.exp(m_ref[...] - row_m), **ALONG)
    rows = m_ref.shape[0]
    for k, v in enumerate((row_m, row_s)):
        flat = jnp.broadcast_to(v, (rows, LANES)).T
        for p in range(rows // LANES):
            at = base + 8 * k + p
            out_ref[at:at + 1, :] = flat[0:1, p * LANES:(p + 1) * LANES]


def z_own_kernel(n_slots, h_hbm, w_hbm, labels_ref, in_len_ref, lab_len_ref, z_hbm, pick_ref, meta_ref, h_ref, hsem, wbuf, wsem, zbuf, zsem, m_ref, s_ref, blank, head, nxt):
    n_tiles = z_hbm.shape[0]
    rows = h_ref.shape[0]
    n_seq = meta_ref.shape[0]
    frames = rows // n_seq
    h_copy = pltpu.make_async_copy(h_hbm, h_ref, hsem.at[0])
    h_copy.start()
    n_lab = n_slots - 1
    for q in range(n_seq):
        def put(k, c, q=q):
            meta_ref[q, k] = labels_ref[q, k]
            return c

        lax.fori_loop(0, n_lab, put, 0)
        meta_ref[q, n_lab] = in_len_ref[q]
        meta_ref[q, n_lab + 1] = lab_len_ref[q]
    group = zbuf.shape[1]
    stream = TileStream(w_hbm, wbuf, wsem, wbuf.shape[0], n_tiles // group, lambda src, j: w_view(src, j, group))
    stream.prime()
    col_start = build_lists([meta_ref], n_tiles * TILE, head, nxt)
    m_ref[...] = jnp.full(m_ref.shape, NEG_BIG, F32)
    s_ref[...] = jnp.zeros(s_ref.shape, F32)
    pick_ref[...] = jnp.zeros(pick_ref.shape, F32)
    blank[...] = jnp.zeros(blank.shape, F32)
    half = frames // 2
    h_copy.wait()
    lane = lax.broadcasted_iota(jnp.int32, (half, LANES), 1)

    def out_copy(j):
        slot = lax.rem(j, zbuf.shape[0])
        return pltpu.make_async_copy(zbuf.at[slot], z_view(z_hbm, j, group), zsem.at[slot])

    def step(j, c):
        slot = stream.get(j)

        @pl.when(j >= 3)
        def _():
            out_copy(j - 3).wait()

        zslot = lax.rem(j, zbuf.shape[0])
        z_group(h_ref, wbuf.at[slot], zbuf.at[zslot], m_ref, s_ref)
        out_copy(j).start()

        for t in range(group):
            def visit(i, t=t):
                seq, item = i // n_slots, lax.rem(i, n_slots)
                off = label_col([meta_ref], i) - col_start - (j * group + t) * TILE
                blk = off // LANES
                r0 = pl.multiple_of(seq * frames, frames)
                src = off - blk * LANES
                c0 = pl.multiple_of(blk * LANES, LANES)

                def moved(p, at):
                    zb = zbuf[zslot, t, pl.ds(r0 + p * half, half), pl.ds(c0, LANES)]
                    return pltpu.roll(zb, lax.rem(at - src + LANES, LANES), 1)

                @pl.when(item > 0)
                def _():
                    for p in range(2):
                        at = item - 1 + n_lab * seq + HALF * p
                        pick_ref[0:half, :] = jnp.where(lane == at, moved(p, at), pick_ref[0:half, :])

                @pl.when(item == 0)
                def _():
                    for p in range(2):
                        at = 2 * seq + p
                        blank[...] = jnp.where(lane == at, moved(p, at), blank[...])

            walk_list(head, nxt, j * group + t, visit)
        return c

    n_groups = n_tiles // group
    lax.fori_loop(0, n_groups, step, 0)
    emit_stats(m_ref, s_ref, pick_ref, half)
    pick_ref[half + 16:half + 24, :] = blank[...].T[0:8]
    for j in range(n_groups - 3, n_groups):
        out_copy(j).wait()


def z_oth_loop(lo, hi, join, h_ref, w_hbm, z_hbm, wbuf, wsem, zbuf, zsem, m_ref, s_ref, sections):
    group = zbuf.shape[1]
    lo, n_groups = lo // group, (hi - lo) // group
    stream = TileStream(w_hbm, wbuf, wsem, wbuf.shape[0], n_groups, lambda src, j: w_view(src, lo + j, group))
    stream.prime()

    def out_copy(j):
        slot = lax.rem(j, zbuf.shape[0])
        return pltpu.make_async_copy(zbuf.at[slot], z_view(z_hbm, lo + j, group), zsem.at[slot])

    base = 0
    join.wait()
    for n, side, make_carry in sections:
        carry = make_carry()

        def step(k, c, base=base, side=side):
            j = base + k
            slot = stream.get(j)

            @pl.when(j >= 3)
            def _():
                out_copy(j - 3).wait()

            z_group(h_ref, wbuf.at[slot], zbuf.at[lax.rem(j, zbuf.shape[0])], m_ref, s_ref)
            c = side(k, c)
            out_copy(j).start()
            return c

        last = lax.fori_loop(0, n, step, carry)
        yield last
        base += n
    for j in range(max(n_groups - 3, 0), n_groups):
        out_copy(j).wait()


class JoinRows:
    def __init__(self, h_got, h_core, h_ref, hsem):
        n = h_got.shape[0]
        core = lax.rem(lax.axis_index("tp"), 2)
        self.copies = [pltpu.make_async_copy(src, h_ref.at[pl.ds(pl.multiple_of(at * n, n), n), :], hsem.at[k])
                       for k, (src, at) in enumerate(((h_got, core), (h_core, 1 - core)))]

    def start(self):
        for c in self.copies:
            c.start()

    def wait(self):
        for c in self.copies:
            c.wait()


def z_lattice_part(lo, hi, n_lat, per_group, n_lab, before_tail, h_got, h_core, w_hbm, p0, p1, p2, p3, meta_ref,
                     z_hbm, stats_ref, occ_ref, loss_ref, m_ref, s_ref,
                     h_ref, hsem, wbuf, wsem, zbuf, zsem, e_lab, e_blk, s_lab, s_blk, r_lab, r_blk, o_t):
    join = JoinRows(h_got, h_core, h_ref, hsem)
    join.start()
    n_blk = e_lab.shape[0]
    frames = n_blk * HALF
    m_ref[...] = jnp.full(m_ref.shape, NEG_BIG, F32)
    s_ref[...] = jnp.zeros(s_ref.shape, F32)
    lane128 = lax.broadcasted_iota(jnp.int32, (LANES, LANES), 1)
    row32 = lax.broadcasted_iota(jnp.int32, (n_lab, LANES), 0)
    row8 = lax.broadcasted_iota(jnp.int32, (8, LANES), 0)
    lane32 = lax.broadcasted_iota(jnp.int32, (n_lab, LANES), 1)
    lane8 = lax.broadcasted_iota(jnp.int32, (8, LANES), 1)
    n_seq = meta_ref.shape[0]
    labs = jnp.zeros((n_lab, LANES), jnp.int32)
    lab_row = jnp.zeros((8, LANES), jnp.int32)
    live8 = jnp.zeros((8, LANES), jnp.int32)
    used8 = jnp.zeros((8, LANES), jnp.int32)
    for s in range(n_seq):
        for k in range(n_lab):
            labs = jnp.where((row32 == k) & ((lane32 == s) | (lane32 == s + n_seq)), meta_ref[s, k], labs)
            lab_row = jnp.where((row8 == s) & (lane8 == k), meta_ref[s, k], lab_row)
        here = (lane8 == s) | (lane8 == s + n_seq)
        live8 = jnp.where(here, meta_ref[s, n_lab], live8)
        used8 = jnp.where(here, meta_ref[s, n_lab + 1], used8)
    live32 = jnp.broadcast_to(live8[0:1], (n_lab, LANES))
    used32 = jnp.broadcast_to(used8[0:1], (n_lab, LANES))
    skip_dn = labs != pltpu.roll(labs, 1, 0)
    skip_up = labs != pltpu.roll(labs, n_lab - 1, 0)
    end_lab = row32 == used32 - 1
    end_blk = row32 == used32
    end_top = (row8 == 0) & (used8 == n_lab)
    shift0 = jnp.zeros((1, LANES), F32)
    seq1 = lane8[0:1] >= HALF
    half_len = jnp.where(seq1, meta_ref[1, n_lab], meta_ref[0, n_lab])
    half = frames // 2
    packed = functools.reduce(jnp.add, [p[0:half, :] for p in (p0, p1, p2, p3)])
    blanks = functools.reduce(jnp.add, [p[half + 16:half + 24, :] for p in (p0, p1, p2, p3)])
    for j in range(n_blk):
        far, near = j // 2, HALF * (j % 2)
        part = packed[near:near + HALF]
        x = jnp.concatenate([pltpu.roll(part, (LANES - HALF * far - n_lab * q) % LANES, 1) for q in range(2)], axis=0).T[0:n_lab]
        rows_b = [pltpu.roll(blanks, (HALF * q - near) % LANES, 1)[2 * q + far:2 * q + far + 1] for q in range(2)]
        x_blank = jnp.where(seq1, rows_b[1], rows_b[0])
        top = jnp.maximum(jnp.max(x, **DOWN), x_blank)
        e_blk[j] = jnp.broadcast_to((x_blank - top) * LOG2E, (8, LANES))
        e_lab[j] = (x - top) * LOG2E
        shift0 = shift0 + jnp.where(lax.rem(lane8[0:1], HALF) + HALF * j < half_len, top, 0.0)
    shift_seq0 = jnp.sum(jnp.where(seq1, 0.0, shift0), **ALONG)
    shift_seq1 = jnp.sum(jnp.where(seq1, shift0, 0.0), **ALONG)

    def lse2(a, b):
        hi_v = jnp.maximum(a, b)
        return hi_v + jnp.log2(1.0 + jnp.exp2(jnp.minimum(a, b) - hi_v))

    def lse3(a, b, c):
        hi_v = jnp.maximum(a, b)
        lo_v = jnp.minimum(a, b)
        top = jnp.maximum(hi_v, c)
        mid = jnp.minimum(hi_v, c)
        return top + jnp.log2(1.0 + (jnp.exp2(lo_v - top) + jnp.exp2(mid - top)))

    fwd8, fwd32 = lane8 < n_seq, lane32 < n_seq
    ahead8 = fwd8 & (row8 == 0)
    behind8 = (lane8 >= n_seq) & (row8 == 7)
    base8 = jnp.where(fwd8, HALF * lane8, HALF * (lane8 - n_seq) + HALF - 1)
    base8 = jnp.where(lane8 < 2 * n_seq, base8, HALF)
    skip = jnp.where(fwd32, jnp.where(skip_dn & (row32 > 0), 1, 0), jnp.where(skip_up & (row32 < n_lab - 1), 1, 0)) > 0

    def lanes_of(x, idx):
        return jnp.take_along_axis(x, idx, axis=1, mode="promise_in_bounds")

    def tall(x):
        return jnp.concatenate([x] * (n_lab // 8), axis=0)

    neg32 = jnp.full((n_lab, LANES), NEG_BIG, F32)
    first_b = jnp.where(fwd32, jnp.where(row32 == 0, 0.0, NEG_BIG), jnp.where(end_blk, 0.0, NEG_BIG))
    first_t = jnp.where(fwd8, NEG_BIG, jnp.where(end_top, 0.0, NEG_BIG))

    def lat_step(i, j, u, carry):
        lab, blk, top_b = carry
        idx8 = base8 + jnp.where(fwd8, u, -u)
        idx32 = tall(idx8)
        back = n_blk - 1 - j
        e_l = jnp.where(fwd32, lanes_of(e_lab[j], idx32), lanes_of(e_lab[back], idx32))
        e_b = jnp.where(fwd8, lanes_of(e_blk[j], idx8), lanes_of(e_blk[back], idx8))
        lab_dn = pltpu.roll(lab, 1, 0)
        lab_up = pltpu.roll(lab, n_lab - 1, 0)
        blk_side = jnp.where(fwd32, blk, pltpu.roll(blk, n_lab - 1, 0))
        blk_side = jnp.concatenate([blk_side[:n_lab - 8], jnp.where(behind8, jnp.broadcast_to(top_b[0:1], (8, LANES)), blk_side[n_lab - 8:])], axis=0)
        lab_side = jnp.where(fwd32, lab_dn, lab)
        lab_side = jnp.concatenate([jnp.where(ahead8, NEG_BIG, lab_side[:8]), lab_side[8:]], axis=0)
        new_l = lse3(lab, blk_side, jnp.where(skip, jnp.where(fwd32, lab_dn, lab_up), NEG_BIG))
        new_b = lse2(blk, lab_side)
        new_t = lse2(top_b, jnp.where(ahead8, lab_dn[:8], NEG_BIG))
        s_lab[i] = new_l
        s_blk[i, 0:n_lab] = new_b
        s_blk[i, n_lab:n_lab + 8] = new_t
        behind = frames - 1 - i + pad
        r_lab[behind] = pltpu.roll(new_l, LANES - n_seq, 1)
        r_blk[behind, 0:n_lab] = pltpu.roll(new_b, LANES - n_seq, 1)
        r_blk[behind, n_lab:n_lab + 8] = pltpu.roll(new_t, LANES - n_seq, 1)
        at8 = jnp.where(fwd8, i, frames - 1 - i)
        live = tall(at8) < live32
        lab = jnp.where(live, e_l + new_l, lab)
        blk = jnp.where(live, tall(e_b) + new_b, blk)
        top_b = jnp.where(at8 < live8, e_b + new_t, top_b)
        return lab, blk, top_b

    group = zbuf.shape[1]
    n_lat_groups = n_lat // group
    pad = s_lab.shape[0] - frames

    def lattice_side(k, carry):
        for u in range(per_group):
            i = k * per_group + u
            j = lax.min(lax.div(i, HALF), n_blk - 1)
            carry = lat_step(i, j, lax.rem(i, HALF), carry)
        return carry

    n_occ = (hi - lo - n_lat) // group
    occ_group = frames // n_occ // HALF
    seq_of8 = jnp.where(lane8 >= HALF, 1, 0)
    run = z_oth_loop(lo, hi, join, h_ref, w_hbm, z_hbm, wbuf, wsem, zbuf, zsem, m_ref, s_ref,
                     [(n_lat_groups, lattice_side, lambda: (neg32, first_b, first_t)),
                      (n_occ, lambda k, c: occ_side(k, c), lambda: 0)])
    al, ab, at = next(run)

    lasts = [jnp.where(end, v, NEG_BIG) for end, v in ((end_lab, al), (end_blk, ab), (end_top, at))]
    top = functools.reduce(jnp.maximum, [jnp.max(v, **DOWN) for v in lasts])
    total = functools.reduce(jnp.add, [jnp.sum(jnp.exp2(v - top), **DOWN) for v in lasts])
    loss = -(top + jnp.log2(total))
    loss_at = lanes_of(jnp.broadcast_to(loss, (8, LANES)), seq_of8)
    lane1 = lane8[0:1]
    loss_ref[...] = jnp.broadcast_to(loss * (1.0 / LOG2E) - jnp.where(lane1 == 0, shift_seq0, jnp.where(lane1 == 1, shift_seq1, 0.0)), (8, LANES))

    def occ_side(k, c):
        for g in range(occ_group):
            j = k * occ_group + g
            seq_of32 = tall(seq_of8)
            logs = [neg32, neg32, neg32[0:8]]
            for u in range(HALF):
                i = j * HALF + u
                here8 = lax.rem(lane8, HALF) == u
                here32 = lax.rem(lane32, HALF) == u
                sum_l = s_lab[i] + r_lab[i + pad]
                sum_b = s_blk[i] + r_blk[i + pad]
                logs[0] = jnp.where(here32, lanes_of(sum_l, seq_of32), logs[0])
                logs[1] = jnp.where(here32, lanes_of(sum_b[:n_lab], seq_of32), logs[1])
                logs[2] = jnp.where(here8, lanes_of(sum_b[n_lab:], seq_of8), logs[2])
            rest = e_blk[j] + loss_at
            live = lax.rem(lane8, HALF) + HALF * j < jnp.broadcast_to(half_len, (8, LANES))
            occ_l = jnp.exp2(logs[0] + e_lab[j] + tall(loss_at))
            occ_b = jnp.sum(jnp.exp2(logs[1] + tall(rest)), **DOWN) + jnp.exp2(logs[2] + rest)[0:1]
            o_t[j, 0:n_lab] = jnp.where(tall(jnp.where(live, 1, 0)) > 0, occ_l, 0.0)
            o_t[j, n_lab:n_lab + 8] = jnp.where(live, jnp.broadcast_to(occ_b, (8, LANES)), 0.0)
            o_t[j, 8 + n_lab:LANES] = jnp.zeros((LANES - 8 - n_lab, LANES), F32)
        return c

    next(run)
    before_tail()
    for _ in run:
        pass
    emit_stats(m_ref, s_ref, stats_ref, 0)
    row128 = lax.broadcasted_iota(jnp.int32, (LANES, LANES), 0)
    same = []
    for s in range(n_seq):
        down = jnp.full((n_lab, LANES), -1, jnp.int32)
        for k in range(n_lab):
            down = jnp.where(row32 == k, meta_ref[s, k], down)
        down = jnp.concatenate([down, jnp.full((LANES - n_lab, LANES), -1, jnp.int32)], axis=0)
        across = pltpu.roll(jnp.broadcast_to(lab_row[s:s + 1], (LANES, LANES)), HALF * s, 1)
        own = lane128 - HALF * s
        inner = (row128 < n_lab) & (own >= 0) & (own < n_lab)
        same.append(jnp.where((inner & (down == across)) | ((row128 == own) & (own < HALF)), 1.0, 0.0))
    for j in range(n_blk):
        y = o_t[j].T
        occ_ref[HALF * j:HALF * (j + 1), :] = functools.reduce(jnp.add, [
            jnp.dot(y[HALF * q:HALF * (q + 1), :], same[q], precision=lax.Precision.HIGHEST, preferred_element_type=F32) for q in range(n_seq)])


def spread_lse(refs, base, meta_ref, lse_ref, r0, frames):
    m = functools.reduce(jnp.maximum, [r[base:base + 8, :] for r in refs])
    tot = functools.reduce(jnp.add, [r[base + 8:base + 16, :] * jnp.exp(r[base:base + 8, :] - m) for r in refs])
    lse = m + jnp.log(tot)
    t = lax.broadcasted_iota(jnp.int32, (LANES, LANES), 0)
    n_part = frames // LANES
    sums = []
    for q in range(meta_ref.shape[0]):
        live_sum = jnp.zeros((1, LANES), F32)
        for p in range(n_part):
            at = q * n_part + p
            part = jnp.broadcast_to(lse[at:at + 1, :], (LANES, LANES)).T
            live = t + p * LANES < meta_ref[q, meta_ref.shape[1] - 2]
            lse_ref[r0 + at * LANES:r0 + (at + 1) * LANES, :] = jnp.where(live, part, 1.0e30)
            live_sum = live_sum + jnp.sum(jnp.where(live, part, 0.0), **DOWN)
        sums.append(live_sum)
    return sums


def patch_tile(n_slots, frames, meta_refs, col_start, j, i, z_block, lse_ref, occ_ref, g_ref, g_col, lane):
    seq, item = i // n_slots, lax.rem(i, n_slots)
    off = label_col(meta_refs, i) - col_start - j * TILE
    blk = off // LANES
    r0 = pl.multiple_of(seq * frames, frames)
    c0 = pl.multiple_of(blk * LANES, LANES)
    zb = z_block(seq, c0)
    slot_lane = jnp.where(item == 0, n_slots - 1, item - 1) + HALF * seq
    occ = jnp.sum(jnp.where(lane == slot_lane, occ_ref[...], 0.0), **ALONG)
    fresh = jnp.exp(zb - lse_ref[pl.ds(r0, frames), :]) - occ
    gc = pl.multiple_of(g_col + c0, LANES)
    old = g_ref[pl.ds(r0, frames), pl.ds(gc, LANES)].astype(F32)
    g_ref[pl.ds(r0, frames), pl.ds(gc, LANES)] = jnp.where(lane == off - blk * LANES, fresh, old).astype(BF16)


def softmax_unit(z, z_row, lse_ref, out, r0, n, c0):
    total = None
    for b in range(n // 32):
        lse = lse_ref[r0 + 32 * b:r0 + 32 * (b + 1), :]
        for k in range(TILE // LANES):
            e = jnp.exp(z[z_row + 32 * b:z_row + 32 * (b + 1), k * LANES:(k + 1) * LANES] - lse)
            out[r0 + 32 * b:r0 + 32 * (b + 1), c0 + k * LANES:c0 + (k + 1) * LANES] = e.astype(BF16)
            total = e if total is None else total + e
    return exact_zero(total)


def grad_h_part(n_slots, z_hbm, w_hbm, st0, st1, st2, st3, occ_ref, part_loss, meta_ref, keep_ref, send_ref, loss_ref, g_hbm,
                  wbuf, wsem, zbuf, zsem, acc, lse_ref, g0, g1, gsem, head, nxt):
    n_tiles, rows = z_hbm.shape[0], z_hbm.shape[1]
    frames = rows // meta_ref.shape[0]
    meta_refs = [meta_ref]
    group = zbuf.shape[1]
    n_groups = n_tiles // group
    stream = TileStream(w_hbm, wbuf, wsem, wbuf.shape[0], n_groups, lambda src, j: w_view(src, j, group))
    zs = TileStream(z_hbm, zbuf, zsem, zbuf.shape[0], n_groups, lambda src, j: z_view(src, j, group))
    zs.prime()
    yield stream.prime
    col_start = build_lists(meta_refs, n_tiles * TILE, head, nxt)
    sums = spread_lse([st0, st1, st2, st3], frames // 2, meta_ref, lse_ref, 0, frames)
    lane1 = lax.broadcasted_iota(jnp.int32, (8, LANES), 1)
    loss_ref[...] = part_loss[...] + jnp.where(lane1 == 0, sums[0], sums[1])
    lane = lax.broadcasted_iota(jnp.int32, (frames, LANES), 1)

    def patch(j, slot, g):
        for t in range(group):
            def z_block(seq, c0, t=t):
                return zbuf[slot, t, pl.ds(pl.multiple_of(seq * frames, frames), frames), pl.ds(c0, LANES)]

            walk_list(head, nxt, j * group + t,
                      lambda i, t=t, z_block=z_block: patch_tile(n_slots, frames, meta_refs, col_start, j * group + t, i, z_block, lse_ref, occ_ref, g, t * TILE, lane))

    def make_g(slot, u, g):
        t, r = u // 2, u % 2
        return softmax_unit(zbuf.at[slot, t], r * rows // 2, lse_ref, g, r * rows // 2, rows // 2, t * TILE)

    acc[...] = jnp.zeros(acc.shape, F32)
    slot0 = zs.get(0)
    for u in range(2 * group):
        make_g(slot0, u, g0)
    patch(0, slot0, g0)
    n_units = acc.shape[0] // 256

    def g_copy(j, g, k):
        return pltpu.make_async_copy(g, g_hbm.at[j], gsem.at[k])

    def half(j, g_now, g_next, k):
        slot = stream.get(j)
        nj = lax.min(j + 1, n_groups - 1)

        @pl.when(j + 1 < n_groups)
        def _():
            zs.get(nj)

        @pl.when(j >= 1)
        def _():
            g_copy(j - 1, g_next, 1 - k).wait()

        g_copy(j, g_now, k).start()

        zslot = lax.rem(nj, zbuf.shape[0])
        zero = None
        for u in range(n_units):
            d_rows = slice(u * 256, (u + 1) * 256)
            lhs = after(wbuf[slot, d_rows, :], zero)
            acc[d_rows, :] += lax.dot_general(lhs, g_now[...], (((1,), (1,)), ((), ())), preferred_element_type=F32)
            if u < 2 * group:
                zero = make_g(zslot, u, g_next)
        patch(nj, zslot, g_next)

    def step(i, c):
        half(2 * i, g0, g1, 0)
        half(2 * i + 1, g1, g0, 1)
        return c

    lax.fori_loop(0, n_groups // 2, step, 0)
    g_copy(n_groups - 1, g1, 1).wait()
    core = lax.rem(lax.axis_index("tp"), 2)
    n = rows // 2
    keep_ref[...] = acc[:, pl.ds(pl.multiple_of(core * n, n), n)].T
    send_ref[...] = acc[:, pl.ds(pl.multiple_of((1 - core) * n, n), n)].T


def mid_kernel(lo, hi, n_lat, per_group, n_lab, h_got, h_core, w_hbm, p0, p1, p2, p3, z_own, meta_ref,
               z_hbm, stats_ref, occ_ref, keep_ref, send_ref, loss_ref, g_hbm,
               part_loss, m_ref, s_ref, h_ref, hsem, wbuf, wsem, zbuf, zsem, e_lab, e_blk, s_lab, s_blk, r_lab, r_blk, o_t,
               zin_buf, zin_sem, acc, lse_ref, g0, g1, gsem, head, nxt):
    second = grad_h_part(n_lab + 1, z_own, w_hbm, p0, p1, p2, p3, occ_ref, part_loss, meta_ref, keep_ref, send_ref, loss_ref, g_hbm,
                         wbuf, wsem, zin_buf, zin_sem, acc, lse_ref, g0, g1, gsem, head, nxt)
    prime_w = next(second)
    z_lattice_part(lo, hi, n_lat, per_group, n_lab, prime_w, h_got, h_core, w_hbm, p0, p1, p2, p3, meta_ref,
                   z_hbm, stats_ref, occ_ref, part_loss, m_ref, s_ref,
                   h_ref, hsem, wbuf, wsem, zbuf, zsem, e_lab, e_blk, s_lab, s_blk, r_lab, r_blk, o_t)
    for _ in second:
        pass


def grad_w_kernel(n_slots, g_hbm, z_hbm, h_own_hbm, h_got, h_core, st0, st1, st2, st3, occ_ref, meta_ref, gw_hbm,
                  h_ref, hsem, h_own_ref, zbuf, zsem, gsem, obuf, osem, ht, lse_ref, g0, g1, head, nxt):
    n_tiles, rows = z_hbm.shape[0], z_hbm.shape[1]
    frames = rows // meta_ref.shape[0]
    d_loc = ht.shape[0]
    group = zbuf.shape[1]
    n_groups = n_tiles // group
    zs = TileStream(z_hbm, zbuf, zsem, zbuf.shape[0], n_groups, lambda src, j: z_view(src, j, group))

    def g_copy(j, g, k):
        return pltpu.make_async_copy(g_hbm.at[j], g.at[0:rows, :], gsem.at[k])

    join = JoinRows(h_got, h_core, h_ref, hsem)
    own_copy = pltpu.make_async_copy(h_own_hbm, h_own_ref, hsem.at[2])
    own_copy.start()
    join.start()
    zs.prime()
    g_copy(0, g0, 0).start()
    col_start = build_lists([meta_ref], n_tiles * TILE, head, nxt)
    d0 = pl.multiple_of(lax.axis_index("dp") * d_loc, LANES)
    own_copy.wait()
    ht[:, 0:rows] = h_own_ref[:, pl.ds(d0, d_loc)].T
    spread_lse([st0, st1, st2, st3], 0, meta_ref, lse_ref, 0, frames)
    join.wait()
    ht[:, rows:2 * rows] = h_ref[:, pl.ds(d0, d_loc)].T
    lane = lax.broadcasted_iota(jnp.int32, (frames, LANES), 1)
    n_units = 2 * group

    def make_g(slot, u, g):
        t, r = u // 2, u % 2
        return softmax_unit(zbuf.at[slot, t], r * rows // 2, lse_ref, g.at[rows:2 * rows, :], r * rows // 2, rows // 2, t * TILE)

    def patch(j, slot, g):
        for t in range(group):
            def z_block(seq, c0, t=t):
                return zbuf[slot, t, pl.ds(pl.multiple_of(seq * frames, frames), frames), pl.ds(c0, LANES)]

            walk_list(head, nxt, j * group + t,
                      lambda i, t=t, z_block=z_block: patch_tile(n_slots, frames, [meta_ref], col_start, j * group + t, i, z_block, lse_ref, occ_ref, g.at[rows:2 * rows, :], t * TILE, lane))

    def out_copy(j):
        slot = lax.rem(j, obuf.shape[0])
        return pltpu.make_async_copy(obuf.at[slot], w_view(gw_hbm, j, group), osem.at[slot])

    slot0 = zs.get(0)
    for u in range(n_units):
        make_g(slot0, u, g0)
    patch(0, slot0, g0)
    d_half = d_loc // 2
    n_out = obuf.shape[0]

    def half(j, g_now, g_next, k):
        @pl.when(j >= n_out)
        def _():
            out_copy(j - n_out).wait()

        nj = lax.min(j + 1, n_groups - 1)

        @pl.when(j + 1 < n_groups)
        def _():
            zs.get(nj)
            g_copy(nj, g_next, 1 - k).start()

        g_copy(j, g_now, k).wait()
        slot = lax.rem(nj, zbuf.shape[0])
        oslot = lax.rem(j, obuf.shape[0])
        zero = None
        for u in range(n_units):
            t, r = u // 2, u % 2
            d_rows = slice(r * d_half, (r + 1) * d_half)
            lhs = after(ht[d_rows, :], zero)
            obuf[oslot, d_rows, t * TILE:(t + 1) * TILE] = jnp.dot(lhs, g_now[:, t * TILE:(t + 1) * TILE], preferred_element_type=F32)
            zero = make_g(slot, u, g_next)
        out_copy(j).start()
        patch(nj, slot, g_next)

    def step(i, c):
        half(2 * i, g0, g1, 0)
        half(2 * i + 1, g1, g0, 1)
        return c

    lax.fori_loop(0, n_groups // 2, step, 0)
    for j in range(n_groups - n_out, n_groups):
        out_copy(j).wait()


def cost(flops, nbytes):
    return pl.CostEstimate(flops=flops, bytes_accessed=nbytes, transcendentals=0)


def solution(mesh):
    batch_axes = ("part", "dp")
    n_tp = mesh.shape["tp"]
    n_dp = mesh.shape["dp"]
    dp_swap = [(i, n_dp - 1 - i) for i in range(n_dp)]

    others = range(1, n_tp)

    def tp_xor(x, mask):
        return lax.ppermute(x, "tp", [(i, i ^ mask) for i in range(n_tp)])

    def in_hbm(x):
        return pltpu.with_memory_space_constraint(x, pltpu.HBM)

    def swap_dp(x):
        return lax.ppermute(x, "dp", dp_swap)

    def local_body(hidden, w_loc, labels, in_len, lab_len):
        batch_loc, frames, model_dim = hidden.shape
        vocab_loc = w_loc.shape[1]
        n_lab = labels.shape[1]
        n_slots = n_lab + 1
        rows = batch_loc * frames
        n_tiles = vocab_loc // TILE
        d_loc = model_dim // n_dp
        dma = pltpu.SemaphoreType.DMA
        i32 = jnp.int32
        out_slots = 4
        n_lat, lat_steps, lat_pad = 24, 22, 8
        h_own = hidden.reshape(rows, model_dim)
        core = lax.rem(lax.axis_index("tp"), 2)
        h_half = lax.dynamic_index_in_dim(h_own.reshape(2, rows // 2, model_dim), core, 0, keepdims=False)
        h_got = swap_dp(h_half)
        flops = 2 * rows * model_dim * TILE
        wbytes = model_dim * TILE * 2
        zbytes = rows * TILE * 4
        z_type = jax.ShapeDtypeStruct((n_tiles, rows, TILE), F32)
        pick_type = jax.ShapeDtypeStruct((frames // 2 + 24, LANES), F32)
        meta_type = jax.ShapeDtypeStruct((batch_loc, n_slots + 1), i32)
        g_type = jax.ShapeDtypeStruct((n_tiles // 2, rows, 2 * TILE), BF16)
        stat_type = jax.ShapeDtypeStruct((16, LANES), F32)
        g_scratch = [pltpu.VMEM((rows, 2 * TILE), BF16)] * 2

        def w_scratch(n, slots):
            return [pltpu.VMEM((slots, model_dim, n * TILE), BF16), dma((slots,))]

        def z_scratch(n, slots=3):
            return [pltpu.VMEM((slots, n, rows, TILE), F32), dma((slots,))]

        h_scratch = [pltpu.VMEM((rows, model_dim), BF16), dma((3,))]
        run_scratch = [pltpu.VMEM((rows, LANES), F32), pltpu.VMEM((rows, LANES), F32)]

        def lists(n_sets):
            return [pltpu.SMEM((n_tiles,), i32), pltpu.SMEM((n_sets * batch_loc * n_slots,), i32)]

        z_own, pick, meta = kernel_call(
            functools.partial(z_own_kernel, n_slots),
            out_shape=(z_type, pick_type, meta_type),
            in_specs=[any_spec(), any_spec(), smem_spec(), smem_spec(), smem_spec()],
            out_specs=(any_spec(), vmem_spec(), smem_spec()),
            scratch_shapes=h_scratch + w_scratch(4, 4) + z_scratch(4) + run_scratch + [pltpu.VMEM((frames // 2, LANES), F32)] + lists(1),
            compiler_params=params(),
            cost_estimate=cost(n_tiles * flops, n_tiles * (wbytes + zbytes)),
        )(in_hbm(h_own), w_loc, labels, in_len, lab_len)

        h_got, pick = lax.optimization_barrier((h_got, pick))
        h_core = in_hbm(tp_xor(h_got, 1))
        h_got = in_hbm(h_got)
        picks = [pick] + [tp_xor(pick, k) for k in others]

        n_blk = frames // HALF
        half_type = jax.ShapeDtypeStruct((rows // 2, model_dim), F32)
        occ_type = jax.ShapeDtypeStruct((frames, LANES), F32)
        loss_type = jax.ShapeDtypeStruct((8, LANES), F32)
        z_oth, stats_oth, occ, keep, send, loss, g_own = kernel_call(
            functools.partial(mid_kernel, 0, n_tiles, n_lat, lat_steps, n_lab),
            out_shape=(z_type, stat_type, occ_type, half_type, half_type, loss_type, g_type),
            in_specs=[any_spec()] * 3 + [vmem_spec()] * 4 + [any_spec(), smem_spec()],
            out_specs=(any_spec(),) + (vmem_spec(),) * 5 + (any_spec(),),
            scratch_shapes=[pltpu.VMEM((8, LANES), F32)] + run_scratch + h_scratch + w_scratch(2, 5) + z_scratch(2) + [
                pltpu.VMEM((n_blk, n_lab, LANES), F32), pltpu.VMEM((n_blk, 8, LANES), F32),
                *[pltpu.VMEM((frames + lat_pad, n, LANES), F32) for n in (n_lab, n_lab + 8) * 2],
                pltpu.VMEM((n_blk, LANES, LANES), F32)] + z_scratch(2, 4) + [
                pltpu.VMEM((model_dim, rows), F32), pltpu.VMEM((rows, LANES), F32)] + g_scratch + [dma((2,))] + lists(1),
            compiler_params=params(),
            cost_estimate=cost((2 * n_tiles) * flops, (2 * n_tiles) * (wbytes + zbytes)),
        )(h_got, h_core, w_loc, *picks, z_own, meta)
        st_oth = [stats_oth] + [tp_xor(stats_oth, k) for k in others]
        occ_oth = swap_dp(occ)
        meta_oth = swap_dp(meta)
        recv = tp_xor(send, 1)
        chip_sum = keep + recv
        across = tp_xor(chip_sum, 2)

        grad_weight = kernel_call(
            functools.partial(grad_w_kernel, n_slots),
            out_shape=jax.ShapeDtypeStruct((d_loc, vocab_loc), F32),
            in_specs=[any_spec()] * 5 + [vmem_spec()] * 5 + [smem_spec()],
            out_specs=any_spec(),
            scratch_shapes=h_scratch + [h_scratch[0]] + z_scratch(2, 5) + [
                dma((2,)), pltpu.VMEM((out_slots, d_loc, 2 * TILE), F32), dma((out_slots,)),
                pltpu.VMEM((d_loc, 2 * rows), BF16), pltpu.VMEM((rows, LANES), F32),
                pltpu.VMEM((2 * rows, 2 * TILE), BF16), pltpu.VMEM((2 * rows, 2 * TILE), BF16)] + lists(1),
            compiler_params=params(),
            cost_estimate=cost(n_tiles * flops, n_tiles * (2 * zbytes + d_loc * TILE * 4)),
        )(g_own, z_oth, in_hbm(h_own), h_got, h_core, *st_oth, occ_oth, meta_oth)

        chip_sum, grad_weight = lax.optimization_barrier((chip_sum, grad_weight))
        full_half = chip_sum + across
        other_half = tp_xor(full_half, 1)
        grad_hidden = jnp.where(core == 0, jnp.stack([full_half, other_half]), jnp.stack([other_half, full_half])).reshape(batch_loc, frames, model_dim)
        return loss[0, :batch_loc], grad_weight, grad_hidden


    return jax.shard_map(
        local_body,
        mesh=mesh,
        in_specs=(P(batch_axes, None, None), P(None, "tp"), P(batch_axes, None), P(batch_axes), P(batch_axes)),
        out_specs=(P(batch_axes), P(batch_axes, "tp"), P(batch_axes, None, None)),
        check_vma=False,
    )
```

```python
import functools

import jax
import jax.numpy as jnp
from jax import lax
from jax.experimental import pallas as pl
from jax.experimental.pallas import tpu as pltpu
from jax.sharding import PartitionSpec as P

NEG_BIG = -1.0e30
LOG2E = 1.4426950408889634
F32 = jnp.float32
DOWN = dict(axis=0, keepdims=True)
ALONG = dict(axis=1, keepdims=True)
BF16 = jnp.bfloat16
TILE = 512
LANES = 128
HALF = LANES // 2
MIB = 1 << 20


def vmem_spec():
    return pl.BlockSpec(memory_space=pltpu.VMEM)


def smem_spec():
    return pl.BlockSpec(memory_space=pltpu.SMEM)


def any_spec():
    return pl.BlockSpec(memory_space=pl.ANY)


def kernel_call(*args, **kw):
    return pl.pallas_call(*args, **kw)


def params():
    return pltpu.CompilerParams(vmem_limit_bytes=56 * MIB)


def label_col(meta_refs, i):
    n_slots = meta_refs[0].shape[1] - 1
    seq, item = i // n_slots, lax.rem(i, n_slots)
    n_seq = meta_refs[0].shape[0]
    at = lax.max(item - 1, 0)
    col = meta_refs[0][lax.rem(seq, n_seq), at]
    for k in range(1, len(meta_refs)):
        col = jnp.where(seq >= k * n_seq, meta_refs[k][lax.rem(seq, n_seq), at], col)
    return jnp.where(item == 0, 0, col)


def build_lists(meta_refs, vocab_loc, head, nxt):
    n_items = len(meta_refs) * meta_refs[0].shape[0] * (meta_refs[0].shape[1] - 1)
    col_start = lax.axis_index("tp") * vocab_loc
    n_tiles = vocab_loc // TILE

    def clear(i, c):
        head[i] = -1
        return c

    lax.fori_loop(0, n_tiles, clear, 0)

    def insert(i, c):
        loc = label_col(meta_refs, i) - col_start
        tile = lax.max(loc, 0) // TILE

        @pl.when((loc >= 0) & (loc < vocab_loc))
        def _():
            nxt[i] = head[tile]
            head[tile] = i

        return c

    lax.fori_loop(0, n_items, insert, 0)
    return col_start


def walk_list(head, nxt, tile, visit):
    def body(i):
        visit(i)
        return nxt[i]

    lax.while_loop(lambda i: i >= 0, body, head[tile])


class TileStream:
    def __init__(self, src, buf, sem, depth, n_tiles, view):
        self.src, self.buf, self.sem, self.depth, self.n, self.view = src, buf, sem, depth, n_tiles, view

    def copy(self, j):
        slot = lax.rem(j, self.depth)
        return pltpu.make_async_copy(self.view(self.src, j), self.buf.at[slot], self.sem.at[slot])

    def prime(self):
        for j in range(min(self.depth - 1, self.n)):
            self.copy(j).start()

    def get(self, j):
        self.copy(j).wait()

        @pl.when(j + self.depth - 1 < self.n)
        def _():
            self.copy(j + self.depth - 1).start()

        return lax.rem(j, self.depth)


def w_view(src, j, n=1):
    return src.at[:, pl.ds(pl.multiple_of(j * n * TILE, TILE), n * TILE)]


def z_view(src, j, n):
    return src.at[pl.ds(j * n, n)]


def exact_zero(total):
    return jnp.minimum(total[0:16] + total[16:32], 0.0).astype(BF16)


def after(lhs, zero):
    if zero is None:
        return lhs
    corner = lhs[0:16, 0:LANES] + zero
    return jnp.concatenate([jnp.concatenate([corner, lhs[0:16, LANES:]], axis=1), lhs[16:]], axis=0)


def unit_stats(z, m_ref, s_ref, r0):
    n_chunks = z.shape[1] // LANES
    total = None
    for b in range(z.shape[0] // 32):
        zb = [z[32 * b:32 * (b + 1), k * LANES:(k + 1) * LANES] for k in range(n_chunks)]
        rows = slice(r0 + 32 * b, r0 + 32 * (b + 1))
        m_old = m_ref[rows, :]
        m_new = functools.reduce(jnp.maximum, zb, m_old)
        s_new = s_ref[rows, :] * jnp.exp(m_old - m_new)
        for part in zb:
            s_new = s_new + jnp.exp(part - m_new)
        m_ref[rows, :] = m_new
        s_ref[rows, :] = s_new
        total = s_new if total is None else total + s_new
    return exact_zero(total)


def z_group(h_ref, w, z_out, m_ref, s_ref):
    n_tiles = z_out.shape[0]
    n = h_ref.shape[0] // 2
    zeros = []
    for t in range(n_tiles):
        for r in range(2):
            rows = slice(r * n, (r + 1) * n)
            lhs = after(h_ref[rows, :], zeros[-2] if len(zeros) >= 2 else None)
            z = jnp.dot(lhs, w[:, t * TILE:(t + 1) * TILE], preferred_element_type=F32)
            z_out[t, rows, :] = z
            zeros.append(unit_stats(z, m_ref, s_ref, r * n))


def emit_stats(m_ref, s_ref, out_ref, base):
    row_m = jnp.max(m_ref[...], **ALONG)
    row_s = jnp.sum(s_ref[...] * jnp.exp(m_ref[...] - row_m), **ALONG)
    rows = m_ref.shape[0]
    for k, v in enumerate((row_m, row_s)):
        flat = jnp.broadcast_to(v, (rows, LANES)).T
        for p in range(rows // LANES):
            at = base + 8 * k + p
            out_ref[at:at + 1, :] = flat[0:1, p * LANES:(p + 1) * LANES]


def z_own_kernel(n_slots, h_hbm, w_hbm, labels_ref, in_len_ref, lab_len_ref, z_hbm, pick_ref, meta_ref, h_ref, hsem, wbuf, wsem, zbuf, zsem, m_ref, s_ref, blank, head, nxt):
    n_tiles = z_hbm.shape[0]
    rows = h_ref.shape[0]
    n_seq = meta_ref.shape[0]
    frames = rows // n_seq
    h_copy = pltpu.make_async_copy(h_hbm, h_ref, hsem.at[0])
    h_copy.start()
    n_lab = n_slots - 1
    for q in range(n_seq):
        def put(k, c, q=q):
            meta_ref[q, k] = labels_ref[q, k]
            return c

        lax.fori_loop(0, n_lab, put, 0)
        meta_ref[q, n_lab] = in_len_ref[q]
        meta_ref[q, n_lab + 1] = lab_len_ref[q]
    group = zbuf.shape[1]
    stream = TileStream(w_hbm, wbuf, wsem, wbuf.shape[0], n_tiles // group, lambda src, j: w_view(src, j, group))
    stream.prime()
    col_start = build_lists([meta_ref], n_tiles * TILE, head, nxt)
    m_ref[...] = jnp.full(m_ref.shape, NEG_BIG, F32)
    s_ref[...] = jnp.zeros(s_ref.shape, F32)
    pick_ref[...] = jnp.zeros(pick_ref.shape, F32)
    blank[...] = jnp.zeros(blank.shape, F32)
    half = frames // 2
    h_copy.wait()
    lane = lax.broadcasted_iota(jnp.int32, (half, LANES), 1)

    def out_copy(j):
        slot = lax.rem(j, zbuf.shape[0])
        return pltpu.make_async_copy(zbuf.at[slot], z_view(z_hbm, j, group), zsem.at[slot])

    def step(j, c):
        slot = stream.get(j)

        @pl.when(j >= 3)
        def _():
            out_copy(j - 3).wait()

        zslot = lax.rem(j, zbuf.shape[0])
        z_group(h_ref, wbuf.at[slot], zbuf.at[zslot], m_ref, s_ref)
        out_copy(j).start()

        for t in range(group):
            def visit(i, t=t):
                seq, item = i // n_slots, lax.rem(i, n_slots)
                off = label_col([meta_ref], i) - col_start - (j * group + t) * TILE
                blk = off // LANES
                r0 = pl.multiple_of(seq * frames, frames)
                src = off - blk * LANES
                c0 = pl.multiple_of(blk * LANES, LANES)

                def moved(p, at):
                    zb = zbuf[zslot, t, pl.ds(r0 + p * half, half), pl.ds(c0, LANES)]
                    return pltpu.roll(zb, lax.rem(at - src + LANES, LANES), 1)

                @pl.when(item > 0)
                def _():
                    for p in range(2):
                        at = item - 1 + n_lab * seq + HALF * p
                        pick_ref[0:half, :] = jnp.where(lane == at, moved(p, at), pick_ref[0:half, :])

                @pl.when(item == 0)
                def _():
                    for p in range(2):
                        at = 2 * seq + p
                        blank[...] = jnp.where(lane == at, moved(p, at), blank[...])

            walk_list(head, nxt, j * group + t, visit)
        return c

    n_groups = n_tiles // group
    lax.fori_loop(0, n_groups, step, 0)
    emit_stats(m_ref, s_ref, pick_ref, half)
    pick_ref[half + 16:half + 24, :] = blank[...].T[0:8]
    for j in range(n_groups - 3, n_groups):
        out_copy(j).wait()


def z_oth_loop(lo, hi, join, h_ref, w_hbm, z_hbm, wbuf, wsem, zbuf, zsem, m_ref, s_ref, sections):
    group = zbuf.shape[1]
    lo, n_groups = lo // group, (hi - lo) // group
    stream = TileStream(w_hbm, wbuf, wsem, wbuf.shape[0], n_groups, lambda src, j: w_view(src, lo + j, group))
    stream.prime()

    def out_copy(j):
        slot = lax.rem(j, zbuf.shape[0])
        return pltpu.make_async_copy(zbuf.at[slot], z_view(z_hbm, lo + j, group), zsem.at[slot])

    base = 0
    join.wait()
    for n, side, make_carry in sections:
        carry = make_carry()

        def step(k, c, base=base, side=side):
            j = base + k
            slot = stream.get(j)

            @pl.when(j >= 3)
            def _():
                out_copy(j - 3).wait()

            z_group(h_ref, wbuf.at[slot], zbuf.at[lax.rem(j, zbuf.shape[0])], m_ref, s_ref)
            c = side(k, c)
            out_copy(j).start()
            return c

        last = lax.fori_loop(0, n, step, carry)
        yield last
        base += n
    for j in range(max(n_groups - 3, 0), n_groups):
        out_copy(j).wait()


def z_lattice_part(lo, hi, n_lat, per_group, n_lab, before_tail, h_oth, w_hbm, p0, p1, p2, p3, meta_ref,
                     z_hbm, stats_ref, occ_ref, loss_ref, m_ref, s_ref,
                     h_ref, hsem, wbuf, wsem, zbuf, zsem, e_lab, e_blk, s_lab, s_blk, r_lab, r_blk, o_t):
    join = pltpu.make_async_copy(h_oth, h_ref, hsem.at[0])
    join.start()
    n_blk = e_lab.shape[0]
    frames = n_blk * HALF
    m_ref[...] = jnp.full(m_ref.shape, NEG_BIG, F32)
    s_ref[...] = jnp.zeros(s_ref.shape, F32)
    lane128 = lax.broadcasted_iota(jnp.int32, (LANES, LANES), 1)
    row32 = lax.broadcasted_iota(jnp.int32, (n_lab, LANES), 0)
    row8 = lax.broadcasted_iota(jnp.int32, (8, LANES), 0)
    lane32 = lax.broadcasted_iota(jnp.int32, (n_lab, LANES), 1)
    lane8 = lax.broadcasted_iota(jnp.int32, (8, LANES), 1)
    n_seq = meta_ref.shape[0]
    labs = jnp.zeros((n_lab, LANES), jnp.int32)
    lab_row = jnp.zeros((8, LANES), jnp.int32)
    live8 = jnp.zeros((8, LANES), jnp.int32)
    used8 = jnp.zeros((8, LANES), jnp.int32)
    for s in range(n_seq):
        for k in range(n_lab):
            labs = jnp.where((row32 == k) & ((lane32 == s) | (lane32 == s + n_seq)), meta_ref[s, k], labs)
            lab_row = jnp.where((row8 == s) & (lane8 == k), meta_ref[s, k], lab_row)
        here = (lane8 == s) | (lane8 == s + n_seq)
        live8 = jnp.where(here, meta_ref[s, n_lab], live8)
        used8 = jnp.where(here, meta_ref[s, n_lab + 1], used8)
    live32 = jnp.broadcast_to(live8[0:1], (n_lab, LANES))
    used32 = jnp.broadcast_to(used8[0:1], (n_lab, LANES))
    skip_dn = labs != pltpu.roll(labs, 1, 0)
    skip_up = labs != pltpu.roll(labs, n_lab - 1, 0)
    end_lab = row32 == used32 - 1
    end_blk = row32 == used32
    end_top = (row8 == 0) & (used8 == n_lab)
    shift0 = jnp.zeros((1, LANES), F32)
    seq1 = lane8[0:1] >= HALF
    half_len = jnp.where(seq1, meta_ref[1, n_lab], meta_ref[0, n_lab])
    half = frames // 2
    packed = functools.reduce(jnp.add, [p[0:half, :] for p in (p0, p1, p2, p3)])
    blanks = functools.reduce(jnp.add, [p[half + 16:half + 24, :] for p in (p0, p1, p2, p3)])
    for j in range(n_blk):
        far, near = j // 2, HALF * (j % 2)
        part = packed[near:near + HALF]
        x = jnp.concatenate([pltpu.roll(part, (LANES - HALF * far - n_lab * q) % LANES, 1) for q in range(2)], axis=0).T[0:n_lab]
        rows_b = [pltpu.roll(blanks, (HALF * q - near) % LANES, 1)[2 * q + far:2 * q + far + 1] for q in range(2)]
        x_blank = jnp.where(seq1, rows_b[1], rows_b[0])
        top = jnp.maximum(jnp.max(x, **DOWN), x_blank)
        e_blk[j] = jnp.broadcast_to((x_blank - top) * LOG2E, (8, LANES))
        e_lab[j] = (x - top) * LOG2E
        shift0 = shift0 + jnp.where(lax.rem(lane8[0:1], HALF) + HALF * j < half_len, top, 0.0)
    shift_seq0 = jnp.sum(jnp.where(seq1, 0.0, shift0), **ALONG)
    shift_seq1 = jnp.sum(jnp.where(seq1, shift0, 0.0), **ALONG)

    def lse2(a, b):
        hi_v = jnp.maximum(a, b)
        return hi_v + jnp.log2(1.0 + jnp.exp2(jnp.minimum(a, b) - hi_v))

    def lse3(a, b, c):
        hi_v = jnp.maximum(a, b)
        lo_v = jnp.minimum(a, b)
        top = jnp.maximum(hi_v, c)
        mid = jnp.minimum(hi_v, c)
        return top + jnp.log2(1.0 + (jnp.exp2(lo_v - top) + jnp.exp2(mid - top)))

    fwd8, fwd32 = lane8 < n_seq, lane32 < n_seq
    ahead8 = fwd8 & (row8 == 0)
    behind8 = (lane8 >= n_seq) & (row8 == 7)
    base8 = jnp.where(fwd8, HALF * lane8, HALF * (lane8 - n_seq) + HALF - 1)
    base8 = jnp.where(lane8 < 2 * n_seq, base8, HALF)
    skip = jnp.where(fwd32, jnp.where(skip_dn & (row32 > 0), 1, 0), jnp.where(skip_up & (row32 < n_lab - 1), 1, 0)) > 0

    def lanes_of(x, idx):
        return jnp.take_along_axis(x, idx, axis=1, mode="promise_in_bounds")

    def tall(x):
        return jnp.concatenate([x] * (n_lab // 8), axis=0)

    neg32 = jnp.full((n_lab, LANES), NEG_BIG, F32)
    first_b = jnp.where(fwd32, jnp.where(row32 == 0, 0.0, NEG_BIG), jnp.where(end_blk, 0.0, NEG_BIG))
    first_t = jnp.where(fwd8, NEG_BIG, jnp.where(end_top, 0.0, NEG_BIG))

    def lat_step(i, j, u, carry):
        lab, blk, top_b = carry
        idx8 = base8 + jnp.where(fwd8, u, -u)
        idx32 = tall(idx8)
        back = n_blk - 1 - j
        e_l = jnp.where(fwd32, lanes_of(e_lab[j], idx32), lanes_of(e_lab[back], idx32))
        e_b = jnp.where(fwd8, lanes_of(e_blk[j], idx8), lanes_of(e_blk[back], idx8))
        lab_dn = pltpu.roll(lab, 1, 0)
        lab_up = pltpu.roll(lab, n_lab - 1, 0)
        blk_side = jnp.where(fwd32, blk, pltpu.roll(blk, n_lab - 1, 0))
        blk_side = jnp.concatenate([blk_side[:n_lab - 8], jnp.where(behind8, jnp.broadcast_to(top_b[0:1], (8, LANES)), blk_side[n_lab - 8:])], axis=0)
        lab_side = jnp.where(fwd32, lab_dn, lab)
        lab_side = jnp.concatenate([jnp.where(ahead8, NEG_BIG, lab_side[:8]), lab_side[8:]], axis=0)
        new_l = lse3(lab, blk_side, jnp.where(skip, jnp.where(fwd32, lab_dn, lab_up), NEG_BIG))
        new_b = lse2(blk, lab_side)
        new_t = lse2(top_b, jnp.where(ahead8, lab_dn[:8], NEG_BIG))
        s_lab[i] = new_l
        s_blk[i, 0:n_lab] = new_b
        s_blk[i, n_lab:n_lab + 8] = new_t
        behind = frames - 1 - i + pad
        r_lab[behind] = pltpu.roll(new_l, LANES - n_seq, 1)
        r_blk[behind, 0:n_lab] = pltpu.roll(new_b, LANES - n_seq, 1)
        r_blk[behind, n_lab:n_lab + 8] = pltpu.roll(new_t, LANES - n_seq, 1)
        at8 = jnp.where(fwd8, i, frames - 1 - i)
        live = tall(at8) < live32
        lab = jnp.where(live, e_l + new_l, lab)
        blk = jnp.where(live, tall(e_b) + new_b, blk)
        top_b = jnp.where(at8 < live8, e_b + new_t, top_b)
        return lab, blk, top_b

    group = zbuf.shape[1]
    n_lat_groups = n_lat // group
    pad = s_lab.shape[0] - frames

    def lattice_side(k, carry):
        for u in range(per_group):
            i = k * per_group + u
            j = lax.min(lax.div(i, HALF), n_blk - 1)
            carry = lat_step(i, j, lax.rem(i, HALF), carry)
        return carry

    n_occ = (hi - lo - n_lat) // group
    occ_group = frames // n_occ // HALF
    seq_of8 = jnp.where(lane8 >= HALF, 1, 0)
    run = z_oth_loop(lo, hi, join, h_ref, w_hbm, z_hbm, wbuf, wsem, zbuf, zsem, m_ref, s_ref,
                     [(n_lat_groups, lattice_side, lambda: (neg32, first_b, first_t)),
                      (n_occ, lambda k, c: occ_side(k, c), lambda: 0)])
    al, ab, at = next(run)

    lasts = [jnp.where(end, v, NEG_BIG) for end, v in ((end_lab, al), (end_blk, ab), (end_top, at))]
    top = functools.reduce(jnp.maximum, [jnp.max(v, **DOWN) for v in lasts])
    total = functools.reduce(jnp.add, [jnp.sum(jnp.exp2(v - top), **DOWN) for v in lasts])
    loss = -(top + jnp.log2(total))
    loss_at = lanes_of(jnp.broadcast_to(loss, (8, LANES)), seq_of8)
    lane1 = lane8[0:1]
    loss_ref[...] = jnp.broadcast_to(loss * (1.0 / LOG2E) - jnp.where(lane1 == 0, shift_seq0, jnp.where(lane1 == 1, shift_seq1, 0.0)), (8, LANES))

    def occ_side(k, c):
        for g in range(occ_group):
            j = k * occ_group + g
            seq_of32 = tall(seq_of8)
            logs = [neg32, neg32, neg32[0:8]]
            for u in range(HALF):
                i = j * HALF + u
                here8 = lax.rem(lane8, HALF) == u
                here32 = lax.rem(lane32, HALF) == u
                sum_l = s_lab[i] + r_lab[i + pad]
                sum_b = s_blk[i] + r_blk[i + pad]
                logs[0] = jnp.where(here32, lanes_of(sum_l, seq_of32), logs[0])
                logs[1] = jnp.where(here32, lanes_of(sum_b[:n_lab], seq_of32), logs[1])
                logs[2] = jnp.where(here8, lanes_of(sum_b[n_lab:], seq_of8), logs[2])
            rest = e_blk[j] + loss_at
            live = lax.rem(lane8, HALF) + HALF * j < jnp.broadcast_to(half_len, (8, LANES))
            occ_l = jnp.exp2(logs[0] + e_lab[j] + tall(loss_at))
            occ_b = jnp.sum(jnp.exp2(logs[1] + tall(rest)), **DOWN) + jnp.exp2(logs[2] + rest)[0:1]
            o_t[j, 0:n_lab] = jnp.where(tall(jnp.where(live, 1, 0)) > 0, occ_l, 0.0)
            o_t[j, n_lab:n_lab + 8] = jnp.where(live, jnp.broadcast_to(occ_b, (8, LANES)), 0.0)
            o_t[j, 8 + n_lab:LANES] = jnp.zeros((LANES - 8 - n_lab, LANES), F32)
        return c

    next(run)
    before_tail()
    for _ in run:
        pass
    emit_stats(m_ref, s_ref, stats_ref, 0)
    row128 = lax.broadcasted_iota(jnp.int32, (LANES, LANES), 0)
    same = []
    for s in range(n_seq):
        down = jnp.full((n_lab, LANES), -1, jnp.int32)
        for k in range(n_lab):
            down = jnp.where(row32 == k, meta_ref[s, k], down)
        down = jnp.concatenate([down, jnp.full((LANES - n_lab, LANES), -1, jnp.int32)], axis=0)
        across = pltpu.roll(jnp.broadcast_to(lab_row[s:s + 1], (LANES, LANES)), HALF * s, 1)
        own = lane128 - HALF * s
        inner = (row128 < n_lab) & (own >= 0) & (own < n_lab)
        same.append(jnp.where((inner & (down == across)) | ((row128 == own) & (own < HALF)), 1.0, 0.0))
    for j in range(n_blk):
        y = o_t[j].T
        occ_ref[HALF * j:HALF * (j + 1), :] = functools.reduce(jnp.add, [
            jnp.dot(y[HALF * q:HALF * (q + 1), :], same[q], precision=lax.Precision.HIGHEST, preferred_element_type=F32) for q in range(n_seq)])


def spread_lse(refs, base, meta_ref, lse_ref, r0, frames):
    m = functools.reduce(jnp.maximum, [r[base:base + 8, :] for r in refs])
    tot = functools.reduce(jnp.add, [r[base + 8:base + 16, :] * jnp.exp(r[base:base + 8, :] - m) for r in refs])
    lse = m + jnp.log(tot)
    t = lax.broadcasted_iota(jnp.int32, (LANES, LANES), 0)
    n_part = frames // LANES
    sums = []
    for q in range(meta_ref.shape[0]):
        live_sum = jnp.zeros((1, LANES), F32)
        for p in range(n_part):
            at = q * n_part + p
            part = jnp.broadcast_to(lse[at:at + 1, :], (LANES, LANES)).T
            live = t + p * LANES < meta_ref[q, meta_ref.shape[1] - 2]
            lse_ref[r0 + at * LANES:r0 + (at + 1) * LANES, :] = jnp.where(live, part, 1.0e30)
            live_sum = live_sum + jnp.sum(jnp.where(live, part, 0.0), **DOWN)
        sums.append(live_sum)
    return sums


def patch_tile(n_slots, frames, meta_refs, col_start, j, i, z_block, lse_ref, occ_ref, g_ref, g_col, lane):
    seq, item = i // n_slots, lax.rem(i, n_slots)
    off = label_col(meta_refs, i) - col_start - j * TILE
    blk = off // LANES
    r0 = pl.multiple_of(seq * frames, frames)
    c0 = pl.multiple_of(blk * LANES, LANES)
    zb = z_block(seq, c0)
    slot_lane = jnp.where(item == 0, n_slots - 1, item - 1) + HALF * seq
    at = off - blk * LANES
    occ = pltpu.roll(occ_ref[...], lax.rem(at - slot_lane + LANES, LANES), 1)
    fresh = jnp.exp(zb - lse_ref[pl.ds(r0, frames), :]) - occ
    gc = pl.multiple_of(g_col + c0, LANES)
    old = g_ref[pl.ds(r0, frames), pl.ds(gc, LANES)].astype(F32)
    g_ref[pl.ds(r0, frames), pl.ds(gc, LANES)] = jnp.where(lane == at, fresh, old).astype(BF16)


def softmax_unit(z, z_row, lse_ref, out, r0, n, c0):
    total = None
    for b in range(n // 32):
        lse = lse_ref[r0 + 32 * b:r0 + 32 * (b + 1), :]
        for k in range(TILE // LANES):
            e = jnp.exp(z[z_row + 32 * b:z_row + 32 * (b + 1), k * LANES:(k + 1) * LANES] - lse)
            out[r0 + 32 * b:r0 + 32 * (b + 1), c0 + k * LANES:c0 + (k + 1) * LANES] = e.astype(BF16)
            total = e if total is None else total + e
    return exact_zero(total)


def grad_h_part(n_slots, z_hbm, w_hbm, st0, st1, st2, st3, occ_ref, part_loss, meta_ref, keep_ref, send_ref, loss_ref, g_hbm,
                  wbuf, wsem, zbuf, zsem, acc, lse_ref, g0, g1, gsem, head, nxt):
    n_tiles, rows = z_hbm.shape[0], z_hbm.shape[1]
    frames = rows // meta_ref.shape[0]
    meta_refs = [meta_ref]
    group = zbuf.shape[1]
    n_groups = n_tiles // group
    stream = TileStream(w_hbm, wbuf, wsem, wbuf.shape[0], n_groups, lambda src, j: w_view(src, j, group))
    zs = TileStream(z_hbm, zbuf, zsem, zbuf.shape[0], n_groups, lambda src, j: z_view(src, j, group))
    zs.prime()
    yield stream.prime
    col_start = build_lists(meta_refs, n_tiles * TILE, head, nxt)
    sums = spread_lse([st0, st1, st2, st3], frames // 2, meta_ref, lse_ref, 0, frames)
    lane1 = lax.broadcasted_iota(jnp.int32, (8, LANES), 1)
    loss_ref[...] = part_loss[...] + jnp.where(lane1 == 0, sums[0], sums[1])
    lane = lax.broadcasted_iota(jnp.int32, (frames, LANES), 1)

    def patch(j, slot, g):
        for t in range(group):
            def z_block(seq, c0, t=t):
                return zbuf[slot, t, pl.ds(pl.multiple_of(seq * frames, frames), frames), pl.ds(c0, LANES)]

            walk_list(head, nxt, j * group + t,
                      lambda i, t=t, z_block=z_block: patch_tile(n_slots, frames, meta_refs, col_start, j * group + t, i, z_block, lse_ref, occ_ref, g, t * TILE, lane))

    def make_g(slot, u, g):
        t, r = u // 2, u % 2
        return softmax_unit(zbuf.at[slot, t], r * rows // 2, lse_ref, g, r * rows // 2, rows // 2, t * TILE)

    acc[...] = jnp.zeros(acc.shape, F32)
    slot0 = zs.get(0)
    for u in range(2 * group):
        make_g(slot0, u, g0)
    patch(0, slot0, g0)
    n_units = acc.shape[0] // 256

    def g_copy(j, g, k):
        return pltpu.make_async_copy(g, g_hbm.at[j], gsem.at[k])

    def half(j, g_now, g_next, k):
        slot = stream.get(j)
        nj = lax.min(j + 1, n_groups - 1)

        @pl.when(j + 1 < n_groups)
        def _():
            zs.get(nj)

        @pl.when(j >= 1)
        def _():
            g_copy(j - 1, g_next, 1 - k).wait()

        g_copy(j, g_now, k).start()

        zslot = lax.rem(nj, zbuf.shape[0])
        zero = None
        for u in range(n_units):
            d_rows = slice(u * 256, (u + 1) * 256)
            lhs = after(wbuf[slot, d_rows, :], zero)
            acc[d_rows, :] += lax.dot_general(lhs, g_now[...], (((1,), (1,)), ((), ())), preferred_element_type=F32)
            if u < 2 * group:
                zero = make_g(zslot, u, g_next)
        patch(nj, zslot, g_next)

    def step(i, c):
        half(2 * i, g0, g1, 0)
        half(2 * i + 1, g1, g0, 1)
        return c

    lax.fori_loop(0, n_groups // 2, step, 0)
    g_copy(n_groups - 1, g1, 1).wait()
    core = lax.rem(lax.axis_index("tp"), 2)
    n = rows // 2
    keep_ref[...] = acc[:, pl.ds(pl.multiple_of(core * n, n), n)].T
    send_ref[...] = acc[:, pl.ds(pl.multiple_of((1 - core) * n, n), n)].T


def mid_kernel(lo, hi, n_lat, per_group, n_lab, h_oth, w_hbm, p0, p1, p2, p3, z_own, meta_ref,
               z_hbm, stats_ref, occ_ref, keep_ref, send_ref, loss_ref, g_hbm,
               part_loss, m_ref, s_ref, h_ref, hsem, wbuf, wsem, zbuf, zsem, e_lab, e_blk, s_lab, s_blk, r_lab, r_blk, o_t,
               zin_buf, zin_sem, acc, lse_ref, g0, g1, gsem, head, nxt):
    second = grad_h_part(n_lab + 1, z_own, w_hbm, p0, p1, p2, p3, occ_ref, part_loss, meta_ref, keep_ref, send_ref, loss_ref, g_hbm,
                         wbuf, wsem, zin_buf, zin_sem, acc, lse_ref, g0, g1, gsem, head, nxt)
    prime_w = next(second)
    z_lattice_part(lo, hi, n_lat, per_group, n_lab, prime_w, h_oth, w_hbm, p0, p1, p2, p3, meta_ref,
                   z_hbm, stats_ref, occ_ref, part_loss, m_ref, s_ref,
                   h_ref, hsem, wbuf, wsem, zbuf, zsem, e_lab, e_blk, s_lab, s_blk, r_lab, r_blk, o_t)
    for _ in second:
        pass


def grad_w_kernel(n_slots, g_hbm, z_hbm, h_own_hbm, h_oth, st0, st1, st2, st3, occ_ref, meta_ref, gw_hbm,
                  h_ref, hsem, h_own_ref, zbuf, zsem, gsem, obuf, osem, ht, lse_ref, g0, g1, head, nxt):
    n_tiles, rows = z_hbm.shape[0], z_hbm.shape[1]
    frames = rows // meta_ref.shape[0]
    d_loc = ht.shape[0]
    group = zbuf.shape[1]
    n_groups = n_tiles // group
    zs = TileStream(z_hbm, zbuf, zsem, zbuf.shape[0], n_groups, lambda src, j: z_view(src, j, group))

    def g_copy(j, g, k):
        return pltpu.make_async_copy(g_hbm.at[j], g.at[0:rows, :], gsem.at[k])

    join = pltpu.make_async_copy(h_oth, h_ref, hsem.at[0])
    own_copy = pltpu.make_async_copy(h_own_hbm, h_own_ref, hsem.at[1])
    own_copy.start()
    join.start()
    zs.prime()
    g_copy(0, g0, 0).start()
    col_start = build_lists([meta_ref], n_tiles * TILE, head, nxt)
    d0 = pl.multiple_of(lax.axis_index("dp") * d_loc, LANES)
    own_copy.wait()
    ht[:, 0:rows] = h_own_ref[:, pl.ds(d0, d_loc)].T
    spread_lse([st0, st1, st2, st3], 0, meta_ref, lse_ref, 0, frames)
    join.wait()
    ht[:, rows:2 * rows] = h_ref[:, pl.ds(d0, d_loc)].T
    lane = lax.broadcasted_iota(jnp.int32, (frames, LANES), 1)
    n_units = 2 * group

    def make_g(slot, u, g):
        t, r = u // 2, u % 2
        return softmax_unit(zbuf.at[slot, t], r * rows // 2, lse_ref, g.at[rows:2 * rows, :], r * rows // 2, rows // 2, t * TILE)

    def patch(j, slot, g):
        for t in range(group):
            def z_block(seq, c0, t=t):
                return zbuf[slot, t, pl.ds(pl.multiple_of(seq * frames, frames), frames), pl.ds(c0, LANES)]

            walk_list(head, nxt, j * group + t,
                      lambda i, t=t, z_block=z_block: patch_tile(n_slots, frames, [meta_ref], col_start, j * group + t, i, z_block, lse_ref, occ_ref, g.at[rows:2 * rows, :], t * TILE, lane))

    def out_copy(j):
        slot = lax.rem(j, obuf.shape[0])
        return pltpu.make_async_copy(obuf.at[slot], w_view(gw_hbm, j, group), osem.at[slot])

    slot0 = zs.get(0)
    for u in range(n_units):
        make_g(slot0, u, g0)
    patch(0, slot0, g0)
    d_half = d_loc // 2

    def half(j, g_now, g_next, k):
        @pl.when(j >= 3)
        def _():
            out_copy(j - 3).wait()

        nj = lax.min(j + 1, n_groups - 1)

        @pl.when(j + 1 < n_groups)
        def _():
            zs.get(nj)
            g_copy(nj, g_next, 1 - k).start()

        g_copy(j, g_now, k).wait()
        slot = lax.rem(nj, zbuf.shape[0])
        oslot = lax.rem(j, obuf.shape[0])
        zero = None
        for u in range(n_units):
            t, r = u // 2, u % 2
            d_rows = slice(r * d_half, (r + 1) * d_half)
            lhs = after(ht[d_rows, :], zero)
            obuf[oslot, d_rows, t * TILE:(t + 1) * TILE] = jnp.dot(lhs, g_now[:, t * TILE:(t + 1) * TILE], preferred_element_type=F32)
            zero = make_g(slot, u, g_next)
        out_copy(j).start()
        patch(nj, slot, g_next)

    def step(i, c):
        half(2 * i, g0, g1, 0)
        half(2 * i + 1, g1, g0, 1)
        return c

    lax.fori_loop(0, n_groups // 2, step, 0)
    for j in range(n_groups - 3, n_groups):
        out_copy(j).wait()


def cost(flops, nbytes):
    return pl.CostEstimate(flops=flops, bytes_accessed=nbytes, transcendentals=0)


def solution(mesh):
    batch_axes = ("part", "dp")
    n_tp = mesh.shape["tp"]
    n_dp = mesh.shape["dp"]
    dp_swap = [(i, n_dp - 1 - i) for i in range(n_dp)]

    others = range(1, n_tp)

    def tp_xor(x, mask):
        return lax.ppermute(x, "tp", [(i, i ^ mask) for i in range(n_tp)])

    def in_hbm(x):
        return pltpu.with_memory_space_constraint(x, pltpu.HBM)

    def swap_dp(x):
        return lax.ppermute(x, "dp", dp_swap)

    def local_body(hidden, w_loc, labels, in_len, lab_len):
        batch_loc, frames, model_dim = hidden.shape
        vocab_loc = w_loc.shape[1]
        n_lab = labels.shape[1]
        n_slots = n_lab + 1
        rows = batch_loc * frames
        n_tiles = vocab_loc // TILE
        d_loc = model_dim // n_dp
        dma = pltpu.SemaphoreType.DMA
        i32 = jnp.int32
        n_lat, lat_steps, lat_pad = 24, 22, 8
        h_own = hidden.reshape(rows, model_dim)
        core = lax.rem(lax.axis_index("tp"), 2)
        h_oth = swap_dp(h_own)
        flops = 2 * rows * model_dim * TILE
        wbytes = model_dim * TILE * 2
        zbytes = rows * TILE * 4
        z_type = jax.ShapeDtypeStruct((n_tiles, rows, TILE), F32)
        pick_type = jax.ShapeDtypeStruct((frames // 2 + 24, LANES), F32)
        meta_type = jax.ShapeDtypeStruct((batch_loc, n_slots + 1), i32)
        g_type = jax.ShapeDtypeStruct((n_tiles // 2, rows, 2 * TILE), BF16)
        stat_type = jax.ShapeDtypeStruct((16, LANES), F32)
        g_scratch = [pltpu.VMEM((rows, 2 * TILE), BF16)] * 2

        def w_scratch(n):
            return [pltpu.VMEM((3, model_dim, n * TILE), BF16), dma((3,))]

        def z_scratch(n):
            return [pltpu.VMEM((3, n, rows, TILE), F32), dma((3,))]

        h_scratch = [pltpu.VMEM((rows, model_dim), BF16), dma((2,))]
        run_scratch = [pltpu.VMEM((rows, LANES), F32), pltpu.VMEM((rows, LANES), F32)]

        def lists(n_sets):
            return [pltpu.SMEM((n_tiles,), i32), pltpu.SMEM((n_sets * batch_loc * n_slots,), i32)]

        z_own, pick, meta = kernel_call(
            functools.partial(z_own_kernel, n_slots),
            out_shape=(z_type, pick_type, meta_type),
            in_specs=[any_spec(), any_spec(), smem_spec(), smem_spec(), smem_spec()],
            out_specs=(any_spec(), vmem_spec(), smem_spec()),
            scratch_shapes=h_scratch + w_scratch(4) + z_scratch(4) + run_scratch + [pltpu.VMEM((frames // 2, LANES), F32)] + lists(1),
            compiler_params=params(),
            cost_estimate=cost(n_tiles * flops, n_tiles * (wbytes + zbytes)),
        )(in_hbm(h_own), w_loc, labels, in_len, lab_len)

        h_oth = in_hbm(h_oth)
        picks = [pick] + [tp_xor(pick, k) for k in others]

        n_blk = frames // HALF
        half_type = jax.ShapeDtypeStruct((rows // 2, model_dim), F32)
        occ_type = jax.ShapeDtypeStruct((frames, LANES), F32)
        loss_type = jax.ShapeDtypeStruct((8, LANES), F32)
        z_oth, stats_oth, occ, keep, send, loss, g_own = kernel_call(
            functools.partial(mid_kernel, 0, n_tiles, n_lat, lat_steps, n_lab),
            out_shape=(z_type, stat_type, occ_type, half_type, half_type, loss_type, g_type),
            in_specs=[any_spec()] * 2 + [vmem_spec()] * 4 + [any_spec(), smem_spec()],
            out_specs=(any_spec(),) + (vmem_spec(),) * 5 + (any_spec(),),
            scratch_shapes=[pltpu.VMEM((8, LANES), F32)] + run_scratch + h_scratch + w_scratch(2) + z_scratch(2) + [
                pltpu.VMEM((n_blk, n_lab, LANES), F32), pltpu.VMEM((n_blk, 8, LANES), F32),
                *[pltpu.VMEM((frames + lat_pad, n, LANES), F32) for n in (n_lab, n_lab + 8) * 2],
                pltpu.VMEM((n_blk, LANES, LANES), F32)] + z_scratch(2) + [
                pltpu.VMEM((model_dim, rows), F32), pltpu.VMEM((rows, LANES), F32)] + g_scratch + [dma((2,))] + lists(1),
            compiler_params=params(),
            cost_estimate=cost((2 * n_tiles) * flops, (2 * n_tiles) * (wbytes + zbytes)),
        )(h_oth, w_loc, *picks, z_own, meta)
        st_oth = [stats_oth] + [tp_xor(stats_oth, k) for k in others]
        occ_oth = swap_dp(occ)
        meta_oth = swap_dp(meta)
        recv = tp_xor(send, 1)
        chip_sum = keep + recv
        across = tp_xor(chip_sum, 2)

        grad_weight = kernel_call(
            functools.partial(grad_w_kernel, n_slots),
            out_shape=jax.ShapeDtypeStruct((d_loc, vocab_loc), F32),
            in_specs=[any_spec(), any_spec(), any_spec(), any_spec()] + [vmem_spec()] * 5 + [smem_spec()],
            out_specs=any_spec(),
            scratch_shapes=h_scratch + h_scratch[:1] + z_scratch(2) + [
                dma((2,)), pltpu.VMEM((3, d_loc, 2 * TILE), F32), dma((3,)),
                pltpu.VMEM((d_loc, 2 * rows), BF16), pltpu.VMEM((rows, LANES), F32),
                pltpu.VMEM((2 * rows, 2 * TILE), BF16), pltpu.VMEM((2 * rows, 2 * TILE), BF16)] + lists(1),
            compiler_params=params(),
            cost_estimate=cost(n_tiles * flops, n_tiles * (2 * zbytes + d_loc * TILE * 4)),
        )(g_own, z_oth, in_hbm(h_own), h_oth, *st_oth, occ_oth, meta_oth)

        chip_sum, grad_weight = lax.optimization_barrier((chip_sum, grad_weight))
        full_half = chip_sum + across
        other_half = tp_xor(full_half, 1)
        grad_hidden = jnp.where(core == 0, jnp.stack([full_half, other_half]), jnp.stack([other_half, full_half])).reshape(batch_loc, frames, model_dim)
        return loss[0, :batch_loc], grad_weight, grad_hidden


    return jax.shard_map(
        local_body,
        mesh=mesh,
        in_specs=(P(batch_axes, None, None), P(None, "tp"), P(batch_axes, None), P(batch_axes), P(batch_axes)),
        out_specs=(P(batch_axes), P(batch_axes, "tp"), P(batch_axes, None, None)),
        check_vma=False,
    )
```

```python
import functools

import jax
import jax.numpy as jnp
from jax import lax
from jax.experimental import pallas as pl
from jax.experimental.pallas import tpu as pltpu
from jax.sharding import PartitionSpec as P

NEG_BIG = -1.0e30
LOG2E = 1.4426950408889634
F32 = jnp.float32
DOWN = dict(axis=0, keepdims=True)
ALONG = dict(axis=1, keepdims=True)
BF16 = jnp.bfloat16
TILE = 512
W_PARTS = 5
LANES = 128
HALF = LANES // 2
MIB = 1 << 20


def vmem_spec():
    return pl.BlockSpec(memory_space=pltpu.VMEM)


def smem_spec():
    return pl.BlockSpec(memory_space=pltpu.SMEM)


def any_spec():
    return pl.BlockSpec(memory_space=pl.ANY)


def kernel_call(*args, **kw):
    return pl.pallas_call(*args, **kw)


def params():
    return pltpu.CompilerParams(vmem_limit_bytes=56 * MIB)


def label_col(meta_refs, i):
    n_slots = meta_refs[0].shape[1] - 1
    seq, item = i // n_slots, lax.rem(i, n_slots)
    n_seq = meta_refs[0].shape[0]
    at = lax.max(item - 1, 0)
    col = meta_refs[0][lax.rem(seq, n_seq), at]
    for k in range(1, len(meta_refs)):
        col = jnp.where(seq >= k * n_seq, meta_refs[k][lax.rem(seq, n_seq), at], col)
    return jnp.where(item == 0, 0, col)


def build_lists(meta_refs, vocab_loc, head, nxt):
    n_items = len(meta_refs) * meta_refs[0].shape[0] * (meta_refs[0].shape[1] - 1)
    col_start = lax.axis_index("tp") * vocab_loc
    n_tiles = vocab_loc // TILE

    def clear(i, c):
        head[i] = -1
        return c

    lax.fori_loop(0, n_tiles, clear, 0)

    def insert(i, c):
        loc = label_col(meta_refs, i) - col_start
        tile = lax.max(loc, 0) // TILE

        @pl.when((loc >= 0) & (loc < vocab_loc))
        def _():
            nxt[i] = head[tile]
            head[tile] = i

        return c

    lax.fori_loop(0, n_items, insert, 0)
    return col_start


def walk_list(head, nxt, tile, visit):
    def body(i):
        visit(i)
        return nxt[i]

    lax.while_loop(lambda i: i >= 0, body, head[tile])


class SplitCopy:
    def __init__(self, src, dst, sem, parts):
        n = src.shape[0] // parts
        self.copies = [pltpu.make_async_copy(src.at[pl.ds(p * n, n)], dst.at[pl.ds(p * n, n)], sem) for p in range(parts)]

    def start(self):
        for p, c in enumerate(self.copies):
            c.start(priority=p % 2)

    def wait(self):
        for c in self.copies:
            c.wait()


class TileStream:
    def __init__(self, src, buf, sem, depth, n_tiles, view, parts):
        self.src, self.buf, self.sem, self.depth, self.n, self.view, self.parts = src, buf, sem, depth, n_tiles, view, parts

    def copy(self, j):
        slot = lax.rem(j, self.depth)
        return SplitCopy(self.view(self.src, j), self.buf.at[slot], self.sem.at[slot], self.parts)

    def prime(self):
        for j in range(min(self.depth - 1, self.n)):
            self.copy(j).start()

    def get(self, j):
        self.copy(j).wait()

        @pl.when(j + self.depth - 1 < self.n)
        def _():
            self.copy(j + self.depth - 1).start()

        return lax.rem(j, self.depth)


def w_view(src, j, n=1):
    return src.at[:, pl.ds(pl.multiple_of(j * n * TILE, TILE), n * TILE)]


def z_view(src, j, n):
    return src.at[pl.ds(j * n, n)]


def exact_zero(total):
    return jnp.minimum(total[0:16] + total[16:32], 0.0).astype(BF16)


def after(lhs, zero):
    if zero is None:
        return lhs
    corner = lhs[0:16, 0:LANES] + zero
    return jnp.concatenate([jnp.concatenate([corner, lhs[0:16, LANES:]], axis=1), lhs[16:]], axis=0)


def unit_stats(z, m_ref, s_ref, r0):
    n_chunks = z.shape[1] // LANES
    total = None
    for b in range(z.shape[0] // 32):
        zb = [z[32 * b:32 * (b + 1), k * LANES:(k + 1) * LANES] for k in range(n_chunks)]
        rows = slice(r0 + 32 * b, r0 + 32 * (b + 1))
        m_old = m_ref[rows, :]
        m_new = functools.reduce(jnp.maximum, zb, m_old)
        s_new = s_ref[rows, :] * jnp.exp(m_old - m_new)
        for part in zb:
            s_new = s_new + jnp.exp(part - m_new)
        m_ref[rows, :] = m_new
        s_ref[rows, :] = s_new
        total = s_new if total is None else total + s_new
    return exact_zero(total)


def z_group(h_ref, w, z_out, m_ref, s_ref):
    n_tiles = z_out.shape[0]
    n = h_ref.shape[0] // 2
    zeros = []
    for t in range(n_tiles):
        for r in range(2):
            rows = slice(r * n, (r + 1) * n)
            lhs = after(h_ref[rows, :], zeros[-2] if len(zeros) >= 2 else None)
            z = jnp.dot(lhs, w[:, t * TILE:(t + 1) * TILE], preferred_element_type=F32)
            z_out[t, rows, :] = z
            zeros.append(unit_stats(z, m_ref, s_ref, r * n))


def emit_stats(m_ref, s_ref, out_ref, base):
    row_m = jnp.max(m_ref[...], **ALONG)
    row_s = jnp.sum(s_ref[...] * jnp.exp(m_ref[...] - row_m), **ALONG)
    rows = m_ref.shape[0]
    for k, v in enumerate((row_m, row_s)):
        flat = jnp.broadcast_to(v, (rows, LANES)).T
        for p in range(rows // LANES):
            at = base + 8 * k + p
            out_ref[at:at + 1, :] = flat[0:1, p * LANES:(p + 1) * LANES]


def z_own_kernel(n_slots, h_hbm, w_hbm, labels_ref, in_len_ref, lab_len_ref, z_hbm, pick_ref, meta_ref, h_ref, hsem, wbuf, wsem, zbuf, zsem, m_ref, s_ref, blank, head, nxt):
    n_tiles = z_hbm.shape[0]
    rows = h_ref.shape[0]
    n_seq = meta_ref.shape[0]
    frames = rows // n_seq
    h_copy = pltpu.make_async_copy(h_hbm, h_ref, hsem.at[0])
    h_copy.start()
    n_lab = n_slots - 1
    for q in range(n_seq):
        def put(k, c, q=q):
            meta_ref[q, k] = labels_ref[q, k]
            return c

        lax.fori_loop(0, n_lab, put, 0)
        meta_ref[q, n_lab] = in_len_ref[q]
        meta_ref[q, n_lab + 1] = lab_len_ref[q]
    group = zbuf.shape[1]
    stream = TileStream(w_hbm, wbuf, wsem, wbuf.shape[0], n_tiles // group, lambda src, j: w_view(src, j, group), W_PARTS)
    stream.prime()
    col_start = build_lists([meta_ref], n_tiles * TILE, head, nxt)
    m_ref[...] = jnp.full(m_ref.shape, NEG_BIG, F32)
    s_ref[...] = jnp.zeros(s_ref.shape, F32)
    pick_ref[...] = jnp.zeros(pick_ref.shape, F32)
    blank[...] = jnp.zeros(blank.shape, F32)
    half = frames // 2
    h_copy.wait()
    lane = lax.broadcasted_iota(jnp.int32, (half, LANES), 1)

    def out_copy(j):
        slot = lax.rem(j, zbuf.shape[0])
        return SplitCopy(zbuf.at[slot], z_view(z_hbm, j, group), zsem.at[slot], group)

    def step(j, c):
        slot = stream.get(j)

        @pl.when(j >= 3)
        def _():
            out_copy(j - 3).wait()

        zslot = lax.rem(j, zbuf.shape[0])
        z_group(h_ref, wbuf.at[slot], zbuf.at[zslot], m_ref, s_ref)
        out_copy(j).start()

        for t in range(group):
            def visit(i, t=t):
                seq, item = i // n_slots, lax.rem(i, n_slots)
                off = label_col([meta_ref], i) - col_start - (j * group + t) * TILE
                blk = off // LANES
                r0 = pl.multiple_of(seq * frames, frames)
                src = off - blk * LANES
                c0 = pl.multiple_of(blk * LANES, LANES)

                def moved(p, at):
                    zb = zbuf[zslot, t, pl.ds(r0 + p * half, half), pl.ds(c0, LANES)]
                    return pltpu.roll(zb, lax.rem(at - src + LANES, LANES), 1)

                @pl.when(item > 0)
                def _():
                    for p in range(2):
                        at = item - 1 + n_lab * seq + HALF * p
                        pick_ref[0:half, :] = jnp.where(lane == at, moved(p, at), pick_ref[0:half, :])

                @pl.when(item == 0)
                def _():
                    for p in range(2):
                        at = 2 * seq + p
                        blank[...] = jnp.where(lane == at, moved(p, at), blank[...])

            walk_list(head, nxt, j * group + t, visit)
        return c

    n_groups = n_tiles // group
    lax.fori_loop(0, n_groups, step, 0)
    emit_stats(m_ref, s_ref, pick_ref, half)
    pick_ref[half + 16:half + 24, :] = blank[...].T[0:8]
    for j in range(n_groups - 3, n_groups):
        out_copy(j).wait()


def z_oth_loop(lo, hi, join, h_ref, w_hbm, z_hbm, wbuf, wsem, zbuf, zsem, m_ref, s_ref, sections):
    group = zbuf.shape[1]
    lo, n_groups = lo // group, (hi - lo) // group
    stream = TileStream(w_hbm, wbuf, wsem, wbuf.shape[0], n_groups, lambda src, j: w_view(src, lo + j, group), W_PARTS)
    stream.prime()

    def out_copy(j):
        slot = lax.rem(j, zbuf.shape[0])
        return SplitCopy(zbuf.at[slot], z_view(z_hbm, lo + j, group), zsem.at[slot], group)

    base = 0
    join.wait()
    for n, side, make_carry in sections:
        carry = make_carry()

        def step(k, c, base=base, side=side):
            j = base + k
            slot = stream.get(j)

            @pl.when(j >= 3)
            def _():
                out_copy(j - 3).wait()

            z_group(h_ref, wbuf.at[slot], zbuf.at[lax.rem(j, zbuf.shape[0])], m_ref, s_ref)
            c = side(k, c)
            out_copy(j).start()
            return c

        last = lax.fori_loop(0, n, step, carry)
        yield last
        base += n
    for j in range(max(n_groups - 3, 0), n_groups):
        out_copy(j).wait()


def z_lattice_part(lo, hi, n_lat, per_group, n_lab, before_tail, h_oth, w_hbm, p0, p1, p2, p3, meta_ref,
                     z_hbm, stats_ref, occ_ref, loss_ref, m_ref, s_ref,
                     h_ref, hsem, wbuf, wsem, zbuf, zsem, e_lab, e_blk, s_lab, s_blk, r_lab, r_blk, o_t):
    join = pltpu.make_async_copy(h_oth, h_ref, hsem.at[0])
    join.start()
    n_blk = e_lab.shape[0]
    frames = n_blk * HALF
    m_ref[...] = jnp.full(m_ref.shape, NEG_BIG, F32)
    s_ref[...] = jnp.zeros(s_ref.shape, F32)
    lane128 = lax.broadcasted_iota(jnp.int32, (LANES, LANES), 1)
    row32 = lax.broadcasted_iota(jnp.int32, (n_lab, LANES), 0)
    row8 = lax.broadcasted_iota(jnp.int32, (8, LANES), 0)
    lane32 = lax.broadcasted_iota(jnp.int32, (n_lab, LANES), 1)
    lane8 = lax.broadcasted_iota(jnp.int32, (8, LANES), 1)
    n_seq = meta_ref.shape[0]
    labs = jnp.zeros((n_lab, LANES), jnp.int32)
    lab_row = jnp.zeros((8, LANES), jnp.int32)
    live8 = jnp.zeros((8, LANES), jnp.int32)
    used8 = jnp.zeros((8, LANES), jnp.int32)
    for s in range(n_seq):
        for k in range(n_lab):
            labs = jnp.where((row32 == k) & ((lane32 == s) | (lane32 == s + n_seq)), meta_ref[s, k], labs)
            lab_row = jnp.where((row8 == s) & (lane8 == k), meta_ref[s, k], lab_row)
        here = (lane8 == s) | (lane8 == s + n_seq)
        live8 = jnp.where(here, meta_ref[s, n_lab], live8)
        used8 = jnp.where(here, meta_ref[s, n_lab + 1], used8)
    live32 = jnp.broadcast_to(live8[0:1], (n_lab, LANES))
    used32 = jnp.broadcast_to(used8[0:1], (n_lab, LANES))
    skip_dn = labs != pltpu.roll(labs, 1, 0)
    skip_up = labs != pltpu.roll(labs, n_lab - 1, 0)
    end_lab = row32 == used32 - 1
    end_blk = row32 == used32
    end_top = (row8 == 0) & (used8 == n_lab)
    shift0 = jnp.zeros((1, LANES), F32)
    seq1 = lane8[0:1] >= HALF
    half_len = jnp.where(seq1, meta_ref[1, n_lab], meta_ref[0, n_lab])
    half = frames // 2
    packed = functools.reduce(jnp.add, [p[0:half, :] for p in (p0, p1, p2, p3)])
    blanks = functools.reduce(jnp.add, [p[half + 16:half + 24, :] for p in (p0, p1, p2, p3)])
    for j in range(n_blk):
        far, near = j // 2, HALF * (j % 2)
        part = packed[near:near + HALF]
        x = jnp.concatenate([pltpu.roll(part, (LANES - HALF * far - n_lab * q) % LANES, 1) for q in range(2)], axis=0).T[0:n_lab]
        rows_b = [pltpu.roll(blanks, (HALF * q - near) % LANES, 1)[2 * q + far:2 * q + far + 1] for q in range(2)]
        x_blank = jnp.where(seq1, rows_b[1], rows_b[0])
        top = jnp.maximum(jnp.max(x, **DOWN), x_blank)
        e_blk[j] = jnp.broadcast_to((x_blank - top) * LOG2E, (8, LANES))
        e_lab[j] = (x - top) * LOG2E
        shift0 = shift0 + jnp.where(lax.rem(lane8[0:1], HALF) + HALF * j < half_len, top, 0.0)
    shift_seq0 = jnp.sum(jnp.where(seq1, 0.0, shift0), **ALONG)
    shift_seq1 = jnp.sum(jnp.where(seq1, shift0, 0.0), **ALONG)

    def lse2(a, b):
        hi_v = jnp.maximum(a, b)
        return hi_v + jnp.log2(1.0 + jnp.exp2(jnp.minimum(a, b) - hi_v))

    def lse3(a, b, c):
        hi_v = jnp.maximum(a, b)
        lo_v = jnp.minimum(a, b)
        top = jnp.maximum(hi_v, c)
        mid = jnp.minimum(hi_v, c)
        return top + jnp.log2(1.0 + (jnp.exp2(lo_v - top) + jnp.exp2(mid - top)))

    fwd8, fwd32 = lane8 < n_seq, lane32 < n_seq
    ahead8 = fwd8 & (row8 == 0)
    behind8 = (lane8 >= n_seq) & (row8 == 7)
    base8 = jnp.where(fwd8, HALF * lane8, HALF * (lane8 - n_seq) + HALF - 1)
    base8 = jnp.where(lane8 < 2 * n_seq, base8, HALF)
    skip = jnp.where(fwd32, jnp.where(skip_dn & (row32 > 0), 1, 0), jnp.where(skip_up & (row32 < n_lab - 1), 1, 0)) > 0

    def lanes_of(x, idx):
        return jnp.take_along_axis(x, idx, axis=1, mode="promise_in_bounds")

    def tall(x):
        return jnp.concatenate([x] * (n_lab // 8), axis=0)

    neg32 = jnp.full((n_lab, LANES), NEG_BIG, F32)
    first_b = jnp.where(fwd32, jnp.where(row32 == 0, 0.0, NEG_BIG), jnp.where(end_blk, 0.0, NEG_BIG))
    first_t = jnp.where(fwd8, NEG_BIG, jnp.where(end_top, 0.0, NEG_BIG))

    def lat_step(i, j, u, carry):
        lab, blk, top_b = carry
        idx8 = base8 + jnp.where(fwd8, u, -u)
        idx32 = tall(idx8)
        back = n_blk - 1 - j
        e_l = jnp.where(fwd32, lanes_of(e_lab[j], idx32), lanes_of(e_lab[back], idx32))
        e_b = jnp.where(fwd8, lanes_of(e_blk[j], idx8), lanes_of(e_blk[back], idx8))
        lab_dn = pltpu.roll(lab, 1, 0)
        lab_up = pltpu.roll(lab, n_lab - 1, 0)
        blk_side = jnp.where(fwd32, blk, pltpu.roll(blk, n_lab - 1, 0))
        blk_side = jnp.concatenate([blk_side[:n_lab - 8], jnp.where(behind8, jnp.broadcast_to(top_b[0:1], (8, LANES)), blk_side[n_lab - 8:])], axis=0)
        lab_side = jnp.where(fwd32, lab_dn, lab)
        lab_side = jnp.concatenate([jnp.where(ahead8, NEG_BIG, lab_side[:8]), lab_side[8:]], axis=0)
        new_l = lse3(lab, blk_side, jnp.where(skip, jnp.where(fwd32, lab_dn, lab_up), NEG_BIG))
        new_b = lse2(blk, lab_side)
        new_t = lse2(top_b, jnp.where(ahead8, lab_dn[:8], NEG_BIG))
        s_lab[i] = new_l
        s_blk[i, 0:n_lab] = new_b
        s_blk[i, n_lab:n_lab + 8] = new_t
        behind = frames - 1 - i + pad
        r_lab[behind] = pltpu.roll(new_l, LANES - n_seq, 1)
        r_blk[behind, 0:n_lab] = pltpu.roll(new_b, LANES - n_seq, 1)
        r_blk[behind, n_lab:n_lab + 8] = pltpu.roll(new_t, LANES - n_seq, 1)
        at8 = jnp.where(fwd8, i, frames - 1 - i)
        live = tall(at8) < live32
        lab = jnp.where(live, e_l + new_l, lab)
        blk = jnp.where(live, tall(e_b) + new_b, blk)
        top_b = jnp.where(at8 < live8, e_b + new_t, top_b)
        return lab, blk, top_b

    group = zbuf.shape[1]
    n_lat_groups = n_lat // group
    pad = s_lab.shape[0] - frames

    def lattice_side(k, carry):
        for u in range(per_group):
            i = k * per_group + u
            j = lax.min(lax.div(i, HALF), n_blk - 1)
            carry = lat_step(i, j, lax.rem(i, HALF), carry)
        return carry

    n_occ = (hi - lo - n_lat) // group
    occ_group = frames // n_occ // HALF
    seq_of8 = jnp.where(lane8 >= HALF, 1, 0)
    run = z_oth_loop(lo, hi, join, h_ref, w_hbm, z_hbm, wbuf, wsem, zbuf, zsem, m_ref, s_ref,
                     [(n_lat_groups, lattice_side, lambda: (neg32, first_b, first_t)),
                      (n_occ, lambda k, c: occ_side(k, c), lambda: 0)])
    al, ab, at = next(run)

    lasts = [jnp.where(end, v, NEG_BIG) for end, v in ((end_lab, al), (end_blk, ab), (end_top, at))]
    top = functools.reduce(jnp.maximum, [jnp.max(v, **DOWN) for v in lasts])
    total = functools.reduce(jnp.add, [jnp.sum(jnp.exp2(v - top), **DOWN) for v in lasts])
    loss = -(top + jnp.log2(total))
    loss_at = lanes_of(jnp.broadcast_to(loss, (8, LANES)), seq_of8)
    lane1 = lane8[0:1]
    loss_ref[...] = jnp.broadcast_to(loss * (1.0 / LOG2E) - jnp.where(lane1 == 0, shift_seq0, jnp.where(lane1 == 1, shift_seq1, 0.0)), (8, LANES))

    def occ_side(k, c):
        for g in range(occ_group):
            j = k * occ_group + g
            seq_of32 = tall(seq_of8)
            logs = [neg32, neg32, neg32[0:8]]
            for u in range(HALF):
                i = j * HALF + u
                here8 = lax.rem(lane8, HALF) == u
                here32 = lax.rem(lane32, HALF) == u
                sum_l = s_lab[i] + r_lab[i + pad]
                sum_b = s_blk[i] + r_blk[i + pad]
                logs[0] = jnp.where(here32, lanes_of(sum_l, seq_of32), logs[0])
                logs[1] = jnp.where(here32, lanes_of(sum_b[:n_lab], seq_of32), logs[1])
                logs[2] = jnp.where(here8, lanes_of(sum_b[n_lab:], seq_of8), logs[2])
            rest = e_blk[j] + loss_at
            live = lax.rem(lane8, HALF) + HALF * j < jnp.broadcast_to(half_len, (8, LANES))
            occ_l = jnp.exp2(logs[0] + e_lab[j] + tall(loss_at))
            occ_b = jnp.sum(jnp.exp2(logs[1] + tall(rest)), **DOWN) + jnp.exp2(logs[2] + rest)[0:1]
            o_t[j, 0:n_lab] = jnp.where(tall(jnp.where(live, 1, 0)) > 0, occ_l, 0.0)
            o_t[j, n_lab:n_lab + 8] = jnp.where(live, jnp.broadcast_to(occ_b, (8, LANES)), 0.0)
            o_t[j, 8 + n_lab:LANES] = jnp.zeros((LANES - 8 - n_lab, LANES), F32)
        return c

    next(run)
    before_tail()
    for _ in run:
        pass
    emit_stats(m_ref, s_ref, stats_ref, 0)
    row128 = lax.broadcasted_iota(jnp.int32, (LANES, LANES), 0)
    same = []
    for s in range(n_seq):
        down = jnp.full((n_lab, LANES), -1, jnp.int32)
        for k in range(n_lab):
            down = jnp.where(row32 == k, meta_ref[s, k], down)
        down = jnp.concatenate([down, jnp.full((LANES - n_lab, LANES), -1, jnp.int32)], axis=0)
        across = pltpu.roll(jnp.broadcast_to(lab_row[s:s + 1], (LANES, LANES)), HALF * s, 1)
        own = lane128 - HALF * s
        inner = (row128 < n_lab) & (own >= 0) & (own < n_lab)
        same.append(jnp.where((inner & (down == across)) | ((row128 == own) & (own < HALF)), 1.0, 0.0))
    for j in range(n_blk):
        y = o_t[j].T
        occ_ref[HALF * j:HALF * (j + 1), :] = functools.reduce(jnp.add, [
            jnp.dot(y[HALF * q:HALF * (q + 1), :], same[q], precision=lax.Precision.HIGHEST, preferred_element_type=F32) for q in range(n_seq)])


def spread_lse(refs, base, meta_ref, lse_ref, r0, frames):
    m = functools.reduce(jnp.maximum, [r[base:base + 8, :] for r in refs])
    tot = functools.reduce(jnp.add, [r[base + 8:base + 16, :] * jnp.exp(r[base:base + 8, :] - m) for r in refs])
    lse = m + jnp.log(tot)
    t = lax.broadcasted_iota(jnp.int32, (LANES, LANES), 0)
    n_part = frames // LANES
    sums = []
    for q in range(meta_ref.shape[0]):
        live_sum = jnp.zeros((1, LANES), F32)
        for p in range(n_part):
            at = q * n_part + p
            part = jnp.broadcast_to(lse[at:at + 1, :], (LANES, LANES)).T
            live = t + p * LANES < meta_ref[q, meta_ref.shape[1] - 2]
            lse_ref[r0 + at * LANES:r0 + (at + 1) * LANES, :] = jnp.where(live, part, 1.0e30)
            live_sum = live_sum + jnp.sum(jnp.where(live, part, 0.0), **DOWN)
        sums.append(live_sum)
    return sums


def patch_tile(n_slots, frames, meta_refs, col_start, j, i, z_block, lse_ref, occ_ref, g_ref, g_col, lane):
    seq, item = i // n_slots, lax.rem(i, n_slots)
    off = label_col(meta_refs, i) - col_start - j * TILE
    blk = off // LANES
    r0 = pl.multiple_of(seq * frames, frames)
    c0 = pl.multiple_of(blk * LANES, LANES)
    zb = z_block(seq, c0)
    slot_lane = jnp.where(item == 0, n_slots - 1, item - 1) + HALF * seq
    at = off - blk * LANES
    occ = pltpu.roll(occ_ref[...], lax.rem(at - slot_lane + LANES, LANES), 1)
    fresh = jnp.exp(zb - lse_ref[pl.ds(r0, frames), :]) - occ
    gc = pl.multiple_of(g_col + c0, LANES)
    old = g_ref[pl.ds(r0, frames), pl.ds(gc, LANES)].astype(F32)
    g_ref[pl.ds(r0, frames), pl.ds(gc, LANES)] = jnp.where(lane == at, fresh, old).astype(BF16)


def softmax_unit(z, z_row, lse_ref, out, r0, n, c0):
    total = None
    for b in range(n // 32):
        lse = lse_ref[r0 + 32 * b:r0 + 32 * (b + 1), :]
        for k in range(TILE // LANES):
            e = jnp.exp(z[z_row + 32 * b:z_row + 32 * (b + 1), k * LANES:(k + 1) * LANES] - lse)
            out[r0 + 32 * b:r0 + 32 * (b + 1), c0 + k * LANES:c0 + (k + 1) * LANES] = e.astype(BF16)
            total = e if total is None else total + e
    return exact_zero(total)


def grad_h_part(n_slots, z_hbm, w_hbm, st0, st1, st2, st3, occ_ref, part_loss, meta_ref, keep_ref, send_ref, loss_ref, g_hbm,
                  wbuf, wsem, zbuf, zsem, acc, lse_ref, g0, g1, gsem, head, nxt):
    n_tiles, rows = z_hbm.shape[0], z_hbm.shape[1]
    frames = rows // meta_ref.shape[0]
    meta_refs = [meta_ref]
    group = zbuf.shape[1]
    n_groups = n_tiles // group
    stream = TileStream(w_hbm, wbuf, wsem, wbuf.shape[0], n_groups, lambda src, j: w_view(src, j, group), W_PARTS)
    zs = TileStream(z_hbm, zbuf, zsem, zbuf.shape[0], n_groups, lambda src, j: z_view(src, j, group), group)
    zs.prime()
    yield stream.prime
    col_start = build_lists(meta_refs, n_tiles * TILE, head, nxt)
    sums = spread_lse([st0, st1, st2, st3], frames // 2, meta_ref, lse_ref, 0, frames)
    lane1 = lax.broadcasted_iota(jnp.int32, (8, LANES), 1)
    loss_ref[...] = part_loss[...] + jnp.where(lane1 == 0, sums[0], sums[1])
    lane = lax.broadcasted_iota(jnp.int32, (frames, LANES), 1)

    def patch(j, slot, g):
        for t in range(group):
            def z_block(seq, c0, t=t):
                return zbuf[slot, t, pl.ds(pl.multiple_of(seq * frames, frames), frames), pl.ds(c0, LANES)]

            walk_list(head, nxt, j * group + t,
                      lambda i, t=t, z_block=z_block: patch_tile(n_slots, frames, meta_refs, col_start, j * group + t, i, z_block, lse_ref, occ_ref, g, t * TILE, lane))

    def make_g(slot, u, g):
        t, r = u // 2, u % 2
        return softmax_unit(zbuf.at[slot, t], r * rows // 2, lse_ref, g, r * rows // 2, rows // 2, t * TILE)

    acc[...] = jnp.zeros(acc.shape, F32)
    slot0 = zs.get(0)
    for u in range(2 * group):
        make_g(slot0, u, g0)
    patch(0, slot0, g0)
    n_units = acc.shape[0] // 256

    def g_copy(j, g, k):
        return pltpu.make_async_copy(g, g_hbm.at[j], gsem.at[k])

    def half(j, g_now, g_next, k):
        slot = stream.get(j)
        nj = lax.min(j + 1, n_groups - 1)

        @pl.when(j + 1 < n_groups)
        def _():
            zs.get(nj)

        @pl.when(j >= 1)
        def _():
            g_copy(j - 1, g_next, 1 - k).wait()

        g_copy(j, g_now, k).start()

        zslot = lax.rem(nj, zbuf.shape[0])
        zero = None
        for u in range(n_units):
            d_rows = slice(u * 256, (u + 1) * 256)
            lhs = after(wbuf[slot, d_rows, :], zero)
            acc[d_rows, :] += lax.dot_general(lhs, g_now[...], (((1,), (1,)), ((), ())), preferred_element_type=F32)
            if u < 2 * group:
                zero = make_g(zslot, u, g_next)
        patch(nj, zslot, g_next)

    def step(i, c):
        half(2 * i, g0, g1, 0)
        half(2 * i + 1, g1, g0, 1)
        return c

    lax.fori_loop(0, n_groups // 2, step, 0)
    g_copy(n_groups - 1, g1, 1).wait()
    core = lax.rem(lax.axis_index("tp"), 2)
    n = rows // 2
    keep_ref[...] = acc[:, pl.ds(pl.multiple_of(core * n, n), n)].T
    send_ref[...] = acc[:, pl.ds(pl.multiple_of((1 - core) * n, n), n)].T


def mid_kernel(lo, hi, n_lat, per_group, n_lab, h_oth, w_hbm, p0, p1, p2, p3, z_own, meta_ref,
               z_hbm, stats_ref, occ_ref, keep_ref, send_ref, loss_ref, g_hbm,
               part_loss, m_ref, s_ref, h_ref, hsem, wbuf, wsem, zbuf, zsem, e_lab, e_blk, s_lab, s_blk, r_lab, r_blk, o_t,
               zin_buf, zin_sem, acc, lse_ref, g0, g1, gsem, head, nxt):
    second = grad_h_part(n_lab + 1, z_own, w_hbm, p0, p1, p2, p3, occ_ref, part_loss, meta_ref, keep_ref, send_ref, loss_ref, g_hbm,
                         wbuf, wsem, zin_buf, zin_sem, acc, lse_ref, g0, g1, gsem, head, nxt)
    prime_w = next(second)
    z_lattice_part(lo, hi, n_lat, per_group, n_lab, prime_w, h_oth, w_hbm, p0, p1, p2, p3, meta_ref,
                   z_hbm, stats_ref, occ_ref, part_loss, m_ref, s_ref,
                   h_ref, hsem, wbuf, wsem, zbuf, zsem, e_lab, e_blk, s_lab, s_blk, r_lab, r_blk, o_t)
    for _ in second:
        pass


def grad_w_kernel(n_slots, g_hbm, z_hbm, h_own_hbm, h_oth, st0, st1, st2, st3, occ_ref, meta_ref, gw_hbm,
                  h_ref, hsem, h_own_ref, zbuf, zsem, gsem, obuf, osem, ht, lse_ref, g0, g1, head, nxt):
    n_tiles, rows = z_hbm.shape[0], z_hbm.shape[1]
    frames = rows // meta_ref.shape[0]
    d_loc = ht.shape[0]
    group = zbuf.shape[1]
    n_groups = n_tiles // group
    zs = TileStream(z_hbm, zbuf, zsem, zbuf.shape[0], n_groups, lambda src, j: z_view(src, j, group), group)

    def g_copy(j, g, k):
        return pltpu.make_async_copy(g_hbm.at[j], g.at[0:rows, :], gsem.at[k])

    join = pltpu.make_async_copy(h_oth, h_ref, hsem.at[0])
    own_copy = pltpu.make_async_copy(h_own_hbm, h_own_ref, hsem.at[1])
    own_copy.start()
    join.start()
    zs.prime()
    g_copy(0, g0, 0).start()
    col_start = build_lists([meta_ref], n_tiles * TILE, head, nxt)
    d0 = pl.multiple_of(lax.axis_index("dp") * d_loc, LANES)
    own_copy.wait()
    ht[:, 0:rows] = h_own_ref[:, pl.ds(d0, d_loc)].T
    spread_lse([st0, st1, st2, st3], 0, meta_ref, lse_ref, 0, frames)
    join.wait()
    ht[:, rows:2 * rows] = h_ref[:, pl.ds(d0, d_loc)].T
    lane = lax.broadcasted_iota(jnp.int32, (frames, LANES), 1)
    n_units = 2 * group

    def make_g(slot, u, g):
        t, r = u // 2, u % 2
        return softmax_unit(zbuf.at[slot, t], r * rows // 2, lse_ref, g.at[rows:2 * rows, :], r * rows // 2, rows // 2, t * TILE)

    def patch(j, slot, g):
        for t in range(group):
            def z_block(seq, c0, t=t):
                return zbuf[slot, t, pl.ds(pl.multiple_of(seq * frames, frames), frames), pl.ds(c0, LANES)]

            walk_list(head, nxt, j * group + t,
                      lambda i, t=t, z_block=z_block: patch_tile(n_slots, frames, [meta_ref], col_start, j * group + t, i, z_block, lse_ref, occ_ref, g.at[rows:2 * rows, :], t * TILE, lane))

    def out_copy(j):
        slot = lax.rem(j, obuf.shape[0])
        return SplitCopy(obuf.at[slot], w_view(gw_hbm, j, group), osem.at[slot], W_PARTS)

    slot0 = zs.get(0)
    for u in range(n_units):
        make_g(slot0, u, g0)
    patch(0, slot0, g0)
    d_half = d_loc // 2

    def half(j, g_now, g_next, k):
        @pl.when(j >= 3)
        def _():
            out_copy(j - 3).wait()

        nj = lax.min(j + 1, n_groups - 1)

        @pl.when(j + 1 < n_groups)
        def _():
            zs.get(nj)
            g_copy(nj, g_next, 1 - k).start()

        g_copy(j, g_now, k).wait()
        slot = lax.rem(nj, zbuf.shape[0])
        oslot = lax.rem(j, obuf.shape[0])
        zero = None
        for u in range(n_units):
            t, r = u // 2, u % 2
            d_rows = slice(r * d_half, (r + 1) * d_half)
            lhs = after(ht[d_rows, :], zero)
            obuf[oslot, d_rows, t * TILE:(t + 1) * TILE] = jnp.dot(lhs, g_now[:, t * TILE:(t + 1) * TILE], preferred_element_type=F32)
            zero = make_g(slot, u, g_next)
        out_copy(j).start()
        patch(nj, slot, g_next)

    def step(i, c):
        half(2 * i, g0, g1, 0)
        half(2 * i + 1, g1, g0, 1)
        return c

    lax.fori_loop(0, n_groups // 2, step, 0)
    for j in range(n_groups - 3, n_groups):
        out_copy(j).wait()


def cost(flops, nbytes):
    return pl.CostEstimate(flops=flops, bytes_accessed=nbytes, transcendentals=0)


def solution(mesh):
    batch_axes = ("part", "dp")
    n_tp = mesh.shape["tp"]
    n_dp = mesh.shape["dp"]
    dp_swap = [(i, n_dp - 1 - i) for i in range(n_dp)]

    others = range(1, n_tp)

    def tp_xor(x, mask):
        return lax.ppermute(x, "tp", [(i, i ^ mask) for i in range(n_tp)])

    def in_hbm(x):
        return pltpu.with_memory_space_constraint(x, pltpu.HBM)

    def swap_dp(x):
        return lax.ppermute(x, "dp", dp_swap)

    def local_body(hidden, w_loc, labels, in_len, lab_len):
        batch_loc, frames, model_dim = hidden.shape
        vocab_loc = w_loc.shape[1]
        n_lab = labels.shape[1]
        n_slots = n_lab + 1
        rows = batch_loc * frames
        n_tiles = vocab_loc // TILE
        d_loc = model_dim // n_dp
        dma = pltpu.SemaphoreType.DMA
        i32 = jnp.int32
        n_lat, lat_steps, lat_pad = 24, 22, 8
        h_own = hidden.reshape(rows, model_dim)
        core = lax.rem(lax.axis_index("tp"), 2)
        h_oth = swap_dp(h_own)
        flops = 2 * rows * model_dim * TILE
        wbytes = model_dim * TILE * 2
        zbytes = rows * TILE * 4
        z_type = jax.ShapeDtypeStruct((n_tiles, rows, TILE), F32)
        pick_type = jax.ShapeDtypeStruct((frames // 2 + 24, LANES), F32)
        meta_type = jax.ShapeDtypeStruct((batch_loc, n_slots + 1), i32)
        g_type = jax.ShapeDtypeStruct((n_tiles // 2, rows, 2 * TILE), BF16)
        stat_type = jax.ShapeDtypeStruct((16, LANES), F32)
        g_scratch = [pltpu.VMEM((rows, 2 * TILE), BF16)] * 2

        def w_scratch(n):
            return [pltpu.VMEM((3, model_dim, n * TILE), BF16), dma((3,))]

        def z_scratch(n):
            return [pltpu.VMEM((3, n, rows, TILE), F32), dma((3,))]

        h_scratch = [pltpu.VMEM((rows, model_dim), BF16), dma((2,))]
        run_scratch = [pltpu.VMEM((rows, LANES), F32), pltpu.VMEM((rows, LANES), F32)]

        def lists(n_sets):
            return [pltpu.SMEM((n_tiles,), i32), pltpu.SMEM((n_sets * batch_loc * n_slots,), i32)]

        z_own, pick, meta = kernel_call(
            functools.partial(z_own_kernel, n_slots),
            out_shape=(z_type, pick_type, meta_type),
            in_specs=[any_spec(), any_spec(), smem_spec(), smem_spec(), smem_spec()],
            out_specs=(any_spec(), vmem_spec(), smem_spec()),
            scratch_shapes=h_scratch + w_scratch(4) + z_scratch(4) + run_scratch + [pltpu.VMEM((frames // 2, LANES), F32)] + lists(1),
            compiler_params=params(),
            cost_estimate=cost(n_tiles * flops, n_tiles * (wbytes + zbytes)),
        )(in_hbm(h_own), w_loc, labels, in_len, lab_len)

        h_oth = in_hbm(h_oth)
        picks = [pick] + [tp_xor(pick, k) for k in others]

        n_blk = frames // HALF
        half_type = jax.ShapeDtypeStruct((rows // 2, model_dim), F32)
        occ_type = jax.ShapeDtypeStruct((frames, LANES), F32)
        loss_type = jax.ShapeDtypeStruct((8, LANES), F32)
        z_oth, stats_oth, occ, keep, send, loss, g_own = kernel_call(
            functools.partial(mid_kernel, 0, n_tiles, n_lat, lat_steps, n_lab),
            out_shape=(z_type, stat_type, occ_type, half_type, half_type, loss_type, g_type),
            in_specs=[any_spec()] * 2 + [vmem_spec()] * 4 + [any_spec(), smem_spec()],
            out_specs=(any_spec(),) + (vmem_spec(),) * 5 + (any_spec(),),
            scratch_shapes=[pltpu.VMEM((8, LANES), F32)] + run_scratch + h_scratch + w_scratch(2) + z_scratch(2) + [
                pltpu.VMEM((n_blk, n_lab, LANES), F32), pltpu.VMEM((n_blk, 8, LANES), F32),
                *[pltpu.VMEM((frames + lat_pad, n, LANES), F32) for n in (n_lab, n_lab + 8) * 2],
                pltpu.VMEM((n_blk, LANES, LANES), F32)] + z_scratch(2) + [
                pltpu.VMEM((model_dim, rows), F32), pltpu.VMEM((rows, LANES), F32)] + g_scratch + [dma((2,))] + lists(1),
            compiler_params=params(),
            cost_estimate=cost((2 * n_tiles) * flops, (2 * n_tiles) * (wbytes + zbytes)),
        )(h_oth, w_loc, *picks, z_own, meta)
        st_oth = [stats_oth] + [tp_xor(stats_oth, k) for k in others]
        occ_oth = swap_dp(occ)
        meta_oth = swap_dp(meta)
        recv = tp_xor(send, 1)
        chip_sum = keep + recv
        across = tp_xor(chip_sum, 2)

        grad_weight = kernel_call(
            functools.partial(grad_w_kernel, n_slots),
            out_shape=jax.ShapeDtypeStruct((d_loc, vocab_loc), F32),
            in_specs=[any_spec(), any_spec(), any_spec(), any_spec()] + [vmem_spec()] * 5 + [smem_spec()],
            out_specs=any_spec(),
            scratch_shapes=h_scratch + h_scratch[:1] + z_scratch(2) + [
                dma((2,)), pltpu.VMEM((3, d_loc, 2 * TILE), F32), dma((3,)),
                pltpu.VMEM((d_loc, 2 * rows), BF16), pltpu.VMEM((rows, LANES), F32),
                pltpu.VMEM((2 * rows, 2 * TILE), BF16), pltpu.VMEM((2 * rows, 2 * TILE), BF16)] + lists(1),
            compiler_params=params(),
            cost_estimate=cost(n_tiles * flops, n_tiles * (2 * zbytes + d_loc * TILE * 4)),
        )(g_own, z_oth, in_hbm(h_own), h_oth, *st_oth, occ_oth, meta_oth)

        chip_sum, grad_weight = lax.optimization_barrier((chip_sum, grad_weight))
        full_half = chip_sum + across
        other_half = tp_xor(full_half, 1)
        grad_hidden = jnp.where(core == 0, jnp.stack([full_half, other_half]), jnp.stack([other_half, full_half])).reshape(batch_loc, frames, model_dim)
        return loss[0, :batch_loc], grad_weight, grad_hidden


    return jax.shard_map(
        local_body,
        mesh=mesh,
        in_specs=(P(batch_axes, None, None), P(None, "tp"), P(batch_axes, None), P(batch_axes), P(batch_axes)),
        out_specs=(P(batch_axes), P(batch_axes, "tp"), P(batch_axes, None, None)),
        check_vma=False,
    )
```

```python
import functools

import jax
import jax.numpy as jnp
from jax import lax
from jax.experimental import pallas as pl
from jax.experimental.pallas import tpu as pltpu
from jax.sharding import PartitionSpec as P

NEG_BIG = -1.0e30
LOG2E = 1.4426950408889634
F32 = jnp.float32
DOWN = dict(axis=0, keepdims=True)
ALONG = dict(axis=1, keepdims=True)
BF16 = jnp.bfloat16
TILE = 512
W_PARTS = 5
LANES = 128
HALF = LANES // 2
MIB = 1 << 20


def vmem_spec():
    return pl.BlockSpec(memory_space=pltpu.VMEM)


def smem_spec():
    return pl.BlockSpec(memory_space=pltpu.SMEM)


def any_spec():
    return pl.BlockSpec(memory_space=pl.ANY)


def kernel_call(*args, **kw):
    return pl.pallas_call(*args, **kw)


def params():
    return pltpu.CompilerParams(vmem_limit_bytes=56 * MIB)


def label_col(meta_refs, i):
    n_slots = meta_refs[0].shape[1] - 1
    seq, item = i // n_slots, lax.rem(i, n_slots)
    n_seq = meta_refs[0].shape[0]
    at = lax.max(item - 1, 0)
    col = meta_refs[0][lax.rem(seq, n_seq), at]
    for k in range(1, len(meta_refs)):
        col = jnp.where(seq >= k * n_seq, meta_refs[k][lax.rem(seq, n_seq), at], col)
    return jnp.where(item == 0, 0, col)


def build_lists(meta_refs, vocab_loc, head, nxt):
    n_items = len(meta_refs) * meta_refs[0].shape[0] * (meta_refs[0].shape[1] - 1)
    col_start = lax.axis_index("tp") * vocab_loc
    n_tiles = vocab_loc // TILE

    def clear(i, c):
        head[i] = -1
        return c

    lax.fori_loop(0, n_tiles, clear, 0)

    def insert(i, c):
        loc = label_col(meta_refs, i) - col_start
        tile = lax.max(loc, 0) // TILE

        @pl.when((loc >= 0) & (loc < vocab_loc))
        def _():
            nxt[i] = head[tile]
            head[tile] = i

        return c

    lax.fori_loop(0, n_items, insert, 0)
    return col_start


def walk_list(head, nxt, tile, visit):
    def body(i):
        visit(i)
        return nxt[i]

    lax.while_loop(lambda i: i >= 0, body, head[tile])


class SplitCopy:
    def __init__(self, src, dst, sem, parts):
        n = src.shape[0] // parts
        self.copies = [pltpu.make_async_copy(src.at[pl.ds(p * n, n)], dst.at[pl.ds(p * n, n)], sem) for p in range(parts)]

    def start(self):
        for p, c in enumerate(self.copies):
            c.start(priority=p % 2)

    def wait(self):
        for c in self.copies:
            c.wait()


class TileStream:
    def __init__(self, src, buf, sem, depth, n_tiles, view, parts):
        self.src, self.buf, self.sem, self.depth, self.n, self.view, self.parts = src, buf, sem, depth, n_tiles, view, parts

    def copy(self, j):
        slot = lax.rem(j, self.depth)
        return SplitCopy(self.view(self.src, j), self.buf.at[slot], self.sem.at[slot], self.parts)

    def prime(self):
        for j in range(min(self.depth - 1, self.n)):
            self.copy(j).start()

    def get(self, j):
        self.copy(j).wait()

        @pl.when(j + self.depth - 1 < self.n)
        def _():
            self.copy(j + self.depth - 1).start()

        return lax.rem(j, self.depth)


def w_view(src, j, n=1):
    return src.at[:, pl.ds(pl.multiple_of(j * n * TILE, TILE), n * TILE)]


def z_view(src, j, n):
    return src.at[pl.ds(j * n, n)]


def exact_zero(total):
    return jnp.minimum(total[0:16] + total[16:32], 0.0).astype(BF16)


def after(lhs, zero):
    if zero is None:
        return lhs
    corner = lhs[0:16, 0:LANES] + zero
    return jnp.concatenate([jnp.concatenate([corner, lhs[0:16, LANES:]], axis=1), lhs[16:]], axis=0)


def unit_stats(z, m_ref, s_ref, r0):
    n_chunks = z.shape[1] // LANES
    total = None
    for b in range(z.shape[0] // 32):
        zb = [z[32 * b:32 * (b + 1), k * LANES:(k + 1) * LANES] for k in range(n_chunks)]
        rows = slice(r0 + 32 * b, r0 + 32 * (b + 1))
        m_old = m_ref[rows, :]
        m_new = functools.reduce(jnp.maximum, zb, m_old)
        s_new = s_ref[rows, :] * jnp.exp(m_old - m_new)
        for part in zb:
            s_new = s_new + jnp.exp(part - m_new)
        m_ref[rows, :] = m_new
        s_ref[rows, :] = s_new
        total = s_new if total is None else total + s_new
    return exact_zero(total)


def z_group(h_ref, w, z_out, m_ref, s_ref):
    n_tiles = z_out.shape[0]
    n = h_ref.shape[0] // 2
    zeros = []
    for t in range(n_tiles):
        for r in range(2):
            rows = slice(r * n, (r + 1) * n)
            lhs = after(h_ref[rows, :], zeros[-2] if len(zeros) >= 2 else None)
            z = jnp.dot(lhs, w[:, t * TILE:(t + 1) * TILE], preferred_element_type=F32)
            z_out[t, rows, :] = z
            zeros.append(None if m_ref is None else unit_stats(z, m_ref, s_ref, r * n))


def emit_stats(m_ref, s_ref, out_ref, base):
    row_m = jnp.max(m_ref[...], **ALONG)
    row_s = jnp.sum(s_ref[...] * jnp.exp(m_ref[...] - row_m), **ALONG)
    rows = m_ref.shape[0]
    for k, v in enumerate((row_m, row_s)):
        flat = jnp.broadcast_to(v, (rows, LANES)).T
        for p in range(rows // LANES):
            at = base + 8 * k + p
            out_ref[at:at + 1, :] = flat[0:1, p * LANES:(p + 1) * LANES]


def z_own_kernel(n_slots, h_hbm, w_hbm, labels_ref, in_len_ref, lab_len_ref, z_hbm, pick_ref, meta_ref, h_ref, hsem, wbuf, wsem, zbuf, zsem, m_ref, s_ref, blank, head, nxt):
    n_tiles = z_hbm.shape[0]
    rows = h_ref.shape[0]
    n_seq = meta_ref.shape[0]
    frames = rows // n_seq
    h_copy = pltpu.make_async_copy(h_hbm, h_ref, hsem.at[0])
    h_copy.start()
    n_lab = n_slots - 1
    for q in range(n_seq):
        def put(k, c, q=q):
            meta_ref[q, k] = labels_ref[q, k]
            return c

        lax.fori_loop(0, n_lab, put, 0)
        meta_ref[q, n_lab] = in_len_ref[q]
        meta_ref[q, n_lab + 1] = lab_len_ref[q]
    group = zbuf.shape[1]
    stream = TileStream(w_hbm, wbuf, wsem, wbuf.shape[0], n_tiles // group, lambda src, j: w_view(src, j, group), W_PARTS)
    stream.prime()
    col_start = build_lists([meta_ref], n_tiles * TILE, head, nxt)
    m_ref[...] = jnp.full(m_ref.shape, NEG_BIG, F32)
    s_ref[...] = jnp.zeros(s_ref.shape, F32)
    pick_ref[...] = jnp.zeros(pick_ref.shape, F32)
    blank[...] = jnp.zeros(blank.shape, F32)
    half = frames // 2
    h_copy.wait()
    lane = lax.broadcasted_iota(jnp.int32, (half, LANES), 1)

    def out_copy(j):
        slot = lax.rem(j, zbuf.shape[0])
        return SplitCopy(zbuf.at[slot], z_view(z_hbm, j, group), zsem.at[slot], group)

    def step(j, c):
        slot = stream.get(j)

        @pl.when(j >= 3)
        def _():
            out_copy(j - 3).wait()

        zslot = lax.rem(j, zbuf.shape[0])
        z_group(h_ref, wbuf.at[slot], zbuf.at[zslot], m_ref, s_ref)
        out_copy(j).start()

        for t in range(group):
            def visit(i, t=t):
                seq, item = i // n_slots, lax.rem(i, n_slots)
                off = label_col([meta_ref], i) - col_start - (j * group + t) * TILE
                blk = off // LANES
                r0 = pl.multiple_of(seq * frames, frames)
                src = off - blk * LANES
                c0 = pl.multiple_of(blk * LANES, LANES)

                def moved(p, at):
                    zb = zbuf[zslot, t, pl.ds(r0 + p * half, half), pl.ds(c0, LANES)]
                    return pltpu.roll(zb, lax.rem(at - src + LANES, LANES), 1)

                @pl.when(item > 0)
                def _():
                    for p in range(2):
                        at = item - 1 + n_lab * seq + HALF * p
                        pick_ref[0:half, :] = jnp.where(lane == at, moved(p, at), pick_ref[0:half, :])

                @pl.when(item == 0)
                def _():
                    for p in range(2):
                        at = 2 * seq + p
                        blank[...] = jnp.where(lane == at, moved(p, at), blank[...])

            walk_list(head, nxt, j * group + t, visit)
        return c

    n_groups = n_tiles // group
    lax.fori_loop(0, n_groups, step, 0)
    emit_stats(m_ref, s_ref, pick_ref, half)
    pick_ref[half + 16:half + 24, :] = blank[...].T[0:8]
    for j in range(n_groups - 3, n_groups):
        out_copy(j).wait()


def z_oth_loop(lo, hi, join, h_ref, w_hbm, z_hbm, wbuf, wsem, zbuf, zsem, sections):
    group = zbuf.shape[1]
    lo, n_groups = lo // group, (hi - lo) // group
    stream = TileStream(w_hbm, wbuf, wsem, wbuf.shape[0], n_groups, lambda src, j: w_view(src, lo + j, group), W_PARTS)
    stream.prime()

    def out_copy(j):
        slot = lax.rem(j, zbuf.shape[0])
        return SplitCopy(zbuf.at[slot], z_view(z_hbm, lo + j, group), zsem.at[slot], group)

    base = 0
    join.wait()
    for n, side, make_carry in sections:
        carry = make_carry()

        def step(k, c, base=base, side=side):
            j = base + k
            slot = stream.get(j)

            @pl.when(j >= 3)
            def _():
                out_copy(j - 3).wait()

            z_group(h_ref, wbuf.at[slot], zbuf.at[lax.rem(j, zbuf.shape[0])], None, None)
            c = side(k, c)
            out_copy(j).start()
            return c

        last = lax.fori_loop(0, n, step, carry)
        yield last
        base += n
    for j in range(max(n_groups - 3, 0), n_groups):
        out_copy(j).wait()


def z_lattice_part(lo, hi, n_lat, per_group, n_lab, before_tail, h_oth, w_hbm, p0, p1, p2, p3, meta_ref,
                     z_hbm, occ_ref, loss_ref,
                     h_ref, hsem, wbuf, wsem, zbuf, zsem, e_lab, e_blk, s_lab, s_blk, r_lab, r_blk, o_t):
    join = pltpu.make_async_copy(h_oth, h_ref, hsem.at[0])
    join.start()
    n_blk = e_lab.shape[0]
    frames = n_blk * HALF
    lane128 = lax.broadcasted_iota(jnp.int32, (LANES, LANES), 1)
    row32 = lax.broadcasted_iota(jnp.int32, (n_lab, LANES), 0)
    row8 = lax.broadcasted_iota(jnp.int32, (8, LANES), 0)
    lane32 = lax.broadcasted_iota(jnp.int32, (n_lab, LANES), 1)
    lane8 = lax.broadcasted_iota(jnp.int32, (8, LANES), 1)
    n_seq = meta_ref.shape[0]
    labs = jnp.zeros((n_lab, LANES), jnp.int32)
    lab_row = jnp.zeros((8, LANES), jnp.int32)
    live8 = jnp.zeros((8, LANES), jnp.int32)
    used8 = jnp.zeros((8, LANES), jnp.int32)
    for s in range(n_seq):
        for k in range(n_lab):
            labs = jnp.where((row32 == k) & ((lane32 == s) | (lane32 == s + n_seq)), meta_ref[s, k], labs)
            lab_row = jnp.where((row8 == s) & (lane8 == k), meta_ref[s, k], lab_row)
        here = (lane8 == s) | (lane8 == s + n_seq)
        live8 = jnp.where(here, meta_ref[s, n_lab], live8)
        used8 = jnp.where(here, meta_ref[s, n_lab + 1], used8)
    live32 = jnp.broadcast_to(live8[0:1], (n_lab, LANES))
    used32 = jnp.broadcast_to(used8[0:1], (n_lab, LANES))
    skip_dn = labs != pltpu.roll(labs, 1, 0)
    skip_up = labs != pltpu.roll(labs, n_lab - 1, 0)
    end_lab = row32 == used32 - 1
    end_blk = row32 == used32
    end_top = (row8 == 0) & (used8 == n_lab)
    shift0 = jnp.zeros((1, LANES), F32)
    seq1 = lane8[0:1] >= HALF
    half_len = jnp.where(seq1, meta_ref[1, n_lab], meta_ref[0, n_lab])
    half = frames // 2
    packed = functools.reduce(jnp.add, [p[0:half, :] for p in (p0, p1, p2, p3)])
    blanks = functools.reduce(jnp.add, [p[half + 16:half + 24, :] for p in (p0, p1, p2, p3)])
    for j in range(n_blk):
        far, near = j // 2, HALF * (j % 2)
        part = packed[near:near + HALF]
        x = jnp.concatenate([pltpu.roll(part, (LANES - HALF * far - n_lab * q) % LANES, 1) for q in range(2)], axis=0).T[0:n_lab]
        rows_b = [pltpu.roll(blanks, (HALF * q - near) % LANES, 1)[2 * q + far:2 * q + far + 1] for q in range(2)]
        x_blank = jnp.where(seq1, rows_b[1], rows_b[0])
        top = jnp.maximum(jnp.max(x, **DOWN), x_blank)
        e_blk[j] = jnp.broadcast_to((x_blank - top) * LOG2E, (8, LANES))
        e_lab[j] = (x - top) * LOG2E
        shift0 = shift0 + jnp.where(lax.rem(lane8[0:1], HALF) + HALF * j < half_len, top, 0.0)
    shift_seq0 = jnp.sum(jnp.where(seq1, 0.0, shift0), **ALONG)
    shift_seq1 = jnp.sum(jnp.where(seq1, shift0, 0.0), **ALONG)

    def lse2(a, b):
        hi_v = jnp.maximum(a, b)
        return hi_v + jnp.log2(1.0 + jnp.exp2(jnp.minimum(a, b) - hi_v))

    def lse3(a, b, c):
        hi_v = jnp.maximum(a, b)
        lo_v = jnp.minimum(a, b)
        top = jnp.maximum(hi_v, c)
        mid = jnp.minimum(hi_v, c)
        return top + jnp.log2(1.0 + (jnp.exp2(lo_v - top) + jnp.exp2(mid - top)))

    fwd8, fwd32 = lane8 < n_seq, lane32 < n_seq
    ahead8 = fwd8 & (row8 == 0)
    behind8 = (lane8 >= n_seq) & (row8 == 7)
    base8 = jnp.where(fwd8, HALF * lane8, HALF * (lane8 - n_seq) + HALF - 1)
    base8 = jnp.where(lane8 < 2 * n_seq, base8, HALF)
    skip = jnp.where(fwd32, jnp.where(skip_dn & (row32 > 0), 1, 0), jnp.where(skip_up & (row32 < n_lab - 1), 1, 0)) > 0

    def lanes_of(x, idx):
        return jnp.take_along_axis(x, idx, axis=1, mode="promise_in_bounds")

    def tall(x):
        return jnp.concatenate([x] * (n_lab // 8), axis=0)

    neg32 = jnp.full((n_lab, LANES), NEG_BIG, F32)
    first_b = jnp.where(fwd32, jnp.where(row32 == 0, 0.0, NEG_BIG), jnp.where(end_blk, 0.0, NEG_BIG))
    first_t = jnp.where(fwd8, NEG_BIG, jnp.where(end_top, 0.0, NEG_BIG))

    def lat_step(i, j, u, carry):
        lab, blk, top_b = carry
        idx8 = base8 + jnp.where(fwd8, u, -u)
        idx32 = tall(idx8)
        back = n_blk - 1 - j
        e_l = jnp.where(fwd32, lanes_of(e_lab[j], idx32), lanes_of(e_lab[back], idx32))
        e_b = jnp.where(fwd8, lanes_of(e_blk[j], idx8), lanes_of(e_blk[back], idx8))
        lab_dn = pltpu.roll(lab, 1, 0)
        lab_up = pltpu.roll(lab, n_lab - 1, 0)
        blk_side = jnp.where(fwd32, blk, pltpu.roll(blk, n_lab - 1, 0))
        blk_side = jnp.concatenate([blk_side[:n_lab - 8], jnp.where(behind8, jnp.broadcast_to(top_b[0:1], (8, LANES)), blk_side[n_lab - 8:])], axis=0)
        lab_side = jnp.where(fwd32, lab_dn, lab)
        lab_side = jnp.concatenate([jnp.where(ahead8, NEG_BIG, lab_side[:8]), lab_side[8:]], axis=0)
        new_l = lse3(lab, blk_side, jnp.where(skip, jnp.where(fwd32, lab_dn, lab_up), NEG_BIG))
        new_b = lse2(blk, lab_side)
        new_t = lse2(top_b, jnp.where(ahead8, lab_dn[:8], NEG_BIG))
        s_lab[i] = new_l
        s_blk[i, 0:n_lab] = new_b
        s_blk[i, n_lab:n_lab + 8] = new_t
        behind = frames - 1 - i + pad
        r_lab[behind] = pltpu.roll(new_l, LANES - n_seq, 1)
        r_blk[behind, 0:n_lab] = pltpu.roll(new_b, LANES - n_seq, 1)
        r_blk[behind, n_lab:n_lab + 8] = pltpu.roll(new_t, LANES - n_seq, 1)
        at8 = jnp.where(fwd8, i, frames - 1 - i)
        live = tall(at8) < live32
        lab = jnp.where(live, e_l + new_l, lab)
        blk = jnp.where(live, tall(e_b) + new_b, blk)
        top_b = jnp.where(at8 < live8, e_b + new_t, top_b)
        return lab, blk, top_b

    group = zbuf.shape[1]
    n_lat_groups = n_lat // group
    pad = s_lab.shape[0] - frames

    def lattice_side(k, carry):
        for u in range(per_group):
            i = k * per_group + u
            j = lax.min(lax.div(i, HALF), n_blk - 1)
            carry = lat_step(i, j, lax.rem(i, HALF), carry)
        return carry

    n_occ = (hi - lo - n_lat) // group
    occ_group = frames // n_occ // HALF
    seq_of8 = jnp.where(lane8 >= HALF, 1, 0)
    run = z_oth_loop(lo, hi, join, h_ref, w_hbm, z_hbm, wbuf, wsem, zbuf, zsem,
                     [(n_lat_groups, lattice_side, lambda: (neg32, first_b, first_t)),
                      (n_occ, lambda k, c: occ_side(k, c), lambda: 0)])
    al, ab, at = next(run)

    lasts = [jnp.where(end, v, NEG_BIG) for end, v in ((end_lab, al), (end_blk, ab), (end_top, at))]
    top = functools.reduce(jnp.maximum, [jnp.max(v, **DOWN) for v in lasts])
    total = functools.reduce(jnp.add, [jnp.sum(jnp.exp2(v - top), **DOWN) for v in lasts])
    loss = -(top + jnp.log2(total))
    loss_at = lanes_of(jnp.broadcast_to(loss, (8, LANES)), seq_of8)
    lane1 = lane8[0:1]
    loss_ref[...] = jnp.broadcast_to(loss * (1.0 / LOG2E) - jnp.where(lane1 == 0, shift_seq0, jnp.where(lane1 == 1, shift_seq1, 0.0)), (8, LANES))

    def occ_side(k, c):
        for g in range(occ_group):
            j = k * occ_group + g
            seq_of32 = tall(seq_of8)
            logs = [neg32, neg32, neg32[0:8]]
            for u in range(HALF):
                i = j * HALF + u
                here8 = lax.rem(lane8, HALF) == u
                here32 = lax.rem(lane32, HALF) == u
                sum_l = s_lab[i] + r_lab[i + pad]
                sum_b = s_blk[i] + r_blk[i + pad]
                logs[0] = jnp.where(here32, lanes_of(sum_l, seq_of32), logs[0])
                logs[1] = jnp.where(here32, lanes_of(sum_b[:n_lab], seq_of32), logs[1])
                logs[2] = jnp.where(here8, lanes_of(sum_b[n_lab:], seq_of8), logs[2])
            rest = e_blk[j] + loss_at
            live = lax.rem(lane8, HALF) + HALF * j < jnp.broadcast_to(half_len, (8, LANES))
            occ_l = jnp.exp2(logs[0] + e_lab[j] + tall(loss_at))
            occ_b = jnp.sum(jnp.exp2(logs[1] + tall(rest)), **DOWN) + jnp.exp2(logs[2] + rest)[0:1]
            o_t[j, 0:n_lab] = jnp.where(tall(jnp.where(live, 1, 0)) > 0, occ_l, 0.0)
            o_t[j, n_lab:n_lab + 8] = jnp.where(live, jnp.broadcast_to(occ_b, (8, LANES)), 0.0)
            o_t[j, 8 + n_lab:LANES] = jnp.zeros((LANES - 8 - n_lab, LANES), F32)
        return c

    next(run)
    before_tail()
    for _ in run:
        pass
    row128 = lax.broadcasted_iota(jnp.int32, (LANES, LANES), 0)
    same = []
    for s in range(n_seq):
        down = jnp.full((n_lab, LANES), -1, jnp.int32)
        for k in range(n_lab):
            down = jnp.where(row32 == k, meta_ref[s, k], down)
        down = jnp.concatenate([down, jnp.full((LANES - n_lab, LANES), -1, jnp.int32)], axis=0)
        across = pltpu.roll(jnp.broadcast_to(lab_row[s:s + 1], (LANES, LANES)), HALF * s, 1)
        own = lane128 - HALF * s
        inner = (row128 < n_lab) & (own >= 0) & (own < n_lab)
        same.append(jnp.where((inner & (down == across)) | ((row128 == own) & (own < HALF)), 1.0, 0.0))
    for j in range(n_blk):
        y = o_t[j].T
        occ_ref[HALF * j:HALF * (j + 1), :] = functools.reduce(jnp.add, [
            jnp.dot(y[HALF * q:HALF * (q + 1), :], same[q], precision=lax.Precision.HIGHEST, preferred_element_type=F32) for q in range(n_seq)])


def combine_lse(refs, base):
    m = functools.reduce(jnp.maximum, [r[base:base + 8, :] for r in refs])
    tot = functools.reduce(jnp.add, [r[base + 8:base + 16, :] * jnp.exp(r[base:base + 8, :] - m) for r in refs])
    return m + jnp.log(tot)


def spread_lse(lse, meta_ref, lse_ref, r0, frames):
    t = lax.broadcasted_iota(jnp.int32, (LANES, LANES), 0)
    n_part = frames // LANES
    sums = []
    for q in range(meta_ref.shape[0]):
        live_sum = jnp.zeros((1, LANES), F32)
        for p in range(n_part):
            at = q * n_part + p
            part = jnp.broadcast_to(lse[at:at + 1, :], (LANES, LANES)).T
            live = t + p * LANES < meta_ref[q, meta_ref.shape[1] - 2]
            lse_ref[r0 + at * LANES:r0 + (at + 1) * LANES, :] = jnp.where(live, part, 1.0e30)
            live_sum = live_sum + jnp.sum(jnp.where(live, part, 0.0), **DOWN)
        sums.append(live_sum)
    return sums


def patch_tile(n_slots, frames, meta_refs, col_start, j, i, z_block, lse_ref, occ_ref, g_ref, g_col, lane):
    seq, item = i // n_slots, lax.rem(i, n_slots)
    off = label_col(meta_refs, i) - col_start - j * TILE
    blk = off // LANES
    r0 = pl.multiple_of(seq * frames, frames)
    c0 = pl.multiple_of(blk * LANES, LANES)
    zb = z_block(seq, c0)
    slot_lane = jnp.where(item == 0, n_slots - 1, item - 1) + HALF * seq
    at = off - blk * LANES
    occ = pltpu.roll(occ_ref[0:frames, :], lax.rem(at - slot_lane + LANES, LANES), 1)
    fresh = jnp.exp(zb - lse_ref[pl.ds(r0, frames), :]) - occ
    gc = pl.multiple_of(g_col + c0, LANES)
    old = g_ref[pl.ds(r0, frames), pl.ds(gc, LANES)].astype(F32)
    g_ref[pl.ds(r0, frames), pl.ds(gc, LANES)] = jnp.where(lane == at, fresh, old).astype(BF16)


def softmax_unit(z, z_row, lse_ref, out, r0, n, c0):
    total = None
    for b in range(n // 32):
        lse = lse_ref[r0 + 32 * b:r0 + 32 * (b + 1), :]
        for k in range(TILE // LANES):
            e = jnp.exp(z[z_row + 32 * b:z_row + 32 * (b + 1), k * LANES:(k + 1) * LANES] - lse)
            out[r0 + 32 * b:r0 + 32 * (b + 1), c0 + k * LANES:c0 + (k + 1) * LANES] = e.astype(BF16)
            total = e if total is None else total + e
    return exact_zero(total)


def grad_h_part(n_slots, z_hbm, w_hbm, st0, st1, st2, st3, occ_ref, part_loss, meta_ref, keep_ref, send_ref, loss_ref, g_hbm,
                  wbuf, wsem, zbuf, zsem, acc, lse_ref, g0, g1, gsem, head, nxt):
    n_tiles, rows = z_hbm.shape[0], z_hbm.shape[1]
    frames = rows // meta_ref.shape[0]
    meta_refs = [meta_ref]
    group = zbuf.shape[1]
    n_groups = n_tiles // group
    stream = TileStream(w_hbm, wbuf, wsem, wbuf.shape[0], n_groups, lambda src, j: w_view(src, j, group), W_PARTS)
    zs = TileStream(z_hbm, zbuf, zsem, zbuf.shape[0], n_groups, lambda src, j: z_view(src, j, group), group)
    zs.prime()
    yield stream.prime
    col_start = build_lists(meta_refs, n_tiles * TILE, head, nxt)
    lse = combine_lse([st0, st1, st2, st3], frames // 2)
    occ_ref[frames:frames + 8, :] = lse
    sums = spread_lse(lse, meta_ref, lse_ref, 0, frames)
    lane1 = lax.broadcasted_iota(jnp.int32, (8, LANES), 1)
    loss_ref[...] = part_loss[...] + jnp.where(lane1 == 0, sums[0], sums[1])
    lane = lax.broadcasted_iota(jnp.int32, (frames, LANES), 1)

    def patch(j, slot, g):
        for t in range(group):
            def z_block(seq, c0, t=t):
                return zbuf[slot, t, pl.ds(pl.multiple_of(seq * frames, frames), frames), pl.ds(c0, LANES)]

            walk_list(head, nxt, j * group + t,
                      lambda i, t=t, z_block=z_block: patch_tile(n_slots, frames, meta_refs, col_start, j * group + t, i, z_block, lse_ref, occ_ref, g, t * TILE, lane))

    def make_g(slot, u, g):
        t, r = u // 2, u % 2
        return softmax_unit(zbuf.at[slot, t], r * rows // 2, lse_ref, g, r * rows // 2, rows // 2, t * TILE)

    acc[...] = jnp.zeros(acc.shape, F32)
    slot0 = zs.get(0)
    for u in range(2 * group):
        make_g(slot0, u, g0)
    patch(0, slot0, g0)
    n_units = acc.shape[0] // 256

    def g_copy(j, g, k):
        return pltpu.make_async_copy(g, g_hbm.at[j], gsem.at[k])

    def half(j, g_now, g_next, k):
        slot = stream.get(j)
        nj = lax.min(j + 1, n_groups - 1)

        @pl.when(j + 1 < n_groups)
        def _():
            zs.get(nj)

        @pl.when(j >= 1)
        def _():
            g_copy(j - 1, g_next, 1 - k).wait()

        g_copy(j, g_now, k).start()

        zslot = lax.rem(nj, zbuf.shape[0])
        zero = None
        for u in range(n_units):
            d_rows = slice(u * 256, (u + 1) * 256)
            lhs = after(wbuf[slot, d_rows, :], zero)
            acc[d_rows, :] += lax.dot_general(lhs, g_now[...], (((1,), (1,)), ((), ())), preferred_element_type=F32)
            if u < 2 * group:
                zero = make_g(zslot, u, g_next)
        patch(nj, zslot, g_next)

    def step(i, c):
        half(2 * i, g0, g1, 0)
        half(2 * i + 1, g1, g0, 1)
        return c

    lax.fori_loop(0, n_groups // 2, step, 0)
    g_copy(n_groups - 1, g1, 1).wait()
    core = lax.rem(lax.axis_index("tp"), 2)
    n = rows // 2
    keep_ref[...] = acc[:, pl.ds(pl.multiple_of(core * n, n), n)].T
    send_ref[...] = acc[:, pl.ds(pl.multiple_of((1 - core) * n, n), n)].T


def mid_kernel(lo, hi, n_lat, per_group, n_lab, h_oth, w_hbm, p0, p1, p2, p3, z_own, meta_ref,
               z_hbm, occ_ref, keep_ref, send_ref, loss_ref, g_hbm,
               part_loss, h_ref, hsem, wbuf, wsem, zbuf, zsem, e_lab, e_blk, s_lab, s_blk, r_lab, r_blk, o_t,
               zin_buf, zin_sem, acc, lse_ref, g0, g1, gsem, head, nxt):
    second = grad_h_part(n_lab + 1, z_own, w_hbm, p0, p1, p2, p3, occ_ref, part_loss, meta_ref, keep_ref, send_ref, loss_ref, g_hbm,
                         wbuf, wsem, zin_buf, zin_sem, acc, lse_ref, g0, g1, gsem, head, nxt)
    prime_w = next(second)
    z_lattice_part(lo, hi, n_lat, per_group, n_lab, prime_w, h_oth, w_hbm, p0, p1, p2, p3, meta_ref,
                   z_hbm, occ_ref, part_loss,
                   h_ref, hsem, wbuf, wsem, zbuf, zsem, e_lab, e_blk, s_lab, s_blk, r_lab, r_blk, o_t)
    for _ in second:
        pass


def grad_w_kernel(n_slots, g_hbm, z_hbm, h_own_hbm, h_oth, occ_ref, meta_ref, gw_hbm,
                  h_ref, hsem, h_own_ref, zbuf, zsem, gsem, obuf, osem, ht, lse_ref, g0, g1, head, nxt):
    n_tiles, rows = z_hbm.shape[0], z_hbm.shape[1]
    frames = rows // meta_ref.shape[0]
    d_loc = ht.shape[0]
    group = zbuf.shape[1]
    n_groups = n_tiles // group
    zs = TileStream(z_hbm, zbuf, zsem, zbuf.shape[0], n_groups, lambda src, j: z_view(src, j, group), group)

    def g_copy(j, g, k):
        return pltpu.make_async_copy(g_hbm.at[j], g.at[0:rows, :], gsem.at[k])

    join = pltpu.make_async_copy(h_oth, h_ref, hsem.at[0])
    own_copy = pltpu.make_async_copy(h_own_hbm, h_own_ref, hsem.at[1])
    own_copy.start()
    join.start()
    zs.prime()
    g_copy(0, g0, 0).start()
    col_start = build_lists([meta_ref], n_tiles * TILE, head, nxt)
    d0 = pl.multiple_of(lax.axis_index("dp") * d_loc, LANES)
    own_copy.wait()
    ht[:, 0:rows] = h_own_ref[:, pl.ds(d0, d_loc)].T
    spread_lse(occ_ref[frames:frames + 8, :], meta_ref, lse_ref, 0, frames)
    join.wait()
    ht[:, rows:2 * rows] = h_ref[:, pl.ds(d0, d_loc)].T
    lane = lax.broadcasted_iota(jnp.int32, (frames, LANES), 1)
    n_units = 2 * group

    def make_g(slot, u, g):
        t, r = u // 2, u % 2
        return softmax_unit(zbuf.at[slot, t], r * rows // 2, lse_ref, g.at[rows:2 * rows, :], r * rows // 2, rows // 2, t * TILE)

    def patch(j, slot, g):
        for t in range(group):
            def z_block(seq, c0, t=t):
                return zbuf[slot, t, pl.ds(pl.multiple_of(seq * frames, frames), frames), pl.ds(c0, LANES)]

            walk_list(head, nxt, j * group + t,
                      lambda i, t=t, z_block=z_block: patch_tile(n_slots, frames, [meta_ref], col_start, j * group + t, i, z_block, lse_ref, occ_ref, g.at[rows:2 * rows, :], t * TILE, lane))

    def out_copy(j):
        slot = lax.rem(j, obuf.shape[0])
        return SplitCopy(obuf.at[slot], w_view(gw_hbm, j, group), osem.at[slot], W_PARTS)

    slot0 = zs.get(0)
    for u in range(n_units):
        make_g(slot0, u, g0)
    patch(0, slot0, g0)
    d_half = d_loc // 2

    def half(j, g_now, g_next, k):
        @pl.when(j >= 3)
        def _():
            out_copy(j - 3).wait()

        nj = lax.min(j + 1, n_groups - 1)

        @pl.when(j + 1 < n_groups)
        def _():
            zs.get(nj)
            g_copy(nj, g_next, 1 - k).start()

        g_copy(j, g_now, k).wait()
        slot = lax.rem(nj, zbuf.shape[0])
        oslot = lax.rem(j, obuf.shape[0])
        zero = None
        for u in range(n_units):
            t, r = u // 2, u % 2
            d_rows = slice(r * d_half, (r + 1) * d_half)
            lhs = after(ht[d_rows, :], zero)
            obuf[oslot, d_rows, t * TILE:(t + 1) * TILE] = jnp.dot(lhs, g_now[:, t * TILE:(t + 1) * TILE], preferred_element_type=F32)
            zero = make_g(slot, u, g_next)
        out_copy(j).start()
        patch(nj, slot, g_next)

    def step(i, c):
        half(2 * i, g0, g1, 0)
        half(2 * i + 1, g1, g0, 1)
        return c

    lax.fori_loop(0, n_groups // 2, step, 0)
    for j in range(n_groups - 3, n_groups):
        out_copy(j).wait()


def cost(flops, nbytes):
    return pl.CostEstimate(flops=flops, bytes_accessed=nbytes, transcendentals=0)


def solution(mesh):
    batch_axes = ("part", "dp")
    n_tp = mesh.shape["tp"]
    n_dp = mesh.shape["dp"]
    dp_swap = [(i, n_dp - 1 - i) for i in range(n_dp)]

    others = range(1, n_tp)

    def tp_xor(x, mask):
        return lax.ppermute(x, "tp", [(i, i ^ mask) for i in range(n_tp)])

    def in_hbm(x):
        return pltpu.with_memory_space_constraint(x, pltpu.HBM)

    def swap_dp(x):
        return lax.ppermute(x, "dp", dp_swap)

    def local_body(hidden, w_loc, labels, in_len, lab_len):
        batch_loc, frames, model_dim = hidden.shape
        vocab_loc = w_loc.shape[1]
        n_lab = labels.shape[1]
        n_slots = n_lab + 1
        rows = batch_loc * frames
        n_tiles = vocab_loc // TILE
        d_loc = model_dim // n_dp
        dma = pltpu.SemaphoreType.DMA
        i32 = jnp.int32
        n_lat, lat_steps, lat_pad = 24, 22, 8
        h_own = hidden.reshape(rows, model_dim)
        core = lax.rem(lax.axis_index("tp"), 2)
        h_oth = swap_dp(h_own)
        flops = 2 * rows * model_dim * TILE
        wbytes = model_dim * TILE * 2
        zbytes = rows * TILE * 4
        z_type = jax.ShapeDtypeStruct((n_tiles, rows, TILE), F32)
        pick_type = jax.ShapeDtypeStruct((frames // 2 + 24, LANES), F32)
        meta_type = jax.ShapeDtypeStruct((batch_loc, n_slots + 1), i32)
        g_type = jax.ShapeDtypeStruct((n_tiles // 2, rows, 2 * TILE), BF16)
        g_scratch = [pltpu.VMEM((rows, 2 * TILE), BF16)] * 2

        def w_scratch(n):
            return [pltpu.VMEM((3, model_dim, n * TILE), BF16), dma((3,))]

        def z_scratch(n):
            return [pltpu.VMEM((3, n, rows, TILE), F32), dma((3,))]

        h_scratch = [pltpu.VMEM((rows, model_dim), BF16), dma((2,))]
        run_scratch = [pltpu.VMEM((rows, LANES), F32), pltpu.VMEM((rows, LANES), F32)]

        def lists(n_sets):
            return [pltpu.SMEM((n_tiles,), i32), pltpu.SMEM((n_sets * batch_loc * n_slots,), i32)]

        z_own, pick, meta = kernel_call(
            functools.partial(z_own_kernel, n_slots),
            out_shape=(z_type, pick_type, meta_type),
            in_specs=[any_spec(), any_spec(), smem_spec(), smem_spec(), smem_spec()],
            out_specs=(any_spec(), vmem_spec(), smem_spec()),
            scratch_shapes=h_scratch + w_scratch(4) + z_scratch(4) + run_scratch + [pltpu.VMEM((frames // 2, LANES), F32)] + lists(1),
            compiler_params=params(),
            cost_estimate=cost(n_tiles * flops, n_tiles * (wbytes + zbytes)),
        )(in_hbm(h_own), w_loc, labels, in_len, lab_len)

        h_oth = in_hbm(h_oth)
        picks = [pick] + [tp_xor(pick, k) for k in others]

        n_blk = frames // HALF
        half_type = jax.ShapeDtypeStruct((rows // 2, model_dim), F32)
        occ_type = jax.ShapeDtypeStruct((frames + 8, LANES), F32)
        loss_type = jax.ShapeDtypeStruct((8, LANES), F32)
        z_oth, occ, keep, send, loss, g_own = kernel_call(
            functools.partial(mid_kernel, 0, n_tiles, n_lat, lat_steps, n_lab),
            out_shape=(z_type, occ_type, half_type, half_type, loss_type, g_type),
            in_specs=[any_spec()] * 2 + [vmem_spec()] * 4 + [any_spec(), smem_spec()],
            out_specs=(any_spec(),) + (vmem_spec(),) * 4 + (any_spec(),),
            scratch_shapes=[pltpu.VMEM((8, LANES), F32)] + h_scratch + w_scratch(2) + z_scratch(2) + [
                pltpu.VMEM((n_blk, n_lab, LANES), F32), pltpu.VMEM((n_blk, 8, LANES), F32),
                *[pltpu.VMEM((frames + lat_pad, n, LANES), F32) for n in (n_lab, n_lab + 8) * 2],
                pltpu.VMEM((n_blk, LANES, LANES), F32)] + z_scratch(2) + [
                pltpu.VMEM((model_dim, rows), F32), pltpu.VMEM((rows, LANES), F32)] + g_scratch + [dma((2,))] + lists(1),
            compiler_params=params(),
            cost_estimate=cost((2 * n_tiles) * flops, (2 * n_tiles) * (wbytes + zbytes)),
        )(h_oth, w_loc, *picks, z_own, meta)
        occ_oth = swap_dp(occ)
        meta_oth = swap_dp(meta)
        recv = tp_xor(send, 1)
        chip_sum = keep + recv
        across = tp_xor(chip_sum, 2)

        grad_weight = kernel_call(
            functools.partial(grad_w_kernel, n_slots),
            out_shape=jax.ShapeDtypeStruct((d_loc, vocab_loc), F32),
            in_specs=[any_spec(), any_spec(), any_spec(), any_spec(), vmem_spec(), smem_spec()],
            out_specs=any_spec(),
            scratch_shapes=h_scratch + h_scratch[:1] + z_scratch(2) + [
                dma((2,)), pltpu.VMEM((3, d_loc, 2 * TILE), F32), dma((3,)),
                pltpu.VMEM((d_loc, 2 * rows), BF16), pltpu.VMEM((rows, LANES), F32),
                pltpu.VMEM((2 * rows, 2 * TILE), BF16), pltpu.VMEM((2 * rows, 2 * TILE), BF16)] + lists(1),
            compiler_params=params(),
            cost_estimate=cost(n_tiles * flops, n_tiles * (2 * zbytes + d_loc * TILE * 4)),
        )(g_own, z_oth, in_hbm(h_own), h_oth, occ_oth, meta_oth)

        chip_sum, grad_weight = lax.optimization_barrier((chip_sum, grad_weight))
        full_half = chip_sum + across
        other_half = tp_xor(full_half, 1)
        grad_hidden = jnp.where(core == 0, jnp.stack([full_half, other_half]), jnp.stack([other_half, full_half])).reshape(batch_loc, frames, model_dim)
        return loss[0, :batch_loc], grad_weight, grad_hidden


    return jax.shard_map(
        local_body,
        mesh=mesh,
        in_specs=(P(batch_axes, None, None), P(None, "tp"), P(batch_axes, None), P(batch_axes), P(batch_axes)),
        out_specs=(P(batch_axes), P(batch_axes, "tp"), P(batch_axes, None, None)),
        check_vma=False,
    )
```

```python
import functools

import jax
import jax.numpy as jnp
from jax import lax
from jax.experimental import pallas as pl
from jax.experimental.pallas import tpu as pltpu
from jax.sharding import PartitionSpec as P

NEG_BIG = -1.0e30
LOG2E = 1.4426950408889634
F32 = jnp.float32
DOWN = dict(axis=0, keepdims=True)
ALONG = dict(axis=1, keepdims=True)
BF16 = jnp.bfloat16
TILE = 512
W_PARTS = 5
LANES = 128
HALF = LANES // 2
MIB = 1 << 20


def vmem_spec():
    return pl.BlockSpec(memory_space=pltpu.VMEM)


def smem_spec():
    return pl.BlockSpec(memory_space=pltpu.SMEM)


def any_spec():
    return pl.BlockSpec(memory_space=pl.ANY)


def kernel_call(*args, **kw):
    return pl.pallas_call(*args, **kw)


def params():
    return pltpu.CompilerParams(vmem_limit_bytes=56 * MIB)


def label_col(meta_refs, i):
    n_slots = meta_refs[0].shape[1] - 1
    seq, item = i // n_slots, lax.rem(i, n_slots)
    n_seq = meta_refs[0].shape[0]
    at = lax.max(item - 1, 0)
    col = meta_refs[0][lax.rem(seq, n_seq), at]
    for k in range(1, len(meta_refs)):
        col = jnp.where(seq >= k * n_seq, meta_refs[k][lax.rem(seq, n_seq), at], col)
    return jnp.where(item == 0, 0, col)


def build_lists(meta_refs, vocab_loc, head, nxt):
    n_items = len(meta_refs) * meta_refs[0].shape[0] * (meta_refs[0].shape[1] - 1)
    col_start = lax.axis_index("tp") * vocab_loc
    n_tiles = vocab_loc // TILE

    def clear(i, c):
        head[i] = -1
        return c

    lax.fori_loop(0, n_tiles, clear, 0)

    def insert(i, c):
        loc = label_col(meta_refs, i) - col_start
        tile = lax.max(loc, 0) // TILE

        @pl.when((loc >= 0) & (loc < vocab_loc))
        def _():
            nxt[i] = head[tile]
            head[tile] = i

        return c

    lax.fori_loop(0, n_items, insert, 0)
    return col_start


def walk_list(head, nxt, tile, visit):
    def body(i):
        visit(i)
        return nxt[i]

    lax.while_loop(lambda i: i >= 0, body, head[tile])


class SplitCopy:
    def __init__(self, src, dst, sem, parts):
        n = src.shape[0] // parts
        self.copies = [pltpu.make_async_copy(src.at[pl.ds(p * n, n)], dst.at[pl.ds(p * n, n)], sem) for p in range(parts)]

    def start(self):
        for p, c in enumerate(self.copies):
            c.start(priority=p % 2)

    def wait(self):
        for c in self.copies:
            c.wait()


class TileStream:
    def __init__(self, src, buf, sem, depth, n_tiles, view, parts):
        self.src, self.buf, self.sem, self.depth, self.n, self.view, self.parts = src, buf, sem, depth, n_tiles, view, parts

    def copy(self, j):
        slot = lax.rem(j, self.depth)
        return SplitCopy(self.view(self.src, j), self.buf.at[slot], self.sem.at[slot], self.parts)

    def prime(self):
        for j in range(min(self.depth - 1, self.n)):
            self.copy(j).start()

    def get(self, j):
        self.copy(j).wait()

        @pl.when(j + self.depth - 1 < self.n)
        def _():
            self.copy(j + self.depth - 1).start()

        return lax.rem(j, self.depth)


def w_view(src, j, n=1):
    return src.at[:, pl.ds(pl.multiple_of(j * n * TILE, TILE), n * TILE)]


def z_view(src, j, n):
    return src.at[pl.ds(j * n, n)]


def exact_zero(total):
    return jnp.minimum(total[0:16] + total[16:32], 0.0).astype(BF16)


def after(lhs, zero):
    if zero is None:
        return lhs
    corner = lhs[0:16, 0:LANES] + zero
    return jnp.concatenate([jnp.concatenate([corner, lhs[0:16, LANES:]], axis=1), lhs[16:]], axis=0)


def unit_stats(z, m_ref, s_ref, r0):
    n_chunks = z.shape[1] // LANES
    total = None
    for b in range(z.shape[0] // 32):
        zb = [z[32 * b:32 * (b + 1), k * LANES:(k + 1) * LANES] for k in range(n_chunks)]
        rows = slice(r0 + 32 * b, r0 + 32 * (b + 1))
        m_old = m_ref[rows, :]
        m_new = functools.reduce(jnp.maximum, zb, m_old)
        s_new = s_ref[rows, :] * jnp.exp(m_old - m_new)
        for part in zb:
            s_new = s_new + jnp.exp(part - m_new)
        m_ref[rows, :] = m_new
        s_ref[rows, :] = s_new
        total = s_new if total is None else total + s_new
    return exact_zero(total)


def z_group(h_ref, w, z_out, m_ref, s_ref):
    n_tiles = z_out.shape[0]
    n = h_ref.shape[0] // 2
    zeros = []
    if m_ref is None:
        for t in range(n_tiles):
            z_out[t] = jnp.dot(h_ref[...], w[:, t * TILE:(t + 1) * TILE], preferred_element_type=F32)
        return
    for t in range(n_tiles):
        for r in range(2):
            rows = slice(r * n, (r + 1) * n)
            lhs = after(h_ref[rows, :], zeros[-2] if len(zeros) >= 2 else None)
            z = jnp.dot(lhs, w[:, t * TILE:(t + 1) * TILE], preferred_element_type=F32)
            z_out[t, rows, :] = z
            zeros.append(unit_stats(z, m_ref, s_ref, r * n))


def emit_stats(m_ref, s_ref, out_ref, base):
    row_m = jnp.max(m_ref[...], **ALONG)
    row_s = jnp.sum(s_ref[...] * jnp.exp(m_ref[...] - row_m), **ALONG)
    rows = m_ref.shape[0]
    for k, v in enumerate((row_m, row_s)):
        flat = jnp.broadcast_to(v, (rows, LANES)).T
        for p in range(rows // LANES):
            at = base + 8 * k + p
            out_ref[at:at + 1, :] = flat[0:1, p * LANES:(p + 1) * LANES]


def z_own_kernel(n_slots, h_hbm, w_hbm, labels_ref, in_len_ref, lab_len_ref, z_hbm, pick_ref, meta_ref, h_ref, hsem, wbuf, wsem, zbuf, zsem, m_ref, s_ref, blank, head, nxt):
    n_tiles = z_hbm.shape[0]
    rows = h_ref.shape[0]
    n_seq = meta_ref.shape[0]
    frames = rows // n_seq
    h_copy = pltpu.make_async_copy(h_hbm, h_ref, hsem.at[0])
    h_copy.start()
    n_lab = n_slots - 1
    for q in range(n_seq):
        def put(k, c, q=q):
            meta_ref[q, k] = labels_ref[q, k]
            return c

        lax.fori_loop(0, n_lab, put, 0)
        meta_ref[q, n_lab] = in_len_ref[q]
        meta_ref[q, n_lab + 1] = lab_len_ref[q]
    group = zbuf.shape[1]
    stream = TileStream(w_hbm, wbuf, wsem, wbuf.shape[0], n_tiles // group, lambda src, j: w_view(src, j, group), W_PARTS)
    stream.prime()
    col_start = build_lists([meta_ref], n_tiles * TILE, head, nxt)
    m_ref[...] = jnp.full(m_ref.shape, NEG_BIG, F32)
    s_ref[...] = jnp.zeros(s_ref.shape, F32)
    pick_ref[...] = jnp.zeros(pick_ref.shape, F32)
    blank[...] = jnp.zeros(blank.shape, F32)
    half = frames // 2
    h_copy.wait()
    lane = lax.broadcasted_iota(jnp.int32, (half, LANES), 1)

    def out_copy(j):
        slot = lax.rem(j, zbuf.shape[0])
        return SplitCopy(zbuf.at[slot], z_view(z_hbm, j, group), zsem.at[slot], group)

    def step(j, c):
        slot = stream.get(j)

        @pl.when(j >= 3)
        def _():
            out_copy(j - 3).wait()

        zslot = lax.rem(j, zbuf.shape[0])
        z_group(h_ref, wbuf.at[slot], zbuf.at[zslot], m_ref, s_ref)
        out_copy(j).start()

        for t in range(group):
            def visit(i, t=t):
                seq, item = i // n_slots, lax.rem(i, n_slots)
                off = label_col([meta_ref], i) - col_start - (j * group + t) * TILE
                blk = off // LANES
                r0 = pl.multiple_of(seq * frames, frames)
                src = off - blk * LANES
                c0 = pl.multiple_of(blk * LANES, LANES)

                def moved(p, at):
                    zb = zbuf[zslot, t, pl.ds(r0 + p * half, half), pl.ds(c0, LANES)]
                    return pltpu.roll(zb, lax.rem(at - src + LANES, LANES), 1)

                @pl.when(item > 0)
                def _():
                    for p in range(2):
                        at = item - 1 + n_lab * seq + HALF * p
                        pick_ref[0:half, :] = jnp.where(lane == at, moved(p, at), pick_ref[0:half, :])

                @pl.when(item == 0)
                def _():
                    for p in range(2):
                        at = 2 * seq + p
                        blank[...] = jnp.where(lane == at, moved(p, at), blank[...])

            walk_list(head, nxt, j * group + t, visit)
        return c

    n_groups = n_tiles // group
    lax.fori_loop(0, n_groups, step, 0)
    emit_stats(m_ref, s_ref, pick_ref, half)
    pick_ref[half + 16:half + 24, :] = blank[...].T[0:8]
    for j in range(n_groups - 3, n_groups):
        out_copy(j).wait()


def z_oth_loop(lo, hi, join, h_ref, w_hbm, z_hbm, wbuf, wsem, zbuf, zsem, sections):
    group = zbuf.shape[1]
    lo, n_groups = lo // group, (hi - lo) // group
    stream = TileStream(w_hbm, wbuf, wsem, wbuf.shape[0], n_groups, lambda src, j: w_view(src, lo + j, group), W_PARTS)
    stream.prime()

    def out_copy(j):
        slot = lax.rem(j, zbuf.shape[0])
        return SplitCopy(zbuf.at[slot], z_view(z_hbm, lo + j, group), zsem.at[slot], group)

    base = 0
    join.wait()
    for n, side, make_carry in sections:
        carry = make_carry()

        def step(k, c, base=base, side=side):
            j = base + k
            slot = stream.get(j)

            @pl.when(j >= 3)
            def _():
                out_copy(j - 3).wait()

            z_group(h_ref, wbuf.at[slot], zbuf.at[lax.rem(j, zbuf.shape[0])], None, None)
            c = side(k, c)
            out_copy(j).start()
            return c

        last = lax.fori_loop(0, n, step, carry)
        yield last
        base += n
    for j in range(max(n_groups - 3, 0), n_groups):
        out_copy(j).wait()


def z_lattice_part(lo, hi, n_lat, per_group, n_lab, before_tail, h_oth, w_hbm, p0, p1, p2, p3, meta_ref,
                     z_hbm, occ_ref, loss_ref,
                     h_ref, hsem, wbuf, wsem, zbuf, zsem, e_lab, e_blk, s_lab, s_blk, r_lab, r_blk, o_t):
    join = pltpu.make_async_copy(h_oth, h_ref, hsem.at[0])
    join.start()
    n_blk = e_lab.shape[0]
    frames = n_blk * HALF
    lane128 = lax.broadcasted_iota(jnp.int32, (LANES, LANES), 1)
    row32 = lax.broadcasted_iota(jnp.int32, (n_lab, LANES), 0)
    row8 = lax.broadcasted_iota(jnp.int32, (8, LANES), 0)
    lane32 = lax.broadcasted_iota(jnp.int32, (n_lab, LANES), 1)
    lane8 = lax.broadcasted_iota(jnp.int32, (8, LANES), 1)
    n_seq = meta_ref.shape[0]
    labs = jnp.zeros((n_lab, LANES), jnp.int32)
    lab_row = jnp.zeros((8, LANES), jnp.int32)
    live8 = jnp.zeros((8, LANES), jnp.int32)
    used8 = jnp.zeros((8, LANES), jnp.int32)
    for s in range(n_seq):
        for k in range(n_lab):
            labs = jnp.where((row32 == k) & ((lane32 == s) | (lane32 == s + n_seq)), meta_ref[s, k], labs)
            lab_row = jnp.where((row8 == s) & (lane8 == k), meta_ref[s, k], lab_row)
        here = (lane8 == s) | (lane8 == s + n_seq)
        live8 = jnp.where(here, meta_ref[s, n_lab], live8)
        used8 = jnp.where(here, meta_ref[s, n_lab + 1], used8)
    live32 = jnp.broadcast_to(live8[0:1], (n_lab, LANES))
    used32 = jnp.broadcast_to(used8[0:1], (n_lab, LANES))
    skip_dn = labs != pltpu.roll(labs, 1, 0)
    skip_up = labs != pltpu.roll(labs, n_lab - 1, 0)
    end_lab = row32 == used32 - 1
    end_blk = row32 == used32
    end_top = (row8 == 0) & (used8 == n_lab)
    shift0 = jnp.zeros((1, LANES), F32)
    seq1 = lane8[0:1] >= HALF
    half_len = jnp.where(seq1, meta_ref[1, n_lab], meta_ref[0, n_lab])
    half = frames // 2
    packed = functools.reduce(jnp.add, [p[0:half, :] for p in (p0, p1, p2, p3)])
    blanks = functools.reduce(jnp.add, [p[half + 16:half + 24, :] for p in (p0, p1, p2, p3)])
    for j in range(n_blk):
        far, near = j // 2, HALF * (j % 2)
        part = packed[near:near + HALF]
        x = jnp.concatenate([pltpu.roll(part, (LANES - HALF * far - n_lab * q) % LANES, 1) for q in range(2)], axis=0).T[0:n_lab]
        rows_b = [pltpu.roll(blanks, (HALF * q - near) % LANES, 1)[2 * q + far:2 * q + far + 1] for q in range(2)]
        x_blank = jnp.where(seq1, rows_b[1], rows_b[0])
        top = jnp.maximum(jnp.max(x, **DOWN), x_blank)
        e_blk[j] = jnp.broadcast_to((x_blank - top) * LOG2E, (8, LANES))
        e_lab[j] = (x - top) * LOG2E
        shift0 = shift0 + jnp.where(lax.rem(lane8[0:1], HALF) + HALF * j < half_len, top, 0.0)
    shift_seq0 = jnp.sum(jnp.where(seq1, 0.0, shift0), **ALONG)
    shift_seq1 = jnp.sum(jnp.where(seq1, shift0, 0.0), **ALONG)

    def lse2(a, b):
        hi_v = jnp.maximum(a, b)
        return hi_v + jnp.log2(1.0 + jnp.exp2(jnp.minimum(a, b) - hi_v))

    def lse3(a, b, c):
        hi_v = jnp.maximum(a, b)
        lo_v = jnp.minimum(a, b)
        top = jnp.maximum(hi_v, c)
        mid = jnp.minimum(hi_v, c)
        return top + jnp.log2(1.0 + (jnp.exp2(lo_v - top) + jnp.exp2(mid - top)))

    fwd8, fwd32 = lane8 < n_seq, lane32 < n_seq
    ahead8 = fwd8 & (row8 == 0)
    behind8 = (lane8 >= n_seq) & (row8 == 7)
    base8 = jnp.where(fwd8, HALF * lane8, HALF * (lane8 - n_seq) + HALF - 1)
    base8 = jnp.where(lane8 < 2 * n_seq, base8, HALF)
    skip = jnp.where(fwd32, jnp.where(skip_dn & (row32 > 0), 1, 0), jnp.where(skip_up & (row32 < n_lab - 1), 1, 0)) > 0

    def lanes_of(x, idx):
        return jnp.take_along_axis(x, idx, axis=1, mode="promise_in_bounds")

    def tall(x):
        return jnp.concatenate([x] * (n_lab // 8), axis=0)

    neg32 = jnp.full((n_lab, LANES), NEG_BIG, F32)
    first_b = jnp.where(fwd32, jnp.where(row32 == 0, 0.0, NEG_BIG), jnp.where(end_blk, 0.0, NEG_BIG))
    first_t = jnp.where(fwd8, NEG_BIG, jnp.where(end_top, 0.0, NEG_BIG))

    def lat_step(i, j, u, carry):
        lab, blk, top_b = carry
        idx8 = base8 + jnp.where(fwd8, u, -u)
        idx32 = tall(idx8)
        back = n_blk - 1 - j
        e_l = jnp.where(fwd32, lanes_of(e_lab[j], idx32), lanes_of(e_lab[back], idx32))
        e_b = jnp.where(fwd8, lanes_of(e_blk[j], idx8), lanes_of(e_blk[back], idx8))
        lab_dn = pltpu.roll(lab, 1, 0)
        lab_up = pltpu.roll(lab, n_lab - 1, 0)
        blk_side = jnp.where(fwd32, blk, pltpu.roll(blk, n_lab - 1, 0))
        blk_side = jnp.concatenate([blk_side[:n_lab - 8], jnp.where(behind8, jnp.broadcast_to(top_b[0:1], (8, LANES)), blk_side[n_lab - 8:])], axis=0)
        lab_side = jnp.where(fwd32, lab_dn, lab)
        lab_side = jnp.concatenate([jnp.where(ahead8, NEG_BIG, lab_side[:8]), lab_side[8:]], axis=0)
        new_l = lse3(lab, blk_side, jnp.where(skip, jnp.where(fwd32, lab_dn, lab_up), NEG_BIG))
        new_b = lse2(blk, lab_side)
        new_t = lse2(top_b, jnp.where(ahead8, lab_dn[:8], NEG_BIG))
        s_lab[i] = new_l
        s_blk[i, 0:n_lab] = new_b
        s_blk[i, n_lab:n_lab + 8] = new_t
        behind = frames - 1 - i + pad
        r_lab[behind] = pltpu.roll(new_l, LANES - n_seq, 1)
        r_blk[behind, 0:n_lab] = pltpu.roll(new_b, LANES - n_seq, 1)
        r_blk[behind, n_lab:n_lab + 8] = pltpu.roll(new_t, LANES - n_seq, 1)
        at8 = jnp.where(fwd8, i, frames - 1 - i)
        live = tall(at8) < live32
        lab = jnp.where(live, e_l + new_l, lab)
        blk = jnp.where(live, tall(e_b) + new_b, blk)
        top_b = jnp.where(at8 < live8, e_b + new_t, top_b)
        return lab, blk, top_b

    group = zbuf.shape[1]
    n_lat_groups = n_lat // group
    pad = s_lab.shape[0] - frames

    def lattice_side(k, carry):
        for u in range(per_group):
            i = k * per_group + u
            j = lax.min(lax.div(i, HALF), n_blk - 1)
            carry = lat_step(i, j, lax.rem(i, HALF), carry)
        return carry

    n_occ = (hi - lo - n_lat) // group
    occ_group = frames // n_occ // HALF
    seq_of8 = jnp.where(lane8 >= HALF, 1, 0)
    run = z_oth_loop(lo, hi, join, h_ref, w_hbm, z_hbm, wbuf, wsem, zbuf, zsem,
                     [(n_lat_groups, lattice_side, lambda: (neg32, first_b, first_t)),
                      (n_occ, lambda k, c: occ_side(k, c), lambda: 0)])
    al, ab, at = next(run)

    lasts = [jnp.where(end, v, NEG_BIG) for end, v in ((end_lab, al), (end_blk, ab), (end_top, at))]
    top = functools.reduce(jnp.maximum, [jnp.max(v, **DOWN) for v in lasts])
    total = functools.reduce(jnp.add, [jnp.sum(jnp.exp2(v - top), **DOWN) for v in lasts])
    loss = -(top + jnp.log2(total))
    loss_at = lanes_of(jnp.broadcast_to(loss, (8, LANES)), seq_of8)
    lane1 = lane8[0:1]
    loss_ref[...] = jnp.broadcast_to(loss * (1.0 / LOG2E) - jnp.where(lane1 == 0, shift_seq0, jnp.where(lane1 == 1, shift_seq1, 0.0)), (8, LANES))

    def occ_side(k, c):
        for g in range(occ_group):
            j = k * occ_group + g
            seq_of32 = tall(seq_of8)
            logs = [neg32, neg32, neg32[0:8]]
            for u in range(HALF):
                i = j * HALF + u
                here8 = lax.rem(lane8, HALF) == u
                here32 = lax.rem(lane32, HALF) == u
                sum_l = s_lab[i] + r_lab[i + pad]
                sum_b = s_blk[i] + r_blk[i + pad]
                logs[0] = jnp.where(here32, lanes_of(sum_l, seq_of32), logs[0])
                logs[1] = jnp.where(here32, lanes_of(sum_b[:n_lab], seq_of32), logs[1])
                logs[2] = jnp.where(here8, lanes_of(sum_b[n_lab:], seq_of8), logs[2])
            rest = e_blk[j] + loss_at
            live = lax.rem(lane8, HALF) + HALF * j < jnp.broadcast_to(half_len, (8, LANES))
            occ_l = jnp.exp2(logs[0] + e_lab[j] + tall(loss_at))
            occ_b = jnp.sum(jnp.exp2(logs[1] + tall(rest)), **DOWN) + jnp.exp2(logs[2] + rest)[0:1]
            o_t[j, 0:n_lab] = jnp.where(tall(jnp.where(live, 1, 0)) > 0, occ_l, 0.0)
            o_t[j, n_lab:n_lab + 8] = jnp.where(live, jnp.broadcast_to(occ_b, (8, LANES)), 0.0)
            o_t[j, 8 + n_lab:LANES] = jnp.zeros((LANES - 8 - n_lab, LANES), F32)
        return c

    next(run)
    before_tail()
    for _ in run:
        pass
    row128 = lax.broadcasted_iota(jnp.int32, (LANES, LANES), 0)
    same = []
    for s in range(n_seq):
        down = jnp.full((n_lab, LANES), -1, jnp.int32)
        for k in range(n_lab):
            down = jnp.where(row32 == k, meta_ref[s, k], down)
        down = jnp.concatenate([down, jnp.full((LANES - n_lab, LANES), -1, jnp.int32)], axis=0)
        across = pltpu.roll(jnp.broadcast_to(lab_row[s:s + 1], (LANES, LANES)), HALF * s, 1)
        own = lane128 - HALF * s
        inner = (row128 < n_lab) & (own >= 0) & (own < n_lab)
        same.append(jnp.where((inner & (down == across)) | ((row128 == own) & (own < HALF)), 1.0, 0.0))
    for j in range(n_blk):
        y = o_t[j].T
        occ_ref[HALF * j:HALF * (j + 1), :] = functools.reduce(jnp.add, [
            jnp.dot(y[HALF * q:HALF * (q + 1), :], same[q], precision=lax.Precision.HIGHEST, preferred_element_type=F32) for q in range(n_seq)])


def combine_lse(refs, base):
    m = functools.reduce(jnp.maximum, [r[base:base + 8, :] for r in refs])
    tot = functools.reduce(jnp.add, [r[base + 8:base + 16, :] * jnp.exp(r[base:base + 8, :] - m) for r in refs])
    return m + jnp.log(tot)


def spread_lse(lse, meta_ref, lse_ref, r0, frames):
    t = lax.broadcasted_iota(jnp.int32, (LANES, LANES), 0)
    n_part = frames // LANES
    sums = []
    for q in range(meta_ref.shape[0]):
        live_sum = jnp.zeros((1, LANES), F32)
        for p in range(n_part):
            at = q * n_part + p
            part = jnp.broadcast_to(lse[at:at + 1, :], (LANES, LANES)).T
            live = t + p * LANES < meta_ref[q, meta_ref.shape[1] - 2]
            lse_ref[r0 + at * LANES:r0 + (at + 1) * LANES, :] = jnp.where(live, part, 1.0e30)
            live_sum = live_sum + jnp.sum(jnp.where(live, part, 0.0), **DOWN)
        sums.append(live_sum)
    return sums


def patch_tile(n_slots, frames, meta_refs, col_start, j, i, z_block, lse_ref, occ_ref, g_ref, g_col, lane):
    seq, item = i // n_slots, lax.rem(i, n_slots)
    off = label_col(meta_refs, i) - col_start - j * TILE
    blk = off // LANES
    r0 = pl.multiple_of(seq * frames, frames)
    c0 = pl.multiple_of(blk * LANES, LANES)
    zb = z_block(seq, c0)
    slot_lane = jnp.where(item == 0, n_slots - 1, item - 1) + HALF * seq
    at = off - blk * LANES
    occ = pltpu.roll(occ_ref[0:frames, :], lax.rem(at - slot_lane + LANES, LANES), 1)
    fresh = jnp.exp(zb - lse_ref[pl.ds(r0, frames), :]) - occ
    gc = pl.multiple_of(g_col + c0, LANES)
    old = g_ref[pl.ds(r0, frames), pl.ds(gc, LANES)].astype(F32)
    g_ref[pl.ds(r0, frames), pl.ds(gc, LANES)] = jnp.where(lane == at, fresh, old).astype(BF16)


def softmax_unit(z, z_row, lse_ref, out, r0, n, c0):
    total = None
    for b in range(n // 32):
        lse = lse_ref[r0 + 32 * b:r0 + 32 * (b + 1), :]
        for k in range(TILE // LANES):
            e = jnp.exp(z[z_row + 32 * b:z_row + 32 * (b + 1), k * LANES:(k + 1) * LANES] - lse)
            out[r0 + 32 * b:r0 + 32 * (b + 1), c0 + k * LANES:c0 + (k + 1) * LANES] = e.astype(BF16)
            total = e if total is None else total + e
    return exact_zero(total)


def grad_h_part(n_slots, z_hbm, w_hbm, st0, st1, st2, st3, occ_ref, part_loss, meta_ref, keep_ref, send_ref, loss_ref, g_hbm,
                  wbuf, wsem, zbuf, zsem, acc, lse_ref, g0, g1, gsem, head, nxt):
    n_tiles, rows = z_hbm.shape[0], z_hbm.shape[1]
    frames = rows // meta_ref.shape[0]
    meta_refs = [meta_ref]
    group = zbuf.shape[1]
    n_groups = n_tiles // group
    stream = TileStream(w_hbm, wbuf, wsem, wbuf.shape[0], n_groups, lambda src, j: w_view(src, j, group), W_PARTS)
    zs = TileStream(z_hbm, zbuf, zsem, zbuf.shape[0], n_groups, lambda src, j: z_view(src, j, group), group)
    zs.prime()
    yield stream.prime
    col_start = build_lists(meta_refs, n_tiles * TILE, head, nxt)
    lse = combine_lse([st0, st1, st2, st3], frames // 2)
    occ_ref[frames:frames + 8, :] = lse
    sums = spread_lse(lse, meta_ref, lse_ref, 0, frames)
    lane1 = lax.broadcasted_iota(jnp.int32, (8, LANES), 1)
    loss_ref[...] = part_loss[...] + jnp.where(lane1 == 0, sums[0], sums[1])
    lane = lax.broadcasted_iota(jnp.int32, (frames, LANES), 1)

    def patch(j, slot, g):
        for t in range(group):
            def z_block(seq, c0, t=t):
                return zbuf[slot, t, pl.ds(pl.multiple_of(seq * frames, frames), frames), pl.ds(c0, LANES)]

            walk_list(head, nxt, j * group + t,
                      lambda i, t=t, z_block=z_block: patch_tile(n_slots, frames, meta_refs, col_start, j * group + t, i, z_block, lse_ref, occ_ref, g, t * TILE, lane))

    def make_g(slot, u, g):
        t, r = u // 2, u % 2
        return softmax_unit(zbuf.at[slot, t], r * rows // 2, lse_ref, g, r * rows // 2, rows // 2, t * TILE)

    acc[...] = jnp.zeros(acc.shape, F32)
    slot0 = zs.get(0)
    for u in range(2 * group):
        make_g(slot0, u, g0)
    patch(0, slot0, g0)
    n_units = acc.shape[0] // 256

    def g_copy(j, g, k):
        return pltpu.make_async_copy(g, g_hbm.at[j], gsem.at[k])

    def half(j, g_now, g_next, k):
        slot = stream.get(j)
        nj = lax.min(j + 1, n_groups - 1)

        @pl.when(j + 1 < n_groups)
        def _():
            zs.get(nj)

        @pl.when(j >= 1)
        def _():
            g_copy(j - 1, g_next, 1 - k).wait()

        g_copy(j, g_now, k).start()

        zslot = lax.rem(nj, zbuf.shape[0])
        zero = None
        for u in range(n_units):
            d_rows = slice(u * 256, (u + 1) * 256)
            lhs = after(wbuf[slot, d_rows, :], zero)
            acc[d_rows, :] += lax.dot_general(lhs, g_now[...], (((1,), (1,)), ((), ())), preferred_element_type=F32)
            if u < 2 * group:
                zero = make_g(zslot, u, g_next)
        patch(nj, zslot, g_next)

    def step(i, c):
        half(2 * i, g0, g1, 0)
        half(2 * i + 1, g1, g0, 1)
        return c

    lax.fori_loop(0, n_groups // 2, step, 0)
    g_copy(n_groups - 1, g1, 1).wait()
    core = lax.rem(lax.axis_index("tp"), 2)
    n = rows // 2
    keep_ref[...] = acc[:, pl.ds(pl.multiple_of(core * n, n), n)].T
    send_ref[...] = acc[:, pl.ds(pl.multiple_of((1 - core) * n, n), n)].T


def mid_kernel(lo, hi, n_lat, per_group, n_lab, h_oth, w_hbm, p0, p1, p2, p3, z_own, meta_ref,
               z_hbm, occ_ref, keep_ref, send_ref, loss_ref, g_hbm,
               part_loss, h_ref, hsem, wbuf, wsem, zbuf, zsem, e_lab, e_blk, s_lab, s_blk, r_lab, r_blk, o_t,
               zin_buf, zin_sem, acc, lse_ref, g0, g1, gsem, head, nxt):
    second = grad_h_part(n_lab + 1, z_own, w_hbm, p0, p1, p2, p3, occ_ref, part_loss, meta_ref, keep_ref, send_ref, loss_ref, g_hbm,
                         wbuf, wsem, zin_buf, zin_sem, acc, lse_ref, g0, g1, gsem, head, nxt)
    prime_w = next(second)
    z_lattice_part(lo, hi, n_lat, per_group, n_lab, prime_w, h_oth, w_hbm, p0, p1, p2, p3, meta_ref,
                   z_hbm, occ_ref, part_loss,
                   h_ref, hsem, wbuf, wsem, zbuf, zsem, e_lab, e_blk, s_lab, s_blk, r_lab, r_blk, o_t)
    for _ in second:
        pass


def grad_w_kernel(n_slots, g_hbm, z_hbm, h_own_hbm, h_oth, occ_ref, meta_ref, gw_hbm,
                  h_ref, hsem, h_own_ref, zbuf, zsem, gsem, obuf, osem, ht, lse_ref, g0, g1, head, nxt):
    n_tiles, rows = z_hbm.shape[0], z_hbm.shape[1]
    frames = rows // meta_ref.shape[0]
    d_loc = ht.shape[0]
    group = zbuf.shape[1]
    n_groups = n_tiles // group
    zs = TileStream(z_hbm, zbuf, zsem, zbuf.shape[0], n_groups, lambda src, j: z_view(src, j, group), group)

    def g_copy(j, g, k):
        return pltpu.make_async_copy(g_hbm.at[j], g.at[0:rows, :], gsem.at[k])

    join = pltpu.make_async_copy(h_oth, h_ref, hsem.at[0])
    own_copy = pltpu.make_async_copy(h_own_hbm, h_own_ref, hsem.at[1])
    own_copy.start()
    join.start()
    zs.prime()
    g_copy(0, g0, 0).start()
    col_start = build_lists([meta_ref], n_tiles * TILE, head, nxt)
    d0 = pl.multiple_of(lax.axis_index("dp") * d_loc, LANES)
    own_copy.wait()
    ht[:, 0:rows] = h_own_ref[:, pl.ds(d0, d_loc)].T
    spread_lse(occ_ref[frames:frames + 8, :], meta_ref, lse_ref, 0, frames)
    join.wait()
    ht[:, rows:2 * rows] = h_ref[:, pl.ds(d0, d_loc)].T
    lane = lax.broadcasted_iota(jnp.int32, (frames, LANES), 1)
    n_units = 2 * group

    def make_g(slot, u, g):
        t, r = u // 2, u % 2
        return softmax_unit(zbuf.at[slot, t], r * rows // 2, lse_ref, g.at[rows:2 * rows, :], r * rows // 2, rows // 2, t * TILE)

    def patch(j, slot, g):
        for t in range(group):
            def z_block(seq, c0, t=t):
                return zbuf[slot, t, pl.ds(pl.multiple_of(seq * frames, frames), frames), pl.ds(c0, LANES)]

            walk_list(head, nxt, j * group + t,
                      lambda i, t=t, z_block=z_block: patch_tile(n_slots, frames, [meta_ref], col_start, j * group + t, i, z_block, lse_ref, occ_ref, g.at[rows:2 * rows, :], t * TILE, lane))

    def out_copy(j):
        slot = lax.rem(j, obuf.shape[0])
        return SplitCopy(obuf.at[slot], w_view(gw_hbm, j, group), osem.at[slot], W_PARTS)

    slot0 = zs.get(0)
    for u in range(n_units):
        make_g(slot0, u, g0)
    patch(0, slot0, g0)
    d_half = d_loc // 2

    def half(j, g_now, g_next, k):
        @pl.when(j >= 3)
        def _():
            out_copy(j - 3).wait()

        nj = lax.min(j + 1, n_groups - 1)

        @pl.when(j + 1 < n_groups)
        def _():
            zs.get(nj)
            g_copy(nj, g_next, 1 - k).start()

        g_copy(j, g_now, k).wait()
        slot = lax.rem(nj, zbuf.shape[0])
        oslot = lax.rem(j, obuf.shape[0])
        zero = None
        for u in range(n_units):
            t, r = u // 2, u % 2
            d_rows = slice(r * d_half, (r + 1) * d_half)
            lhs = after(ht[d_rows, :], zero)
            obuf[oslot, d_rows, t * TILE:(t + 1) * TILE] = jnp.dot(lhs, g_now[:, t * TILE:(t + 1) * TILE], preferred_element_type=F32)
            zero = make_g(slot, u, g_next)
        out_copy(j).start()
        patch(nj, slot, g_next)

    def step(i, c):
        half(2 * i, g0, g1, 0)
        half(2 * i + 1, g1, g0, 1)
        return c

    lax.fori_loop(0, n_groups // 2, step, 0)
    for j in range(n_groups - 3, n_groups):
        out_copy(j).wait()


def cost(flops, nbytes):
    return pl.CostEstimate(flops=flops, bytes_accessed=nbytes, transcendentals=0)


def solution(mesh):
    batch_axes = ("part", "dp")
    n_tp = mesh.shape["tp"]
    n_dp = mesh.shape["dp"]
    dp_swap = [(i, n_dp - 1 - i) for i in range(n_dp)]

    others = range(1, n_tp)

    def tp_xor(x, mask):
        return lax.ppermute(x, "tp", [(i, i ^ mask) for i in range(n_tp)])

    def in_hbm(x):
        return pltpu.with_memory_space_constraint(x, pltpu.HBM)

    def swap_dp(x):
        return lax.ppermute(x, "dp", dp_swap)

    def local_body(hidden, w_loc, labels, in_len, lab_len):
        batch_loc, frames, model_dim = hidden.shape
        vocab_loc = w_loc.shape[1]
        n_lab = labels.shape[1]
        n_slots = n_lab + 1
        rows = batch_loc * frames
        n_tiles = vocab_loc // TILE
        d_loc = model_dim // n_dp
        dma = pltpu.SemaphoreType.DMA
        i32 = jnp.int32
        n_lat, lat_steps, lat_pad = 24, 22, 8
        h_own = hidden.reshape(rows, model_dim)
        core = lax.rem(lax.axis_index("tp"), 2)
        h_oth = swap_dp(h_own)
        flops = 2 * rows * model_dim * TILE
        wbytes = model_dim * TILE * 2
        zbytes = rows * TILE * 4
        z_type = jax.ShapeDtypeStruct((n_tiles, rows, TILE), F32)
        pick_type = jax.ShapeDtypeStruct((frames // 2 + 24, LANES), F32)
        meta_type = jax.ShapeDtypeStruct((batch_loc, n_slots + 1), i32)
        g_type = jax.ShapeDtypeStruct((n_tiles // 2, rows, 2 * TILE), BF16)
        g_scratch = [pltpu.VMEM((rows, 2 * TILE), BF16)] * 2

        def w_scratch(n):
            return [pltpu.VMEM((3, model_dim, n * TILE), BF16), dma((3,))]

        def z_scratch(n):
            return [pltpu.VMEM((3, n, rows, TILE), F32), dma((3,))]

        h_scratch = [pltpu.VMEM((rows, model_dim), BF16), dma((2,))]
        run_scratch = [pltpu.VMEM((rows, LANES), F32), pltpu.VMEM((rows, LANES), F32)]

        def lists(n_sets):
            return [pltpu.SMEM((n_tiles,), i32), pltpu.SMEM((n_sets * batch_loc * n_slots,), i32)]

        z_own, pick, meta = kernel_call(
            functools.partial(z_own_kernel, n_slots),
            out_shape=(z_type, pick_type, meta_type),
            in_specs=[any_spec(), any_spec(), smem_spec(), smem_spec(), smem_spec()],
            out_specs=(any_spec(), vmem_spec(), smem_spec()),
            scratch_shapes=h_scratch + w_scratch(4) + z_scratch(4) + run_scratch + [pltpu.VMEM((frames // 2, LANES), F32)] + lists(1),
            compiler_params=params(),
            cost_estimate=cost(n_tiles * flops, n_tiles * (wbytes + zbytes)),
        )(in_hbm(h_own), w_loc, labels, in_len, lab_len)

        h_oth = in_hbm(h_oth)
        picks = [pick] + [tp_xor(pick, k) for k in others]

        n_blk = frames // HALF
        half_type = jax.ShapeDtypeStruct((rows // 2, model_dim), F32)
        occ_type = jax.ShapeDtypeStruct((frames + 8, LANES), F32)
        loss_type = jax.ShapeDtypeStruct((8, LANES), F32)
        z_oth, occ, keep, send, loss, g_own = kernel_call(
            functools.partial(mid_kernel, 0, n_tiles, n_lat, lat_steps, n_lab),
            out_shape=(z_type, occ_type, half_type, half_type, loss_type, g_type),
            in_specs=[any_spec()] * 2 + [vmem_spec()] * 4 + [any_spec(), smem_spec()],
            out_specs=(any_spec(),) + (vmem_spec(),) * 4 + (any_spec(),),
            scratch_shapes=[pltpu.VMEM((8, LANES), F32)] + h_scratch + w_scratch(2) + z_scratch(2) + [
                pltpu.VMEM((n_blk, n_lab, LANES), F32), pltpu.VMEM((n_blk, 8, LANES), F32),
                *[pltpu.VMEM((frames + lat_pad, n, LANES), F32) for n in (n_lab, n_lab + 8) * 2],
                pltpu.VMEM((n_blk, LANES, LANES), F32)] + z_scratch(2) + [
                pltpu.VMEM((model_dim, rows), F32), pltpu.VMEM((rows, LANES), F32)] + g_scratch + [dma((2,))] + lists(1),
            compiler_params=params(),
            cost_estimate=cost((2 * n_tiles) * flops, (2 * n_tiles) * (wbytes + zbytes)),
        )(h_oth, w_loc, *picks, z_own, meta)
        occ_oth = swap_dp(occ)
        meta_oth = swap_dp(meta)
        recv = tp_xor(send, 1)
        chip_sum = keep + recv
        across = tp_xor(chip_sum, 2)

        grad_weight = kernel_call(
            functools.partial(grad_w_kernel, n_slots),
            out_shape=jax.ShapeDtypeStruct((d_loc, vocab_loc), F32),
            in_specs=[any_spec(), any_spec(), any_spec(), any_spec(), vmem_spec(), smem_spec()],
            out_specs=any_spec(),
            scratch_shapes=h_scratch + h_scratch[:1] + z_scratch(2) + [
                dma((2,)), pltpu.VMEM((3, d_loc, 2 * TILE), F32), dma((3,)),
                pltpu.VMEM((d_loc, 2 * rows), BF16), pltpu.VMEM((rows, LANES), F32),
                pltpu.VMEM((2 * rows, 2 * TILE), BF16), pltpu.VMEM((2 * rows, 2 * TILE), BF16)] + lists(1),
            compiler_params=params(),
            cost_estimate=cost(n_tiles * flops, n_tiles * (2 * zbytes + d_loc * TILE * 4)),
        )(g_own, z_oth, in_hbm(h_own), h_oth, occ_oth, meta_oth)

        chip_sum, grad_weight = lax.optimization_barrier((chip_sum, grad_weight))
        full_half = chip_sum + across
        other_half = tp_xor(full_half, 1)
        grad_hidden = jnp.where(core == 0, jnp.stack([full_half, other_half]), jnp.stack([other_half, full_half])).reshape(batch_loc, frames, model_dim)
        return loss[0, :batch_loc], grad_weight, grad_hidden


    return jax.shard_map(
        local_body,
        mesh=mesh,
        in_specs=(P(batch_axes, None, None), P(None, "tp"), P(batch_axes, None), P(batch_axes), P(batch_axes)),
        out_specs=(P(batch_axes), P(batch_axes, "tp"), P(batch_axes, None, None)),
        check_vma=False,
    )
```
